32 devices in a mesh: section: 2 (over x), dp: 4 (over z), expert: 4 (over y, core).
Axes of the slice: x: 2, y: 2, z: 4, core: 2. Of those that a mesh axis runs over, the one named last changes fastest.
Arguments:
- boundary: bfloat16 [2, 1, 2048, 2048], P('section', None, ('dp', 'expert')), may hold values from -6 to 6
- lengths: int32 [1, 4, 4, 3], P(None, 'dp'), may hold values from 1 to 64, 128 in all within a row
- routes: int32 [2, 1, 2048, 6], P('section', None, ('dp', 'expert')), may hold values from 0 to 15, all different within a row; in each aligned block of 128 rows (0 to 127, 128 to 255, ..., all dimensions but the last counted through in order) at most 64 rows name the same one
- attn_gain: float32 [2, 2048], P('section'), may hold values from 0.5 to 1.5
- query_weight: bfloat16 [2, 2048, 3072], P('section', None, 'expert'), may hold values from -0.125 to 0.125
- compress_weight: bfloat16 [2, 2048, 576], P('section'), may hold values from -0.125 to 0.125
- latent_gain: float32 [2, 512], P('section'), may hold values from 0.5 to 1.5
- expand_weight: bfloat16 [2, 512, 4096], P('section', None, 'expert'), may hold values from -0.25 to 0.25
- output_weight: bfloat16 [2, 2048, 2048], P('section', 'expert'), may hold values from -1 to 1
- ffn_gain: float32 [2, 2048], P('section'), may hold values from 0.5 to 1.5
- router_weight: bfloat16 [2, 2048, 16], P('section'), may hold values from -0.375 to 0.375
- shared_in: bfloat16 [2, 2048, 2, 2816], P('section', None, None, 'expert'), may hold values from -0.125 to 0.125
- shared_out: bfloat16 [2, 2816, 2048], P('section', 'expert'), may hold values from -0.109375 to 0.109375
- expert_in: bfloat16 [2, 16, 2048, 2, 768], P('section', ('dp', 'expert')), may hold values from -0.125 to 0.125
- expert_out: bfloat16 [2, 16, 768, 2048], P('section', ('dp', 'expert')), may hold values from -0.875 to 0.875
Outputs:
- ends: float32 [2, 1, 2048, 2048], P('section', None, ('dp', 'expert'))
- attn_gain_grad: float32 [2, 2048], P('section')
- query_grad: float32 [2, 2048, 3072], P('section', None, 'expert')
- compress_grad: float32 [2, 2048, 576], P('section')
- latent_gain_grad: float32 [2, 512], P('section')
- expand_grad: float32 [2, 512, 4096], P('section', None, 'expert')
- output_grad: float32 [2, 2048, 2048], P('section', 'expert')
- ffn_gain_grad: float32 [2, 2048], P('section')
- router_grad: float32 [2, 2048, 16], P('section')
- shared_in_grad: float32 [2, 2048, 2, 2816], P('section', None, None, 'expert')
- shared_out_grad: float32 [2, 2816, 2048], P('section', 'expert')
- expert_in_grad: float32 [2, 16, 2048, 2, 768], P('section', ('dp', 'expert'))
- expert_out_grad: float32 [2, 16, 768, 2048], P('section', ('dp', 'expert'))
The draws below stay inside these ranges and needn't reach their ends.
Inputs may be any that keep to these rules, and one draw needn't show every extreme that they name: The lengths of each row of 3 sum to 128, and the largest of each row is exactly 64. `routes`: each row names 6 different experts. In the rows of one device (aligned blocks of 128 rows, section, micro-batch and rows taken together) no expert is named by more than 64 rows, and in every draw some block has an expert named by exactly 64.
All inputs are finite; a program needn't handle non-finite values.
Results may differ from the reference program's by a relative error of at most 0.034.
Values may be sent and summed in bfloat16 or wider, within the bound.
A program may use at most 448 MiB of HBM per device.

```python
import math
import jax
import jax.numpy as jnp
import numpy as np
from jax import lax

D = 2048
HEADS = 16
NOPE = 128
ROPE = 64
VD = 128
LAT = 512
FE = 768
SFF = 2816
TOP = 6
MICRO = 1
NSEQ = 3
TOK_DEV = 128
PACK = 512
ROWS = 2048
SEQ_MAX = 64
EXPERTS = 16
CAP = 64
N_DP = 4
N_EXPERT = 4


def levels(rng, extent, pieces, smallest, largest):
    gain, own = 1.0, jax.random.fold_in(rng, 6)
    for dim, shards_of in pieces:
        steps = jnp.exp(jax.random.uniform(jax.random.fold_in(own, dim), (shards_of,), jnp.float32, smallest / len(pieces), largest / len(pieces)))
        gain = gain * jnp.repeat(steps, extent[dim] // shards_of).reshape([-1 if axis == dim else 1 for axis in range(len(extent))])
    return gain


def profile(amount, total, reach, skew):
    weights = [(1 << 20) // math.isqrt(standing ** skew) + 1 for standing in range(2, amount + 1)]
    surplus, holding = total - reach - (amount - 1), [1] * (amount - 1)
    while surplus > 0:
        candidates = [i for i in range(amount - 1) if holding[i] < reach]
        whole, remaining = sum([weights[i] for i in candidates]), surplus
        for i in candidates:
            addition = min(reach - holding[i], max(1, remaining * weights[i] // whole), surplus)
            holding[i] = holding[i] + addition
            surplus = surplus - addition
    return np.array([reach] + holding)


def ragged(key, count, total, most, lean):
    if count == 2:
        one = jax.random.randint(key, (), max(1, total - most), min(most, total - 1) + 1)
        return jnp.stack([one, total - one])
    sizes = jnp.asarray(profile(count, total, most, lean), jnp.int32)
    couples = (count - 1) // 2
    donor, sink = sizes[1:1 + 2 * couples:2], sizes[2:2 + 2 * couples:2]
    margin = jnp.minimum(donor - 1, most - sink)
    shifted = jax.random.randint(jax.random.fold_in(key, 1), (couples,), 0, 1 << 20) % (margin + 1)
    sizes = sizes.at[1:1 + 2 * couples:2].set(donor - shifted).at[2:2 + 2 * couples:2].set(sink + shifted)
    return sizes[jax.random.permutation(jax.random.fold_in(key, 2), count)]


def deal_out(key, own, number, rows, count, top, limit, skew):
    order = jax.random.permutation(key, count)
    crowded, common = shares(count, rows * top, limit, skew, True), shares(count, rows * top, limit, skew, False)
    places = jnp.arange(count)

    def named(tallies, offset_by):
        used = int((tallies > 0).sum())
        fixed = max(1, used // 4)
        shifted = fixed + (places - fixed + offset_by * (used - fixed)) % max(1, count - fixed)
        return jnp.zeros((count,), jnp.int32).at[order[jnp.where(places < fixed, places, shifted)]].set(jnp.asarray(tallies, jnp.int32))

    tallies = jnp.where(number % 4 == 0, named(crowded, number // 4), named(common, number - number // 4 - 1))
    mixed = jax.random.permutation(jax.random.fold_in(own, 3), count)
    source_of, taker = mixed[0:count // 2 * 2:2], mixed[1:count // 2 * 2:2]
    margin = jnp.minimum(tallies[source_of] - 1, limit - tallies[taker]) // 2
    margin = jnp.where((source_of == order[0]) | (taker == order[0]) | (tallies[taker] == 0), 0, jnp.maximum(margin, 0))
    shifted = jax.random.randint(jax.random.fold_in(own, 4), (count // 2,), 0, 1 << 20) % (margin + 1)
    tallies = tallies.at[source_of].add(-shifted).at[taker].add(shifted)
    items = jnp.searchsorted(jnp.cumsum(tallies), jnp.arange(rows * top), side="right").astype(jnp.int32)
    table = items.reshape(top, rows).T
    table = table[jax.random.permutation(jax.random.fold_in(own, 1), rows)]
    offset_by = jax.random.randint(jax.random.fold_in(own, 2), (rows, 1), 0, top)
    return jnp.take_along_axis(table, (jnp.arange(top)[None, :] + offset_by) % top, axis=1)


def shares(count, total, bound, lean, full):
    portions = [(1 << 20) // math.isqrt(grade ** lean) + 1 for grade in range(1, count + 1)]
    largest = bound if full else min(bound, max(-(-total // count), total * portions[0] // sum(portions)))
    least = 1 if total - largest >= count - 1 else 0
    holding, rest = [largest] + [least] * (count - 1), total - largest - least * (count - 1)
    while rest > 0:
        candidates = [i for i in range(1, count) if holding[i] < largest] or [i for i in range(1, count) if holding[i] < bound]
        mass, budget = sum([portions[i] for i in candidates]), rest
        for i in candidates:
            addition = min(bound - holding[i], max(1, budget * portions[i] // mass), rest)
            holding[i] = holding[i] + addition
            rest = rest - addition
    return np.array(holding)


def centred(stream_key, extent, scale, limit, cuts=(), kind=jnp.bfloat16):
    drawn = scale * jax.random.normal(stream_key, extent, jnp.float32)
    if cuts:
        drawn = drawn * levels(stream_key, extent, cuts, -0.22, 0.18)
    return jnp.clip(drawn, -limit, limit).astype(kind)


def setup_inputs(seed: int = 0) -> dict:
    key_of = jax.random.split(jax.random.key(seed), 16)
    boundary = centred(key_of[0], (2, MICRO, ROWS, D), 1.0, 6.0, ((0, 2), (2, 16)))
    lengths = jax.vmap(lambda own: ragged(own, NSEQ, TOK_DEV, SEQ_MAX, 2))(jax.random.split(key_of[1], MICRO * N_DP * N_EXPERT)).reshape((MICRO, N_DP, N_EXPERT, NSEQ)).astype(jnp.int32)
    routes_keys = jax.random.split(jax.random.fold_in(key_of[2], 1), 2 * MICRO * ROWS // TOK_DEV)
    routes_turns = jax.random.permutation(jax.random.fold_in(key_of[2], 3), 2 * MICRO * ROWS // TOK_DEV)
    routes = jax.vmap(lambda own, number: deal_out(jax.random.fold_in(key_of[2], 2), own, number, TOK_DEV, EXPERTS, TOP, CAP, 2))(routes_keys, routes_turns).reshape((2, MICRO, ROWS, TOP))
    attn_gain = jnp.clip(1.0 + 0.1 * jax.random.normal(key_of[3], (2, D), jnp.float32), 0.5, 1.5)
    query_weight = centred(key_of[4], (2, D, HEADS * (NOPE + ROPE)), D ** -0.5, 0.125, ((0, 2), (2, 4)))
    compress_weight = centred(key_of[5], (2, D, LAT + ROPE), D ** -0.5, 0.125, ((0, 2),))
    latent_gain = jnp.clip(1.0 + 0.1 * jax.random.normal(key_of[6], (2, LAT), jnp.float32), 0.5, 1.5)
    expand_weight = centred(key_of[7], (2, LAT, HEADS * (NOPE + VD)), LAT ** -0.5, 0.25, ((0, 2), (2, 4)))
    output_weight = centred(key_of[8], (2, HEADS * VD, D), (VD // 4) ** -0.5, 1.0, ((0, 2), (1, 4)))
    ffn_gain = jnp.clip(1.0 + 0.1 * jax.random.normal(key_of[9], (2, D), jnp.float32), 0.5, 1.5)
    router_weight = centred(key_of[10], (2, D, EXPERTS), (D // 9) ** -0.5, 0.375, ((0, 2),))
    shared_in = centred(key_of[11], (2, D, 2, SFF), D ** -0.5, 0.125, ((0, 2), (3, 4)))
    shared_out = centred(key_of[12], (2, SFF, D), SFF ** -0.5, 0.109375, ((0, 2), (1, 4)))
    expert_in = centred(key_of[13], (2, EXPERTS, D, 2, FE), D ** -0.5, 0.125, ((0, 2), (1, 16)))
    expert_out = centred(key_of[14], (2, EXPERTS, FE, D), (FE // 16) ** -0.5, 0.875, ((0, 2), (1, 16)))
    return dict(boundary=boundary, lengths=lengths, routes=routes, attn_gain=attn_gain, query_weight=query_weight, compress_weight=compress_weight, latent_gain=latent_gain, expand_weight=expand_weight, output_weight=output_weight, ffn_gain=ffn_gain, router_weight=router_weight, shared_in=shared_in, shared_out=shared_out, expert_in=expert_in, expert_out=expert_out)


epsilon = 1e-06
rope_base = 10000.0
masked_score = -1e+30
block_limit = 512

def contract(form, left, right):
    return jnp.einsum(form, left.astype(jnp.float32), right.astype(jnp.float32), preferred_element_type=jnp.float32)

def rms_forward(inputs, gain_vec):
    norm_scale = lax.rsqrt(lax.optimization_barrier(jnp.mean(inputs * inputs, axis=-1, keepdims=True)) + epsilon)
    return (inputs * norm_scale * gain_vec, norm_scale)

def rms_backward(inputs, norm_scale, gain_vec, upstream):
    weighted = upstream * gain_vec
    grad_gain = lax.optimization_barrier(jnp.sum(upstream * inputs * norm_scale, axis=0))
    cubed = norm_scale * norm_scale * norm_scale
    grad_inputs = norm_scale * weighted - inputs * cubed * lax.optimization_barrier(jnp.mean(weighted * inputs, axis=-1, keepdims=True))
    return (grad_inputs, grad_gain)

def rope_tables(position, half_width):
    freqs = rope_base ** (-jnp.arange(half_width, dtype=jnp.float32) / half_width)
    angles = position.astype(jnp.float32)[:, None] * freqs[None, :]
    return (jnp.cos(angles), jnp.sin(angles))

def rotate(inputs, cosine, sine_table):
    half_width = cosine.shape[-1]
    former = inputs[..., :half_width]
    latter = inputs[..., half_width:]
    return jnp.concatenate([former * cosine - latter * sine_table, latter * cosine + former * sine_table], axis=-1)

def pack_layout(pack_lengths, pack_rows):
    starts = (jnp.cumsum(pack_lengths) - pack_lengths).astype(jnp.int32)
    row_index = jnp.arange(pack_rows, dtype=jnp.int32)
    begun = row_index[:, None] >= starts[None, :]
    segment = lax.optimization_barrier(jnp.sum(begun.astype(jnp.int32), axis=1)).astype(jnp.int32)
    opening = lax.optimization_barrier(jnp.max(jnp.where(begun, starts[None, :], 0), axis=1)).astype(jnp.int32)
    return (segment, row_index - opening)

def group_layout(group_lengths, group_rows):
    segment, position = jax.vmap(lambda one: pack_layout(one, group_rows))(group_lengths)
    seq_count = group_lengths.shape[1]
    offsets = jnp.arange(group_lengths.shape[0], dtype=jnp.int32)[:, None] * seq_count
    return ((segment + offsets).reshape(-1).astype(jnp.int32), position.reshape(-1).astype(jnp.int32))

def block_size(row_count):
    return min(row_count, TOK_DEV * max(1, block_limit // TOK_DEV))

def visible(segment, offset, block_rows):
    seg_block = segment[offset:offset + block_rows]
    row_index = jnp.arange(block_rows, dtype=jnp.int32)
    same_seq = seg_block[:, None] == seg_block[None, :]
    return same_seq & (row_index[None, :] <= row_index[:, None])

def silu_parts(pre_gate):
    sigmoid_part = jax.nn.sigmoid(pre_gate)
    activated = pre_gate * sigmoid_part
    slope = sigmoid_part * (1.0 + pre_gate * (1.0 - sigmoid_part))
    return (activated, slope)

def project_heads(row_block, key_block, query_weight, expand_weight, cosine, sine_table):
    row_count = row_block.shape[0]
    head_count = query_weight.shape[1] // (NOPE + ROPE)
    query_raw = jnp.dot(row_block, query_weight, preferred_element_type=jnp.float32).reshape(row_count, head_count, NOPE + ROPE)
    query_heads = jnp.concatenate([query_raw[..., :NOPE], rotate(query_raw[..., NOPE:], cosine[:, None, :], sine_table[:, None, :])], axis=-1).astype(jnp.bfloat16)
    latent = jnp.dot(key_block[:, :LAT], expand_weight, preferred_element_type=jnp.float32).reshape(row_count, head_count, NOPE + VD).astype(jnp.bfloat16)
    shared_key = jnp.broadcast_to(key_block[:, None, LAT:], (row_count, head_count, ROPE))
    key_heads = jnp.concatenate([latent[..., :NOPE], shared_key], axis=-1)
    return (query_heads, key_heads, latent[..., NOPE:])

def attention_forward(query_heads, key_heads, value_heads, segment):
    row_count = query_heads.shape[0]
    block_rows = block_size(row_count)
    factor = (NOPE + ROPE) ** (-0.5)
    out_blocks = []
    log_blocks = []
    for offset in range(0, row_count, block_rows):
        allowed = visible(segment, offset, block_rows)
        scores = contract('bhc,khc->hbk', query_heads[offset:offset + block_rows], key_heads[offset:offset + block_rows]) * factor
        scores = jnp.where(allowed[None], scores, masked_score)
        row_max = lax.optimization_barrier(jnp.max(scores, axis=-1, keepdims=True))
        log_total = row_max + jnp.log(lax.optimization_barrier(jnp.sum(jnp.exp(scores - row_max), axis=-1, keepdims=True)))
        weights = jnp.exp(scores - log_total).astype(jnp.bfloat16)
        out_blocks.append(contract('hbk,khv->bhv', weights, value_heads[offset:offset + block_rows]).astype(jnp.bfloat16))
        log_blocks.append(log_total[..., 0])
    attended = jnp.concatenate(out_blocks, axis=0)
    return (attended.reshape(row_count, -1), jnp.concatenate(log_blocks, axis=1))

def attention_backward(query_heads, key_heads, value_heads, segment, log_totals, grad_attended):
    row_count, head_count, qk_width = query_heads.shape
    block_rows = block_size(row_count)
    factor = (NOPE + ROPE) ** (-0.5)
    grad_out = grad_attended.reshape(row_count, head_count, VD)
    key_blocks = []
    value_blocks = []
    query_blocks = []
    for offset in range(0, row_count, block_rows):
        allowed = visible(segment, offset, block_rows)
        query_part = query_heads[offset:offset + block_rows]
        key_part = key_heads[offset:offset + block_rows]
        value_part = value_heads[offset:offset + block_rows]
        scores = contract('bhc,khc->hbk', query_part, key_part) * factor
        scores = jnp.where(allowed[None], scores, masked_score)
        weights = jnp.exp(scores - log_totals[:, offset:offset + block_rows, None])
        grad_part = grad_out[offset:offset + block_rows]
        value_blocks.append(contract('hbk,bhv->khv', weights.astype(jnp.bfloat16), grad_part))
        grad_weights = contract('bhv,khv->hbk', grad_part, value_part)
        centre = lax.optimization_barrier(jnp.sum(weights * grad_weights, axis=-1, keepdims=True))
        grad_scores = (weights * (grad_weights - centre) * factor).astype(jnp.bfloat16)
        query_blocks.append(contract('hbk,khc->bhc', grad_scores, key_part))
        key_blocks.append(contract('hbk,bhc->khc', grad_scores, query_part))
    return (jnp.concatenate(query_blocks, axis=0), jnp.concatenate(key_blocks, axis=0), jnp.concatenate(value_blocks, axis=0))

def project_backward(row_block, key_block, query_weight, expand_weight, cosine, sine_table, grad_query, grad_keys, grad_values):
    row_count, head_count, qk_width = grad_query.shape
    grad_q = jnp.concatenate([grad_query[..., :NOPE], rotate(grad_query[..., NOPE:], cosine[:, None, :], -sine_table[:, None, :])], axis=-1)
    grad_q = grad_q.reshape(row_count, head_count * qk_width).astype(jnp.bfloat16)
    grad_latent = jnp.concatenate([grad_keys[..., :NOPE], grad_values], axis=-1).reshape(row_count, -1).astype(jnp.bfloat16)
    grad_shared = lax.optimization_barrier(jnp.sum(grad_keys[..., NOPE:], axis=1))
    query_part = jnp.dot(row_block.T, grad_q, preferred_element_type=jnp.float32)
    expand_part = jnp.dot(key_block[:, :LAT].T, grad_latent, preferred_element_type=jnp.float32)
    grad_rows = jnp.dot(grad_q, query_weight.T, preferred_element_type=jnp.float32)
    grad_keyed = jnp.concatenate([jnp.dot(grad_latent, expand_weight.T, preferred_element_type=jnp.float32), grad_shared], axis=1)
    return (query_part, expand_part, grad_rows, grad_keyed)

def slot_rank(flat_routes, expert_count, capacity):
    onehot = (flat_routes[:, None] == jnp.arange(expert_count, dtype=jnp.int32)[None, :]).astype(jnp.int32)
    earlier = (jnp.cumsum(onehot, axis=0) - onehot).astype(jnp.int32)
    return (flat_routes * capacity + lax.optimization_barrier(jnp.sum(earlier * onehot, axis=1))).astype(jnp.int32)

def expert_forward(operands):
    arrived, weight_in, weight_out = operands
    model_width = arrived.shape[1]
    pre_act = jnp.dot(arrived, weight_in.reshape(model_width, -1), preferred_element_type=jnp.float32).reshape(arrived.shape[0], 2, FE)
    activated, slope = silu_parts(pre_act[:, 0])
    hidden_units = (activated * pre_act[:, 1]).astype(jnp.bfloat16)
    return jnp.dot(hidden_units, weight_out, preferred_element_type=jnp.float32).astype(jnp.bfloat16)

def expert_backward(operands):
    arrived, weight_in, weight_out, grad_out = operands
    model_width = arrived.shape[1]
    flat_in = weight_in.reshape(model_width, -1)
    pre_act = jnp.dot(arrived, flat_in, preferred_element_type=jnp.float32).reshape(arrived.shape[0], 2, FE)
    activated, slope = silu_parts(pre_act[:, 0])
    hidden_units = (activated * pre_act[:, 1]).astype(jnp.bfloat16)
    grad_hidden = jnp.dot(grad_out, weight_out.T, preferred_element_type=jnp.float32)
    grad_weight_out = jnp.dot(hidden_units.T, grad_out, preferred_element_type=jnp.float32)
    grad_pre = jnp.stack([grad_hidden * pre_act[:, 1] * slope, grad_hidden * activated], axis=1).reshape(arrived.shape[0], -1).astype(jnp.bfloat16)
    grad_weight_in = jnp.dot(arrived.T, grad_pre, preferred_element_type=jnp.float32).reshape(model_width, 2, FE)
    grad_arrived = jnp.dot(grad_pre, flat_in.T, preferred_element_type=jnp.float32).astype(jnp.bfloat16)
    return (grad_arrived, grad_weight_in, grad_weight_out)

def layer_forward(hidden, lengths_mb, routes_mb, params):
    attn_gain, query_weight, compress_weight, latent_gain, expand_weight, output_weight, ffn_gain, router_weight, shared_in, shared_out, expert_in, expert_out = params
    packs = ROWS // PACK
    dev_count = N_DP * N_EXPERT
    segment, position = group_layout(lengths_mb.reshape(dev_count, NSEQ), TOK_DEV)
    segment = segment.reshape(packs, PACK)
    cosine, sine_table = rope_tables(position, ROPE // 2)
    normed32, scale_attn = rms_forward(hidden, attn_gain)
    normed = normed32.astype(jnp.bfloat16)
    compressed = jnp.dot(normed, compress_weight, preferred_element_type=jnp.float32)
    latent32, scale_latent = rms_forward(compressed[:, :LAT], latent_gain)
    keyed = jnp.concatenate([latent32, rotate(compressed[:, LAT:], cosine, sine_table)], axis=1).astype(jnp.bfloat16)

    def attend_pack(operands):
        row_block, key_block, seg_block, cos_block, sin_block = operands
        query_heads, key_heads, value_heads = project_heads(row_block, key_block, query_weight, expand_weight, cos_block, sin_block)
        return attention_forward(query_heads, key_heads, value_heads, seg_block)
    attended, log_totals = lax.map(attend_pack, (normed.reshape(packs, PACK, D), keyed.reshape(packs, PACK, LAT + ROPE), segment, cosine.reshape(packs, PACK, -1), sine_table.reshape(packs, PACK, -1)))
    attended = attended.reshape(ROWS, -1)
    mixed_rows = hidden + jnp.dot(attended, output_weight, preferred_element_type=jnp.float32)
    ffn32, scale_ffn = rms_forward(mixed_rows, ffn_gain)
    ffn_in = ffn32.astype(jnp.bfloat16)
    router_prob = jax.nn.softmax(jnp.dot(ffn_in, router_weight, preferred_element_type=jnp.float32), axis=-1)
    gate_values = jnp.take_along_axis(router_prob, routes_mb, axis=1)
    shared_pre = jnp.dot(ffn_in, shared_in.reshape(D, -1), preferred_element_type=jnp.float32).reshape(ROWS, 2, SFF)
    shared_act, shared_slope = silu_parts(shared_pre[:, 0])
    shared_hid = (shared_act * shared_pre[:, 1]).astype(jnp.bfloat16)
    shared_sum = jnp.dot(shared_hid, shared_out, preferred_element_type=jnp.float32)
    local_slot = jax.vmap(lambda device_routes: slot_rank(device_routes, EXPERTS, CAP))(routes_mb.reshape(dev_count, TOK_DEV * TOP))
    device_ids = jnp.arange(dev_count, dtype=jnp.int32)[:, None]
    global_slot = ((local_slot // CAP * dev_count + device_ids) * CAP + local_slot % CAP).reshape(-1).astype(jnp.int32)
    owner_row = jnp.arange(ROWS * TOP, dtype=jnp.int32) // TOP
    arrived = jnp.zeros((EXPERTS * dev_count * CAP, D), jnp.bfloat16).at[global_slot].set(ffn_in[owner_row])
    arrived = arrived.reshape(EXPERTS, dev_count * CAP, D)
    produced = lax.map(expert_forward, (arrived, expert_in, expert_out)).reshape(-1, D)
    picked = produced[global_slot].reshape(ROWS, TOP, D)
    routed = lax.optimization_barrier(jnp.sum(gate_values[..., None] * picked.astype(jnp.float32), axis=1))
    result = mixed_rows + shared_sum + routed
    stored = {'segment': segment, 'cosine': cosine, 'sine_table': sine_table, 'normed': normed, 'compressed': compressed, 'scale_attn': scale_attn, 'scale_latent': scale_latent, 'keyed': keyed, 'attended': attended, 'log_totals': log_totals, 'mixed_rows': mixed_rows, 'scale_ffn': scale_ffn, 'ffn_in': ffn_in, 'router_prob': router_prob, 'gate_values': gate_values, 'shared_pre': shared_pre, 'shared_hid': shared_hid, 'global_slot': global_slot, 'arrived': arrived, 'picked': picked}
    return (result, stored)

def layer_backward(hidden, routes_mb, params, stored, upstream):
    attn_gain, query_weight, compress_weight, latent_gain, expand_weight, output_weight, ffn_gain, router_weight, shared_in, shared_out, expert_in, expert_out = params
    packs = ROWS // PACK
    dev_count = N_DP * N_EXPERT
    global_slot = stored['global_slot']
    grad_gates = lax.optimization_barrier(jnp.sum(upstream[:, None, :] * stored['picked'].astype(jnp.float32), axis=-1))
    grad_picked = (stored['gate_values'][..., None] * upstream[:, None, :]).astype(jnp.bfloat16)
    grad_produced = jnp.zeros((EXPERTS * dev_count * CAP, D), jnp.bfloat16).at[global_slot].set(grad_picked.reshape(-1, D))
    grad_arrived, grad_expert_in, grad_expert_out = lax.map(expert_backward, (stored['arrived'], expert_in, expert_out, grad_produced.reshape(EXPERTS, dev_count * CAP, D)))
    grad_ffn = lax.optimization_barrier(jnp.sum(grad_arrived.reshape(-1, D)[global_slot].reshape(ROWS, TOP, D).astype(jnp.float32), axis=1))
    choose = (routes_mb[..., None] == jnp.arange(EXPERTS, dtype=jnp.int32)).astype(jnp.float32)
    grad_prob = lax.optimization_barrier(jnp.sum(grad_gates[..., None] * choose, axis=1))
    router_prob = stored['router_prob']
    grad_logits = (router_prob * (grad_prob - lax.optimization_barrier(jnp.sum(router_prob * grad_prob, axis=-1, keepdims=True)))).astype(jnp.bfloat16)
    ffn_in = stored['ffn_in']
    grad_router = jnp.dot(ffn_in.T, grad_logits, preferred_element_type=jnp.float32)
    grad_ffn = grad_ffn + jnp.dot(grad_logits, router_weight.T, preferred_element_type=jnp.float32)
    upstream16 = upstream.astype(jnp.bfloat16)
    grad_shared_hid = jnp.dot(upstream16, shared_out.T, preferred_element_type=jnp.float32)
    grad_shared_out = jnp.dot(stored['shared_hid'].T, upstream16, preferred_element_type=jnp.float32)
    shared_pre = stored['shared_pre']
    shared_act, shared_slope = silu_parts(shared_pre[:, 0])
    grad_shared_pre = jnp.stack([grad_shared_hid * shared_pre[:, 1] * shared_slope, grad_shared_hid * shared_act], axis=1).reshape(ROWS, -1).astype(jnp.bfloat16)
    grad_shared_in = jnp.dot(ffn_in.T, grad_shared_pre, preferred_element_type=jnp.float32).reshape(D, 2, SFF)
    grad_ffn = grad_ffn + jnp.dot(grad_shared_pre, shared_in.reshape(D, -1).T, preferred_element_type=jnp.float32)
    grad_mixed_norm, grad_ffn_gain = rms_backward(stored['mixed_rows'], stored['scale_ffn'], ffn_gain, grad_ffn)
    grad_mixed = upstream + grad_mixed_norm
    grad_mixed16 = grad_mixed.astype(jnp.bfloat16)
    grad_attended = jnp.dot(grad_mixed16, output_weight.T, preferred_element_type=jnp.float32).astype(jnp.bfloat16)
    grad_output = jnp.dot(stored['attended'].T, grad_mixed16, preferred_element_type=jnp.float32)

    def back_pack(carry, operands):
        row_block, key_block, seg_block, cos_block, sin_block, log_block, grad_block = operands
        query_heads, key_heads, value_heads = project_heads(row_block, key_block, query_weight, expand_weight, cos_block, sin_block)
        grad_query, grad_keys, grad_values = attention_backward(query_heads, key_heads, value_heads, seg_block, log_block, grad_block)
        query_part, expand_part, grad_rows, grad_keyed = project_backward(row_block, key_block, query_weight, expand_weight, cos_block, sin_block, grad_query, grad_keys, grad_values)
        return ((carry[0] + query_part, carry[1] + expand_part), (grad_rows, grad_keyed))
    initial = (jnp.zeros(query_weight.shape, jnp.float32), jnp.zeros(expand_weight.shape, jnp.float32))
    cosine = stored['cosine']
    sine_table = stored['sine_table']
    (grad_query_w, grad_expand_w), (grad_rows, grad_keyed) = lax.scan(back_pack, initial, (stored['normed'].reshape(packs, PACK, D), stored['keyed'].reshape(packs, PACK, LAT + ROPE), stored['segment'], cosine.reshape(packs, PACK, -1), sine_table.reshape(packs, PACK, -1), stored['log_totals'], grad_attended.reshape(packs, PACK, -1)))
    grad_rows = grad_rows.reshape(ROWS, D)
    grad_keyed = grad_keyed.reshape(ROWS, LAT + ROPE)
    grad_latent, grad_latent_gain = rms_backward(stored['compressed'][:, :LAT], stored['scale_latent'], latent_gain, grad_keyed[:, :LAT])
    grad_compressed = jnp.concatenate([grad_latent, rotate(grad_keyed[:, LAT:], cosine, -sine_table)], axis=1).astype(jnp.bfloat16)
    grad_compress = jnp.dot(stored['normed'].T, grad_compressed, preferred_element_type=jnp.float32)
    grad_normed = grad_rows + jnp.dot(grad_compressed, compress_weight.T, preferred_element_type=jnp.float32)
    grad_hidden_norm, grad_attn_gain = rms_backward(hidden, stored['scale_attn'], attn_gain, grad_normed)
    grads = (grad_attn_gain, grad_query_w, grad_compress, grad_latent_gain, grad_expand_w, grad_output, grad_ffn_gain, grad_router, grad_shared_in, grad_shared_out, grad_expert_in, grad_expert_out)
    return (grad_mixed + grad_hidden_norm, grads)

def reference(boundary, lengths, routes, attn_gain, query_weight, compress_weight, latent_gain, expand_weight, output_weight, ffn_gain, router_weight, shared_in, shared_out, expert_in, expert_out):
    stacked = (attn_gain, query_weight, compress_weight, latent_gain, expand_weight, output_weight, ffn_gain, router_weight, shared_in, shared_out, expert_in, expert_out)
    layer_params = [tuple((member[layer_id] for member in stacked)) for layer_id in range(2)]
    sums_first = None
    sums_second = None
    input_grads = []
    outputs = []
    for batch_idx in range(MICRO):
        layer_input = boundary[0, batch_idx].astype(jnp.float32)
        out_first, stored_first = layer_forward(layer_input, lengths[batch_idx], routes[0, batch_idx], layer_params[0])
        second_input = lax.optimization_barrier(out_first.astype(jnp.bfloat16)).astype(jnp.float32)
        out_second, stored_second = layer_forward(second_input, lengths[batch_idx], routes[1, batch_idx], layer_params[1])
        outputs.append(out_second)
        grad_middle, grads_second = layer_backward(second_input, routes[1, batch_idx], layer_params[1], stored_second, boundary[1, batch_idx].astype(jnp.float32))
        grad_input, grads_first = layer_backward(layer_input, routes[0, batch_idx], layer_params[0], stored_first, grad_middle)
        input_grads.append(grad_input)
        if sums_first is None:
            sums_first = grads_first
            sums_second = grads_second
        else:
            sums_first = tuple((left_term + right_term for left_term, right_term in zip(sums_first, grads_first)))
            sums_second = tuple((left_term + right_term for left_term, right_term in zip(sums_second, grads_second)))
    ends = jnp.stack([jnp.stack(input_grads), jnp.stack(outputs)])
    merged = [jnp.stack([left_term, right_term]) for left_term, right_term in zip(sums_first, sums_second)]
    return (ends, merged[0], merged[1], merged[2], merged[3], merged[4], merged[5], merged[6], merged[7], merged[8], merged[9], merged[10], merged[11])
```

```python
import functools

import jax
import jax.numpy as jnp
from jax import lax
from jax.experimental import pallas as pl
from jax.experimental.pallas import tpu as pltpu
from jax.sharding import PartitionSpec as P

NOPE = 128
ROPE = 64
VD = 128
LAT = 512

QK = NOPE + ROPE
KV = NOPE + VD
HALF = ROPE // 2
epsilon = 1e-06
rope_base = 10000.0
masked_score = -1e30
BOTH = ("dp", "expert")


def dot(left, right):
    return jnp.dot(left, right, preferred_element_type=jnp.float32)


def dot_t(left, right):
    return lax.dot_general(
        left, right, (((1,), (1,)), ((), ())), preferred_element_type=jnp.float32
    )


def t_dot(left, right):
    return lax.dot_general(
        left, right, (((0,), (0,)), ((), ())), preferred_element_type=jnp.float32
    )


def bf16(value):
    return value.astype(jnp.bfloat16)


def gather_all(rows):
    return lax.all_gather(rows, BOTH, axis=0, tiled=True)


def gather_pack(rows):
    return lax.all_gather(rows, "expert", axis=0, tiled=True)


def scatter_all(partial_rows):
    return lax.psum_scatter(partial_rows, BOTH, scatter_dimension=0, tiled=True)


def scatter_pack(partial_rows):
    return lax.psum_scatter(partial_rows, "expert", scatter_dimension=0, tiled=True)


def rms_forward(inputs, gain_vec):
    norm_scale = lax.rsqrt(jnp.mean(inputs * inputs, axis=-1, keepdims=True) + epsilon)
    return (inputs * norm_scale * gain_vec, norm_scale)


def rms_backward(inputs, norm_scale, gain_vec, upstream):
    weighted = upstream * gain_vec
    grad_gain = jnp.sum(upstream * inputs * norm_scale, axis=0)
    cubed = norm_scale * norm_scale * norm_scale
    grad_inputs = norm_scale * weighted - inputs * cubed * jnp.mean(
        weighted * inputs, axis=-1, keepdims=True
    )
    return (grad_inputs, grad_gain)


def rotate(inputs, cosine, sine):
    half = cosine.shape[-1]
    former = inputs[..., :half]
    latter = inputs[..., half:]
    return jnp.concatenate(
        [former * cosine - latter * sine, latter * cosine + former * sine], axis=-1
    )


def silu_parts(pre_gate):
    sigmoid = jax.nn.sigmoid(pre_gate)
    return (pre_gate * sigmoid, sigmoid * (1.0 + pre_gate * (1.0 - sigmoid)))


def block_layout(block_lengths, rows):
    starts = jnp.cumsum(block_lengths, axis=1) - block_lengths
    index = jnp.arange(rows, dtype=jnp.int32)
    begun = index[None, :, None] >= starts[:, None, :]
    segment = jnp.sum(begun.astype(jnp.int32), axis=2)
    opening = jnp.max(jnp.where(begun, starts[:, None, :], 0), axis=2)
    return segment, index[None, :] - opening


def allowed_pairs(seg_col, seg_row):
    rows = seg_col.shape[0]
    later = lax.broadcasted_iota(jnp.int32, (rows, rows), 0)
    earlier = lax.broadcasted_iota(jnp.int32, (rows, rows), 1)
    return (seg_col == seg_row) & (earlier <= later)


def attend_kernel(heads, q_ref, lat_ref, key_ref, cos_ref, sin_ref, col_ref, row_ref, out_ref, rot_ref):
    factor = QK**-0.5
    allowed = allowed_pairs(col_ref[...], row_ref[0])
    cosine, sine = cos_ref[...], sin_ref[...]
    shared = key_ref[:, LAT:]
    for head in range(heads):
        raw = q_ref[:, head * QK : (head + 1) * QK]
        query = bf16(
            jnp.concatenate([raw[:, :NOPE], rotate(raw[:, NOPE:], cosine, sine)], axis=1)
        )
        rot_ref[:, head * QK : (head + 1) * QK] = query
        key = jnp.concatenate([lat_ref[:, head * KV : head * KV + NOPE], shared], axis=1)
        value = lat_ref[:, head * KV + NOPE : (head + 1) * KV]
        scores = jnp.where(allowed, dot_t(query, key) * factor, masked_score)
        top = jnp.max(scores, axis=1, keepdims=True)
        powers = jnp.exp(scores - top)
        probs = powers / jnp.sum(powers, axis=1, keepdims=True)
        out_ref[:, head * VD : (head + 1) * VD] = bf16(dot(bf16(probs), value))


def attend(query_raw, latent, keyed, tables):
    cosine, sine, seg_col, seg_row = tables
    count, _, rows = seg_row.shape
    heads = query_raw.shape[1] // QK
    block = lambda width: pl.BlockSpec((rows, width), lambda i: (i, 0))
    return pl.pallas_call(
        functools.partial(attend_kernel, heads),
        grid=(count,),
        in_specs=[
            block(heads * QK),
            block(heads * KV),
            block(LAT + ROPE),
            block(HALF),
            block(HALF),
            block(1),
            pl.BlockSpec((1, 1, rows), lambda i: (i, 0, 0)),
        ],
        out_specs=[block(heads * VD), block(heads * QK)],
        out_shape=[
            jax.ShapeDtypeStruct((count * rows, heads * VD), jnp.bfloat16),
            jax.ShapeDtypeStruct((count * rows, heads * QK), jnp.bfloat16),
        ],
        name="attend",
        cost_estimate=pl.CostEstimate(
            flops=2 * count * heads * rows * rows * (QK + VD),
            bytes_accessed=count * rows * heads * (QK * 6 + KV * 2 + VD * 2),
            transcendentals=count * heads * rows * rows,
        ),
    )(query_raw, latent, keyed, cosine, sine, seg_col, seg_row)


def attend_back_kernel(
    heads, q_ref, lat_ref, key_ref, grad_ref, cos_ref, sin_ref, col_ref, row_ref, dq_ref, dlat_ref, dkey_ref
):
    factor = QK**-0.5
    allowed = allowed_pairs(col_ref[...], row_ref[0])
    cosine, sine = cos_ref[...], sin_ref[...]
    shared = key_ref[:, LAT:]
    total = None
    for head in range(heads):
        query = q_ref[:, head * QK : (head + 1) * QK]
        key = jnp.concatenate([lat_ref[:, head * KV : head * KV + NOPE], shared], axis=1)
        value = lat_ref[:, head * KV + NOPE : (head + 1) * KV]
        grad = grad_ref[:, head * VD : (head + 1) * VD]
        scores = jnp.where(allowed, dot_t(query, key) * factor, masked_score)
        top = jnp.max(scores, axis=1, keepdims=True)
        powers = jnp.exp(scores - top)
        probs = powers / jnp.sum(powers, axis=1, keepdims=True)
        grad_value = t_dot(bf16(probs), grad)
        grad_probs = dot_t(grad, value)
        centre = jnp.sum(probs * grad_probs, axis=1, keepdims=True)
        grad_scores = bf16(probs * (grad_probs - centre) * factor)
        grad_query = dot(grad_scores, key)
        grad_key = t_dot(grad_scores, query)
        dq_ref[:, head * QK : (head + 1) * QK] = bf16(
            jnp.concatenate(
                [grad_query[:, :NOPE], rotate(grad_query[:, NOPE:], cosine, -sine)], axis=1
            )
        )
        dlat_ref[:, head * KV : head * KV + NOPE] = bf16(grad_key[:, :NOPE])
        dlat_ref[:, head * KV + NOPE : (head + 1) * KV] = bf16(grad_value)
        part = grad_key[:, NOPE:]
        total = part if total is None else total + part
    dkey_ref[...] = total


def attend_back(query, latent, keyed, grad, tables):
    cosine, sine, seg_col, seg_row = tables
    count, _, rows = seg_row.shape
    heads = query.shape[1] // QK
    block = lambda width: pl.BlockSpec((rows, width), lambda i: (i, 0))
    return pl.pallas_call(
        functools.partial(attend_back_kernel, heads),
        grid=(count,),
        in_specs=[
            block(heads * QK),
            block(heads * KV),
            block(LAT + ROPE),
            block(heads * VD),
            block(HALF),
            block(HALF),
            block(1),
            pl.BlockSpec((1, 1, rows), lambda i: (i, 0, 0)),
        ],
        out_specs=[block(heads * QK), block(heads * KV), block(ROPE)],
        out_shape=[
            jax.ShapeDtypeStruct((count * rows, heads * QK), jnp.bfloat16),
            jax.ShapeDtypeStruct((count * rows, heads * KV), jnp.bfloat16),
            jax.ShapeDtypeStruct((count * rows, ROPE), jnp.float32),
        ],
        name="attend_back",
        cost_estimate=pl.CostEstimate(
            flops=2 * count * heads * rows * rows * (3 * QK + 2 * VD),
            bytes_accessed=count * rows * heads * (QK * 4 + KV * 4 + VD * 2),
            transcendentals=count * heads * rows * rows,
        ),
    )(query, latent, keyed, grad, cosine, sine, seg_col, seg_row)


def split_in(flat):
    half = flat.shape[1] // 2
    return flat[:, :half], flat[:, half:]


def gated_hidden(pre):
    gate, up = split_in(pre)
    return silu_parts(gate)[0] * up


def gated_back(pre, grad_hidden):
    gate, up = split_in(pre)
    act, slope = silu_parts(gate)
    return bf16(jnp.concatenate([grad_hidden * up * slope, grad_hidden * act], axis=1))


def body(
    boundary,
    lengths,
    routes,
    attn_gain,
    query_weight,
    compress_weight,
    latent_gain,
    expand_weight,
    output_weight,
    ffn_gain,
    router_weight,
    shared_in,
    shared_out,
    expert_in,
    expert_out,
):
    attn_gain, latent_gain, ffn_gain = attn_gain[0], latent_gain[0], ffn_gain[0]
    query_weight, compress_weight = query_weight[0], compress_weight[0]
    expand_weight, output_weight = expand_weight[0], output_weight[0]
    router_weight, shared_out, expert_out = router_weight[0], shared_out[0], expert_out[0, 0]
    width = boundary.shape[3]
    rows = boundary.shape[2]
    shared_in_shape, expert_in_shape = shared_in.shape, expert_in.shape
    shared_in = shared_in.reshape(width, -1)
    expert_in = expert_in.reshape(width, -1)

    packs, members = lax.axis_size("dp"), lax.axis_size("expert")
    count = packs * members
    pack, member = lax.axis_index("dp"), lax.axis_index("expert")
    me = pack * members + member
    is_first = lax.axis_index("section") == 0
    pack_rows = members * rows
    top = routes.shape[3]
    experts = router_weight.shape[1]

    def own_pack(value, per_block=None):
        size = value.shape[0] // packs
        return lax.dynamic_slice_in_dim(value, pack * size, size, 0)

    own_lengths = lax.dynamic_index_in_dim(lengths[0, 0], member, 0, keepdims=True)
    whole = gather_all(jnp.concatenate([routes.reshape(1, rows * top), own_lengths], axis=1))
    routes_all = whole[:, : rows * top].reshape(count * rows, top)
    routed = jnp.any(routes_all == me, axis=1, keepdims=True).astype(jnp.float32)
    segment, position = block_layout(whole[:, rows * top :], rows)
    freqs = rope_base ** (-jnp.arange(HALF, dtype=jnp.float32) / HALF)
    angles = position.reshape(-1).astype(jnp.float32)[:, None] * freqs[None, :]
    tables_all = (
        jnp.cos(angles),
        jnp.sin(angles),
        segment.reshape(count * rows, 1),
        segment.reshape(count, 1, rows),
    )
    tables_pack = tuple(own_pack(table) for table in tables_all)
    own_cos, own_sin = (
        lax.dynamic_slice_in_dim(table, me * rows, rows, 0) for table in tables_all[:2]
    )
    own_column = (lax.broadcasted_iota(jnp.int32, (1, experts), 1) == me).astype(jnp.float32)

    def forward(hidden, keep):
        normed32, scale_attn = rms_forward(hidden, attn_gain)
        normed = bf16(normed32)
        compressed = dot(normed, compress_weight)
        latent32, scale_latent = rms_forward(compressed[:, :LAT], latent_gain)
        keyed = bf16(
            jnp.concatenate([latent32, rotate(compressed[:, LAT:], own_cos, own_sin)], axis=1)
        )
        if keep:
            normed_all, keyed_all = gather_all(normed), gather_all(keyed)
            normed_pack, keyed_pack = own_pack(normed_all), own_pack(keyed_all)
        else:
            normed_pack, keyed_pack = gather_pack(normed), gather_pack(keyed)
        query_raw = dot(normed_pack, query_weight)
        latent = bf16(dot(keyed_pack[:, :LAT], expand_weight))
        attended, query = attend(query_raw, latent, keyed_pack, tables_pack)
        mixed = hidden + scatter_pack(bf16(dot(attended, output_weight))).astype(jnp.float32)
        ffn32, scale_ffn = rms_forward(mixed, ffn_gain)
        ffn = bf16(ffn32)
        ffn_all = gather_all(ffn)
        prob_all = jax.nn.softmax(dot(ffn_all, router_weight), axis=-1)
        own_prob = jnp.sum(prob_all * own_column, axis=1, keepdims=True)
        gate = own_prob * routed
        expert_pre = dot(ffn_all, expert_in)
        expert_hid = gated_hidden(expert_pre)
        gated = bf16(gate * expert_hid)
        ffn_pack = own_pack(ffn_all)
        shared_pre = dot(ffn_pack, shared_in)
        shared_hid = bf16(gated_hidden(shared_pre))
        partial = dot(gated, expert_out)
        shared_part = dot(shared_hid, shared_out)
        partial = bf16(
            lax.dynamic_update_slice_in_dim(
                partial, own_pack(partial) + shared_part, pack * pack_rows, 0
            )
        )
        result = mixed + scatter_all(partial).astype(jnp.float32)
        if not keep:
            return result, None
        stored = dict(
            normed=normed,
            compressed=compressed,
            scale_attn=scale_attn,
            scale_latent=scale_latent,
            normed_all=normed_all,
            keyed_all=keyed_all,
            keyed_pack=keyed_pack,
            latent=latent,
            query=query,
            mixed=mixed,
            scale_ffn=scale_ffn,
            ffn_all=ffn_all,
            prob_all=prob_all,
            own_prob=own_prob,
            gate=gate,
            expert_pre=expert_pre,
            gated=gated,
            shared_pre=shared_pre,
        )
        return result, stored

    def backward(hidden, stored, upstream, weights):
        upstream_all = gather_all(bf16(upstream))
        grad_units = dot_t(upstream_all, expert_out)
        expert_pre = stored["expert_pre"]
        grad_pre = gated_back(expert_pre, stored["gate"] * grad_units)
        grad_gate = jnp.sum(grad_units * gated_hidden(expert_pre), axis=1, keepdims=True)
        moved = stored["own_prob"] * grad_gate * routed
        grad_logits = bf16(moved * (own_column - stored["prob_all"]))
        upstream_pack = own_pack(upstream_all)
        grad_shared = gated_back(stored["shared_pre"], dot_t(upstream_pack, shared_out))
        shared_part = dot_t(grad_shared, shared_in)
        partial = dot_t(grad_pre, expert_in) + dot_t(grad_logits, router_weight)
        partial = bf16(
            lax.dynamic_update_slice_in_dim(
                partial, own_pack(partial) + shared_part, pack * pack_rows, 0
            )
        )
        grad_ffn = scatter_all(partial).astype(jnp.float32)
        grad_mixed_norm, grad_ffn_gain = rms_backward(
            stored["mixed"], stored["scale_ffn"], ffn_gain, grad_ffn
        )
        grad_mixed = upstream + grad_mixed_norm
        if weights:
            grad_mixed_all = gather_all(bf16(grad_mixed))
            query_all_raw = dot(stored["normed_all"], query_weight)
            latent_all = bf16(dot(stored["keyed_all"][:, :LAT], expand_weight))
            attended_all, query_all = attend(
                query_all_raw, latent_all, stored["keyed_all"], tables_all
            )
            grad_attended = bf16(dot_t(grad_mixed_all, output_weight))
            grad_query_all, grad_latent_all, grad_shared_key = attend_back(
                query_all, latent_all, stored["keyed_all"], grad_attended, tables_all
            )
            grad_query, grad_latent_heads, grad_shared_key = (
                own_pack(value) for value in (grad_query_all, grad_latent_all, grad_shared_key)
            )
        else:
            grad_mixed_pack = gather_pack(bf16(grad_mixed))
            grad_attended = bf16(dot_t(grad_mixed_pack, output_weight))
            grad_query, grad_latent_heads, grad_shared_key = attend_back(
                stored["query"], stored["latent"], stored["keyed_pack"], grad_attended, tables_pack
            )
        own = scatter_pack(
            bf16(
                jnp.concatenate(
                    [
                        dot_t(grad_query, query_weight),
                        dot_t(grad_latent_heads, expand_weight),
                        grad_shared_key,
                    ],
                    axis=1,
                )
            )
        ).astype(jnp.float32)
        grad_latent, grad_latent_gain = rms_backward(
            stored["compressed"][:, :LAT],
            stored["scale_latent"],
            latent_gain,
            own[:, width : width + LAT],
        )
        grad_compressed = bf16(
            jnp.concatenate([grad_latent, rotate(own[:, width + LAT :], own_cos, -own_sin)], axis=1)
        )
        grad_normed = own[:, :width] + dot_t(grad_compressed, compress_weight)
        grad_hidden_norm, grad_attn_gain = rms_backward(
            hidden, stored["scale_attn"], attn_gain, grad_normed
        )
        grad_hidden = grad_mixed + grad_hidden_norm
        if not weights:
            return grad_hidden, None
        shared_pre = dot(stored["ffn_all"], shared_in)
        shared_hid = bf16(gated_hidden(shared_pre))
        grad_shared_all = gated_back(shared_pre, dot_t(upstream_all, shared_out))
        grads = dict(
            query=t_dot(stored["normed_all"], grad_query_all),
            expand=t_dot(stored["keyed_all"][:, :LAT], grad_latent_all),
            output=t_dot(attended_all, grad_mixed_all),
            shared_in=t_dot(stored["ffn_all"], grad_shared_all),
            shared_out=t_dot(shared_hid, upstream_all),
            expert_in=t_dot(stored["ffn_all"], grad_pre),
            expert_out=t_dot(stored["gated"], upstream_all),
            compress=t_dot(stored["normed_all"], gather_all(grad_compressed)),
        )
        small = jnp.concatenate([grad_attn_gain, grad_latent_gain, grad_ffn_gain])
        small = jnp.sum(gather_all(small[None]), axis=0)
        router = lax.psum(t_dot(stored["ffn_all"], grad_logits), BOTH)
        grads["attn_gain"] = small[:width]
        grads["latent_gain"] = small[width : width + LAT]
        grads["ffn_gain"] = small[width + LAT :]
        grads["router"] = router
        return grad_hidden, grads

    fresh = boundary[0, 0].astype(jnp.float32)
    first_result, _ = forward(fresh, False)
    inbound = lax.ppermute(bf16(first_result), "section", [(0, 1)])
    hidden = jnp.where(is_first, fresh, inbound.astype(jnp.float32))
    result, stored = forward(hidden, True)
    grad_first, _ = backward(hidden, stored, fresh, False)
    downbound = lax.ppermute(grad_first, "section", [(1, 0)])
    upstream = jnp.where(is_first, downbound, fresh)
    grad_hidden, grads = backward(hidden, stored, upstream, True)
    ends = jnp.where(is_first, grad_hidden, result)
    return (
        ends[None, None],
        grads["attn_gain"][None],
        grads["query"][None],
        grads["compress"][None],
        grads["latent_gain"][None],
        grads["expand"][None],
        grads["output"][None],
        grads["ffn_gain"][None],
        grads["router"][None],
        grads["shared_in"].reshape(shared_in_shape),
        grads["shared_out"][None],
        grads["expert_in"].reshape(expert_in_shape),
        grads["expert_out"][None, None],
    )


def solution(mesh):
    return jax.shard_map(
        body,
        mesh=mesh,
        in_specs=(
            P("section", None, BOTH, None),
            P(None, "dp", None, None),
            P("section", None, BOTH, None),
            P("section", None),
            P("section", None, "expert"),
            P("section", None, None),
            P("section", None),
            P("section", None, "expert"),
            P("section", "expert", None),
            P("section", None),
            P("section", None, None),
            P("section", None, None, "expert"),
            P("section", "expert", None),
            P("section", BOTH, None, None, None),
            P("section", BOTH, None, None),
        ),
        out_specs=(
            P("section", None, BOTH, None),
            P("section", None),
            P("section", None, "expert"),
            P("section", None, None),
            P("section", None),
            P("section", None, "expert"),
            P("section", "expert", None),
            P("section", None),
            P("section", None, None),
            P("section", None, None, "expert"),
            P("section", "expert", None),
            P("section", BOTH, None, None, None),
            P("section", BOTH, None, None),
        ),
        check_vma=False,
    )
```

```python
import functools

import jax
import jax.numpy as jnp
from jax import lax
from jax.experimental import pallas as pl
from jax.experimental.pallas import tpu as pltpu
from jax.sharding import PartitionSpec as P

NOPE = 128
ROPE = 64
VD = 128
LAT = 512

QK = NOPE + ROPE
KV = NOPE + VD
HALF = ROPE // 2
epsilon = 1e-06
rope_base = 10000.0
masked_score = -1e30
BOTH = ("dp", "expert")
MESH = pl.DeviceIdType.MESH
IDS = {
    name: index
    for index, name in enumerate(
        (
            "gather_target",
            "gather_inputs_first",
            "gather_ffn_first",
            "gather_inputs_second",
            "gather_ffn_second",
            "gather_mixed",
            "gather_upstream",
            "gather_keyed_first",
            "gather_keyed_second",
            "scatter_attended_first",
            "scatter_ffn_first",
            "scatter_attended_second",
            "scatter_result",
            "scatter_ffn_back_second",
            "scatter_heads_second",
            "scatter_ffn_back_first",
        )
    )
}


def dot(left, right):
    return jnp.dot(left, right, preferred_element_type=jnp.float32)


def dot_t(left, right):
    return lax.dot_general(
        left, right, (((1,), (1,)), ((), ())), preferred_element_type=jnp.float32
    )


def t_dot(left, right):
    return lax.dot_general(
        left, right, (((0,), (0,)), ((), ())), preferred_element_type=jnp.float32
    )


def bf16(value):
    return value.astype(jnp.bfloat16)


def rms_forward(inputs, gain_vec):
    norm_scale = lax.rsqrt(jnp.mean(inputs * inputs, axis=-1, keepdims=True) + epsilon)
    return (inputs * norm_scale * gain_vec, norm_scale)


def rms_backward(inputs, norm_scale, gain_vec, upstream):
    weighted = upstream * gain_vec
    grad_gain = jnp.sum(upstream * inputs * norm_scale, axis=0)
    cubed = norm_scale * norm_scale * norm_scale
    grad_inputs = norm_scale * weighted - inputs * cubed * jnp.mean(
        weighted * inputs, axis=-1, keepdims=True
    )
    return (grad_inputs, grad_gain)


def rotate(inputs, cosine, sine):
    half = cosine.shape[-1]
    former = inputs[..., :half]
    latter = inputs[..., half:]
    return jnp.concatenate(
        [former * cosine - latter * sine, latter * cosine + former * sine], axis=-1
    )


def silu_parts(pre_gate):
    sigmoid = jax.nn.sigmoid(pre_gate)
    return (pre_gate * sigmoid, sigmoid * (1.0 + pre_gate * (1.0 - sigmoid)))


def block_layout(block_lengths, rows):
    starts = jnp.cumsum(block_lengths, axis=1) - block_lengths
    index = jnp.arange(rows, dtype=jnp.int32)
    begun = index[None, :, None] >= starts[:, None, :]
    segment = jnp.sum(begun.astype(jnp.int32), axis=2)
    opening = jnp.max(jnp.where(begun, starts[:, None, :], 0), axis=2)
    return segment, index[None, :] - opening


def places(spots):
    member = lax.axis_index("expert")
    spot = lax.axis_index("dp") if spots > 1 else 0
    return spot, member // 2, lax.rem(member, 2)


def to_partner(chip, core):
    return {"expert": chip * 2 + 1 - core}


def to_other(chip, core):
    return {"expert": (1 - chip) * 2 + core}


def when(condition, action):
    if condition is True:
        action()
    else:
        pl.when(condition)(action)


def greet(spots, spot, chip, core):
    barrier = pltpu.get_barrier_semaphore()

    def signal(target):
        pl.semaphore_signal(barrier, inc=1, device_id=target, device_id_type=MESH)

    signal(to_partner(chip, core))
    signal(to_other(chip, core))
    if spots > 1:
        pl.when(spot > 0)(lambda: signal({"dp": spot - 1}))
        pl.when(spot < spots - 1)(lambda: signal({"dp": spot + 1}))
        ends = jnp.where(spot > 0, 1, 0) + jnp.where(spot < spots - 1, 1, 0)
        pl.semaphore_wait(barrier, 2 + ends)
    else:
        pl.semaphore_wait(barrier, 2)


def remote(source, target_ref, target, out_sem, in_sem):
    return pltpu.make_async_remote_copy(
        src_ref=source,
        dst_ref=target_ref,
        send_sem=out_sem,
        recv_sem=in_sem,
        device_id=target,
        device_id_type=MESH,
    )


def slot(spot, chip, core):
    return spot * 4 + chip * 2 + core


def gather_kernel(spots, cuts, active, *refs):
    arrays = len(cuts)
    x_refs, o_refs, sems = refs[:arrays], refs[-9 - arrays : -9], refs[-9:]
    own_sem, up_out, up_in, down_out, down_in, over_out, over_in, pair_out, pair_in = sems
    units = [
        (a, pl.ds(part * (x_refs[a].shape[0] // parts), x_refs[a].shape[0] // parts))
        for a, parts in enumerate(cuts)
        for part in range(parts)
    ]

    def run():
        spot, chip, core = places(spots)
        greet(spots, spot, chip, core)

        def piece(unit, index):
            array, cut = units[unit]
            return o_refs[array].at[index, cut]

        def first(unit):
            array, cut = units[unit]
            return x_refs[array].at[cut]

        def up(source, at, unit, reach):
            return remote(
                source, piece(unit, slot(at, chip, core)), {"dp": spot + 1}, up_out.at[reach, unit], up_in.at[reach, unit]
            )

        def down(source, at, unit, reach):
            return remote(
                source,
                piece(unit, slot(at, chip, core)),
                {"dp": spot - 1},
                down_out.at[reach, unit],
                down_in.at[reach, unit],
            )

        def over(source, at, unit):
            return remote(
                source, piece(unit, slot(at, chip, core)), to_other(chip, core), over_out.at[at, unit], over_in.at[at, unit]
            )

        def pair(source, at, c, unit):
            return remote(
                source,
                piece(unit, slot(at, c, core)),
                to_partner(chip, core),
                pair_out.at[c, at, unit],
                pair_in.at[c, at, unit],
            )

        mine = slot(spot, chip, core)
        for unit in range(len(units)):
            source = first(unit)
            over(source, spot, unit).start()
            if spots > 1:
                pl.when(spot < spots - 1)(lambda: up(source, spot, unit, 0).start())
                pl.when(spot > 0)(lambda: down(source, spot, unit, 0).start())
            pair(source, spot, chip, unit).start()
        own = [pltpu.make_async_copy(x_refs[a], o_refs[a].at[mine], own_sem.at[a]) for a in range(arrays)]
        for copy in own:
            copy.start()
        for reach in range(1, spots):
            for unit in range(len(units)):

                def below(reach=reach, unit=unit):
                    at = spot - reach
                    source = piece(unit, slot(at, chip, core))
                    up(source, at, unit, reach - 1).wait_recv()
                    pl.when(spot < spots - 1)(lambda: up(source, at, unit, reach).start())
                    over(source, at, unit).start()
                    pair(source, at, chip, unit).start()

                def above(reach=reach, unit=unit):
                    at = spot + reach
                    source = piece(unit, slot(at, chip, core))
                    down(source, at, unit, reach - 1).wait_recv()
                    pl.when(spot > 0)(lambda: down(source, at, unit, reach).start())
                    over(source, at, unit).start()
                    pair(source, at, chip, unit).start()

                pl.when(spot >= reach)(below)
                pl.when(spot + reach < spots)(above)
        for reach in range(spots):
            sides = [(True, spot)]
            if reach > 0:
                sides = [(spot >= reach, spot - reach), (spot + reach < spots, spot + reach)]
            for unit in range(len(units)):
                for there, at in sides:

                    def hand_on(at=at, unit=unit):
                        source = piece(unit, slot(at, 1 - chip, core))
                        over(source, at, unit).wait_recv()
                        pair(source, at, 1 - chip, unit).start()

                    when(there, hand_on)
        for copy in own:
            copy.wait()
        for unit in range(len(units)):
            source = piece(unit, mine)
            for at in range(spots):
                over(source, at, unit).wait_send()
                for c in range(2):
                    pair(source, at, c, unit).wait()
            for reach in range(spots - 1):
                pl.when((spot >= reach) & (spot < spots - 1))(lambda: up(source, spot, unit, reach).wait_send())
                pl.when((spot + reach < spots) & (spot > 0))(lambda: down(source, spot, unit, reach).wait_send())

    if active is None:
        run()
    else:
        pl.when(lax.axis_index("section") == active)(run)


def gather_blocks(values, across, name, active=None, into=None, parts=4):
    axes = BOTH if across else "expert"
    if lax.axis_size("expert") != 4:
        found = [lax.all_gather(value, axes, axis=0, tiled=True) for value in values]
        if into is None:
            return found
        chosen = lax.axis_index("section") == active
        return [jnp.where(chosen, new, old) for new, old in zip(found, into)]
    spots = lax.axis_size("dp") if across else 1
    cuts = [parts if value.shape[0] % (16 * parts) == 0 else 1 for value in values]
    units = sum(cuts)
    dma = pltpu.SemaphoreType.DMA
    hops = max(spots - 1, 1)
    shapes = [jax.ShapeDtypeStruct((spots * 4, *value.shape), value.dtype) for value in values]
    held = [] if into is None else [old.reshape(shape.shape) for old, shape in zip(into, shapes)]
    outs = pl.pallas_call(
        functools.partial(gather_kernel, spots, cuts, active),
        out_shape=shapes,
        in_specs=[pl.BlockSpec(memory_space=pltpu.VMEM)] * len(values)
        + [pl.BlockSpec(memory_space=pl.ANY)] * len(held),
        out_specs=[pl.BlockSpec(memory_space=pl.ANY)] * len(values),
        input_output_aliases={len(values) + index: index for index in range(len(held))},
        scratch_shapes=[
            dma((len(values),)),
            dma((hops, units)),
            dma((hops, units)),
            dma((hops, units)),
            dma((hops, units)),
            dma((spots, units)),
            dma((spots, units)),
            dma((2, spots, units)),
            dma((2, spots, units)),
        ],
        compiler_params=pltpu.CompilerParams(collective_id=IDS[name], has_side_effects=True),
        name=name,
    )(*values, *held)
    return [out.reshape(-1, out.shape[2]) for out in outs]


def add_into(target, sources, rows, step=16):
    def some(index, carry):
        at = pl.ds(pl.multiple_of(index * step, step), step)
        total = sources[0][at, :].astype(jnp.float32)
        for source in sources[1:]:
            total = total + source[at, :].astype(jnp.float32)
        target[at, :] = total.astype(target.dtype)
        return carry

    lax.fori_loop(0, rows // step, some, 0)


def scatter_kernel(
    spots,
    parts,
    active,
    x_ref,
    o_ref,
    pair_buf,
    over_src,
    over_buf,
    line_src,
    up_buf,
    down_buf,
    pair_out,
    pair_in,
    over_out,
    over_in,
    line_out,
    up_in,
    down_in,
):
    rows = x_ref.shape[1] // parts
    cut = lambda part: pl.ds(part * rows, rows)

    def run():
        spot, chip, core = places(spots)
        greet(spots, spot, chip, core)

        def order(step):
            if step == spots - 1:
                return spot
            fall = spots - 1 - step
            fall = jnp.where(fall <= spot, fall - 1, fall)
            rise = jnp.where(step >= spot, step + 1, step)
            return jnp.where(2 * spot < spots - 1, fall, rise)

        def pair(at, c, part):
            return remote(
                x_ref.at[slot(at, c, 1 - core), cut(part)],
                pair_buf.at[at, c, cut(part)],
                to_partner(chip, core),
                pair_out.at[at, c, part],
                pair_in.at[at, c, part],
            )

        def over(at, part):
            return remote(
                over_src.at[at, cut(part)],
                over_buf.at[at, cut(part)],
                to_other(chip, core),
                over_out.at[at, part],
                over_in.at[at, part],
            )

        def up(at, part):
            return remote(
                line_src.at[at, cut(part)],
                up_buf.at[at, cut(part)],
                {"dp": spot + 1},
                line_out.at[at, part],
                up_in.at[at, part],
            )

        def down(at, part):
            return remote(
                line_src.at[at, cut(part)],
                down_buf.at[at, cut(part)],
                {"dp": spot - 1},
                line_out.at[at, part],
                down_in.at[at, part],
            )

        for c in (1 - chip, chip):
            for step in range(spots):
                for part in range(parts):
                    pair(order(step), c, part).start()
        for step in range(spots):
            at = order(step)
            for part in range(parts):
                pair(at, 1 - chip, part).wait_recv()
                add_into(
                    over_src.at[at, cut(part)],
                    [x_ref.at[slot(at, 1 - chip, core), cut(part)], pair_buf.at[at, 1 - chip, cut(part)]],
                    rows,
                )
                over(at, part).start()
        for step in range(spots):
            at = order(step)
            for part in range(parts):
                pair(at, chip, part).wait_recv()
                over(at, part).wait_recv()
                base = [
                    x_ref.at[slot(at, chip, core), cut(part)],
                    pair_buf.at[at, chip, cut(part)],
                    over_buf.at[at, cut(part)],
                ]
                ups, downs = up_buf.at[at, cut(part)], down_buf.at[at, cut(part)]
                if step < spots - 1:
                    target = line_src.at[at, cut(part)]

                    def rising(first):
                        if not first:
                            up(at, part).wait_recv()
                        add_into(target, base if first else base + [ups], rows)
                        up(at, part).start()

                    def falling(first):
                        if not first:
                            down(at, part).wait_recv()
                        add_into(target, base if first else base + [downs], rows)
                        down(at, part).start()

                    pl.when((at > spot) & (spot == 0))(lambda: rising(True))
                    pl.when((at > spot) & (spot > 0))(lambda: rising(False))
                    pl.when((at < spot) & (spot == spots - 1))(lambda: falling(True))
                    pl.when((at < spot) & (spot < spots - 1))(lambda: falling(False))
                elif spots == 1:
                    add_into(o_ref.at[cut(part)], base, rows)
                else:

                    def finish(ends):
                        if ends < 1:
                            up(at, part).wait_recv()
                        if ends > -1:
                            down(at, part).wait_recv()
                        extra = ([ups] if ends < 1 else []) + ([downs] if ends > -1 else [])
                        add_into(o_ref.at[cut(part)], base + extra, rows)

                    pl.when(spot == 0)(lambda: finish(1))
                    pl.when(spot == spots - 1)(lambda: finish(-1))
                    pl.when((spot > 0) & (spot < spots - 1))(lambda: finish(0))
        for part in range(parts):
            for step in range(spots):
                at = order(step)
                pair(at, 0, part).wait_send()
                pair(at, 1, part).wait_send()
                over(at, part).wait_send()
                if step < spots - 1:
                    up(at, part).wait_send()

    if active is None:
        run()
    else:
        pl.when(lax.axis_index("section") == active)(run)


def scatter_blocks(partial, across, name, active=None, parts=4):
    if lax.axis_size("expert") != 4:
        axes = BOTH if across else "expert"
        return lax.psum_scatter(partial, axes, scatter_dimension=0, tiled=True).astype(jnp.float32)
    spots = lax.axis_size("dp") if across else 1
    rows, width = partial.shape[0] // (spots * 4), partial.shape[1]
    dma = pltpu.SemaphoreType.DMA
    hold = lambda *lead: pltpu.VMEM((*lead, rows, width), partial.dtype)
    return pl.pallas_call(
        functools.partial(scatter_kernel, spots, parts, active),
        out_shape=jax.ShapeDtypeStruct((rows, width), jnp.float32),
        in_specs=[pl.BlockSpec(memory_space=pltpu.VMEM)],
        out_specs=pl.BlockSpec(memory_space=pltpu.VMEM),
        scratch_shapes=[
            hold(spots, 2),
            hold(spots),
            hold(spots),
            hold(spots),
            hold(spots),
            hold(spots),
            dma((spots, 2, parts)),
            dma((spots, 2, parts)),
            dma((spots, parts)),
            dma((spots, parts)),
            dma((spots, parts)),
            dma((spots, parts)),
            dma((spots, parts)),
        ],
        compiler_params=pltpu.CompilerParams(collective_id=IDS[name], has_side_effects=True),
        name=name,
    )(partial.reshape(spots * 4, rows, width))


def allowed_pairs(seg_col, seg_row):
    rows = seg_col.shape[0]
    later = lax.broadcasted_iota(jnp.int32, (rows, rows), 0)
    earlier = lax.broadcasted_iota(jnp.int32, (rows, rows), 1)
    return (seg_col == seg_row) & (earlier <= later)


def attend_kernel(heads, q_ref, lat_ref, key_ref, cos_ref, sin_ref, col_ref, row_ref, out_ref, rot_ref):
    factor = QK**-0.5
    allowed = allowed_pairs(col_ref[...], row_ref[0])
    cosine, sine = cos_ref[...], sin_ref[...]
    shared = key_ref[:, LAT:]
    for head in range(heads):
        raw = q_ref[:, head * QK : (head + 1) * QK]
        query = bf16(
            jnp.concatenate([raw[:, :NOPE], rotate(raw[:, NOPE:], cosine, sine)], axis=1)
        )
        rot_ref[:, head * QK : (head + 1) * QK] = query
        key = jnp.concatenate([lat_ref[:, head * KV : head * KV + NOPE], shared], axis=1)
        value = lat_ref[:, head * KV + NOPE : (head + 1) * KV]
        scores = jnp.where(allowed, dot_t(query, key) * factor, masked_score)
        top = jnp.max(scores, axis=1, keepdims=True)
        powers = jnp.exp(scores - top)
        probs = powers / jnp.sum(powers, axis=1, keepdims=True)
        out_ref[:, head * VD : (head + 1) * VD] = bf16(dot(bf16(probs), value))


def attend(query_raw, latent, keyed, tables):
    cosine, sine, seg_col, seg_row = tables
    count, _, rows = seg_row.shape
    heads = query_raw.shape[1] // QK
    block = lambda width: pl.BlockSpec((rows, width), lambda i: (i, 0))
    return pl.pallas_call(
        functools.partial(attend_kernel, heads),
        grid=(count,),
        in_specs=[
            block(heads * QK),
            block(heads * KV),
            block(LAT + ROPE),
            block(HALF),
            block(HALF),
            block(1),
            pl.BlockSpec((1, 1, rows), lambda i: (i, 0, 0)),
        ],
        out_specs=[block(heads * VD), block(heads * QK)],
        out_shape=[
            jax.ShapeDtypeStruct((count * rows, heads * VD), jnp.bfloat16),
            jax.ShapeDtypeStruct((count * rows, heads * QK), jnp.bfloat16),
        ],
        name="attend",
        cost_estimate=pl.CostEstimate(
            flops=2 * count * heads * rows * rows * (QK + VD),
            bytes_accessed=count * rows * heads * (QK * 6 + KV * 2 + VD * 2),
            transcendentals=count * heads * rows * rows,
        ),
    )(query_raw, latent, keyed, cosine, sine, seg_col, seg_row)


def attend_back_kernel(
    heads, q_ref, lat_ref, key_ref, grad_ref, cos_ref, sin_ref, col_ref, row_ref, dq_ref, dlat_ref, dkey_ref
):
    factor = QK**-0.5
    allowed = allowed_pairs(col_ref[...], row_ref[0])
    cosine, sine = cos_ref[...], sin_ref[...]
    shared = key_ref[:, LAT:]
    total = None
    for head in range(heads):
        query = q_ref[:, head * QK : (head + 1) * QK]
        key = jnp.concatenate([lat_ref[:, head * KV : head * KV + NOPE], shared], axis=1)
        value = lat_ref[:, head * KV + NOPE : (head + 1) * KV]
        grad = grad_ref[:, head * VD : (head + 1) * VD]
        scores = jnp.where(allowed, dot_t(query, key) * factor, masked_score)
        top = jnp.max(scores, axis=1, keepdims=True)
        powers = jnp.exp(scores - top)
        probs = powers / jnp.sum(powers, axis=1, keepdims=True)
        grad_value = t_dot(bf16(probs), grad)
        grad_probs = dot_t(grad, value)
        centre = jnp.sum(probs * grad_probs, axis=1, keepdims=True)
        grad_scores = bf16(probs * (grad_probs - centre) * factor)
        grad_query = dot(grad_scores, key)
        grad_key = t_dot(grad_scores, query)
        dq_ref[:, head * QK : (head + 1) * QK] = bf16(
            jnp.concatenate(
                [grad_query[:, :NOPE], rotate(grad_query[:, NOPE:], cosine, -sine)], axis=1
            )
        )
        dlat_ref[:, head * KV : head * KV + NOPE] = bf16(grad_key[:, :NOPE])
        dlat_ref[:, head * KV + NOPE : (head + 1) * KV] = bf16(grad_value)
        part = grad_key[:, NOPE:]
        total = part if total is None else total + part
    dkey_ref[...] = total


def attend_back(query, latent, keyed, grad, tables):
    cosine, sine, seg_col, seg_row = tables
    count, _, rows = seg_row.shape
    heads = query.shape[1] // QK
    block = lambda width: pl.BlockSpec((rows, width), lambda i: (i, 0))
    return pl.pallas_call(
        functools.partial(attend_back_kernel, heads),
        grid=(count,),
        in_specs=[
            block(heads * QK),
            block(heads * KV),
            block(LAT + ROPE),
            block(heads * VD),
            block(HALF),
            block(HALF),
            block(1),
            pl.BlockSpec((1, 1, rows), lambda i: (i, 0, 0)),
        ],
        out_specs=[block(heads * QK), block(heads * KV), block(ROPE)],
        out_shape=[
            jax.ShapeDtypeStruct((count * rows, heads * QK), jnp.bfloat16),
            jax.ShapeDtypeStruct((count * rows, heads * KV), jnp.bfloat16),
            jax.ShapeDtypeStruct((count * rows, ROPE), jnp.float32),
        ],
        name="attend_back",
        cost_estimate=pl.CostEstimate(
            flops=2 * count * heads * rows * rows * (3 * QK + 2 * VD),
            bytes_accessed=count * rows * heads * (QK * 4 + KV * 4 + VD * 2),
            transcendentals=count * heads * rows * rows,
        ),
    )(query, latent, keyed, grad, cosine, sine, seg_col, seg_row)


def gated_hidden(gate, up):
    return silu_parts(gate)[0] * up


def gated_back(gate, up, grad_hidden):
    act, slope = silu_parts(gate)
    return bf16(grad_hidden * up * slope), bf16(grad_hidden * act)


def experts_kernel(
    full,
    here_ref,
    x_ref,
    routed_ref,
    own_ref,
    in_ref,
    out_w_ref,
    router_ref,
    shared_in_ref,
    shared_out_ref,
    pre_ref,
    gated_ref,
    prob_ref,
    shared_pre_ref,
    *partial_ref,
):
    units = gated_ref.shape[1]
    x = x_ref[...]
    logits = dot(x, router_ref[...])
    powers = jnp.exp(logits - jnp.max(logits, axis=1, keepdims=True))
    prob = powers / jnp.sum(powers, axis=1, keepdims=True)
    prob_ref[...] = prob
    gate = jnp.sum(prob * own_ref[...], axis=1, keepdims=True) * routed_ref[...]
    pre = dot(x, in_ref[...])
    pre_ref[...] = bf16(pre)
    gated = bf16(gate * gated_hidden(pre[:, :units], pre[:, units:]))
    gated_ref[...] = gated
    tile = pl.program_id(0)
    inside = (tile >= here_ref[0]) & (tile < here_ref[1])
    half = shared_out_ref.shape[0]

    def shared():
        left = dot_t(x, shared_in_ref[:half])
        right = dot_t(x, shared_in_ref[half:])
        shared_pre_ref[0] = bf16(left)
        shared_pre_ref[1] = bf16(right)
        return left, right

    if full:

        def with_shared():
            hidden = bf16(gated_hidden(*shared()))
            partial_ref[0][...] = bf16(dot(gated, out_w_ref[...]) + dot(hidden, shared_out_ref[...]))

        def without():
            partial_ref[0][...] = bf16(dot(gated, out_w_ref[...]))

        pl.when(inside)(with_shared)
        pl.when(jnp.logical_not(inside))(without)
    else:
        pl.when(inside)(lambda: shared() and None)


def tile_rows(pack_rows):
    return min(256, pack_rows)


def tile_here(pack, pack_rows):
    tiles = pack_rows // tile_rows(pack_rows)
    return jnp.stack([pack * tiles, (pack + 1) * tiles]).astype(jnp.int32)


def specs_of(rows, tile):
    block = lambda width: pl.BlockSpec((tile, width), lambda i, here: (i, 0))
    whole = lambda array: pl.BlockSpec(
        array.shape, lambda i, here: (0,) * array.ndim, pipeline_mode=pl.Buffered(1)
    )
    inner = lambda i, here: jnp.clip(i - here[0], 0, here[1] - here[0] - 1)
    return block, whole, inner


def experts(x, routed, own_column, weights, here, pack_rows, full):
    expert_in, expert_out, router, shared_in, shared_out = weights
    rows, width = x.shape
    tile = tile_rows(pack_rows)
    units, half = expert_out.shape[0], shared_out.shape[0]
    block, whole, inner = specs_of(rows, tile)
    shape = jax.ShapeDtypeStruct
    out_shape = [
        shape((rows, 2 * units), jnp.bfloat16),
        shape((rows, units), jnp.bfloat16),
        shape((rows, router.shape[1]), jnp.float32),
        shape((2, pack_rows, half), jnp.bfloat16),
    ]
    out_specs = [
        block(2 * units),
        block(units),
        block(router.shape[1]),
        pl.BlockSpec((2, tile, half), lambda i, here: (0, inner(i, here), 0)),
    ]
    if full:
        out_shape.append(shape((rows, width), jnp.bfloat16))
        out_specs.append(block(width))
    return pl.pallas_call(
        functools.partial(experts_kernel, full),
        grid_spec=pltpu.PrefetchScalarGridSpec(
            num_scalar_prefetch=1,
            grid=(rows // tile,),
            in_specs=[
                block(width),
                block(1),
                whole(own_column),
                whole(expert_in),
                whole(expert_out),
                whole(router),
                whole(shared_in),
                whole(shared_out),
            ],
            out_specs=out_specs,
        ),
        out_shape=out_shape,
        name="experts_full" if full else "experts_inner",
        cost_estimate=pl.CostEstimate(
            flops=2 * rows * width * units * 3, bytes_accessed=rows * width * 4, transcendentals=rows * units
        ),
    )(here, x, routed, own_column, expert_in, expert_out, router, shared_in, shared_out)


def experts_back_kernel(
    here_ref,
    grad_ref,
    pre_ref,
    prob_ref,
    routed_ref,
    own_ref,
    in_ref,
    out_w_ref,
    router_ref,
    shared_pre_ref,
    shared_in_ref,
    shared_out_ref,
    grad_pre_ref,
    moved_ref,
    partial_ref,
):
    units = out_w_ref.shape[0]
    grad = grad_ref[...]
    prob = prob_ref[...]
    own_prob = jnp.sum(prob * own_ref[...], axis=1, keepdims=True) * routed_ref[...]
    gate, up = pre_ref[:, :units].astype(jnp.float32), pre_ref[:, units:].astype(jnp.float32)
    grad_units = dot_t(grad, out_w_ref[...])
    act, slope = silu_parts(gate)
    grad_gate = jnp.sum(grad_units * act * up, axis=1, keepdims=True)
    moved = own_prob * grad_gate
    moved_ref[...] = moved
    grad_logits = bf16(moved * (own_ref[...] - prob))
    scaled = own_prob * grad_units
    grad_pre_ref[:, :units] = bf16(scaled * up * slope)
    grad_pre_ref[:, units:] = bf16(scaled * act)
    base = dot_t(grad_pre_ref[...], in_ref[...]) + dot_t(grad_logits, router_ref[...])
    tile = pl.program_id(0)
    inside = (tile >= here_ref[0]) & (tile < here_ref[1])
    half = shared_out_ref.shape[0]

    def with_shared():
        left, right = gated_back(
            shared_pre_ref[0].astype(jnp.float32),
            shared_pre_ref[1].astype(jnp.float32),
            dot_t(grad, shared_out_ref[...]),
        )
        partial_ref[...] = bf16(base + dot(left, shared_in_ref[:half]) + dot(right, shared_in_ref[half:]))

    def without():
        partial_ref[...] = bf16(base)

    pl.when(inside)(with_shared)
    pl.when(jnp.logical_not(inside))(without)


def experts_back(grad, stored, routed, own_column, weights, here, pack_rows):
    expert_in, expert_out, router, shared_in, shared_out = weights
    rows, width = grad.shape
    tile = tile_rows(pack_rows)
    units, half = expert_out.shape[0], shared_out.shape[0]
    block, whole, inner = specs_of(rows, tile)
    shape = jax.ShapeDtypeStruct
    return pl.pallas_call(
        experts_back_kernel,
        grid_spec=pltpu.PrefetchScalarGridSpec(
            num_scalar_prefetch=1,
            grid=(rows // tile,),
            in_specs=[
                block(width),
                block(2 * units),
                block(router.shape[1]),
                block(1),
                whole(own_column),
                whole(expert_in),
                whole(expert_out),
                whole(router),
                pl.BlockSpec((2, tile, half), lambda i, here: (0, inner(i, here), 0)),
                whole(shared_in),
                whole(shared_out),
            ],
            out_specs=[block(2 * units), block(1), block(width)],
        ),
        out_shape=[
            shape((rows, 2 * units), jnp.bfloat16),
            shape((rows, 1), jnp.float32),
            shape((rows, width), jnp.bfloat16),
        ],
        name="experts_back",
        cost_estimate=pl.CostEstimate(
            flops=2 * rows * width * units * 3, bytes_accessed=rows * width * 4, transcendentals=rows * units
        ),
    )(
        here,
        grad,
        stored["pre"],
        stored["prob"],
        routed,
        own_column,
        expert_in,
        expert_out,
        router,
        stored["shared_pre"],
        shared_in,
        shared_out,
    )


def pair_grad_kernel(x_ref, grad_ref, out_ref):
    units = out_ref.shape[2]
    x = x_ref[...]
    out_ref[:, 0, :] = t_dot(x, grad_ref[:, :units])
    out_ref[:, 1, :] = t_dot(x, grad_ref[:, units:])


def pair_grad(x, grad):
    rows, width = x.shape
    units = grad.shape[1] // 2
    if rows > 4096:
        return t_dot(x, grad).reshape(width, 2, units)
    tile = 256
    return pl.pallas_call(
        pair_grad_kernel,
        grid=(width // tile,),
        in_specs=[
            pl.BlockSpec((rows, tile), lambda i: (0, i)),
            pl.BlockSpec((rows, 2 * units), lambda i: (0, 0), pipeline_mode=pl.Buffered(1)),
        ],
        out_specs=pl.BlockSpec((tile, 2, units), lambda i: (i, 0, 0)),
        out_shape=jax.ShapeDtypeStruct((width, 2, units), jnp.float32),
        name="pair_grad",
        cost_estimate=pl.CostEstimate(
            flops=4 * rows * width * units, bytes_accessed=rows * (width + 2 * units) * 2 + width * units * 8, transcendentals=0
        ),
    )(x, grad)


def blank(shape, dtype):
    return pl.pallas_call(
        lambda out_ref: None,
        out_shape=jax.ShapeDtypeStruct(shape, dtype),
        out_specs=pl.BlockSpec(memory_space=pl.ANY),
        name="blank",
    )()


def body(
    boundary,
    lengths,
    routes,
    attn_gain,
    query_weight,
    compress_weight,
    latent_gain,
    expand_weight,
    output_weight,
    ffn_gain,
    router_weight,
    shared_in,
    shared_out,
    expert_in,
    expert_out,
):
    attn_gain, latent_gain, ffn_gain = attn_gain[0], latent_gain[0], ffn_gain[0]
    query_weight, compress_weight = query_weight[0], compress_weight[0]
    expand_weight, output_weight = expand_weight[0], output_weight[0]
    router_weight, shared_out, expert_out = router_weight[0], shared_out[0], expert_out[0, 0]
    width = boundary.shape[3]
    rows = boundary.shape[2]
    shared_half = shared_out.shape[0]
    units = expert_out.shape[0]
    shared_in_t = jnp.transpose(shared_in[0], (1, 2, 0)).reshape(2 * shared_half, width)
    expert_in = expert_in.reshape(width, 2 * units)
    weights = (expert_in, expert_out, router_weight, shared_in_t, shared_out)

    packs, members = lax.axis_size("dp"), lax.axis_size("expert")
    count = packs * members
    pack, member = lax.axis_index("dp"), lax.axis_index("expert")
    me = pack * members + member
    is_first = lax.axis_index("section") == 0
    pack_rows = members * rows
    top = routes.shape[3]
    experts_count = router_weight.shape[1]
    here = tile_here(pack, pack_rows)

    def own_pack(value):
        size = value.shape[0] // packs
        return lax.dynamic_slice_in_dim(value, pack * size, size, 0)

    def tables_of(block_lengths):
        segment, position = block_layout(block_lengths, rows)
        blocks = segment.shape[0]
        freqs = rope_base ** (-jnp.arange(HALF, dtype=jnp.float32) / HALF)
        angles = position.reshape(-1).astype(jnp.float32)[:, None] * freqs[None, :]
        return (
            jnp.cos(angles),
            jnp.sin(angles),
            segment.reshape(blocks * rows, 1),
            segment.reshape(blocks, 1, rows),
        )

    own_lengths = lax.dynamic_index_in_dim(lengths[0, 0], member, 0, keepdims=False)
    layout = jnp.concatenate([routes.reshape(rows * top), own_lengths])
    layout = jnp.pad(layout, (0, -layout.shape[0] % 1024)).reshape(8, -1)

    def routed_of(layout_all):
        routes_all = layout_all.reshape(count, -1)[:, : rows * top].reshape(count * rows, top)
        return jnp.any(routes_all == me, axis=1, keepdims=True).astype(jnp.float32)

    tables_pack = tables_of(lengths[0, 0])
    own_cos, own_sin = (
        lax.dynamic_slice_in_dim(table, member * rows, rows, 0) for table in tables_pack[:2]
    )
    own_column = (lax.broadcasted_iota(jnp.int32, (1, experts_count), 1) == me).astype(jnp.float32)

    def inputs_of(hidden):
        normed32, scale_attn = rms_forward(hidden, attn_gain)
        normed = bf16(normed32)
        compressed = dot(normed, compress_weight)
        latent32, scale_latent = rms_forward(compressed[:, :LAT], latent_gain)
        keyed = bf16(
            jnp.concatenate([latent32, rotate(compressed[:, LAT:], own_cos, own_sin)], axis=1)
        )
        return normed, keyed, (compressed, scale_attn, scale_latent)

    def heads_of(normed, keyed, tables):
        query_raw = dot(normed, query_weight)
        latent = bf16(dot(keyed[:, :LAT], expand_weight))
        attended, query = attend(query_raw, latent, keyed, tables)
        return attended, query, latent

    fresh = boundary[0, 0].astype(jnp.float32)

    normed, keyed, _ = inputs_of(fresh)
    pack_inputs = gather_blocks([normed, keyed], False, "gather_inputs_first", 0)
    attended, _, _ = heads_of(*pack_inputs, tables_pack)
    mixed_first = fresh + scatter_blocks(
        bf16(dot(attended, output_weight)), False, "scatter_attended_first", 0
    )
    ffn_all, layout_all = gather_blocks(
        [bf16(rms_forward(mixed_first, ffn_gain)[0]), layout], True, "gather_ffn_first", 0
    )
    *_, partial = experts(ffn_all, routed_of(layout_all), own_column, weights, here, pack_rows, True)
    result_first = mixed_first + scatter_blocks(partial, True, "scatter_ffn_first", 0)
    target_all, layout_all = gather_blocks(
        [boundary[0, 0], layout], True, "gather_target", 1, [blank(ffn_all.shape, jnp.bfloat16), layout_all]
    )
    sent, target_all, layout_all = lax.optimization_barrier((bf16(result_first), target_all, layout_all))
    inbound = lax.ppermute(sent, "section", [(0, 1)])
    routed = routed_of(layout_all)
    tables_all = tables_of(layout_all.reshape(count, -1)[:, rows * top : rows * top + lengths.shape[3]])

    hidden = jnp.where(is_first, fresh, inbound.astype(jnp.float32))
    normed, keyed, (compressed, scale_attn, scale_latent) = inputs_of(hidden)
    normed_pack, keyed_pack = gather_blocks([normed, keyed], False, "gather_inputs_second", 1, pack_inputs)
    attended, query, latent = heads_of(normed_pack, keyed_pack, tables_pack)
    mixed = hidden + scatter_blocks(bf16(dot(attended, output_weight)), False, "scatter_attended_second", 1)
    mixed = jnp.where(is_first, mixed_first, mixed)
    ffn32, scale_ffn = rms_forward(mixed, ffn_gain)
    (ffn_all,) = gather_blocks([bf16(ffn32)], True, "gather_ffn_second", 1, [ffn_all])
    pre, gated, prob, shared_pre = experts(ffn_all, routed, own_column, weights, here, pack_rows, False)
    stored = dict(pre=pre, prob=prob, shared_pre=shared_pre)

    def latent_back(own):
        grad_latent, grad_latent_gain = rms_backward(
            compressed[:, :LAT], scale_latent, latent_gain, own[:, width : width + LAT]
        )
        grad_compressed = bf16(
            jnp.concatenate([grad_latent, rotate(own[:, width + LAT :], own_cos, -own_sin)], axis=1)
        )
        grad_normed = own[:, :width] + dot_t(grad_compressed, compress_weight)
        grad_hidden_norm, grad_attn_gain = rms_backward(hidden, scale_attn, attn_gain, grad_normed)
        return grad_compressed, grad_hidden_norm, grad_attn_gain, grad_latent_gain

    def heads_back(grad_query, grad_latent_heads, grad_shared_key):
        return bf16(
            jnp.concatenate(
                [
                    dot_t(grad_query, query_weight),
                    dot_t(grad_latent_heads, expand_weight),
                    grad_shared_key,
                ],
                axis=1,
            )
        )

    def prepare(normed_all, keyed_all):
        attended_all, query_all, latent_all = heads_of(normed_all, keyed_all, tables_all)
        left = dot_t(ffn_all, shared_in_t[:shared_half])
        right = dot_t(ffn_all, shared_in_t[shared_half:])
        return attended_all, query_all, latent_all, bf16(left), bf16(right), bf16(gated_hidden(left, right))

    grad_pre_second, moved_second, partial = experts_back(
        target_all, stored, routed, own_column, weights, here, pack_rows
    )
    grad_ffn_second = scatter_blocks(partial, True, "scatter_ffn_back_second", 1)
    grad_mixed = fresh + rms_backward(mixed, scale_ffn, ffn_gain, grad_ffn_second)[0]
    (grad_mixed_pack,) = gather_blocks([bf16(grad_mixed)], False, "gather_mixed", 1)
    own_second = scatter_blocks(
        heads_back(
            *attend_back(query, latent, keyed_pack, bf16(dot_t(grad_mixed_pack, output_weight)), tables_pack)
        ),
        False,
        "scatter_heads_second",
        1,
    )
    grad_second = grad_mixed + latent_back(own_second)[1]

    all_inputs = gather_blocks([normed, keyed], True, "gather_keyed_first", 0)
    prepared = lax.cond(
        is_first,
        prepare,
        lambda *_: tuple(blank(like.shape, like.dtype) for like in jax.eval_shape(prepare, *all_inputs)),
        *all_inputs,
    )
    grad_second, prepared, all_inputs = lax.optimization_barrier((grad_second, prepared, all_inputs))
    downbound = lax.ppermute(grad_second, "section", [(1, 0)])

    normed_late, keyed_late, gated_late, _ = lax.optimization_barrier((normed, keyed, gated, grad_second))
    normed_all, keyed_all = gather_blocks([normed_late, keyed_late], True, "gather_keyed_second", 1, all_inputs)
    attended_all, query_all, latent_all, shared_gate, shared_up, shared_hid = lax.cond(
        is_first, lambda *values: values[2:], lambda *values: prepare(*values[:2]), normed_all, keyed_all, *prepared
    )

    def finish(gated_late, shared_hid):
        partial = bf16(dot(gated_late, expert_out))
        addend = dot(own_pack(shared_hid), shared_out)
        return lax.dynamic_update_slice_in_dim(
            partial, bf16(own_pack(partial).astype(jnp.float32) + addend), pack * pack_rows, 0
        )

    partial = lax.cond(
        is_first, lambda *_: blank((count * rows, width), jnp.bfloat16), finish, gated_late, shared_hid
    )
    result = mixed + scatter_blocks(partial, True, "scatter_result", 1)

    upstream = jnp.where(is_first, downbound, fresh)
    (upstream_all,) = gather_blocks([bf16(upstream)], True, "gather_upstream", 0, [target_all])
    grad_pre, moved, partial = lax.cond(
        is_first,
        lambda upstream_all, *_: tuple(
            experts_back(upstream_all, stored, routed, own_column, weights, here, pack_rows)
        ),
        lambda _, *old: (*old, blank((count * rows, width), jnp.bfloat16)),
        upstream_all,
        grad_pre_second,
        moved_second,
    )
    grad_ffn = jnp.where(is_first, scatter_blocks(partial, True, "scatter_ffn_back_first", 0), grad_ffn_second)
    grad_mixed_norm, grad_ffn_gain = rms_backward(mixed, scale_ffn, ffn_gain, grad_ffn)
    grad_mixed = upstream + grad_mixed_norm
    grad_mixed_all = lax.all_gather(bf16(grad_mixed), BOTH, axis=0, tiled=True)
    grad_attended = bf16(dot_t(grad_mixed_all, output_weight))
    grad_query, grad_latent_heads, grad_shared_key = attend_back(
        query_all, latent_all, keyed_all, grad_attended, tables_all
    )
    own = lax.psum_scatter(
        heads_back(own_pack(grad_query), own_pack(grad_latent_heads), own_pack(grad_shared_key)),
        "expert",
        scatter_dimension=0,
        tiled=True,
    ).astype(jnp.float32)
    grad_compressed, grad_hidden_norm, grad_attn_gain, grad_latent_gain = latent_back(own)
    grad_hidden = grad_mixed + grad_hidden_norm

    small = jnp.concatenate([grad_attn_gain, grad_latent_gain, grad_ffn_gain, moved[:, 0]])
    small = jnp.pad(small, (0, -small.shape[0] % 1024)).reshape(8, -1)
    grad_compressed_all = lax.all_gather(grad_compressed, BOTH, axis=0, tiled=True)
    small_all = lax.all_gather(small, BOTH, axis=0, tiled=True).reshape(count, -1)
    gains = jnp.sum(small_all[:, : 2 * width + LAT], axis=0)
    moved_all = small_all[:, 2 * width + LAT : 2 * width + LAT + count * rows].T
    grad_logits = bf16(moved_all - prob * jnp.sum(moved_all, axis=1, keepdims=True))
    left, right = gated_back(
        shared_gate.astype(jnp.float32), shared_up.astype(jnp.float32), dot_t(upstream_all, shared_out)
    )
    grad_shared_in = jnp.stack([t_dot(ffn_all, left), t_dot(ffn_all, right)], axis=1)
    ends = jnp.where(is_first, grad_hidden, result)
    return (
        ends[None, None],
        gains[:width][None],
        t_dot(normed_all, grad_query)[None],
        t_dot(normed_all, grad_compressed_all)[None],
        gains[width : width + LAT][None],
        t_dot(keyed_all[:, :LAT], grad_latent_heads)[None],
        t_dot(attended_all, grad_mixed_all)[None],
        gains[width + LAT :][None],
        t_dot(ffn_all, grad_logits)[None],
        grad_shared_in[None],
        t_dot(shared_hid, upstream_all)[None],
        pair_grad(ffn_all, grad_pre)[None, None],
        t_dot(gated, upstream_all)[None, None],
    )


def solution(mesh):
    return jax.shard_map(
        body,
        mesh=mesh,
        in_specs=(
            P("section", None, BOTH, None),
            P(None, "dp", None, None),
            P("section", None, BOTH, None),
            P("section", None),
            P("section", None, "expert"),
            P("section", None, None),
            P("section", None),
            P("section", None, "expert"),
            P("section", "expert", None),
            P("section", None),
            P("section", None, None),
            P("section", None, None, "expert"),
            P("section", "expert", None),
            P("section", BOTH, None, None, None),
            P("section", BOTH, None, None),
        ),
        out_specs=(
            P("section", None, BOTH, None),
            P("section", None),
            P("section", None, "expert"),
            P("section", None, None),
            P("section", None),
            P("section", None, "expert"),
            P("section", "expert", None),
            P("section", None),
            P("section", None, None),
            P("section", None, None, "expert"),
            P("section", "expert", None),
            P("section", BOTH, None, None, None),
            P("section", BOTH, None, None),
        ),
        check_vma=False,
    )
```

```python
import functools

import jax
import jax.numpy as jnp
from jax import lax
from jax.experimental import pallas as pl
from jax.experimental.pallas import tpu as pltpu
from jax.sharding import PartitionSpec as P

NOPE = 128
ROPE = 64
VD = 128
LAT = 512

QK = NOPE + ROPE
KV = NOPE + VD
HALF = ROPE // 2
epsilon = 1e-06
rope_base = 10000.0
masked_score = -1e30
SECTION, PACKS, MEMBERS = "section", "dp", "expert"
BOTH = (PACKS, MEMBERS)
MESH = pl.DeviceIdType.MESH
def dot(left, right):
    return jnp.dot(left, right, preferred_element_type=jnp.float32)


def dot_t(left, right):
    return lax.dot_general(
        left, right, (((1,), (1,)), ((), ())), preferred_element_type=jnp.float32
    )


def t_dot(left, right):
    return lax.dot_general(
        left, right, (((0,), (0,)), ((), ())), preferred_element_type=jnp.float32
    )


def bf16(value):
    return value.astype(jnp.bfloat16)


def rms_forward(inputs, gain_vec):
    norm_scale = lax.rsqrt(jnp.mean(inputs * inputs, axis=-1, keepdims=True) + epsilon)
    return (inputs * norm_scale * gain_vec, norm_scale)


def rms_backward(inputs, norm_scale, gain_vec, upstream):
    weighted = upstream * gain_vec
    grad_gain = jnp.sum(upstream * inputs * norm_scale, axis=0)
    cubed = norm_scale * norm_scale * norm_scale
    grad_inputs = norm_scale * weighted - inputs * cubed * jnp.mean(
        weighted * inputs, axis=-1, keepdims=True
    )
    return (grad_inputs, grad_gain)


def rotate(inputs, cosine, sine):
    half = cosine.shape[-1]
    former = inputs[..., :half]
    latter = inputs[..., half:]
    return jnp.concatenate(
        [former * cosine - latter * sine, latter * cosine + former * sine], axis=-1
    )


def silu_parts(pre_gate):
    sigmoid = jax.nn.sigmoid(pre_gate)
    return (pre_gate * sigmoid, sigmoid * (1.0 + pre_gate * (1.0 - sigmoid)))


def block_layout(block_lengths, rows):
    starts = jnp.cumsum(block_lengths, axis=1) - block_lengths
    index = jnp.arange(rows, dtype=jnp.int32)
    begun = index[None, :, None] >= starts[:, None, :]
    segment = jnp.sum(begun.astype(jnp.int32), axis=2)
    opening = jnp.max(jnp.where(begun, starts[:, None, :], 0), axis=2)
    return segment, index[None, :] - opening


def places(spots):
    member = lax.axis_index(MEMBERS)
    spot = lax.axis_index(PACKS) if spots > 1 else 0
    return spot, member // 2, lax.rem(member, 2)


def to_partner(chip, core):
    return {MEMBERS: chip * 2 + 1 - core}


def to_other(chip, core):
    return {MEMBERS: (1 - chip) * 2 + core}


def when(condition, action):
    if condition is True:
        action()
    else:
        pl.when(condition)(action)


def greet(spots, spot, chip, core):
    barrier = pltpu.get_barrier_semaphore()

    def signal(target):
        pl.semaphore_signal(barrier, inc=1, device_id=target, device_id_type=MESH)

    signal(to_partner(chip, core))
    signal(to_other(chip, core))
    if spots > 1:
        pl.when(spot > 0)(lambda: signal({PACKS: spot - 1}))
        pl.when(spot < spots - 1)(lambda: signal({PACKS: spot + 1}))
        ends = jnp.where(spot > 0, 1, 0) + jnp.where(spot < spots - 1, 1, 0)
        pl.semaphore_wait(barrier, 2 + ends)
    else:
        pl.semaphore_wait(barrier, 2)


def remote(source, target_ref, target, out_sem, in_sem):
    return pltpu.make_async_remote_copy(
        src_ref=source,
        dst_ref=target_ref,
        send_sem=out_sem,
        recv_sem=in_sem,
        device_id=target,
        device_id_type=MESH,
    )


def slot(spot, chip, core):
    return spot * 4 + chip * 2 + core


def gather_kernel(spots, cuts, active, *refs):
    arrays = len(cuts)
    x_refs, o_refs, sems = refs[:arrays], refs[-9 - arrays : -9], refs[-9:]
    own_sem, up_out, up_in, down_out, down_in, over_out, over_in, pair_out, pair_in = sems
    units = [
        (a, pl.ds(part * (x_refs[a].shape[0] // parts), x_refs[a].shape[0] // parts))
        for a, parts in enumerate(cuts)
        for part in range(parts)
    ]

    def run():
        spot, chip, core = places(spots)
        greet(spots, spot, chip, core)

        def piece(unit, index):
            array, cut = units[unit]
            return o_refs[array].at[index, cut]

        def first(unit):
            array, cut = units[unit]
            return x_refs[array].at[cut]

        def up(source, at, unit, reach):
            return remote(
                source, piece(unit, slot(at, chip, core)), {PACKS: spot + 1}, up_out.at[reach, unit], up_in.at[reach, unit]
            )

        def down(source, at, unit, reach):
            return remote(
                source,
                piece(unit, slot(at, chip, core)),
                {PACKS: spot - 1},
                down_out.at[reach, unit],
                down_in.at[reach, unit],
            )

        def over(source, at, unit):
            return remote(
                source, piece(unit, slot(at, chip, core)), to_other(chip, core), over_out.at[at, unit], over_in.at[at, unit]
            )

        def pair(source, at, c, unit):
            return remote(
                source,
                piece(unit, slot(at, c, core)),
                to_partner(chip, core),
                pair_out.at[c, at, unit],
                pair_in.at[c, at, unit],
            )

        mine = slot(spot, chip, core)
        for unit in range(len(units)):
            source = first(unit)
            over(source, spot, unit).start()
            if spots > 1:
                pl.when(spot < spots - 1)(lambda: up(source, spot, unit, 0).start())
                pl.when(spot > 0)(lambda: down(source, spot, unit, 0).start())
            pair(source, spot, chip, unit).start()
        own = [pltpu.make_async_copy(x_refs[a], o_refs[a].at[mine], own_sem.at[a]) for a in range(arrays)]
        for copy in own:
            copy.start()
        for reach in range(1, spots):
            for unit in range(len(units)):

                def below(reach=reach, unit=unit):
                    at = spot - reach
                    source = piece(unit, slot(at, chip, core))
                    up(source, at, unit, reach - 1).wait_recv()
                    pl.when(spot < spots - 1)(lambda: up(source, at, unit, reach).start())
                    over(source, at, unit).start()
                    pair(source, at, chip, unit).start()

                def above(reach=reach, unit=unit):
                    at = spot + reach
                    source = piece(unit, slot(at, chip, core))
                    down(source, at, unit, reach - 1).wait_recv()
                    pl.when(spot > 0)(lambda: down(source, at, unit, reach).start())
                    over(source, at, unit).start()
                    pair(source, at, chip, unit).start()

                pl.when(spot >= reach)(below)
                pl.when(spot + reach < spots)(above)
        for reach in range(spots):
            sides = [(True, spot)]
            if reach > 0:
                sides = [(spot >= reach, spot - reach), (spot + reach < spots, spot + reach)]
            for unit in range(len(units)):
                for there, at in sides:

                    def hand_on(at=at, unit=unit):
                        source = piece(unit, slot(at, 1 - chip, core))
                        over(source, at, unit).wait_recv()
                        pair(source, at, 1 - chip, unit).start()

                    when(there, hand_on)
        for copy in own:
            copy.wait()
        for unit in range(len(units)):
            source = piece(unit, mine)
            for at in range(spots):
                over(source, at, unit).wait_send()
                for c in range(2):
                    pair(source, at, c, unit).wait()
            for reach in range(spots - 1):
                pl.when((spot >= reach) & (spot < spots - 1))(lambda: up(source, spot, unit, reach).wait_send())
                pl.when((spot + reach < spots) & (spot > 0))(lambda: down(source, spot, unit, reach).wait_send())

    if active is None:
        run()
    else:
        pl.when(lax.axis_index(SECTION) == active)(run)


def gather_blocks(values, across, number, active=None, into=None, parts=4):
    axes = BOTH if across else MEMBERS
    if lax.axis_size(MEMBERS) != 4:
        found = [lax.all_gather(value, axes, axis=0, tiled=True) for value in values]
        if into is None:
            return found
        chosen = lax.axis_index(SECTION) == active
        return [jnp.where(chosen, new, old) for new, old in zip(found, into)]
    spots = lax.axis_size(PACKS) if across else 1
    cuts = [parts if value.shape[0] % (16 * parts) == 0 else 1 for value in values]
    units = sum(cuts)
    dma = pltpu.SemaphoreType.DMA
    hops = max(spots - 1, 1)
    shapes = [jax.ShapeDtypeStruct((spots * 4, *value.shape), value.dtype) for value in values]
    held = [] if into is None else [old.reshape(shape.shape) for old, shape in zip(into, shapes)]
    outs = pl.pallas_call(
        functools.partial(gather_kernel, spots, cuts, active),
        out_shape=shapes,
        in_specs=[pl.BlockSpec(memory_space=pltpu.VMEM)] * len(values)
        + [pl.BlockSpec(memory_space=pl.ANY)] * len(held),
        out_specs=[pl.BlockSpec(memory_space=pl.ANY)] * len(values),
        input_output_aliases={len(values) + index: index for index in range(len(held))},
        scratch_shapes=[
            dma((len(values),)),
            dma((hops, units)),
            dma((hops, units)),
            dma((hops, units)),
            dma((hops, units)),
            dma((spots, units)),
            dma((spots, units)),
            dma((2, spots, units)),
            dma((2, spots, units)),
        ],
        compiler_params=pltpu.CompilerParams(collective_id=number, has_side_effects=True),
    )(*values, *held)
    return [out.reshape(-1, out.shape[2]) for out in outs]


def add_into(target, sources, rows, step=16):
    def some(index, carry):
        at = pl.ds(pl.multiple_of(index * step, step), step)
        total = sources[0][at, :].astype(jnp.float32)
        for source in sources[1:]:
            total = total + source[at, :].astype(jnp.float32)
        target[at, :] = total.astype(target.dtype)
        return carry

    lax.fori_loop(0, rows // step, some, 0)


def scatter_kernel(
    spots,
    parts,
    active,
    x_ref,
    o_ref,
    own_buf,
    pair_buf,
    over_src,
    over_buf,
    line_src,
    up_buf,
    down_buf,
    own_in,
    pair_out,
    pair_in,
    over_out,
    over_in,
    line_out,
    up_in,
    down_in,
):
    rows = x_ref.shape[1] // parts
    cut = lambda part: pl.ds(part * rows, rows)

    def run():
        spot, chip, core = places(spots)
        greet(spots, spot, chip, core)

        def order(step):
            if step == spots - 1:
                return spot
            fall = spots - 1 - step
            fall = jnp.where(fall <= spot, fall - 1, fall)
            rise = jnp.where(step >= spot, step + 1, step)
            return jnp.where(2 * spot < spots - 1, fall, rise)

        def pair(at, c, part):
            return remote(
                x_ref.at[slot(at, c, 1 - core), cut(part)],
                pair_buf.at[at, c, cut(part)],
                to_partner(chip, core),
                pair_out.at[at, c, part],
                pair_in.at[at, c, part],
            )

        def over(at, part):
            return remote(
                over_src.at[at, cut(part)],
                over_buf.at[at, cut(part)],
                to_other(chip, core),
                over_out.at[at, part],
                over_in.at[at, part],
            )

        def up(at, part):
            return remote(
                line_src.at[at, cut(part)],
                up_buf.at[at, cut(part)],
                {PACKS: spot + 1},
                line_out.at[at, part],
                up_in.at[at, part],
            )

        def down(at, part):
            return remote(
                line_src.at[at, cut(part)],
                down_buf.at[at, cut(part)],
                {PACKS: spot - 1},
                line_out.at[at, part],
                down_in.at[at, part],
            )

        def own(at, c):
            return pltpu.make_async_copy(x_ref.at[slot(at, c, core)], own_buf.at[at, c], own_in.at[at, c])

        for c in (1 - chip, chip):
            for step in range(spots):
                own(order(step), c).start()
                for part in range(parts):
                    pair(order(step), c, part).start()
        for step in range(spots):
            at = order(step)
            own(at, 1 - chip).wait()
            for part in range(parts):
                pair(at, 1 - chip, part).wait_recv()
                add_into(
                    over_src.at[at, cut(part)],
                    [own_buf.at[at, 1 - chip, cut(part)], pair_buf.at[at, 1 - chip, cut(part)]],
                    rows,
                )
                over(at, part).start()
        for step in range(spots):
            at = order(step)
            own(at, chip).wait()
            for part in range(parts):
                pair(at, chip, part).wait_recv()
                over(at, part).wait_recv()
                base = [
                    own_buf.at[at, chip, cut(part)],
                    pair_buf.at[at, chip, cut(part)],
                    over_buf.at[at, cut(part)],
                ]
                ups, downs = up_buf.at[at, cut(part)], down_buf.at[at, cut(part)]
                if step < spots - 1:
                    target = line_src.at[at, cut(part)]

                    def rising(first):
                        if not first:
                            up(at, part).wait_recv()
                        add_into(target, base if first else base + [ups], rows)
                        up(at, part).start()

                    def falling(first):
                        if not first:
                            down(at, part).wait_recv()
                        add_into(target, base if first else base + [downs], rows)
                        down(at, part).start()

                    pl.when((at > spot) & (spot == 0))(lambda: rising(True))
                    pl.when((at > spot) & (spot > 0))(lambda: rising(False))
                    pl.when((at < spot) & (spot == spots - 1))(lambda: falling(True))
                    pl.when((at < spot) & (spot < spots - 1))(lambda: falling(False))
                elif spots == 1:
                    add_into(o_ref.at[cut(part)], base, rows)
                else:

                    def finish(ends):
                        if ends < 1:
                            up(at, part).wait_recv()
                        if ends > -1:
                            down(at, part).wait_recv()
                        extra = ([ups] if ends < 1 else []) + ([downs] if ends > -1 else [])
                        add_into(o_ref.at[cut(part)], base + extra, rows)

                    pl.when(spot == 0)(lambda: finish(1))
                    pl.when(spot == spots - 1)(lambda: finish(-1))
                    pl.when((spot > 0) & (spot < spots - 1))(lambda: finish(0))
        for part in range(parts):
            for step in range(spots):
                at = order(step)
                pair(at, 0, part).wait_send()
                pair(at, 1, part).wait_send()
                over(at, part).wait_send()
                if step < spots - 1:
                    up(at, part).wait_send()

    if active is None:
        run()
    else:
        pl.when(lax.axis_index(SECTION) == active)(run)


def scatter_blocks(partial, across, number, active=None, parts=4):
    if lax.axis_size(MEMBERS) != 4:
        axes = BOTH if across else MEMBERS
        return lax.psum_scatter(partial, axes, scatter_dimension=0, tiled=True).astype(jnp.float32)
    spots = lax.axis_size(PACKS) if across else 1
    rows, width = partial.shape[0] // (spots * 4), partial.shape[1]
    dma = pltpu.SemaphoreType.DMA
    hold = lambda *lead: pltpu.VMEM((*lead, rows, width), partial.dtype)
    return pl.pallas_call(
        functools.partial(scatter_kernel, spots, parts, active),
        out_shape=jax.ShapeDtypeStruct((rows, width), jnp.float32),
        in_specs=[pl.BlockSpec(memory_space=pl.ANY)],
        out_specs=pl.BlockSpec(memory_space=pltpu.VMEM),
        scratch_shapes=[
            hold(spots, 2),
            hold(spots, 2),
            hold(spots),
            hold(spots),
            hold(spots),
            hold(spots),
            hold(spots),
            dma((spots, 2)),
            dma((spots, 2, parts)),
            dma((spots, 2, parts)),
            dma((spots, parts)),
            dma((spots, parts)),
            dma((spots, parts)),
            dma((spots, parts)),
            dma((spots, parts)),
        ],
        compiler_params=pltpu.CompilerParams(collective_id=number, has_side_effects=True),
    )(partial.reshape(spots * 4, rows, width))


def allowed_pairs(seg_col, seg_row):
    rows = seg_col.shape[0]
    later = lax.broadcasted_iota(jnp.int32, (rows, rows), 0)
    earlier = lax.broadcasted_iota(jnp.int32, (rows, rows), 1)
    return (seg_col == seg_row) & (earlier <= later)


def attend_kernel(heads, q_ref, lat_ref, key_ref, cos_ref, sin_ref, col_ref, row_ref, out_ref, rot_ref):
    factor = QK**-0.5
    allowed = allowed_pairs(col_ref[...], row_ref[0])
    cosine, sine = cos_ref[...], sin_ref[...]
    shared = key_ref[:, LAT:]
    for head in range(heads):
        raw = q_ref[:, head * QK : (head + 1) * QK]
        query = bf16(
            jnp.concatenate([raw[:, :NOPE], rotate(raw[:, NOPE:], cosine, sine)], axis=1)
        )
        rot_ref[:, head * QK : (head + 1) * QK] = query
        key = jnp.concatenate([lat_ref[:, head * KV : head * KV + NOPE], shared], axis=1)
        value = lat_ref[:, head * KV + NOPE : (head + 1) * KV]
        scores = jnp.where(allowed, dot_t(query, key) * factor, masked_score)
        top = jnp.max(scores, axis=1, keepdims=True)
        powers = jnp.exp(scores - top)
        probs = powers / jnp.sum(powers, axis=1, keepdims=True)
        out_ref[:, head * VD : (head + 1) * VD] = bf16(dot(bf16(probs), value))


def attend(query_raw, latent, keyed, tables):
    cosine, sine, seg_col, seg_row = tables
    count, _, rows = seg_row.shape
    heads = query_raw.shape[1] // QK
    block = lambda width: pl.BlockSpec((rows, width), lambda i: (i, 0))
    return pl.pallas_call(
        functools.partial(attend_kernel, heads),
        grid=(count,),
        in_specs=[
            block(heads * QK),
            block(heads * KV),
            block(LAT + ROPE),
            block(HALF),
            block(HALF),
            block(1),
            pl.BlockSpec((1, 1, rows), lambda i: (i, 0, 0)),
        ],
        out_specs=[block(heads * VD), block(heads * QK)],
        out_shape=[
            jax.ShapeDtypeStruct((count * rows, heads * VD), jnp.bfloat16),
            jax.ShapeDtypeStruct((count * rows, heads * QK), jnp.bfloat16),
        ],
        name="attend",
        cost_estimate=pl.CostEstimate(
            flops=2 * count * heads * rows * rows * (QK + VD),
            bytes_accessed=count * rows * heads * (QK * 6 + KV * 2 + VD * 2),
            transcendentals=count * heads * rows * rows,
        ),
    )(query_raw, latent, keyed, cosine, sine, seg_col, seg_row)


def attend_back_kernel(
    heads, q_ref, lat_ref, key_ref, grad_ref, cos_ref, sin_ref, col_ref, row_ref, dq_ref, dlat_ref, dkey_ref
):
    factor = QK**-0.5
    allowed = allowed_pairs(col_ref[...], row_ref[0])
    cosine, sine = cos_ref[...], sin_ref[...]
    shared = key_ref[:, LAT:]
    total = None
    for head in range(heads):
        query = q_ref[:, head * QK : (head + 1) * QK]
        key = jnp.concatenate([lat_ref[:, head * KV : head * KV + NOPE], shared], axis=1)
        value = lat_ref[:, head * KV + NOPE : (head + 1) * KV]
        grad = grad_ref[:, head * VD : (head + 1) * VD]
        scores = jnp.where(allowed, dot_t(query, key) * factor, masked_score)
        top = jnp.max(scores, axis=1, keepdims=True)
        powers = jnp.exp(scores - top)
        probs = powers / jnp.sum(powers, axis=1, keepdims=True)
        grad_value = t_dot(bf16(probs), grad)
        grad_probs = dot_t(grad, value)
        centre = jnp.sum(probs * grad_probs, axis=1, keepdims=True)
        grad_scores = bf16(probs * (grad_probs - centre) * factor)
        grad_query = dot(grad_scores, key)
        grad_key = t_dot(grad_scores, query)
        dq_ref[:, head * QK : (head + 1) * QK] = bf16(
            jnp.concatenate(
                [grad_query[:, :NOPE], rotate(grad_query[:, NOPE:], cosine, -sine)], axis=1
            )
        )
        dlat_ref[:, head * KV : head * KV + NOPE] = bf16(grad_key[:, :NOPE])
        dlat_ref[:, head * KV + NOPE : (head + 1) * KV] = bf16(grad_value)
        part = grad_key[:, NOPE:]
        total = part if total is None else total + part
    dkey_ref[...] = total


def attend_back(query, latent, keyed, grad, tables):
    cosine, sine, seg_col, seg_row = tables
    count, _, rows = seg_row.shape
    heads = query.shape[1] // QK
    block = lambda width: pl.BlockSpec((rows, width), lambda i: (i, 0))
    return pl.pallas_call(
        functools.partial(attend_back_kernel, heads),
        grid=(count,),
        in_specs=[
            block(heads * QK),
            block(heads * KV),
            block(LAT + ROPE),
            block(heads * VD),
            block(HALF),
            block(HALF),
            block(1),
            pl.BlockSpec((1, 1, rows), lambda i: (i, 0, 0)),
        ],
        out_specs=[block(heads * QK), block(heads * KV), block(ROPE)],
        out_shape=[
            jax.ShapeDtypeStruct((count * rows, heads * QK), jnp.bfloat16),
            jax.ShapeDtypeStruct((count * rows, heads * KV), jnp.bfloat16),
            jax.ShapeDtypeStruct((count * rows, ROPE), jnp.float32),
        ],
        name="attend_back",
        cost_estimate=pl.CostEstimate(
            flops=2 * count * heads * rows * rows * (3 * QK + 2 * VD),
            bytes_accessed=count * rows * heads * (QK * 4 + KV * 4 + VD * 2),
            transcendentals=count * heads * rows * rows,
        ),
    )(query, latent, keyed, grad, cosine, sine, seg_col, seg_row)


def gated_hidden(gate, up):
    return silu_parts(gate)[0] * up


def gated_back(gate, up, grad_hidden):
    act, slope = silu_parts(gate)
    return bf16(grad_hidden * up * slope), bf16(grad_hidden * act)


def experts_kernel(
    full,
    here_ref,
    x_ref,
    routed_ref,
    own_ref,
    in_ref,
    out_w_ref,
    shared_in_ref,
    shared_out_ref,
    pre_ref,
    gated_ref,
    prob_ref,
    shared_pre_ref,
    *partial_ref,
):
    units = gated_ref.shape[1]
    x = x_ref[...]
    pre = dot(x, in_ref[...])
    logits = pre[:, 2 * units : 2 * units + own_ref.shape[1]]
    powers = jnp.exp(logits - jnp.max(logits, axis=1, keepdims=True))
    prob = powers / jnp.sum(powers, axis=1, keepdims=True)
    prob_ref[...] = prob
    gate = jnp.sum(prob * own_ref[...], axis=1, keepdims=True) * routed_ref[...]
    pre_ref[...] = bf16(pre[:, : 2 * units])
    gated = bf16(gate * gated_hidden(pre[:, :units], pre[:, units : 2 * units]))
    gated_ref[...] = gated
    tile = pl.program_id(0)
    inside = (tile >= here_ref[0]) & (tile < here_ref[1])
    half = shared_out_ref.shape[0]

    def shared():
        left = dot_t(x, shared_in_ref[:half])
        right = dot_t(x, shared_in_ref[half:])
        shared_pre_ref[0] = bf16(left)
        shared_pre_ref[1] = bf16(right)
        return left, right

    if full:

        def with_shared():
            hidden = bf16(gated_hidden(*shared()))
            partial_ref[0][...] = bf16(dot(gated, out_w_ref[...]) + dot(hidden, shared_out_ref[...]))

        def without():
            partial_ref[0][...] = bf16(dot(gated, out_w_ref[...]))

        pl.when(inside)(with_shared)
        pl.when(jnp.logical_not(inside))(without)
    else:
        pl.when(inside)(lambda: shared() and None)


def tile_rows(pack_rows):
    return min(256, pack_rows)


def tile_here(pack, pack_rows):
    tiles = pack_rows // tile_rows(pack_rows)
    return jnp.stack([pack * tiles, (pack + 1) * tiles]).astype(jnp.int32)


def specs_of(rows, tile):
    block = lambda width: pl.BlockSpec((tile, width), lambda i, here: (i, 0))
    whole = lambda array: pl.BlockSpec(
        array.shape, lambda i, here: (0,) * array.ndim, pipeline_mode=pl.Buffered(1)
    )
    inner = lambda i, here: jnp.clip(i - here[0], 0, here[1] - here[0] - 1)
    return block, whole, inner


def experts(x, routed, own_column, weights, here, pack_rows, full):
    expert_in, expert_out, shared_in, shared_out = weights
    routes_width = own_column.shape[1]
    rows, width = x.shape
    tile = tile_rows(pack_rows)
    units, half = expert_out.shape[0], shared_out.shape[0]
    block, whole, inner = specs_of(rows, tile)
    shape = jax.ShapeDtypeStruct
    out_shape = [
        shape((rows, 2 * units), jnp.bfloat16),
        shape((rows, units), jnp.bfloat16),
        shape((rows, routes_width), jnp.float32),
        shape((2, pack_rows, half), jnp.bfloat16),
    ]
    out_specs = [
        block(2 * units),
        block(units),
        block(routes_width),
        pl.BlockSpec((2, tile, half), lambda i, here: (0, inner(i, here), 0)),
    ]
    if full:
        out_shape.append(shape((rows, width), jnp.bfloat16))
        out_specs.append(block(width))
    return pl.pallas_call(
        functools.partial(experts_kernel, full),
        grid_spec=pltpu.PrefetchScalarGridSpec(
            num_scalar_prefetch=1,
            grid=(rows // tile,),
            in_specs=[
                block(width),
                block(1),
                whole(own_column),
                whole(expert_in),
                whole(expert_out),
                whole(shared_in),
                whole(shared_out),
            ],
            out_specs=out_specs,
        ),
        out_shape=out_shape,
        name="experts_full" if full else "experts_inner",
        cost_estimate=pl.CostEstimate(
            flops=2 * rows * width * units * 3, bytes_accessed=rows * width * 4, transcendentals=rows * units
        ),
    )(here, x, routed, own_column, expert_in, expert_out, shared_in, shared_out)


def experts_back_kernel(
    here_ref,
    grad_ref,
    pre_ref,
    prob_ref,
    routed_ref,
    own_ref,
    in_ref,
    out_w_ref,
    shared_pre_ref,
    shared_in_ref,
    shared_out_ref,
    grad_pre_ref,
    moved_ref,
    partial_ref,
    joined_ref,
):
    units = out_w_ref.shape[0]
    grad = grad_ref[...]
    prob = prob_ref[...]
    own_prob = jnp.sum(prob * own_ref[...], axis=1, keepdims=True) * routed_ref[...]
    gate, up = pre_ref[:, :units].astype(jnp.float32), pre_ref[:, units:].astype(jnp.float32)
    grad_units = dot_t(grad, out_w_ref[...])
    act, slope = silu_parts(gate)
    grad_gate = jnp.sum(grad_units * act * up, axis=1, keepdims=True)
    moved = own_prob * grad_gate
    moved_ref[...] = moved
    grad_logits = bf16(moved * (own_ref[...] - prob))
    scaled = own_prob * grad_units
    joined_ref[:, :units] = bf16(scaled * up * slope)
    joined_ref[:, units : 2 * units] = bf16(scaled * act)
    joined_ref[:, 2 * units :] = jnp.zeros_like(joined_ref[:, 2 * units :])
    joined_ref[:, 2 * units : 2 * units + own_ref.shape[1]] = grad_logits
    grad_pre_ref[...] = joined_ref[:, : 2 * units]
    base = dot_t(joined_ref[...], in_ref[...])
    tile = pl.program_id(0)
    inside = (tile >= here_ref[0]) & (tile < here_ref[1])
    half = shared_out_ref.shape[0]

    def with_shared():
        left, right = gated_back(
            shared_pre_ref[0].astype(jnp.float32),
            shared_pre_ref[1].astype(jnp.float32),
            dot_t(grad, shared_out_ref[...]),
        )
        partial_ref[...] = bf16(base + dot(left, shared_in_ref[:half]) + dot(right, shared_in_ref[half:]))

    def without():
        partial_ref[...] = bf16(base)

    pl.when(inside)(with_shared)
    pl.when(jnp.logical_not(inside))(without)


def experts_back(grad, stored, routed, own_column, weights, here, pack_rows):
    expert_in, expert_out, shared_in, shared_out = weights
    routes_width = own_column.shape[1]
    rows, width = grad.shape
    tile = tile_rows(pack_rows)
    units, half = expert_out.shape[0], shared_out.shape[0]
    block, whole, inner = specs_of(rows, tile)
    shape = jax.ShapeDtypeStruct
    return pl.pallas_call(
        experts_back_kernel,
        grid_spec=pltpu.PrefetchScalarGridSpec(
            num_scalar_prefetch=1,
            grid=(rows // tile,),
            in_specs=[
                block(width),
                block(2 * units),
                block(routes_width),
                block(1),
                whole(own_column),
                whole(expert_in),
                whole(expert_out),
                pl.BlockSpec((2, tile, half), lambda i, here: (0, inner(i, here), 0)),
                whole(shared_in),
                whole(shared_out),
            ],
            out_specs=[block(2 * units), block(1), block(width)],
            scratch_shapes=[pltpu.VMEM((tile, expert_in.shape[1]), jnp.bfloat16)],
        ),
        out_shape=[
            shape((rows, 2 * units), jnp.bfloat16),
            shape((rows, 1), jnp.float32),
            shape((rows, width), jnp.bfloat16),
        ],
        name="experts_back",
        cost_estimate=pl.CostEstimate(
            flops=2 * rows * width * units * 3, bytes_accessed=rows * width * 4, transcendentals=rows * units
        ),
    )(
        here,
        grad,
        stored["pre"],
        stored["prob"],
        routed,
        own_column,
        expert_in,
        expert_out,
        stored["shared_pre"],
        shared_in,
        shared_out,
    )


def pair_grad_kernel(x_ref, grad_ref, out_ref):
    units = out_ref.shape[2]
    x = x_ref[...]
    out_ref[:, 0, :] = t_dot(x, grad_ref[:, :units])
    out_ref[:, 1, :] = t_dot(x, grad_ref[:, units:])


def pair_grad(x, grad):
    rows, width = x.shape
    units = grad.shape[1] // 2
    if rows > 4096:
        return t_dot(x, grad).reshape(width, 2, units)
    tile = 256
    return pl.pallas_call(
        pair_grad_kernel,
        grid=(width // tile,),
        in_specs=[
            pl.BlockSpec((rows, tile), lambda i: (0, i)),
            pl.BlockSpec((rows, 2 * units), lambda i: (0, 0), pipeline_mode=pl.Buffered(1)),
        ],
        out_specs=pl.BlockSpec((tile, 2, units), lambda i: (i, 0, 0)),
        out_shape=jax.ShapeDtypeStruct((width, 2, units), jnp.float32),
        name="pair_grad",
        cost_estimate=pl.CostEstimate(
            flops=4 * rows * width * units, bytes_accessed=rows * (width + 2 * units) * 2 + width * units * 8, transcendentals=0
        ),
    )(x, grad)


def blank(shape, dtype):
    return pl.pallas_call(
        lambda out_ref: None,
        out_shape=jax.ShapeDtypeStruct(shape, dtype),
        out_specs=pl.BlockSpec(memory_space=pl.ANY),
        compiler_params=pltpu.CompilerParams(has_side_effects=True),
        name="blank",
    )()


def body(
    boundary,
    lengths,
    routes,
    attn_gain,
    query_weight,
    compress_weight,
    latent_gain,
    expand_weight,
    output_weight,
    ffn_gain,
    router_weight,
    shared_in,
    shared_out,
    expert_in,
    expert_out,
):
    attn_gain, latent_gain, ffn_gain = attn_gain[0], latent_gain[0], ffn_gain[0]
    query_weight, compress_weight = query_weight[0], compress_weight[0]
    expand_weight, output_weight = expand_weight[0], output_weight[0]
    router_weight, shared_out, expert_out = router_weight[0], shared_out[0], expert_out[0, 0]
    width = boundary.shape[3]
    rows = boundary.shape[2]
    shared_half = shared_out.shape[0]
    units = expert_out.shape[0]
    shared_in_t = jnp.transpose(shared_in[0], (1, 2, 0)).reshape(2 * shared_half, width)
    experts_count = router_weight.shape[1]
    joined_in = jnp.concatenate(
        [
            expert_in.reshape(width, 2 * units),
            router_weight,
            jnp.zeros((width, -experts_count % 128), jnp.bfloat16),
        ],
        axis=1,
    )
    weights = (joined_in, expert_out, shared_in_t, shared_out)

    packs, members = lax.axis_size(PACKS), lax.axis_size(MEMBERS)
    count = packs * members
    pack, member = lax.axis_index(PACKS), lax.axis_index(MEMBERS)
    me = pack * members + member
    is_first = lax.axis_index(SECTION) == 0
    pack_rows = members * rows
    top = routes.shape[3]
    here = tile_here(pack, pack_rows)

    def own_pack(value):
        size = value.shape[0] // packs
        return lax.dynamic_slice_in_dim(value, pack * size, size, 0)

    def tables_of(block_lengths):
        segment, position = block_layout(block_lengths, rows)
        blocks = segment.shape[0]
        freqs = rope_base ** (-jnp.arange(HALF, dtype=jnp.float32) / HALF)
        angles = position.reshape(-1).astype(jnp.float32)[:, None] * freqs[None, :]
        return (
            jnp.cos(angles),
            jnp.sin(angles),
            segment.reshape(blocks * rows, 1),
            segment.reshape(blocks, 1, rows),
        )

    own_lengths = lax.dynamic_index_in_dim(lengths[0, 0], member, 0, keepdims=False)
    layout = jnp.concatenate([routes.reshape(rows * top), own_lengths])
    layout = jnp.pad(layout, (0, -layout.shape[0] % 1024)).reshape(8, -1)

    def routed_of(layout_all):
        routes_all = layout_all.reshape(count, -1)[:, : rows * top].reshape(count * rows, top)
        return jnp.any(routes_all == me, axis=1, keepdims=True).astype(jnp.float32)

    tables_pack = tables_of(lengths[0, 0])
    own_cos, own_sin = (
        lax.dynamic_slice_in_dim(table, member * rows, rows, 0) for table in tables_pack[:2]
    )
    own_column = (lax.broadcasted_iota(jnp.int32, (1, experts_count), 1) == me).astype(jnp.float32)

    def inputs_of(hidden):
        normed32, scale_attn = rms_forward(hidden, attn_gain)
        normed = bf16(normed32)
        compressed = dot(normed, compress_weight)
        latent32, scale_latent = rms_forward(compressed[:, :LAT], latent_gain)
        keyed = bf16(
            jnp.concatenate([latent32, rotate(compressed[:, LAT:], own_cos, own_sin)], axis=1)
        )
        return normed, keyed, (compressed, scale_attn, scale_latent)

    def heads_of(normed, keyed, tables):
        query_raw = dot(normed, query_weight)
        latent = bf16(dot(keyed[:, :LAT], expand_weight))
        attended, query = attend(query_raw, latent, keyed, tables)
        return attended, query, latent

    fresh = boundary[0, 0].astype(jnp.float32)

    normed, keyed, _ = inputs_of(fresh)
    pack_inputs = gather_blocks([normed, keyed], False, 1, 0)
    attended, _, _ = heads_of(*pack_inputs, tables_pack)
    mixed_first = fresh + scatter_blocks(
        bf16(dot(attended, output_weight)), False, 9, 0
    )
    ffn_all, layout_all = gather_blocks(
        [bf16(rms_forward(mixed_first, ffn_gain)[0]), layout], True, 2, 0
    )
    *_, partial = experts(ffn_all, routed_of(layout_all), own_column, weights, here, pack_rows, True)
    result_first = mixed_first + scatter_blocks(partial, True, 10, 0)
    target_all, layout_all = gather_blocks(
        [boundary[0, 0], layout], True, 0, 1, [blank(ffn_all.shape, jnp.bfloat16), layout_all]
    )
    sent, target_all, layout_all = lax.optimization_barrier((bf16(result_first), target_all, layout_all))
    inbound = lax.ppermute(sent, SECTION, [(0, 1)])
    routed = routed_of(layout_all)
    tables_all = tables_of(layout_all.reshape(count, -1)[:, rows * top : rows * top + lengths.shape[3]])

    hidden = jnp.where(is_first, fresh, inbound.astype(jnp.float32))
    normed, keyed, (compressed, scale_attn, scale_latent) = inputs_of(hidden)
    normed_pack, keyed_pack = gather_blocks([normed, keyed], False, 3, 1, pack_inputs)
    attended, query, latent = heads_of(normed_pack, keyed_pack, tables_pack)
    mixed = hidden + scatter_blocks(bf16(dot(attended, output_weight)), False, 11, 1)
    mixed = jnp.where(is_first, mixed_first, mixed)
    ffn32, scale_ffn = rms_forward(mixed, ffn_gain)
    (ffn_all,) = gather_blocks([bf16(ffn32)], True, 4, 1, [ffn_all])
    pre, gated, prob, shared_pre = experts(ffn_all, routed, own_column, weights, here, pack_rows, False)
    stored = dict(pre=pre, prob=prob, shared_pre=shared_pre)

    def latent_back(own):
        grad_latent, grad_latent_gain = rms_backward(
            compressed[:, :LAT], scale_latent, latent_gain, own[:, width : width + LAT]
        )
        grad_compressed = bf16(
            jnp.concatenate([grad_latent, rotate(own[:, width + LAT :], own_cos, -own_sin)], axis=1)
        )
        grad_normed = own[:, :width] + dot_t(grad_compressed, compress_weight)
        grad_hidden_norm, grad_attn_gain = rms_backward(hidden, scale_attn, attn_gain, grad_normed)
        return grad_compressed, grad_hidden_norm, grad_attn_gain, grad_latent_gain

    def heads_back(grad_query, grad_latent_heads, grad_shared_key):
        return bf16(
            jnp.concatenate(
                [
                    dot_t(grad_query, query_weight),
                    dot_t(grad_latent_heads, expand_weight),
                    grad_shared_key,
                ],
                axis=1,
            )
        )

    def prepare(normed_all, keyed_all):
        attended_all, query_all, latent_all = heads_of(normed_all, keyed_all, tables_all)
        left = dot_t(ffn_all, shared_in_t[:shared_half])
        right = dot_t(ffn_all, shared_in_t[shared_half:])
        return attended_all, query_all, latent_all, bf16(left), bf16(right), bf16(gated_hidden(left, right))

    grad_pre_second, moved_second, partial = experts_back(
        target_all, stored, routed, own_column, weights, here, pack_rows
    )
    grad_ffn_second = scatter_blocks(partial, True, 13, 1)
    grad_mixed = fresh + rms_backward(mixed, scale_ffn, ffn_gain, grad_ffn_second)[0]
    (grad_mixed_pack,) = gather_blocks([bf16(grad_mixed)], False, 5, 1)
    own_second = scatter_blocks(
        heads_back(
            *attend_back(query, latent, keyed_pack, bf16(dot_t(grad_mixed_pack, output_weight)), tables_pack)
        ),
        False,
        14,
        1,
    )
    grad_second = grad_mixed + latent_back(own_second)[1]

    all_inputs = gather_blocks([normed, keyed], True, 7, 0)
    prepared = lax.cond(
        is_first,
        prepare,
        lambda *_: tuple(blank(like.shape, like.dtype) for like in jax.eval_shape(prepare, *all_inputs)),
        *all_inputs,
    )
    grad_second, prepared, all_inputs = lax.optimization_barrier((grad_second, prepared, all_inputs))
    downbound = lax.ppermute(bf16(grad_second), SECTION, [(1, 0)]).astype(jnp.float32)

    normed_late, keyed_late, gated_late, _ = lax.optimization_barrier((normed, keyed, gated, grad_second))
    normed_all, keyed_all = gather_blocks([normed_late, keyed_late], True, 8, 1, all_inputs)
    attended_all, query_all, latent_all, shared_gate, shared_up, shared_hid = lax.cond(
        is_first, lambda *values: values[2:], lambda *values: prepare(*values[:2]), normed_all, keyed_all, *prepared
    )

    def finish(gated_late, shared_hid):
        partial = bf16(dot(gated_late, expert_out))
        addend = dot(own_pack(shared_hid), shared_out)
        return lax.dynamic_update_slice_in_dim(
            partial, bf16(own_pack(partial).astype(jnp.float32) + addend), pack * pack_rows, 0
        )

    partial = lax.cond(
        is_first, lambda *_: blank((count * rows, width), jnp.bfloat16), finish, gated_late, shared_hid
    )
    result = mixed + scatter_blocks(partial, True, 12, 1)

    upstream = jnp.where(is_first, downbound, fresh)
    (upstream_all,) = gather_blocks([bf16(upstream)], True, 6, 0, [target_all])
    grad_pre, moved, partial = lax.cond(
        is_first,
        lambda upstream_all, *_: tuple(
            experts_back(upstream_all, stored, routed, own_column, weights, here, pack_rows)
        ),
        lambda _, *old: (*old, blank((count * rows, width), jnp.bfloat16)),
        upstream_all,
        grad_pre_second,
        moved_second,
    )
    grad_ffn = jnp.where(is_first, scatter_blocks(partial, True, 15, 0), grad_ffn_second)
    grad_mixed_norm, grad_ffn_gain = rms_backward(mixed, scale_ffn, ffn_gain, grad_ffn)
    grad_mixed = upstream + grad_mixed_norm
    grad_mixed_all = lax.all_gather(bf16(grad_mixed), BOTH, axis=0, tiled=True)
    grad_attended = bf16(dot_t(grad_mixed_all, output_weight))
    grad_query, grad_latent_heads, grad_shared_key = attend_back(
        query_all, latent_all, keyed_all, grad_attended, tables_all
    )
    own = lax.psum_scatter(
        heads_back(own_pack(grad_query), own_pack(grad_latent_heads), own_pack(grad_shared_key)),
        MEMBERS,
        scatter_dimension=0,
        tiled=True,
    ).astype(jnp.float32)
    grad_compressed, grad_hidden_norm, grad_attn_gain, grad_latent_gain = latent_back(own)
    grad_hidden = grad_mixed + grad_hidden_norm

    small = jnp.concatenate([grad_attn_gain, grad_latent_gain, grad_ffn_gain, moved[:, 0]])
    small = jnp.pad(small, (0, -small.shape[0] % 1024)).reshape(8, -1)
    grad_compressed_all, small_all = gather_blocks([grad_compressed, small], True, 16)
    small_all = small_all.reshape(count, -1)
    gains = jnp.sum(small_all[:, : 2 * width + LAT], axis=0)
    moved_all = small_all[:, 2 * width + LAT : 2 * width + LAT + count * rows].T
    grad_logits = bf16(moved_all - prob * jnp.sum(moved_all, axis=1, keepdims=True))
    left, right = gated_back(
        shared_gate.astype(jnp.float32), shared_up.astype(jnp.float32), dot_t(upstream_all, shared_out)
    )
    grad_shared_in = lax.dot_general(
        jnp.stack([left, right]), ffn_all, (((1,), (0,)), ((), ())), preferred_element_type=jnp.float32
    )
    ends = jnp.where(is_first, grad_hidden, result)
    return (
        ends[None, None],
        gains[:width][None],
        t_dot(normed_all, grad_query)[None],
        t_dot(normed_all, grad_compressed_all)[None],
        gains[width : width + LAT][None],
        t_dot(keyed_all[:, :LAT], grad_latent_heads)[None],
        t_dot(attended_all, grad_mixed_all)[None],
        gains[width + LAT :][None],
        t_dot(ffn_all, grad_logits)[None],
        jnp.transpose(grad_shared_in, (2, 0, 1))[None],
        t_dot(shared_hid, upstream_all)[None],
        pair_grad(ffn_all, grad_pre)[None, None],
        t_dot(gated, upstream_all)[None, None],
    )


def solution(mesh):
    return jax.shard_map(
        body,
        mesh=mesh,
        in_specs=(
            P(SECTION, None, BOTH, None),
            P(None, PACKS, None, None),
            P(SECTION, None, BOTH, None),
            P(SECTION, None),
            P(SECTION, None, MEMBERS),
            P(SECTION, None, None),
            P(SECTION, None),
            P(SECTION, None, MEMBERS),
            P(SECTION, MEMBERS, None),
            P(SECTION, None),
            P(SECTION, None, None),
            P(SECTION, None, None, MEMBERS),
            P(SECTION, MEMBERS, None),
            P(SECTION, BOTH, None, None, None),
            P(SECTION, BOTH, None, None),
        ),
        out_specs=(
            P(SECTION, None, BOTH, None),
            P(SECTION, None),
            P(SECTION, None, MEMBERS),
            P(SECTION, None, None),
            P(SECTION, None),
            P(SECTION, None, MEMBERS),
            P(SECTION, MEMBERS, None),
            P(SECTION, None),
            P(SECTION, None, None),
            P(SECTION, None, None, MEMBERS),
            P(SECTION, MEMBERS, None),
            P(SECTION, BOTH, None, None, None),
            P(SECTION, BOTH, None, None),
        ),
        check_vma=False,
    )
```

```python
import functools

import jax
import jax.numpy as jnp
from jax import lax
from jax.experimental import pallas as pl
from jax.experimental.pallas import tpu as pltpu
from jax.sharding import PartitionSpec as P

NOPE = 128
ROPE = 64
VD = 128
LAT = 512

QK = NOPE + ROPE
KV = NOPE + VD
HALF = ROPE // 2
epsilon = 1e-06
rope_base = 10000.0
masked_score = -1e30
SECTION, PACKS, MEMBERS = "section", "dp", "expert"
BOTH = (PACKS, MEMBERS)
MESH = pl.DeviceIdType.MESH
def dot(left, right):
    return jnp.dot(left, right, preferred_element_type=jnp.float32)


def dot_t(left, right):
    return lax.dot_general(
        left, right, (((1,), (1,)), ((), ())), preferred_element_type=jnp.float32
    )


def t_dot(left, right):
    return lax.dot_general(
        left, right, (((0,), (0,)), ((), ())), preferred_element_type=jnp.float32
    )


def bf16(value):
    return value.astype(jnp.bfloat16)


def rms_forward(inputs, gain_vec):
    norm_scale = lax.rsqrt(jnp.mean(inputs * inputs, axis=-1, keepdims=True) + epsilon)
    return (inputs * norm_scale * gain_vec, norm_scale)


def rms_backward(inputs, norm_scale, gain_vec, upstream):
    weighted = upstream * gain_vec
    grad_gain = jnp.sum(upstream * inputs * norm_scale, axis=0)
    cubed = norm_scale * norm_scale * norm_scale
    grad_inputs = norm_scale * weighted - inputs * cubed * jnp.mean(
        weighted * inputs, axis=-1, keepdims=True
    )
    return (grad_inputs, grad_gain)


def rotate(inputs, cosine, sine):
    half = cosine.shape[-1]
    former = inputs[..., :half]
    latter = inputs[..., half:]
    return jnp.concatenate(
        [former * cosine - latter * sine, latter * cosine + former * sine], axis=-1
    )


def silu_parts(pre_gate):
    sigmoid = jax.nn.sigmoid(pre_gate)
    return (pre_gate * sigmoid, sigmoid * (1.0 + pre_gate * (1.0 - sigmoid)))


def block_layout(block_lengths, rows):
    starts = jnp.cumsum(block_lengths, axis=1) - block_lengths
    index = jnp.arange(rows, dtype=jnp.int32)
    begun = index[None, :, None] >= starts[:, None, :]
    segment = jnp.sum(begun.astype(jnp.int32), axis=2)
    opening = jnp.max(jnp.where(begun, starts[:, None, :], 0), axis=2)
    return segment, index[None, :] - opening


def places(spots):
    member = lax.axis_index(MEMBERS)
    spot = lax.axis_index(PACKS) if spots > 1 else 0
    return spot, member // 2, lax.rem(member, 2)


def to_partner(chip, core):
    return {MEMBERS: chip * 2 + 1 - core}


def to_other(chip, core):
    return {MEMBERS: (1 - chip) * 2 + core}


def when(condition, action):
    if condition is True:
        action()
    else:
        pl.when(condition)(action)


def greet(spots, spot, chip, core):
    barrier = pltpu.get_barrier_semaphore()

    def signal(target):
        pl.semaphore_signal(barrier, inc=1, device_id=target, device_id_type=MESH)

    signal(to_partner(chip, core))
    signal(to_other(chip, core))
    if spots > 1:
        pl.when(spot > 0)(lambda: signal({PACKS: spot - 1}))
        pl.when(spot < spots - 1)(lambda: signal({PACKS: spot + 1}))
        ends = jnp.where(spot > 0, 1, 0) + jnp.where(spot < spots - 1, 1, 0)
        pl.semaphore_wait(barrier, 2 + ends)
    else:
        pl.semaphore_wait(barrier, 2)


def remote(source, target_ref, target, out_sem, in_sem):
    return pltpu.make_async_remote_copy(
        src_ref=source,
        dst_ref=target_ref,
        send_sem=out_sem,
        recv_sem=in_sem,
        device_id=target,
        device_id_type=MESH,
    )


def slot(spot, chip, core):
    return spot * 4 + chip * 2 + core


def gather_kernel(spots, cuts, active, *refs):
    arrays = len(cuts)
    x_refs, o_refs, sems = refs[:arrays], refs[-9 - arrays : -9], refs[-9:]
    own_sem, up_out, up_in, down_out, down_in, over_out, over_in, pair_out, pair_in = sems
    units = [
        (a, pl.ds(part * (x_refs[a].shape[0] // parts), x_refs[a].shape[0] // parts))
        for a, parts in enumerate(cuts)
        for part in range(parts)
    ]

    def run():
        spot, chip, core = places(spots)
        greet(spots, spot, chip, core)

        def piece(unit, index):
            array, cut = units[unit]
            return o_refs[array].at[index, cut]

        def first(unit):
            array, cut = units[unit]
            return x_refs[array].at[cut]

        def up(source, at, unit, reach):
            return remote(
                source, piece(unit, slot(at, chip, core)), {PACKS: spot + 1}, up_out.at[reach, unit], up_in.at[reach, unit]
            )

        def down(source, at, unit, reach):
            return remote(
                source,
                piece(unit, slot(at, chip, core)),
                {PACKS: spot - 1},
                down_out.at[reach, unit],
                down_in.at[reach, unit],
            )

        def over(source, at, unit):
            return remote(
                source, piece(unit, slot(at, chip, core)), to_other(chip, core), over_out.at[at, unit], over_in.at[at, unit]
            )

        def pair(source, at, c, unit):
            return remote(
                source,
                piece(unit, slot(at, c, core)),
                to_partner(chip, core),
                pair_out.at[c, at, unit],
                pair_in.at[c, at, unit],
            )

        mine = slot(spot, chip, core)
        for unit in range(len(units)):
            source = first(unit)
            over(source, spot, unit).start()
            if spots > 1:
                pl.when(spot < spots - 1)(lambda: up(source, spot, unit, 0).start())
                pl.when(spot > 0)(lambda: down(source, spot, unit, 0).start())
            pair(source, spot, chip, unit).start()
        own = [pltpu.make_async_copy(x_refs[a], o_refs[a].at[mine], own_sem.at[a]) for a in range(arrays)]
        for copy in own:
            copy.start()
        for reach in range(1, spots):
            for unit in range(len(units)):

                def below(reach=reach, unit=unit):
                    at = spot - reach
                    source = piece(unit, slot(at, chip, core))
                    up(source, at, unit, reach - 1).wait_recv()
                    pl.when(spot < spots - 1)(lambda: up(source, at, unit, reach).start())
                    over(source, at, unit).start()
                    pair(source, at, chip, unit).start()

                def above(reach=reach, unit=unit):
                    at = spot + reach
                    source = piece(unit, slot(at, chip, core))
                    down(source, at, unit, reach - 1).wait_recv()
                    pl.when(spot > 0)(lambda: down(source, at, unit, reach).start())
                    over(source, at, unit).start()
                    pair(source, at, chip, unit).start()

                pl.when(spot >= reach)(below)
                pl.when(spot + reach < spots)(above)
        for reach in range(spots):
            sides = [(True, spot)]
            if reach > 0:
                sides = [(spot >= reach, spot - reach), (spot + reach < spots, spot + reach)]
            for unit in range(len(units)):
                for there, at in sides:

                    def hand_on(at=at, unit=unit):
                        source = piece(unit, slot(at, 1 - chip, core))
                        over(source, at, unit).wait_recv()
                        pair(source, at, 1 - chip, unit).start()

                    when(there, hand_on)
        for copy in own:
            copy.wait()
        for unit in range(len(units)):
            source = piece(unit, mine)
            for at in range(spots):
                over(source, at, unit).wait_send()
                for c in range(2):
                    pair(source, at, c, unit).wait()
            for reach in range(spots - 1):
                pl.when((spot >= reach) & (spot < spots - 1))(lambda: up(source, spot, unit, reach).wait_send())
                pl.when((spot + reach < spots) & (spot > 0))(lambda: down(source, spot, unit, reach).wait_send())

    if active is None:
        run()
    else:
        pl.when(lax.axis_index(SECTION) == active)(run)


def gather_blocks(values, across, number, active=None, into=None, parts=4):
    axes = BOTH if across else MEMBERS
    if lax.axis_size(MEMBERS) != 4:
        found = [lax.all_gather(value, axes, axis=0, tiled=True) for value in values]
        if into is None:
            return found
        chosen = lax.axis_index(SECTION) == active
        return [jnp.where(chosen, new, old) for new, old in zip(found, into)]
    spots = lax.axis_size(PACKS) if across else 1
    cuts = [parts if value.shape[0] % (16 * parts) == 0 else 1 for value in values]
    units = sum(cuts)
    dma = pltpu.SemaphoreType.DMA
    hops = max(spots - 1, 1)
    shapes = [jax.ShapeDtypeStruct((spots * 4, *value.shape), value.dtype) for value in values]
    held = [] if into is None else [old.reshape(shape.shape) for old, shape in zip(into, shapes)]
    outs = pl.pallas_call(
        functools.partial(gather_kernel, spots, cuts, active),
        out_shape=shapes,
        in_specs=[pl.BlockSpec(memory_space=pltpu.VMEM)] * len(values)
        + [pl.BlockSpec(memory_space=pl.ANY)] * len(held),
        out_specs=[pl.BlockSpec(memory_space=pl.ANY)] * len(values),
        input_output_aliases={len(values) + index: index for index in range(len(held))},
        scratch_shapes=[
            dma((len(values),)),
            dma((hops, units)),
            dma((hops, units)),
            dma((hops, units)),
            dma((hops, units)),
            dma((spots, units)),
            dma((spots, units)),
            dma((2, spots, units)),
            dma((2, spots, units)),
        ],
        compiler_params=pltpu.CompilerParams(collective_id=number, has_side_effects=True),
        name=f"gather{number}",
    )(*values, *held)
    return [out.reshape(-1, out.shape[2]) for out in outs]


def add_into(target, sources, rows, step=16):
    def some(index, carry):
        at = pl.ds(pl.multiple_of(index * step, step), step)
        total = sources[0][at, :].astype(jnp.float32)
        for source in sources[1:]:
            total = total + source[at, :].astype(jnp.float32)
        target[at, :] = total.astype(target.dtype)
        return carry

    lax.fori_loop(0, rows // step, some, 0)


def scatter_kernel(
    spots,
    parts,
    active,
    x_ref,
    o_ref,
    own_buf,
    pair_buf,
    over_src,
    over_buf,
    line_src,
    up_buf,
    down_buf,
    own_in,
    pair_out,
    pair_in,
    over_out,
    over_in,
    line_out,
    up_in,
    down_in,
):
    rows = x_ref.shape[1] // parts
    cut = lambda part: pl.ds(part * rows, rows)

    def run():
        spot, chip, core = places(spots)
        greet(spots, spot, chip, core)

        def order(step):
            if step == spots - 1:
                return spot
            fall = spots - 1 - step
            fall = jnp.where(fall <= spot, fall - 1, fall)
            rise = jnp.where(step >= spot, step + 1, step)
            return jnp.where(2 * spot < spots - 1, fall, rise)

        def pair(at, c, part):
            return remote(
                x_ref.at[slot(at, c, 1 - core), cut(part)],
                pair_buf.at[at, c, cut(part)],
                to_partner(chip, core),
                pair_out.at[at, c, part],
                pair_in.at[at, c, part],
            )

        def over(at, part):
            return remote(
                over_src.at[at, cut(part)],
                over_buf.at[at, cut(part)],
                to_other(chip, core),
                over_out.at[at, part],
                over_in.at[at, part],
            )

        def up(at, part):
            return remote(
                line_src.at[at, cut(part)],
                up_buf.at[at, cut(part)],
                {PACKS: spot + 1},
                line_out.at[at, part],
                up_in.at[at, part],
            )

        def down(at, part):
            return remote(
                line_src.at[at, cut(part)],
                down_buf.at[at, cut(part)],
                {PACKS: spot - 1},
                line_out.at[at, part],
                down_in.at[at, part],
            )

        def own(at, c):
            return pltpu.make_async_copy(x_ref.at[slot(at, c, core)], own_buf.at[at, c], own_in.at[at, c])

        for c in (1 - chip, chip):
            for step in range(spots):
                own(order(step), c).start()
                for part in range(parts):
                    pair(order(step), c, part).start()
        for step in range(spots):
            at = order(step)
            own(at, 1 - chip).wait()
            for part in range(parts):
                pair(at, 1 - chip, part).wait_recv()
                add_into(
                    over_src.at[at, cut(part)],
                    [own_buf.at[at, 1 - chip, cut(part)], pair_buf.at[at, 1 - chip, cut(part)]],
                    rows,
                )
                over(at, part).start()
        for step in range(spots):
            at = order(step)
            own(at, chip).wait()
            for part in range(parts):
                pair(at, chip, part).wait_recv()
                over(at, part).wait_recv()
                base = [
                    own_buf.at[at, chip, cut(part)],
                    pair_buf.at[at, chip, cut(part)],
                    over_buf.at[at, cut(part)],
                ]
                ups, downs = up_buf.at[at, cut(part)], down_buf.at[at, cut(part)]
                if step < spots - 1:
                    target = line_src.at[at, cut(part)]

                    def rising(first):
                        if not first:
                            up(at, part).wait_recv()
                        add_into(target, base if first else base + [ups], rows)
                        up(at, part).start()

                    def falling(first):
                        if not first:
                            down(at, part).wait_recv()
                        add_into(target, base if first else base + [downs], rows)
                        down(at, part).start()

                    pl.when((at > spot) & (spot == 0))(lambda: rising(True))
                    pl.when((at > spot) & (spot > 0))(lambda: rising(False))
                    pl.when((at < spot) & (spot == spots - 1))(lambda: falling(True))
                    pl.when((at < spot) & (spot < spots - 1))(lambda: falling(False))
                elif spots == 1:
                    add_into(o_ref.at[cut(part)], base, rows)
                else:

                    def finish(ends):
                        if ends < 1:
                            up(at, part).wait_recv()
                        if ends > -1:
                            down(at, part).wait_recv()
                        extra = ([ups] if ends < 1 else []) + ([downs] if ends > -1 else [])
                        add_into(o_ref.at[cut(part)], base + extra, rows)

                    pl.when(spot == 0)(lambda: finish(1))
                    pl.when(spot == spots - 1)(lambda: finish(-1))
                    pl.when((spot > 0) & (spot < spots - 1))(lambda: finish(0))
        for part in range(parts):
            for step in range(spots):
                at = order(step)
                pair(at, 0, part).wait_send()
                pair(at, 1, part).wait_send()
                over(at, part).wait_send()
                if step < spots - 1:
                    up(at, part).wait_send()

    if active is None:
        run()
    else:
        pl.when(lax.axis_index(SECTION) == active)(run)


def scatter_blocks(partial, rows, across, number, active=None, parts=4):
    if lax.axis_size(MEMBERS) != 4:
        axes = BOTH if across else MEMBERS
        taken = partial[: rows * lax.axis_size(axes)]
        return lax.psum_scatter(taken, axes, scatter_dimension=0, tiled=True).astype(jnp.float32)
    spots = lax.axis_size(PACKS) if across else 1
    width = partial.shape[1]
    dma = pltpu.SemaphoreType.DMA
    hold = lambda *lead: pltpu.VMEM((*lead, rows, width), partial.dtype)
    return pl.pallas_call(
        functools.partial(scatter_kernel, spots, parts, active),
        out_shape=jax.ShapeDtypeStruct((rows, width), jnp.float32),
        in_specs=[pl.BlockSpec(memory_space=pl.ANY)],
        out_specs=pl.BlockSpec(memory_space=pltpu.VMEM),
        scratch_shapes=[
            hold(spots, 2),
            hold(spots, 2),
            hold(spots),
            hold(spots),
            hold(spots),
            hold(spots),
            hold(spots),
            dma((spots, 2)),
            dma((spots, 2, parts)),
            dma((spots, 2, parts)),
            dma((spots, parts)),
            dma((spots, parts)),
            dma((spots, parts)),
            dma((spots, parts)),
            dma((spots, parts)),
        ],
        compiler_params=pltpu.CompilerParams(collective_id=number, has_side_effects=True),
        name=f"scatter{number}",
    )(partial.reshape(-1, rows, width))


def allowed_pairs(seg_col, seg_row):
    rows = seg_col.shape[0]
    later = lax.broadcasted_iota(jnp.int32, (rows, rows), 0)
    earlier = lax.broadcasted_iota(jnp.int32, (rows, rows), 1)
    return (seg_col == seg_row) & (earlier <= later)


def attend_kernel(heads, q_ref, lat_ref, key_ref, cos_ref, sin_ref, col_ref, row_ref, out_ref, rot_ref):
    factor = QK**-0.5
    allowed = allowed_pairs(col_ref[...], row_ref[0])
    cosine, sine = cos_ref[...], sin_ref[...]
    shared = key_ref[:, LAT:]
    for head in range(heads):
        raw = q_ref[:, head * QK : (head + 1) * QK]
        query = bf16(
            jnp.concatenate([raw[:, :NOPE], rotate(raw[:, NOPE:], cosine, sine)], axis=1)
        )
        rot_ref[:, head * QK : (head + 1) * QK] = query
        key = jnp.concatenate([lat_ref[:, head * KV : head * KV + NOPE], shared], axis=1)
        value = lat_ref[:, head * KV + NOPE : (head + 1) * KV]
        scores = jnp.where(allowed, dot_t(query, key) * factor, masked_score)
        top = jnp.max(scores, axis=1, keepdims=True)
        powers = jnp.exp(scores - top)
        probs = powers / jnp.sum(powers, axis=1, keepdims=True)
        out_ref[:, head * VD : (head + 1) * VD] = bf16(dot(bf16(probs), value))


def attend(query_raw, latent, keyed, tables, groups=1):
    cosine, sine, seg_col, seg_row = tables
    count, _, rows = seg_row.shape
    heads = query_raw.shape[1] // QK
    block = lambda width: pl.BlockSpec((rows, width), lambda i: (i, 0))
    same = lambda width: pl.BlockSpec((rows, width), lambda i: (0, 0) if groups > 1 else (i, 0))
    count = count * groups
    return pl.pallas_call(
        functools.partial(attend_kernel, heads),
        grid=(count,),
        in_specs=[
            block(heads * QK),
            block(heads * KV),
            same(LAT + ROPE),
            same(HALF),
            same(HALF),
            same(1),
            pl.BlockSpec((1, 1, rows), lambda i: (0, 0, 0) if groups > 1 else (i, 0, 0)),
        ],
        out_specs=[block(heads * VD), block(heads * QK)],
        out_shape=[
            jax.ShapeDtypeStruct((count * rows, heads * VD), jnp.bfloat16),
            jax.ShapeDtypeStruct((count * rows, heads * QK), jnp.bfloat16),
        ],
        name="attend",
        cost_estimate=pl.CostEstimate(
            flops=2 * count * heads * rows * rows * (QK + VD),
            bytes_accessed=count * rows * heads * (QK * 6 + KV * 2 + VD * 2),
            transcendentals=count * heads * rows * rows,
        ),
    )(query_raw, latent, keyed, cosine, sine, seg_col, seg_row)


def attend_back_kernel(
    heads, q_ref, lat_ref, key_ref, grad_ref, cos_ref, sin_ref, col_ref, row_ref, dq_ref, dlat_ref, dkey_ref
):
    factor = QK**-0.5
    allowed = allowed_pairs(col_ref[...], row_ref[0])
    cosine, sine = cos_ref[...], sin_ref[...]
    shared = key_ref[:, LAT:]
    total = None
    for head in range(heads):
        query = q_ref[:, head * QK : (head + 1) * QK]
        key = jnp.concatenate([lat_ref[:, head * KV : head * KV + NOPE], shared], axis=1)
        value = lat_ref[:, head * KV + NOPE : (head + 1) * KV]
        grad = grad_ref[:, head * VD : (head + 1) * VD]
        scores = jnp.where(allowed, dot_t(query, key) * factor, masked_score)
        top = jnp.max(scores, axis=1, keepdims=True)
        powers = jnp.exp(scores - top)
        probs = powers / jnp.sum(powers, axis=1, keepdims=True)
        grad_value = t_dot(bf16(probs), grad)
        grad_probs = dot_t(grad, value)
        centre = jnp.sum(probs * grad_probs, axis=1, keepdims=True)
        grad_scores = bf16(probs * (grad_probs - centre) * factor)
        grad_query = dot(grad_scores, key)
        grad_key = t_dot(grad_scores, query)
        dq_ref[:, head * QK : (head + 1) * QK] = bf16(
            jnp.concatenate(
                [grad_query[:, :NOPE], rotate(grad_query[:, NOPE:], cosine, -sine)], axis=1
            )
        )
        dlat_ref[:, head * KV : head * KV + NOPE] = bf16(grad_key[:, :NOPE])
        dlat_ref[:, head * KV + NOPE : (head + 1) * KV] = bf16(grad_value)
        part = grad_key[:, NOPE:]
        total = part if total is None else total + part
    dkey_ref[...] = total


def attend_back(query, latent, keyed, grad, tables, groups=1):
    cosine, sine, seg_col, seg_row = tables
    count, _, rows = seg_row.shape
    heads = query.shape[1] // QK
    block = lambda width: pl.BlockSpec((rows, width), lambda i: (i, 0))
    same = lambda width: pl.BlockSpec((rows, width), lambda i: (0, 0) if groups > 1 else (i, 0))
    count = count * groups
    return pl.pallas_call(
        functools.partial(attend_back_kernel, heads),
        grid=(count,),
        in_specs=[
            block(heads * QK),
            block(heads * KV),
            same(LAT + ROPE),
            block(heads * VD),
            same(HALF),
            same(HALF),
            same(1),
            pl.BlockSpec((1, 1, rows), lambda i: (0, 0, 0) if groups > 1 else (i, 0, 0)),
        ],
        out_specs=[block(heads * QK), block(heads * KV), block(ROPE)],
        out_shape=[
            jax.ShapeDtypeStruct((count * rows, heads * QK), jnp.bfloat16),
            jax.ShapeDtypeStruct((count * rows, heads * KV), jnp.bfloat16),
            jax.ShapeDtypeStruct((count * rows, ROPE), jnp.float32),
        ],
        name="attend_back",
        cost_estimate=pl.CostEstimate(
            flops=2 * count * heads * rows * rows * (3 * QK + 2 * VD),
            bytes_accessed=count * rows * heads * (QK * 4 + KV * 4 + VD * 2),
            transcendentals=count * heads * rows * rows,
        ),
    )(query, latent, keyed, grad, cosine, sine, seg_col, seg_row)


def gated_hidden(gate, up):
    return silu_parts(gate)[0] * up


def gated_back(gate, up, grad_hidden):
    act, slope = silu_parts(gate)
    return bf16(grad_hidden * up * slope), bf16(grad_hidden * act)


def load(sources, targets, sems):
    copies = [
        pltpu.make_async_copy(source, target, sems.at[index])
        for index, (source, target) in enumerate(zip(sources, targets))
    ]
    for copy in copies:
        copy.start()
    for copy in copies:
        copy.wait()


class Tiles:
    def __init__(self, rows, pack_rows, pack, active):
        self.rows, self.pack_rows = rows, pack_rows
        self.tile = min(256, pack_rows)
        self.count = rows // self.tile
        inner = pack_rows // self.tile
        runs = (lax.axis_index(SECTION) == active).astype(jnp.int32)
        self.control = jnp.stack([pack * inner, (pack + 1) * inner, runs]).astype(jnp.int32)

    def source(self, width):
        return pl.BlockSpec((self.tile, width), lambda i, control: (i * control[2], 0))

    def small(self, array):
        return pl.BlockSpec(array.shape, lambda i, control: (0,) * array.ndim)

    def pack_source(self, width):
        def index(i, control):
            return (0, jnp.clip(i - control[0], 0, control[1] - control[0] - 1), 0)

        return pl.BlockSpec((2, self.tile, width), index)

    def result(self, width, dtype=jnp.bfloat16):
        def index(i, control):
            return (jnp.where(control[2] == 1, i, self.count), 0)

        shape = jax.ShapeDtypeStruct((self.rows + self.tile, width), dtype)
        return shape, pl.BlockSpec((self.tile, width), index)

    def pair_result(self, width):
        def index(i, control):
            return (0, jnp.where(control[2] == 1, i, self.count), 0)

        shape = jax.ShapeDtypeStruct((2, self.rows + self.tile, width), jnp.bfloat16)
        return shape, pl.BlockSpec((2, self.tile, width), index)

    def pack_result(self, width):
        def index(i, control):
            spot = jnp.clip(i - control[0], 0, control[1] - control[0] - 1)
            return (0, jnp.where(control[2] == 1, spot, control[1] - control[0]), 0)

        shape = jax.ShapeDtypeStruct((2, self.pack_rows + self.tile, width), jnp.bfloat16)
        return shape, pl.BlockSpec((2, self.tile, width), index)

    def call(self, kernel, name, sources, weights, results, into=(), scratch=(), flops=0):
        arrays, specs = zip(*sources)
        shapes, out_specs = zip(*results)
        anywhere = pl.BlockSpec(memory_space=pl.ANY)
        first = 1 + len(arrays) + len(weights)
        return pl.pallas_call(
            functools.partial(kernel, len(arrays), len(weights), len(into), len(results)),
            grid_spec=pltpu.PrefetchScalarGridSpec(
                num_scalar_prefetch=1,
                grid=(self.count,),
                in_specs=[*specs, *([anywhere] * (len(weights) + len(into)))],
                out_specs=list(out_specs),
                scratch_shapes=[
                    *[pltpu.VMEM(weight.shape, weight.dtype) for weight in weights],
                    pltpu.SemaphoreType.DMA((len(weights),)),
                    *scratch,
                ],
            ),
            out_shape=list(shapes),
            input_output_aliases={first + index: index for index in range(len(into))},
            name=name,
            cost_estimate=pl.CostEstimate(flops=flops, bytes_accessed=self.rows * 16384, transcendentals=0),
        )(self.control, *arrays, *weights, *into)


def tiled(body):
    def kernel(n_sources, n_weights, n_into, n_results, control, *refs):
        sources, refs = refs[:n_sources], refs[n_sources:]
        stored, refs = refs[:n_weights], refs[n_weights + n_into :]
        results, refs = refs[:n_results], refs[n_results:]
        weights, sems, scratch = refs[:n_weights], refs[n_weights], refs[n_weights + 1 :]

        def run():
            pl.when(pl.program_id(0) == 0)(lambda: load(stored, weights, sems))
            body(control, sources, weights, results, scratch)

        pl.when(control[2] == 1)(run)

    return kernel


def inside_pack(control):
    tile = pl.program_id(0)
    return (tile >= control[0]) & (tile < control[1])


def shared_units(x, shared_in):
    half = shared_in.shape[0] // 2
    return dot_t(x, shared_in[:half]), dot_t(x, shared_in[half:])


def experts_body(control, sources, weights, results, scratch):
    x_ref, routed_ref, own_ref = sources
    in_ref, shared_in_ref = weights[:2]
    pre_ref, gated_ref, prob_ref, shared_pre_ref = results[:4]
    units = gated_ref.shape[1]
    x = x_ref[...]
    pre = dot(x, in_ref[...])
    logits = pre[:, 2 * units : 2 * units + own_ref.shape[1]]
    powers = jnp.exp(logits - jnp.max(logits, axis=1, keepdims=True))
    prob = powers / jnp.sum(powers, axis=1, keepdims=True)
    prob_ref[...] = prob
    gate = jnp.sum(prob * own_ref[...], axis=1, keepdims=True) * routed_ref[...]
    pre_ref[...] = bf16(pre[:, : 2 * units])
    gated = bf16(gate * gated_hidden(pre[:, :units], pre[:, units : 2 * units]))
    gated_ref[...] = gated

    def shared():
        left, right = shared_units(x, shared_in_ref)
        shared_pre_ref[0] = bf16(left)
        shared_pre_ref[1] = bf16(right)
        return left, right

    if len(weights) == 2:
        pl.when(inside_pack(control))(lambda: shared() and None)
        return
    out_ref, shared_out_ref = weights[2:]
    partial_ref = results[4]

    def with_shared():
        hidden = bf16(gated_hidden(*shared()))
        partial_ref[...] = bf16(dot(gated, out_ref[...]) + dot(hidden, shared_out_ref[...]))

    def without():
        partial_ref[...] = bf16(dot(gated, out_ref[...]))

    pl.when(inside_pack(control))(with_shared)
    pl.when(jnp.logical_not(inside_pack(control)))(without)


def finish_body(control, sources, weights, results, scratch):
    gated_ref, shared_pre_ref = sources
    out_ref, shared_out_ref = weights
    (partial_ref,) = results

    def with_shared():
        hidden = bf16(gated_hidden(shared_pre_ref[0].astype(jnp.float32), shared_pre_ref[1].astype(jnp.float32)))
        partial_ref[...] = bf16(dot(gated_ref[...], out_ref[...]) + dot(hidden, shared_out_ref[...]))

    def without():
        partial_ref[...] = bf16(dot(gated_ref[...], out_ref[...]))

    pl.when(inside_pack(control))(with_shared)
    pl.when(jnp.logical_not(inside_pack(control)))(without)


def experts_back_body(control, sources, weights, results, scratch):
    grad_ref, pre_ref, prob_ref, routed_ref, own_ref, shared_pre_ref = sources
    in_ref, shared_in_ref, out_ref, shared_out_ref = weights
    grad_pre_ref, moved_ref, partial_ref = results
    (joined_ref,) = scratch
    units = out_ref.shape[0]
    grad = grad_ref[...]
    prob = prob_ref[...]
    own_prob = jnp.sum(prob * own_ref[...], axis=1, keepdims=True) * routed_ref[...]
    gate, up = pre_ref[:, :units].astype(jnp.float32), pre_ref[:, units:].astype(jnp.float32)
    grad_units = dot_t(grad, out_ref[...])
    act, slope = silu_parts(gate)
    moved = own_prob * jnp.sum(grad_units * act * up, axis=1, keepdims=True)
    moved_ref[...] = moved
    scaled = own_prob * grad_units
    joined_ref[:, :units] = bf16(scaled * up * slope)
    joined_ref[:, units : 2 * units] = bf16(scaled * act)
    joined_ref[:, 2 * units :] = jnp.zeros_like(joined_ref[:, 2 * units :])
    joined_ref[:, 2 * units : 2 * units + own_ref.shape[1]] = bf16(moved * (own_ref[...] - prob))
    grad_pre_ref[...] = joined_ref[:, : 2 * units]
    base = dot_t(joined_ref[...], in_ref[...])
    half = shared_out_ref.shape[0]

    def with_shared():
        left, right = gated_back(
            shared_pre_ref[0].astype(jnp.float32),
            shared_pre_ref[1].astype(jnp.float32),
            dot_t(grad, shared_out_ref[...]),
        )
        partial_ref[...] = bf16(base + dot(left, shared_in_ref[:half]) + dot(right, shared_in_ref[half:]))

    def without():
        partial_ref[...] = bf16(base)

    pl.when(inside_pack(control))(with_shared)
    pl.when(jnp.logical_not(inside_pack(control)))(without)


def shared_body(control, sources, weights, results, scratch):
    pre_ref, hid_ref = results
    left, right = shared_units(sources[0][...], weights[0])
    pre_ref[0] = bf16(left)
    pre_ref[1] = bf16(right)
    hid_ref[...] = bf16(gated_hidden(left, right))


def heads_body(block, control, sources, weights, results, scratch):
    x_ref, key_ref, cos_ref, sin_ref, col_ref, row_ref = sources
    query_w_ref, expand_ref = weights
    out_ref, rot_ref, lat_ref = results
    (q_ref,) = scratch
    heads = q_ref.shape[1] // QK
    q_ref[...] = dot(x_ref[...], query_w_ref[...])
    lat_ref[...] = bf16(dot(key_ref[:, :LAT], expand_ref[...]))
    for start in range(0, x_ref.shape[0], block):
        at = pl.ds(start, block)
        attend_kernel(
            heads,
            q_ref.at[at],
            lat_ref.at[at],
            key_ref.at[at],
            cos_ref.at[at],
            sin_ref.at[at],
            col_ref.at[at],
            row_ref.at[pl.ds(start // block, 1)],
            out_ref.at[at],
            rot_ref.at[at],
        )


def pair_grad_kernel(x_ref, grad_ref, out_ref):
    units = out_ref.shape[2]
    x = x_ref[...]
    out_ref[:, 0, :] = t_dot(x, grad_ref[:, :units])
    out_ref[:, 1, :] = t_dot(x, grad_ref[:, units:])


def pair_grad(x, grad):
    rows, width = x.shape
    units = grad.shape[1] // 2
    if rows > 4096:
        return t_dot(x, grad[:rows]).reshape(width, 2, units)
    tile = 256
    return pl.pallas_call(
        pair_grad_kernel,
        grid=(width // tile,),
        in_specs=[
            pl.BlockSpec((rows, tile), lambda i: (0, i)),
            pl.BlockSpec((rows, 2 * units), lambda i: (0, 0), pipeline_mode=pl.Buffered(1)),
        ],
        out_specs=pl.BlockSpec((tile, 2, units), lambda i: (i, 0, 0)),
        out_shape=jax.ShapeDtypeStruct((width, 2, units), jnp.float32),
        name="pair_grad",
        cost_estimate=pl.CostEstimate(
            flops=4 * rows * width * units, bytes_accessed=rows * (width + 2 * units) * 2 + width * units * 8, transcendentals=0
        ),
    )(x, grad)


def blank(shape, dtype):
    return pl.pallas_call(
        lambda out_ref: None,
        out_shape=jax.ShapeDtypeStruct(shape, dtype),
        out_specs=pl.BlockSpec(memory_space=pl.ANY),
        compiler_params=pltpu.CompilerParams(has_side_effects=True),
        name="blank",
    )()


def body(
    boundary,
    lengths,
    routes,
    attn_gain,
    query_weight,
    compress_weight,
    latent_gain,
    expand_weight,
    output_weight,
    ffn_gain,
    router_weight,
    shared_in,
    shared_out,
    expert_in,
    expert_out,
):
    attn_gain, latent_gain, ffn_gain = attn_gain[0], latent_gain[0], ffn_gain[0]
    query_weight, compress_weight = query_weight[0], compress_weight[0]
    expand_weight, output_weight = expand_weight[0], output_weight[0]
    router_weight, shared_out, expert_out = router_weight[0], shared_out[0], expert_out[0, 0]
    width = boundary.shape[3]
    rows = boundary.shape[2]
    half = shared_out.shape[0]
    units = expert_out.shape[0]
    experts_count = router_weight.shape[1]
    shared_in_t = jnp.transpose(shared_in[0], (1, 2, 0)).reshape(2 * half, width)
    joined_in = jnp.concatenate(
        [
            expert_in.reshape(width, 2 * units),
            router_weight,
            jnp.zeros((width, -experts_count % 128), jnp.bfloat16),
        ],
        axis=1,
    )

    packs, members = lax.axis_size(PACKS), lax.axis_size(MEMBERS)
    count = packs * members
    pack, member = lax.axis_index(PACKS), lax.axis_index(MEMBERS)
    me = pack * members + member
    is_first = lax.axis_index(SECTION) == 0
    pack_rows = members * rows
    all_rows = count * rows
    heads = output_weight.shape[0] // VD
    top = routes.shape[3]
    tiles = [Tiles(all_rows, pack_rows, pack, active) for active in range(2)]

    def own_pack(value):
        size = value.shape[0] // packs
        return lax.dynamic_slice_in_dim(value, pack * size, size, 0)

    def tables_of(block_lengths):
        segment, position = block_layout(block_lengths, rows)
        blocks = segment.shape[0]
        freqs = rope_base ** (-jnp.arange(HALF, dtype=jnp.float32) / HALF)
        angles = position.reshape(-1).astype(jnp.float32)[:, None] * freqs[None, :]
        return (
            jnp.cos(angles),
            jnp.sin(angles),
            segment.reshape(blocks * rows, 1),
            segment.reshape(blocks, 1, rows),
        )

    own_lengths = lax.dynamic_index_in_dim(lengths[0, 0], member, 0, keepdims=False)
    layout = jnp.concatenate([routes.reshape(rows * top), own_lengths])
    layout = jnp.pad(layout, (0, -layout.shape[0] % 1024)).reshape(8, -1)

    def routed_of(layout_all):
        routes_all = layout_all.reshape(count, -1)[:, : rows * top].reshape(all_rows, top)
        return jnp.any(routes_all == me, axis=1, keepdims=True).astype(jnp.float32)

    tables_pack = tables_of(lengths[0, 0])
    tables_own = tables_of(own_lengths[None])
    own_cos, own_sin = tables_own[:2]
    own_column = (lax.broadcasted_iota(jnp.int32, (1, experts_count), 1) == me).astype(jnp.float32)

    def inputs_of(hidden):
        normed32, scale_attn = rms_forward(hidden, attn_gain)
        normed = bf16(normed32)
        compressed = dot(normed, compress_weight)
        latent32, scale_latent = rms_forward(compressed[:, :LAT], latent_gain)
        keyed = bf16(
            jnp.concatenate([latent32, rotate(compressed[:, LAT:], own_cos, own_sin)], axis=1)
        )
        return normed, keyed, (compressed, scale_attn, scale_latent)

    def run_experts(section, x, routed, into, full):
        at = tiles[section]
        results = [
            at.result(2 * units),
            at.result(units),
            at.result(experts_count, jnp.float32),
            at.pack_result(half),
        ]
        weights = [joined_in, shared_in_t]
        if full:
            results.append(at.result(width))
            weights += [expert_out, shared_out]
        return at.call(
            tiled(experts_body),
            "experts",
            [(x, at.source(width)), (routed, at.source(1)), (own_column, at.small(own_column))],
            weights,
            results,
            into,
            flops=6 * all_rows * width * units,
        )

    def run_experts_back(section, grad, routed, stored, into):
        at = tiles[section]
        pre, _, prob, shared_pre = stored
        return at.call(
            tiled(experts_back_body),
            "experts_back",
            [
                (grad, at.source(width)),
                (pre, at.source(2 * units)),
                (prob, at.source(experts_count)),
                (routed, at.source(1)),
                (own_column, at.small(own_column)),
                (shared_pre, at.pack_source(half)),
            ],
            [joined_in, shared_in_t, expert_out, shared_out],
            [at.result(2 * units), at.result(1, jnp.float32), at.result(width)],
            into,
            [pltpu.VMEM((at.tile, joined_in.shape[1]), jnp.bfloat16)],
            flops=6 * all_rows * width * units,
        )

    def prepare(section, normed_all, keyed_all, ffn_all, tables, into):
        at = tiles[section]
        cosine, sine, seg_col, seg_row = tables
        blocks = at.tile // rows
        row_spec = pl.BlockSpec((blocks, 1, rows), lambda i, control: (i * control[2], 0, 0))
        found = at.call(
            tiled(functools.partial(heads_body, rows)),
            "heads",
            [
                (normed_all, at.source(width)),
                (keyed_all, at.source(LAT + ROPE)),
                (cosine, at.source(HALF)),
                (sine, at.source(HALF)),
                (seg_col, at.source(1)),
                (seg_row, row_spec),
            ],
            [query_weight, expand_weight],
            [at.result(heads * VD), at.result(heads * QK), at.result(heads * KV)],
            into[:3],
            [pltpu.VMEM((at.tile, heads * QK), jnp.float32)],
            flops=4 * all_rows * width * heads * QK,
        )
        shared = at.call(
            tiled(shared_body),
            "shared",
            [(ffn_all, at.source(width))],
            [shared_in_t],
            [at.pair_result(half), at.result(half)],
            into[3:],
            flops=4 * all_rows * width * half,
        )
        return [*found, *shared]

    fresh = boundary[0, 0].astype(jnp.float32)

    normed, keyed, _ = inputs_of(fresh)
    normed_pack, keyed_pack = gather_blocks([normed, keyed], False, 0, 0)
    attended, _ = attend(
        dot(normed_pack, query_weight),
        bf16(dot(keyed_pack[:, :LAT], expand_weight)),
        keyed_pack,
        tables_pack,
    )
    mixed_first = fresh + scatter_blocks(bf16(dot(attended, output_weight)), rows, False, 1, 0)
    ffn_all, layout_all = gather_blocks(
        [bf16(rms_forward(mixed_first, ffn_gain)[0]), layout], True, 2, 0
    )
    *stored, partial = run_experts(0, ffn_all, routed_of(layout_all), (), True)
    result_first = mixed_first + scatter_blocks(partial, rows, True, 3, 0)
    heads_weights = gather_blocks([query_weight, expand_weight, output_weight], False, 4, 1, parts=8)
    target_all, layout_all = gather_blocks(
        [boundary[0, 0], layout], True, 5, 1, [blank(ffn_all.shape, jnp.bfloat16), layout_all]
    )
    sent, target_all, layout_all, heads_weights = lax.optimization_barrier(
        (bf16(result_first), target_all, layout_all, heads_weights)
    )
    inbound = lax.ppermute(sent, SECTION, [(0, 1)])
    routed = routed_of(layout_all)
    tables_all = tables_of(layout_all.reshape(count, -1)[:, rows * top : rows * top + lengths.shape[3]])
    query_heads, expand_heads, output_heads = (
        value.reshape(members, -1, value.shape[1]) for value in heads_weights
    )

    hidden = jnp.where(is_first, fresh, inbound.astype(jnp.float32))
    normed, keyed, (compressed, scale_attn, scale_latent) = inputs_of(hidden)
    latent = bf16(jnp.einsum("rd,mdc->mrc", keyed[:, :LAT], expand_heads, preferred_element_type=jnp.float32))
    latent = latent.reshape(members * rows, -1)
    query_raw = jnp.einsum("rd,mdc->mrc", normed, query_heads, preferred_element_type=jnp.float32)
    attended, query = attend(query_raw.reshape(members * rows, -1), latent, keyed, tables_own, members)
    mixed = hidden + jnp.einsum(
        "mrc,mcd->rd", attended.reshape(members, rows, -1), output_heads, preferred_element_type=jnp.float32
    )
    mixed = jnp.where(is_first, mixed_first, mixed)
    ffn32, scale_ffn = rms_forward(mixed, ffn_gain)
    (ffn_all,) = gather_blocks([bf16(ffn32)], True, 6, 1, [ffn_all])
    stored = run_experts(1, ffn_all, routed, stored, False)

    def latent_back(own):
        grad_latent, grad_latent_gain = rms_backward(
            compressed[:, :LAT], scale_latent, latent_gain, own[:, width : width + LAT]
        )
        grad_compressed = bf16(
            jnp.concatenate([grad_latent, rotate(own[:, width + LAT :], own_cos, -own_sin)], axis=1)
        )
        grad_normed = own[:, :width] + dot_t(grad_compressed, compress_weight)
        grad_hidden_norm, grad_attn_gain = rms_backward(hidden, scale_attn, attn_gain, grad_normed)
        return grad_compressed, grad_hidden_norm, grad_attn_gain, grad_latent_gain

    *grad_units, partial = run_experts_back(1, target_all, routed, stored, ())
    grad_ffn_second = scatter_blocks(partial, rows, True, 7, 1)
    grad_mixed = fresh + rms_backward(mixed, scale_ffn, ffn_gain, grad_ffn_second)[0]
    grad_attended = jnp.einsum(
        "rd,mcd->mrc", bf16(grad_mixed), output_heads, preferred_element_type=jnp.float32
    )
    grad_query, grad_latent_heads, grad_shared_key = attend_back(
        query, latent, keyed, bf16(grad_attended).reshape(members * rows, -1), tables_own, members
    )
    own_second = jnp.concatenate(
        [
            jnp.einsum(
                "mrc,mdc->rd",
                grad_query.reshape(members, rows, -1),
                query_heads,
                preferred_element_type=jnp.float32,
            ),
            jnp.einsum(
                "mrc,mdc->rd",
                grad_latent_heads.reshape(members, rows, -1),
                expand_heads,
                preferred_element_type=jnp.float32,
            ),
            jnp.sum(grad_shared_key.reshape(members, rows, -1), axis=0),
        ],
        axis=1,
    )
    grad_second = bf16(grad_mixed + latent_back(own_second)[1])

    all_inputs = gather_blocks([normed, keyed], True, 8, 0)
    prepared = prepare(0, *all_inputs, ffn_all, tables_all, ())
    grad_second, prepared, all_inputs = lax.optimization_barrier((grad_second, prepared, all_inputs))
    downbound = lax.ppermute(grad_second, SECTION, [(1, 0)]).astype(jnp.float32)

    normed_late, keyed_late, gated_late, _ = lax.optimization_barrier((normed, keyed, stored[1], grad_second))
    normed_all, keyed_all = gather_blocks([normed_late, keyed_late], True, 9, 1, all_inputs)
    prepared = prepare(1, normed_all, keyed_all, ffn_all, tables_all, prepared)
    attended_all, query_all, latent_all, shared_pre, shared_hid = prepared
    attended_all, shared_hid = attended_all[:all_rows], shared_hid[:all_rows]
    at = tiles[1]
    (partial,) = at.call(
        tiled(finish_body),
        "finish",
        [(gated_late, at.source(units)), (stored[3], at.pack_source(half))],
        [expert_out, shared_out],
        [at.result(width)],
        flops=2 * all_rows * width * units,
    )
    result = mixed + scatter_blocks(partial, rows, True, 10, 1)

    upstream = jnp.where(is_first, downbound, fresh)
    (upstream_all,) = gather_blocks([bf16(upstream)], True, 11, 0, [target_all])
    grad_pre, moved, partial = run_experts_back(0, upstream_all, routed, stored, grad_units)
    grad_ffn = jnp.where(is_first, scatter_blocks(partial, rows, True, 12, 0), grad_ffn_second)
    grad_mixed_norm, grad_ffn_gain = rms_backward(mixed, scale_ffn, ffn_gain, grad_ffn)
    grad_mixed = upstream + grad_mixed_norm
    grad_mixed_all = lax.all_gather(bf16(grad_mixed), BOTH, axis=0, tiled=True)
    grad_attended = bf16(dot_t(grad_mixed_all, output_weight))
    grad_query, grad_latent_heads, grad_shared_key = attend_back(
        query_all, latent_all, keyed_all, grad_attended, tables_all
    )
    own = lax.psum_scatter(
        bf16(
            jnp.concatenate(
                [
                    dot_t(own_pack(grad_query), query_weight),
                    dot_t(own_pack(grad_latent_heads), expand_weight),
                    own_pack(grad_shared_key),
                ],
                axis=1,
            )
        ),
        MEMBERS,
        scatter_dimension=0,
        tiled=True,
    ).astype(jnp.float32)
    grad_compressed, grad_hidden_norm, grad_attn_gain, grad_latent_gain = latent_back(own)
    grad_hidden = grad_mixed + grad_hidden_norm

    small = jnp.concatenate([grad_attn_gain, grad_latent_gain, grad_ffn_gain, moved[:all_rows, 0]])
    small = jnp.pad(small, (0, -small.shape[0] % 1024)).reshape(8, -1)
    grad_compressed_all, small_all = gather_blocks([grad_compressed, small], True, 13)
    small_all = small_all.reshape(count, -1)
    gains = jnp.sum(small_all[:, : 2 * width + LAT], axis=0)
    moved_all = small_all[:, 2 * width + LAT : 2 * width + LAT + all_rows].T
    prob = stored[2][:all_rows]
    grad_logits = bf16(moved_all - prob * jnp.sum(moved_all, axis=1, keepdims=True))
    left, right = gated_back(
        shared_pre[0, :all_rows].astype(jnp.float32),
        shared_pre[1, :all_rows].astype(jnp.float32),
        dot_t(upstream_all, shared_out),
    )
    grad_shared_in = lax.dot_general(
        jnp.stack([left, right]), ffn_all, (((1,), (0,)), ((), ())), preferred_element_type=jnp.float32
    )
    ends = jnp.where(is_first, grad_hidden, result)
    return (
        ends[None, None],
        gains[:width][None],
        t_dot(normed_all, grad_query)[None],
        t_dot(normed_all, grad_compressed_all)[None],
        gains[width : width + LAT][None],
        t_dot(keyed_all[:, :LAT], grad_latent_heads)[None],
        t_dot(attended_all, grad_mixed_all)[None],
        gains[width + LAT :][None],
        t_dot(ffn_all, grad_logits)[None],
        jnp.transpose(grad_shared_in, (2, 0, 1))[None],
        t_dot(shared_hid, upstream_all)[None],
        pair_grad(ffn_all, grad_pre)[None, None],
        t_dot(stored[1][:all_rows], upstream_all)[None, None],
    )


def solution(mesh):
    return jax.shard_map(
        body,
        mesh=mesh,
        in_specs=(
            P(SECTION, None, BOTH, None),
            P(None, PACKS, None, None),
            P(SECTION, None, BOTH, None),
            P(SECTION, None),
            P(SECTION, None, MEMBERS),
            P(SECTION, None, None),
            P(SECTION, None),
            P(SECTION, None, MEMBERS),
            P(SECTION, MEMBERS, None),
            P(SECTION, None),
            P(SECTION, None, None),
            P(SECTION, None, None, MEMBERS),
            P(SECTION, MEMBERS, None),
            P(SECTION, BOTH, None, None, None),
            P(SECTION, BOTH, None, None),
        ),
        out_specs=(
            P(SECTION, None, BOTH, None),
            P(SECTION, None),
            P(SECTION, None, MEMBERS),
            P(SECTION, None, None),
            P(SECTION, None),
            P(SECTION, None, MEMBERS),
            P(SECTION, MEMBERS, None),
            P(SECTION, None),
            P(SECTION, None, None),
            P(SECTION, None, None, MEMBERS),
            P(SECTION, MEMBERS, None),
            P(SECTION, BOTH, None, None, None),
            P(SECTION, BOTH, None, None),
        ),
        check_vma=False,
    )
```

```python
import functools

import jax
import jax.numpy as jnp
from jax import lax
from jax.experimental import pallas as pl
from jax.experimental.pallas import tpu as pltpu
from jax.sharding import PartitionSpec as P

NOPE = 128
ROPE = 64
VD = 128
LAT = 512

QK = NOPE + ROPE
KV = NOPE + VD
HALF = ROPE // 2
epsilon = 1e-06
rope_base = 10000.0
masked_score = -1e30
SECTION, PACKS, MEMBERS = "section", "dp", "expert"
BOTH = (PACKS, MEMBERS)
MESH = pl.DeviceIdType.MESH
def dot(left, right):
    return jnp.dot(left, right, preferred_element_type=jnp.float32)


def dot_t(left, right):
    return lax.dot_general(
        left, right, (((1,), (1,)), ((), ())), preferred_element_type=jnp.float32
    )


def t_dot(left, right):
    return lax.dot_general(
        left, right, (((0,), (0,)), ((), ())), preferred_element_type=jnp.float32
    )


def bf16(value):
    return value.astype(jnp.bfloat16)


def rms_forward(inputs, gain_vec):
    norm_scale = lax.rsqrt(jnp.mean(inputs * inputs, axis=-1, keepdims=True) + epsilon)
    return (inputs * norm_scale * gain_vec, norm_scale)


def rms_backward(inputs, norm_scale, gain_vec, upstream):
    weighted = upstream * gain_vec
    grad_gain = jnp.sum(upstream * inputs * norm_scale, axis=0)
    cubed = norm_scale * norm_scale * norm_scale
    grad_inputs = norm_scale * weighted - inputs * cubed * jnp.mean(
        weighted * inputs, axis=-1, keepdims=True
    )
    return (grad_inputs, grad_gain)


def rotate(inputs, cosine, sine):
    half = cosine.shape[-1]
    former = inputs[..., :half]
    latter = inputs[..., half:]
    return jnp.concatenate(
        [former * cosine - latter * sine, latter * cosine + former * sine], axis=-1
    )


def silu_parts(pre_gate):
    sigmoid = jax.nn.sigmoid(pre_gate)
    return (pre_gate * sigmoid, sigmoid * (1.0 + pre_gate * (1.0 - sigmoid)))


def block_layout(block_lengths, rows):
    starts = jnp.cumsum(block_lengths, axis=1) - block_lengths
    index = jnp.arange(rows, dtype=jnp.int32)
    begun = index[None, :, None] >= starts[:, None, :]
    segment = jnp.sum(begun.astype(jnp.int32), axis=2)
    opening = jnp.max(jnp.where(begun, starts[:, None, :], 0), axis=2)
    return segment, index[None, :] - opening


def places(spots):
    member = lax.axis_index(MEMBERS)
    spot = lax.axis_index(PACKS) if spots > 1 else 0
    return spot, member // 2, lax.rem(member, 2)


def to_partner(chip, core):
    return {MEMBERS: chip * 2 + 1 - core}


def to_other(chip, core):
    return {MEMBERS: (1 - chip) * 2 + core}


def when(condition, action):
    if condition is True:
        action()
    else:
        pl.when(condition)(action)


def greet(spots, spot, chip, core):
    barrier = pltpu.get_barrier_semaphore()

    def signal(target):
        pl.semaphore_signal(barrier, inc=1, device_id=target, device_id_type=MESH)

    signal(to_partner(chip, core))
    signal(to_other(chip, core))
    if spots > 1:
        pl.when(spot > 0)(lambda: signal({PACKS: spot - 1}))
        pl.when(spot < spots - 1)(lambda: signal({PACKS: spot + 1}))
        ends = jnp.where(spot > 0, 1, 0) + jnp.where(spot < spots - 1, 1, 0)
        pl.semaphore_wait(barrier, 2 + ends)
    else:
        pl.semaphore_wait(barrier, 2)


def remote(source, target_ref, target, out_sem, in_sem):
    return pltpu.make_async_remote_copy(
        src_ref=source,
        dst_ref=target_ref,
        send_sem=out_sem,
        recv_sem=in_sem,
        device_id=target,
        device_id_type=MESH,
    )


def slot(spot, chip, core):
    return spot * 4 + chip * 2 + core


def gather_kernel(spots, cuts, active, *refs):
    arrays = len(cuts)
    x_refs, o_refs, sems = refs[:arrays], refs[-9 - arrays : -9], refs[-9:]
    own_sem, up_out, up_in, down_out, down_in, over_out, over_in, pair_out, pair_in = sems
    units = [
        (a, pl.ds(part * (x_refs[a].shape[0] // parts), x_refs[a].shape[0] // parts))
        for a, parts in enumerate(cuts)
        for part in range(parts)
    ]

    def run():
        spot, chip, core = places(spots)
        greet(spots, spot, chip, core)

        def piece(unit, index):
            array, cut = units[unit]
            return o_refs[array].at[index, cut]

        def first(unit):
            array, cut = units[unit]
            return x_refs[array].at[cut]

        def up(source, at, unit, reach):
            return remote(
                source, piece(unit, slot(at, chip, core)), {PACKS: spot + 1}, up_out.at[reach, unit], up_in.at[reach, unit]
            )

        def down(source, at, unit, reach):
            return remote(
                source,
                piece(unit, slot(at, chip, core)),
                {PACKS: spot - 1},
                down_out.at[reach, unit],
                down_in.at[reach, unit],
            )

        def over(source, at, unit):
            return remote(
                source, piece(unit, slot(at, chip, core)), to_other(chip, core), over_out.at[at, unit], over_in.at[at, unit]
            )

        def pair(source, at, c, unit):
            return remote(
                source,
                piece(unit, slot(at, c, core)),
                to_partner(chip, core),
                pair_out.at[c, at, unit],
                pair_in.at[c, at, unit],
            )

        mine = slot(spot, chip, core)
        for unit in range(len(units)):
            source = first(unit)
            over(source, spot, unit).start()
            if spots > 1:
                pl.when(spot < spots - 1)(lambda: up(source, spot, unit, 0).start())
                pl.when(spot > 0)(lambda: down(source, spot, unit, 0).start())
            pair(source, spot, chip, unit).start()
        own = [pltpu.make_async_copy(x_refs[a], o_refs[a].at[mine], own_sem.at[a]) for a in range(arrays)]
        for copy in own:
            copy.start()
        for reach in range(1, spots):
            for unit in range(len(units)):

                def below(reach=reach, unit=unit):
                    at = spot - reach
                    source = piece(unit, slot(at, chip, core))
                    up(source, at, unit, reach - 1).wait_recv()
                    pl.when(spot < spots - 1)(lambda: up(source, at, unit, reach).start())
                    over(source, at, unit).start()
                    pair(source, at, chip, unit).start()

                def above(reach=reach, unit=unit):
                    at = spot + reach
                    source = piece(unit, slot(at, chip, core))
                    down(source, at, unit, reach - 1).wait_recv()
                    pl.when(spot > 0)(lambda: down(source, at, unit, reach).start())
                    over(source, at, unit).start()
                    pair(source, at, chip, unit).start()

                pl.when(spot >= reach)(below)
                pl.when(spot + reach < spots)(above)
        for reach in range(spots):
            sides = [(True, spot)]
            if reach > 0:
                sides = [(spot >= reach, spot - reach), (spot + reach < spots, spot + reach)]
            for unit in range(len(units)):
                for there, at in sides:

                    def hand_on(at=at, unit=unit):
                        source = piece(unit, slot(at, 1 - chip, core))
                        over(source, at, unit).wait_recv()
                        pair(source, at, 1 - chip, unit).start()

                    when(there, hand_on)
        for copy in own:
            copy.wait()
        for unit in range(len(units)):
            source = piece(unit, mine)
            for at in range(spots):
                over(source, at, unit).wait_send()
                for c in range(2):
                    pair(source, at, c, unit).wait()
            for reach in range(spots - 1):
                pl.when((spot >= reach) & (spot < spots - 1))(lambda: up(source, spot, unit, reach).wait_send())
                pl.when((spot + reach < spots) & (spot > 0))(lambda: down(source, spot, unit, reach).wait_send())

    if active is None:
        run()
    else:
        pl.when(lax.axis_index(SECTION) == active)(run)


def gather_blocks(values, across, number, active=None, into=None, parts=4):
    axes = BOTH if across else MEMBERS
    if lax.axis_size(MEMBERS) != 4:
        found = [lax.all_gather(value, axes, axis=0, tiled=True) for value in values]
        if into is None:
            return found
        chosen = lax.axis_index(SECTION) == active
        return [jnp.where(chosen, new, old) for new, old in zip(found, into)]
    spots = lax.axis_size(PACKS) if across else 1
    cuts = [parts if value.shape[0] % (16 * parts) == 0 else 1 for value in values]
    units = sum(cuts)
    dma = pltpu.SemaphoreType.DMA
    hops = max(spots - 1, 1)
    shapes = [jax.ShapeDtypeStruct((spots * 4, *value.shape), value.dtype) for value in values]
    held = [] if into is None else [old.reshape(shape.shape) for old, shape in zip(into, shapes)]
    outs = pl.pallas_call(
        functools.partial(gather_kernel, spots, cuts, active),
        out_shape=shapes,
        in_specs=[pl.BlockSpec(memory_space=pltpu.VMEM)] * len(values)
        + [pl.BlockSpec(memory_space=pl.ANY)] * len(held),
        out_specs=[pl.BlockSpec(memory_space=pl.ANY)] * len(values),
        input_output_aliases={len(values) + index: index for index in range(len(held))},
        scratch_shapes=[
            dma((len(values),)),
            dma((hops, units)),
            dma((hops, units)),
            dma((hops, units)),
            dma((hops, units)),
            dma((spots, units)),
            dma((spots, units)),
            dma((2, spots, units)),
            dma((2, spots, units)),
        ],
        compiler_params=pltpu.CompilerParams(collective_id=number, has_side_effects=True),
        name=f"gather{number}",
    )(*values, *held)
    return [out.reshape(-1, out.shape[2]) for out in outs]


def spread_kernel(cuts, active, *refs):
    arrays = len(cuts)
    x_refs, o_refs = refs[:arrays], refs[arrays : 2 * arrays]
    own_sem, over_out, over_in, side_out, side_in, pair_out, pair_in = refs[2 * arrays :]
    units = [
        (a, pl.ds(part * (x_refs[a].shape[0] // parts), x_refs[a].shape[0] // parts))
        for a, parts in enumerate(cuts)
        for part in range(parts)
    ]

    def run():
        member, spot = lax.axis_index(MEMBERS), lax.axis_index(PACKS)
        chip, core, odd = member // 2, lax.rem(member, 2), lax.rem(spot, 2)
        beside = {PACKS: spot + 1 - 2 * odd}
        barrier = pltpu.get_barrier_semaphore()
        for target in (to_partner(chip, core), to_other(chip, core), beside):
            pl.semaphore_signal(barrier, inc=1, device_id=target, device_id_type=MESH)
        pl.semaphore_wait(barrier, 3)

        def piece(unit, c):
            array, cut = units[unit]
            return o_refs[array].at[c * 2 + core, cut]

        def first(unit):
            array, cut = units[unit]
            return x_refs[array].at[cut]

        def over(unit):
            return remote(first(unit), piece(unit, chip), to_other(chip, core), over_out.at[unit], over_in.at[unit])

        def side(unit):
            source = piece(unit, 1 - chip)
            return remote(source, source, beside, side_out.at[unit], side_in.at[unit])

        def pair(source, unit, c, index):
            return remote(
                source, piece(unit, c), to_partner(chip, core), pair_out.at[index, unit], pair_in.at[index, unit]
            )

        for unit in range(len(units)):
            pl.when(odd == unit % 2)(lambda: over(unit).start())
        for unit in range(len(units)):
            pair(first(unit), unit, chip, 0).start()
        own = [
            pltpu.make_async_copy(x_refs[a], o_refs[a].at[member], own_sem.at[a]) for a in range(arrays)
        ]
        for copy in own:
            copy.start()
        for unit in range(len(units)):

            def taken(unit=unit):
                over(unit).wait_recv()
                side(unit).start()
                pair(piece(unit, 1 - chip), unit, 1 - chip, 1).start()

            pl.when(odd == unit % 2)(taken)
        for unit in range(len(units)):

            def handed(unit=unit):
                side(unit).wait_recv()
                pair(piece(unit, 1 - chip), unit, 1 - chip, 1).start()

            pl.when(odd != unit % 2)(handed)
        for copy in own:
            copy.wait()
        for unit in range(len(units)):

            def sent(unit=unit):
                over(unit).wait_send()
                side(unit).wait_send()

            pl.when(odd == unit % 2)(sent)
            pair(first(unit), unit, chip, 0).wait()
            pair(first(unit), unit, 1 - chip, 1).wait()

    pl.when(lax.axis_index(SECTION) == active)(run)


def spread_blocks(values, number, active, parts=8):
    if lax.axis_size(MEMBERS) != 4 or lax.axis_size(PACKS) % 2:
        return gather_blocks(values, False, number, active)
    units = parts * len(values)
    dma = pltpu.SemaphoreType.DMA
    outs = pl.pallas_call(
        functools.partial(spread_kernel, [parts] * len(values), active),
        out_shape=[jax.ShapeDtypeStruct((4, *value.shape), value.dtype) for value in values],
        in_specs=[pl.BlockSpec(memory_space=pltpu.VMEM)] * len(values),
        out_specs=[pl.BlockSpec(memory_space=pl.ANY)] * len(values),
        scratch_shapes=[
            dma((len(values),)),
            dma((units,)),
            dma((units,)),
            dma((units,)),
            dma((units,)),
            dma((2, units)),
            dma((2, units)),
        ],
        compiler_params=pltpu.CompilerParams(collective_id=number, has_side_effects=True),
        name=f"spread{number}",
    )(*values)
    return [out.reshape(-1, out.shape[2]) for out in outs]


def add_into(target, sources, rows, step=16):
    def some(index, carry):
        at = pl.ds(pl.multiple_of(index * step, step), step)
        total = sources[0][at, :].astype(jnp.float32)
        for source in sources[1:]:
            total = total + source[at, :].astype(jnp.float32)
        target[at, :] = total.astype(target.dtype)
        return carry

    lax.fori_loop(0, rows // step, some, 0)


def scatter_kernel(
    spots,
    parts,
    active,
    x_ref,
    o_ref,
    own_buf,
    pair_buf,
    over_src,
    over_buf,
    line_src,
    up_buf,
    down_buf,
    own_in,
    pair_out,
    pair_in,
    over_out,
    over_in,
    line_out,
    up_in,
    down_in,
):
    rows = x_ref.shape[1] // parts
    cut = lambda part: pl.ds(part * rows, rows)

    def run():
        spot, chip, core = places(spots)
        greet(spots, spot, chip, core)

        def order(step):
            if step == spots - 1:
                return spot
            fall = spots - 1 - step
            fall = jnp.where(fall <= spot, fall - 1, fall)
            rise = jnp.where(step >= spot, step + 1, step)
            return jnp.where(2 * spot < spots - 1, fall, rise)

        def pair(at, c, part):
            return remote(
                x_ref.at[slot(at, c, 1 - core), cut(part)],
                pair_buf.at[at, c, cut(part)],
                to_partner(chip, core),
                pair_out.at[at, c, part],
                pair_in.at[at, c, part],
            )

        def over(at, part):
            return remote(
                over_src.at[at, cut(part)],
                over_buf.at[at, cut(part)],
                to_other(chip, core),
                over_out.at[at, part],
                over_in.at[at, part],
            )

        def up(at, part):
            return remote(
                line_src.at[at, cut(part)],
                up_buf.at[at, cut(part)],
                {PACKS: spot + 1},
                line_out.at[at, part],
                up_in.at[at, part],
            )

        def down(at, part):
            return remote(
                line_src.at[at, cut(part)],
                down_buf.at[at, cut(part)],
                {PACKS: spot - 1},
                line_out.at[at, part],
                down_in.at[at, part],
            )

        def own(at, c):
            return pltpu.make_async_copy(x_ref.at[slot(at, c, core)], own_buf.at[at, c], own_in.at[at, c])

        for c in (1 - chip, chip):
            for step in range(spots):
                own(order(step), c).start()
                for part in range(parts):
                    pair(order(step), c, part).start()
        for step in range(spots):
            at = order(step)
            own(at, 1 - chip).wait()
            for part in range(parts):
                pair(at, 1 - chip, part).wait_recv()
                add_into(
                    over_src.at[at, cut(part)],
                    [own_buf.at[at, 1 - chip, cut(part)], pair_buf.at[at, 1 - chip, cut(part)]],
                    rows,
                )
                over(at, part).start()
        for step in range(spots):
            at = order(step)
            own(at, chip).wait()
            for part in range(parts):
                pair(at, chip, part).wait_recv()
                over(at, part).wait_recv()
                base = [
                    own_buf.at[at, chip, cut(part)],
                    pair_buf.at[at, chip, cut(part)],
                    over_buf.at[at, cut(part)],
                ]
                ups, downs = up_buf.at[at, cut(part)], down_buf.at[at, cut(part)]
                if step < spots - 1:
                    target = line_src.at[at, cut(part)]

                    def rising(first):
                        if not first:
                            up(at, part).wait_recv()
                        add_into(target, base if first else base + [ups], rows)
                        up(at, part).start()

                    def falling(first):
                        if not first:
                            down(at, part).wait_recv()
                        add_into(target, base if first else base + [downs], rows)
                        down(at, part).start()

                    pl.when((at > spot) & (spot == 0))(lambda: rising(True))
                    pl.when((at > spot) & (spot > 0))(lambda: rising(False))
                    pl.when((at < spot) & (spot == spots - 1))(lambda: falling(True))
                    pl.when((at < spot) & (spot < spots - 1))(lambda: falling(False))
                elif spots == 1:
                    add_into(o_ref.at[cut(part)], base, rows)
                else:

                    def finish(ends):
                        if ends < 1:
                            up(at, part).wait_recv()
                        if ends > -1:
                            down(at, part).wait_recv()
                        extra = ([ups] if ends < 1 else []) + ([downs] if ends > -1 else [])
                        add_into(o_ref.at[cut(part)], base + extra, rows)

                    pl.when(spot == 0)(lambda: finish(1))
                    pl.when(spot == spots - 1)(lambda: finish(-1))
                    pl.when((spot > 0) & (spot < spots - 1))(lambda: finish(0))
        for part in range(parts):
            for step in range(spots):
                at = order(step)
                pair(at, 0, part).wait_send()
                pair(at, 1, part).wait_send()
                over(at, part).wait_send()
                if step < spots - 1:
                    up(at, part).wait_send()

    if active is None:
        run()
    else:
        pl.when(lax.axis_index(SECTION) == active)(run)


def scatter_blocks(partial, rows, across, number, active=None, parts=4):
    if lax.axis_size(MEMBERS) != 4:
        axes = BOTH if across else MEMBERS
        taken = partial[: rows * lax.axis_size(axes)]
        return lax.psum_scatter(taken, axes, scatter_dimension=0, tiled=True).astype(jnp.float32)
    spots = lax.axis_size(PACKS) if across else 1
    width = partial.shape[1]
    dma = pltpu.SemaphoreType.DMA
    hold = lambda *lead: pltpu.VMEM((*lead, rows, width), partial.dtype)
    return pl.pallas_call(
        functools.partial(scatter_kernel, spots, parts, active),
        out_shape=jax.ShapeDtypeStruct((rows, width), jnp.float32),
        in_specs=[pl.BlockSpec(memory_space=pl.ANY)],
        out_specs=pl.BlockSpec(memory_space=pltpu.VMEM),
        scratch_shapes=[
            hold(spots, 2),
            hold(spots, 2),
            hold(spots),
            hold(spots),
            hold(spots),
            hold(spots),
            hold(spots),
            dma((spots, 2)),
            dma((spots, 2, parts)),
            dma((spots, 2, parts)),
            dma((spots, parts)),
            dma((spots, parts)),
            dma((spots, parts)),
            dma((spots, parts)),
            dma((spots, parts)),
        ],
        compiler_params=pltpu.CompilerParams(collective_id=number, has_side_effects=True),
        name=f"scatter{number}",
    )(partial.reshape(-1, rows, width))


def allowed_pairs(seg_col, seg_row):
    rows = seg_col.shape[0]
    later = lax.broadcasted_iota(jnp.int32, (rows, rows), 0)
    earlier = lax.broadcasted_iota(jnp.int32, (rows, rows), 1)
    return (seg_col == seg_row) & (earlier <= later)


def attend_kernel(heads, q_ref, lat_ref, key_ref, cos_ref, sin_ref, col_ref, row_ref, out_ref, rot_ref):
    factor = QK**-0.5
    allowed = allowed_pairs(col_ref[...], row_ref[0])
    cosine, sine = cos_ref[...], sin_ref[...]
    shared = key_ref[:, LAT:]
    for head in range(heads):
        raw = q_ref[:, head * QK : (head + 1) * QK]
        query = bf16(
            jnp.concatenate([raw[:, :NOPE], rotate(raw[:, NOPE:], cosine, sine)], axis=1)
        )
        rot_ref[:, head * QK : (head + 1) * QK] = query
        key = jnp.concatenate([lat_ref[:, head * KV : head * KV + NOPE], shared], axis=1)
        value = lat_ref[:, head * KV + NOPE : (head + 1) * KV]
        scores = jnp.where(allowed, dot_t(query, key) * factor, masked_score)
        top = jnp.max(scores, axis=1, keepdims=True)
        powers = jnp.exp(scores - top)
        probs = powers / jnp.sum(powers, axis=1, keepdims=True)
        out_ref[:, head * VD : (head + 1) * VD] = bf16(dot(bf16(probs), value))


def attend(query_raw, latent, keyed, tables, groups=1):
    cosine, sine, seg_col, seg_row = tables
    count, _, rows = seg_row.shape
    heads = query_raw.shape[1] // QK
    block = lambda width: pl.BlockSpec((rows, width), lambda i: (i, 0))
    same = lambda width: pl.BlockSpec((rows, width), lambda i: (0, 0) if groups > 1 else (i, 0))
    count = count * groups
    return pl.pallas_call(
        functools.partial(attend_kernel, heads),
        grid=(count,),
        in_specs=[
            block(heads * QK),
            block(heads * KV),
            same(LAT + ROPE),
            same(HALF),
            same(HALF),
            same(1),
            pl.BlockSpec((1, 1, rows), lambda i: (0, 0, 0) if groups > 1 else (i, 0, 0)),
        ],
        out_specs=[block(heads * VD), block(heads * QK)],
        out_shape=[
            jax.ShapeDtypeStruct((count * rows, heads * VD), jnp.bfloat16),
            jax.ShapeDtypeStruct((count * rows, heads * QK), jnp.bfloat16),
        ],
        name="attend",
        cost_estimate=pl.CostEstimate(
            flops=2 * count * heads * rows * rows * (QK + VD),
            bytes_accessed=count * rows * heads * (QK * 6 + KV * 2 + VD * 2),
            transcendentals=count * heads * rows * rows,
        ),
    )(query_raw, latent, keyed, cosine, sine, seg_col, seg_row)


def attend_back_kernel(
    heads, q_ref, lat_ref, key_ref, grad_ref, cos_ref, sin_ref, col_ref, row_ref, dq_ref, dlat_ref, dkey_ref
):
    factor = QK**-0.5
    allowed = allowed_pairs(col_ref[...], row_ref[0])
    cosine, sine = cos_ref[...], sin_ref[...]
    shared = key_ref[:, LAT:]
    total = None
    for head in range(heads):
        query = q_ref[:, head * QK : (head + 1) * QK]
        key = jnp.concatenate([lat_ref[:, head * KV : head * KV + NOPE], shared], axis=1)
        value = lat_ref[:, head * KV + NOPE : (head + 1) * KV]
        grad = grad_ref[:, head * VD : (head + 1) * VD]
        scores = jnp.where(allowed, dot_t(query, key) * factor, masked_score)
        top = jnp.max(scores, axis=1, keepdims=True)
        powers = jnp.exp(scores - top)
        probs = powers / jnp.sum(powers, axis=1, keepdims=True)
        grad_value = t_dot(bf16(probs), grad)
        grad_probs = dot_t(grad, value)
        centre = jnp.sum(probs * grad_probs, axis=1, keepdims=True)
        grad_scores = bf16(probs * (grad_probs - centre) * factor)
        grad_query = dot(grad_scores, key)
        grad_key = t_dot(grad_scores, query)
        dq_ref[:, head * QK : (head + 1) * QK] = bf16(
            jnp.concatenate(
                [grad_query[:, :NOPE], rotate(grad_query[:, NOPE:], cosine, -sine)], axis=1
            )
        )
        dlat_ref[:, head * KV : head * KV + NOPE] = bf16(grad_key[:, :NOPE])
        dlat_ref[:, head * KV + NOPE : (head + 1) * KV] = bf16(grad_value)
        part = grad_key[:, NOPE:]
        total = part if total is None else total + part
    dkey_ref[...] = total


def attend_back(query, latent, keyed, grad, tables, groups=1):
    cosine, sine, seg_col, seg_row = tables
    count, _, rows = seg_row.shape
    heads = query.shape[1] // QK
    block = lambda width: pl.BlockSpec((rows, width), lambda i: (i, 0))
    same = lambda width: pl.BlockSpec((rows, width), lambda i: (0, 0) if groups > 1 else (i, 0))
    count = count * groups
    return pl.pallas_call(
        functools.partial(attend_back_kernel, heads),
        grid=(count,),
        in_specs=[
            block(heads * QK),
            block(heads * KV),
            same(LAT + ROPE),
            block(heads * VD),
            same(HALF),
            same(HALF),
            same(1),
            pl.BlockSpec((1, 1, rows), lambda i: (0, 0, 0) if groups > 1 else (i, 0, 0)),
        ],
        out_specs=[block(heads * QK), block(heads * KV), block(ROPE)],
        out_shape=[
            jax.ShapeDtypeStruct((count * rows, heads * QK), jnp.bfloat16),
            jax.ShapeDtypeStruct((count * rows, heads * KV), jnp.bfloat16),
            jax.ShapeDtypeStruct((count * rows, ROPE), jnp.float32),
        ],
        name="attend_back",
        cost_estimate=pl.CostEstimate(
            flops=2 * count * heads * rows * rows * (3 * QK + 2 * VD),
            bytes_accessed=count * rows * heads * (QK * 4 + KV * 4 + VD * 2),
            transcendentals=count * heads * rows * rows,
        ),
    )(query, latent, keyed, grad, cosine, sine, seg_col, seg_row)


def gated_hidden(gate, up):
    return silu_parts(gate)[0] * up


def gated_back(gate, up, grad_hidden):
    act, slope = silu_parts(gate)
    return bf16(grad_hidden * up * slope), bf16(grad_hidden * act)


def load(sources, targets, sems):
    copies = [
        pltpu.make_async_copy(source, target, sems.at[index])
        for index, (source, target) in enumerate(zip(sources, targets))
    ]
    for copy in copies:
        copy.start()
    for copy in copies:
        copy.wait()


class Tiles:
    def __init__(self, rows, pack_rows, pack, active):
        self.rows, self.pack_rows = rows, pack_rows
        self.tile = min(256, pack_rows)
        self.count = rows // self.tile
        inner = pack_rows // self.tile
        runs = (lax.axis_index(SECTION) == active).astype(jnp.int32)
        self.control = jnp.stack([pack * inner, (pack + 1) * inner, runs]).astype(jnp.int32)

    def source(self, width):
        return pl.BlockSpec((self.tile, width), lambda i, control: (i * control[2], 0))

    def small(self, array):
        return pl.BlockSpec(array.shape, lambda i, control: (0,) * array.ndim)

    def pack_source(self, width):
        def index(i, control):
            return (0, jnp.clip(i - control[0], 0, control[1] - control[0] - 1), 0)

        return pl.BlockSpec((2, self.tile, width), index)

    def result(self, width, dtype=jnp.bfloat16):
        def index(i, control):
            return (jnp.where(control[2] == 1, i, self.count), 0)

        shape = jax.ShapeDtypeStruct((self.rows + self.tile, width), dtype)
        return shape, pl.BlockSpec((self.tile, width), index)

    def pair_result(self, width):
        def index(i, control):
            return (0, jnp.where(control[2] == 1, i, self.count), 0)

        shape = jax.ShapeDtypeStruct((2, self.rows + self.tile, width), jnp.bfloat16)
        return shape, pl.BlockSpec((2, self.tile, width), index)

    def pack_result(self, width):
        def index(i, control):
            spot = jnp.clip(i - control[0], 0, control[1] - control[0] - 1)
            return (0, jnp.where(control[2] == 1, spot, control[1] - control[0]), 0)

        shape = jax.ShapeDtypeStruct((2, self.pack_rows + self.tile, width), jnp.bfloat16)
        return shape, pl.BlockSpec((2, self.tile, width), index)

    def call(self, kernel, name, sources, weights, results, into=(), scratch=(), flops=0):
        arrays, specs = zip(*sources)
        shapes, out_specs = zip(*results)
        anywhere = pl.BlockSpec(memory_space=pl.ANY)
        first = 1 + len(arrays) + len(weights)
        return pl.pallas_call(
            functools.partial(kernel, len(arrays), len(weights), len(into), len(results)),
            grid_spec=pltpu.PrefetchScalarGridSpec(
                num_scalar_prefetch=1,
                grid=(self.count,),
                in_specs=[*specs, *([anywhere] * (len(weights) + len(into)))],
                out_specs=list(out_specs),
                scratch_shapes=[
                    *[pltpu.VMEM(weight.shape, weight.dtype) for weight in weights],
                    pltpu.SemaphoreType.DMA((len(weights),)),
                    *scratch,
                ],
            ),
            out_shape=list(shapes),
            input_output_aliases={first + index: index for index in range(len(into))},
            name=name,
            cost_estimate=pl.CostEstimate(flops=flops, bytes_accessed=self.rows * 16384, transcendentals=0),
        )(self.control, *arrays, *weights, *into)


def tiled(body):
    def kernel(n_sources, n_weights, n_into, n_results, control, *refs):
        sources, refs = refs[:n_sources], refs[n_sources:]
        stored, refs = refs[:n_weights], refs[n_weights + n_into :]
        results, refs = refs[:n_results], refs[n_results:]
        weights, sems, scratch = refs[:n_weights], refs[n_weights], refs[n_weights + 1 :]

        def run():
            pl.when(pl.program_id(0) == 0)(lambda: load(stored, weights, sems))
            body(inside_pack(control), [sources[0][...], *sources[1:]], weights, results, scratch)

        pl.when(control[2] == 1)(run)

    return kernel


def inside_pack(control):
    tile = pl.program_id(0)
    return (tile >= control[0]) & (tile < control[1])


def shared_units(x, shared_in):
    half = shared_in.shape[0] // 2
    return dot_t(x, shared_in[:half]), dot_t(x, shared_in[half:])


def experts_body(inside, sources, weights, results, scratch):
    x, own_ref, routed_ref = sources
    in_ref, shared_in_ref = weights[:2]
    pre_ref, gated_ref, prob_ref, shared_pre_ref = results[:4]
    units = gated_ref.shape[1]
    pre = dot(x, in_ref[...])
    logits = pre[:, 2 * units : 2 * units + own_ref.shape[1]]
    powers = jnp.exp(logits - jnp.max(logits, axis=1, keepdims=True))
    prob = powers / jnp.sum(powers, axis=1, keepdims=True)
    prob_ref[...] = prob
    gate = jnp.sum(prob * own_ref[...], axis=1, keepdims=True) * routed_ref[...]
    pre_ref[...] = bf16(pre[:, : 2 * units])
    gated = bf16(gate * gated_hidden(pre[:, :units], pre[:, units : 2 * units]))
    gated_ref[...] = gated

    def shared():
        left, right = shared_units(x, shared_in_ref)
        shared_pre_ref[0] = bf16(left)
        shared_pre_ref[1] = bf16(right)
        return left, right

    if len(weights) == 2:
        pl.when(inside)(lambda: shared() and None)
        return
    out_ref, shared_out_ref = weights[2:]
    partial_ref = results[4]

    def with_shared():
        hidden = bf16(gated_hidden(*shared()))
        partial_ref[...] = bf16(dot(gated, out_ref[...]) + dot(hidden, shared_out_ref[...]))

    def without():
        partial_ref[...] = bf16(dot(gated, out_ref[...]))

    pl.when(inside)(with_shared)
    pl.when(jnp.logical_not(inside))(without)


def finish_body(inside, sources, weights, results, scratch):
    gated, shared_pre_ref = sources
    out_ref, shared_out_ref = weights
    (partial_ref,) = results

    def with_shared():
        hidden = bf16(gated_hidden(shared_pre_ref[0].astype(jnp.float32), shared_pre_ref[1].astype(jnp.float32)))
        partial_ref[...] = bf16(dot(gated, out_ref[...]) + dot(hidden, shared_out_ref[...]))

    def without():
        partial_ref[...] = bf16(dot(gated, out_ref[...]))

    pl.when(inside)(with_shared)
    pl.when(jnp.logical_not(inside))(without)


def experts_back_body(inside, sources, weights, results, scratch):
    grad, own_ref, pre_ref, prob_ref, routed_ref, shared_pre_ref = sources
    in_ref, shared_in_ref, out_ref, shared_out_ref = weights
    grad_pre_ref, moved_ref, partial_ref = results
    (joined_ref,) = scratch
    units = out_ref.shape[0]
    prob = prob_ref[...]
    own_prob = jnp.sum(prob * own_ref[...], axis=1, keepdims=True) * routed_ref[...]
    gate, up = pre_ref[:, :units].astype(jnp.float32), pre_ref[:, units:].astype(jnp.float32)
    grad_units = dot_t(grad, out_ref[...])
    act, slope = silu_parts(gate)
    moved = own_prob * jnp.sum(grad_units * act * up, axis=1, keepdims=True)
    moved_ref[...] = moved
    scaled = own_prob * grad_units
    joined_ref[:, :units] = bf16(scaled * up * slope)
    joined_ref[:, units : 2 * units] = bf16(scaled * act)
    joined_ref[:, 2 * units :] = jnp.zeros_like(joined_ref[:, 2 * units :])
    joined_ref[:, 2 * units : 2 * units + own_ref.shape[1]] = bf16(moved * (own_ref[...] - prob))
    grad_pre_ref[...] = joined_ref[:, : 2 * units]
    base = dot_t(joined_ref[...], in_ref[...])
    half = shared_out_ref.shape[0]

    def with_shared():
        left, right = gated_back(
            shared_pre_ref[0].astype(jnp.float32),
            shared_pre_ref[1].astype(jnp.float32),
            dot_t(grad, shared_out_ref[...]),
        )
        partial_ref[...] = bf16(base + dot(left, shared_in_ref[:half]) + dot(right, shared_in_ref[half:]))

    def without():
        partial_ref[...] = bf16(base)

    pl.when(inside)(with_shared)
    pl.when(jnp.logical_not(inside))(without)


def shared_body(inside, sources, weights, results, scratch):
    pre_ref, hid_ref = results
    left, right = shared_units(sources[0], weights[0])
    pre_ref[0] = bf16(left)
    pre_ref[1] = bf16(right)
    hid_ref[...] = bf16(gated_hidden(left, right))


def heads_body(block, inside, sources, weights, results, scratch):
    x, key_ref, cos_ref, sin_ref, col_ref, row_ref = sources
    query_w_ref, expand_ref = weights
    out_ref, rot_ref, lat_ref = results
    (q_ref,) = scratch
    heads = q_ref.shape[1] // QK
    q_ref[...] = dot(x, query_w_ref[...])
    lat_ref[...] = bf16(dot(key_ref[:, :LAT], expand_ref[...]))
    for start in range(0, x.shape[0], block):
        at = pl.ds(start, block)
        attend_kernel(
            heads,
            q_ref.at[at],
            lat_ref.at[at],
            key_ref.at[at],
            cos_ref.at[at],
            sin_ref.at[at],
            col_ref.at[at],
            row_ref.at[pl.ds(start // block, 1)],
            out_ref.at[at],
            rot_ref.at[at],
        )


def pair_grad_kernel(x_ref, grad_ref, out_ref):
    units = out_ref.shape[2]
    x = x_ref[...]
    out_ref[:, 0, :] = t_dot(x, grad_ref[:, :units])
    out_ref[:, 1, :] = t_dot(x, grad_ref[:, units:])


def pair_grad(x, grad):
    rows, width = x.shape
    units = grad.shape[1] // 2
    if rows > 4096:
        return t_dot(x, grad[:rows]).reshape(width, 2, units)
    tile = 256
    return pl.pallas_call(
        pair_grad_kernel,
        grid=(width // tile,),
        in_specs=[
            pl.BlockSpec((rows, tile), lambda i: (0, i)),
            pl.BlockSpec((rows, 2 * units), lambda i: (0, 0), pipeline_mode=pl.Buffered(1)),
        ],
        out_specs=pl.BlockSpec((tile, 2, units), lambda i: (i, 0, 0)),
        out_shape=jax.ShapeDtypeStruct((width, 2, units), jnp.float32),
        name="pair_grad",
        cost_estimate=pl.CostEstimate(
            flops=4 * rows * width * units, bytes_accessed=rows * (width + 2 * units) * 2 + width * units * 8, transcendentals=0
        ),
    )(x, grad)


def join_kernel(in_ref, router_ref, out_ref):
    units, routes_width = in_ref.shape[2], router_ref.shape[1]
    both = in_ref[...].astype(jnp.float32)
    out_ref[:, :units] = bf16(both[:, 0])
    out_ref[:, units : 2 * units] = bf16(both[:, 1])
    out_ref[:, 2 * units :] = jnp.zeros_like(out_ref[:, 2 * units :])
    out_ref[:, 2 * units : 2 * units + routes_width] = router_ref[...]


def join(expert_in, router):
    width, _, units = expert_in.shape
    total = 2 * units + router.shape[1] + -router.shape[1] % 128
    tile = 256
    return pl.pallas_call(
        join_kernel,
        grid=(width // tile,),
        in_specs=[
            pl.BlockSpec((tile, 2, units), lambda i: (i, 0, 0)),
            pl.BlockSpec((tile, router.shape[1]), lambda i: (i, 0)),
        ],
        out_specs=pl.BlockSpec((tile, total), lambda i: (i, 0)),
        out_shape=jax.ShapeDtypeStruct((width, total), expert_in.dtype),
        name="join",
    )(expert_in, router)


def blank(shape, dtype):
    return pl.pallas_call(
        lambda out_ref: None,
        out_shape=jax.ShapeDtypeStruct(shape, dtype),
        out_specs=pl.BlockSpec(memory_space=pl.ANY),
        compiler_params=pltpu.CompilerParams(has_side_effects=True),
        name="blank",
    )()


def arrival_order(spots):
    tiles = [(rank + 1.1 * over, rank, over) for rank in range(spots) for over in (0, 1)]
    return [(rank, over == 1) for _, rank, over in sorted(tiles)]


def ranked_spots(spots, spot):
    ranks = []
    for rank in range(spots):
        value = 0
        for own in range(spots):
            nearest = sorted(range(spots), key=lambda other: (abs(other - own), other))
            value = value + jnp.where(spot == own, nearest[rank], 0)
        ranks.append(value)
    return ranks


def pick(index, values):
    total = 0
    for position, value in enumerate(values):
        total = total + jnp.where(index == position, value, 0)
    return total


def fused_kernel(spots, parts, active, body, pack_kinds, n_weights, n_into, *refs):
    source_kinds, result_kinds = pack_kinds
    n_sources, n_results = len(source_kinds), len(result_kinds)
    x_ref, small_ref, refs = refs[0], refs[1], refs[2:]
    sources, refs = refs[:n_sources], refs[n_sources:]
    stored, refs = refs[:n_weights], refs[n_weights + n_into :]
    o_ref, refs = refs[0], refs[1:]
    results, refs = refs[:n_results], refs[n_results:]
    x_tile, refs = refs[0], refs[1:]
    source_tiles, refs = refs[:n_sources], refs[n_sources:]
    result_tiles, refs = refs[:n_results], refs[n_results:]
    weights, refs = refs[:n_weights], refs[n_weights:]
    sems, scratch = refs[:12], refs[12:]
    own_sem, weight_sem, tile_sem, out_sem = sems[:4]
    up_out, up_in, down_out, down_in, over_out, over_in, pair_out, pair_in = sems[4:]
    block = x_ref.shape[0]
    rows = block // parts
    tile = 2 * block

    def run():
        loads = [
            pltpu.make_async_copy(source, target, weight_sem.at[index])
            for index, (source, target) in enumerate(zip(stored, weights))
        ]
        for copy in loads:
            copy.start()
        spot, chip, core = places(spots)
        greet(spots, spot, chip, core)
        piece = lambda index, part: o_ref.at[index, pl.ds(part * rows, rows)]
        first = lambda part: x_ref.at[pl.ds(part * rows, rows)]

        def up(source, at, part, reach):
            return remote(
                source, piece(slot(at, chip, core), part), {PACKS: spot + 1}, up_out.at[reach, part], up_in.at[reach, part]
            )

        def down(source, at, part, reach):
            return remote(
                source,
                piece(slot(at, chip, core), part),
                {PACKS: spot - 1},
                down_out.at[reach, part],
                down_in.at[reach, part],
            )

        def over(source, at, part):
            return remote(
                source, piece(slot(at, chip, core), part), to_other(chip, core), over_out.at[at, part], over_in.at[at, part]
            )

        def pair(source, at, c, part):
            return remote(
                source,
                piece(slot(at, c, core), part),
                to_partner(chip, core),
                pair_out.at[c, at, part],
                pair_in.at[c, at, part],
            )

        mine = slot(spot, chip, core)
        for part in range(parts):
            source = first(part)
            pair(source, spot, chip, part).start()
            over(source, spot, part).start()
            pl.when(spot < spots - 1)(lambda: up(source, spot, part, 0).start())
            pl.when(spot > 0)(lambda: down(source, spot, part, 0).start())
        own = pltpu.make_async_copy(x_ref, o_ref.at[mine], own_sem.at[0])
        own.start()
        own.wait()
        ranks = ranked_spots(spots, spot)
        order = arrival_order(spots)

        def arrive(rank, across):
            at = ranks[rank]
            if across:
                for part in range(parts):
                    source = piece(slot(at, 1 - chip, core), part)
                    over(source, at, part).wait_recv()
                    pair(source, at, 1 - chip, part).start()
                for part in range(parts):
                    pair(first(part), at, 1 - chip, part).wait_recv()
                return
            if rank > 0:
                for reach in range(1, spots):
                    for part in range(parts):

                        def below(reach=reach, part=part):
                            source = piece(slot(at, chip, core), part)
                            up(source, at, part, reach - 1).wait_recv()
                            pl.when(spot < spots - 1)(lambda: up(source, at, part, reach).start())
                            over(source, at, part).start()
                            pair(source, at, chip, part).start()

                        def above(reach=reach, part=part):
                            source = piece(slot(at, chip, core), part)
                            down(source, at, part, reach - 1).wait_recv()
                            pl.when(spot > 0)(lambda: down(source, at, part, reach).start())
                            over(source, at, part).start()
                            pair(source, at, chip, part).start()

                        pl.when(spot - at == reach)(below)
                        pl.when(at - spot == reach)(above)
            for part in range(parts):
                pair(first(part), at, chip, part).wait_recv()

        def window(ref, kind, at, c):
            if kind:
                return ref.at[:, pl.ds(pl.multiple_of(c * tile, tile), tile)]
            return ref.at[pl.ds(pl.multiple_of((at * 2 + c) * tile, tile), tile)]

        def outward(index, which, at, c):
            return pltpu.make_async_copy(
                result_tiles[index].at[which], window(results[index], result_kinds[index], at, c), out_sem.at[which, index]
            )

        def step(number, carry):
            for position, (rank, across) in enumerate(order):
                pl.when(number == position)(functools.partial(arrive, rank, across))
            at = pick(number, [ranks[rank] for rank, _ in order])
            c = pick(number, [1 - chip if across else chip for _, across in order])
            inside = at == spot
            inputs = [pltpu.make_async_copy(o_ref.at[pl.ds(slot(at, c, 0), 2)], x_tile, tile_sem.at[0])]
            for index, kind in enumerate(source_kinds):
                if not kind:
                    inputs.append(
                        pltpu.make_async_copy(
                            window(sources[index], kind, at, c), source_tiles[index], tile_sem.at[1 + index]
                        )
                    )
            for copy in inputs:
                copy.start()
            for index, kind in enumerate(source_kinds):
                if kind:

                    def fetch(index=index, kind=kind):
                        copy = pltpu.make_async_copy(
                            window(sources[index], kind, at, c), source_tiles[index], tile_sem.at[1 + index]
                        )
                        copy.start()
                        copy.wait()

                    pl.when(inside)(fetch)

            @pl.when(number == 0)
            def _():
                for copy in loads:
                    copy.wait()

            which = lax.rem(number, 2)

            @pl.when(number >= 2)
            def _():
                for index, kind in enumerate(result_kinds):
                    if not kind:
                        outward(index, which, at, c).wait()

            for copy in inputs:
                copy.wait()
            body(
                inside,
                [x_tile[...].reshape(tile, x_tile.shape[2]), small_ref, *source_tiles],
                weights,
                [target.at[which] for target in result_tiles],
                scratch,
            )
            for index, kind in enumerate(result_kinds):
                if kind:

                    def put(index=index):
                        copy = outward(index, which, at, c)
                        copy.start()
                        copy.wait()

                    pl.when(inside)(put)
                else:
                    outward(index, which, at, c).start()
            return carry

        lax.fori_loop(0, 2 * spots, step, 0)
        for which in range(2):
            for index, kind in enumerate(result_kinds):
                if not kind:
                    outward(index, which, spot, chip).wait()
        for part in range(parts):
            for at in range(spots):
                over(first(part), at, part).wait_send()
                for c in range(2):
                    pair(first(part), at, c, part).wait_send()
            for reach in range(spots - 1):
                pl.when((spot >= reach) & (spot < spots - 1))(lambda: up(first(part), spot, part, reach).wait_send())
                pl.when((spot + reach < spots) & (spot > 0))(lambda: down(first(part), spot, part, reach).wait_send())

    pl.when(lax.axis_index(SECTION) == active)(run)


def fused_call(tiles, rows_in, number, active, body, small, sources, weights, results, gathered, into, scratch=(), parts=4):
    spots = lax.axis_size(PACKS)
    block, width = rows_in.shape
    tile = 2 * block
    dma = pltpu.SemaphoreType.DMA
    hops = max(spots - 1, 1)
    anywhere = pl.BlockSpec(memory_space=pl.ANY)
    inside = pl.BlockSpec(memory_space=pltpu.VMEM)
    shapes = [jax.ShapeDtypeStruct((spots * 4, block, width), rows_in.dtype), *(shape for shape, _ in results)]
    held = [gathered.reshape(shapes[0].shape), *into]
    first = 2 + len(sources) + len(weights)

    def hold(array, kind, *lead):
        shape = (2, tile, array.shape[2]) if kind else (tile, array.shape[1])
        return pltpu.VMEM((*lead, *shape), array.dtype)

    outs = pl.pallas_call(
        functools.partial(
            fused_kernel,
            spots,
            parts,
            active,
            body,
            ([kind for _, kind in sources], [kind for _, kind in results]),
            len(weights),
            len(held),
        ),
        out_shape=shapes,
        in_specs=[inside, inside, *([anywhere] * (len(sources) + len(weights) + len(held)))],
        out_specs=[anywhere] * len(shapes),
        input_output_aliases={first + index: index for index in range(len(held))},
        scratch_shapes=[
            pltpu.VMEM((2, block, width), rows_in.dtype),
            *(hold(array, kind) for array, kind in sources),
            *(hold(shape, kind, 2) for shape, kind in results),
            *(pltpu.VMEM(weight.shape, weight.dtype) for weight in weights),
            dma((1,)),
            dma((len(weights),)),
            dma((1 + len(sources),)),
            dma((2, len(results))),
            dma((hops, parts)),
            dma((hops, parts)),
            dma((hops, parts)),
            dma((hops, parts)),
            dma((spots, parts)),
            dma((spots, parts)),
            dma((2, spots, parts)),
            dma((2, spots, parts)),
            *scratch,
        ],
        compiler_params=pltpu.CompilerParams(collective_id=number, has_side_effects=True),
        name=f"fused{number}",
    )(rows_in, small, *(array for array, _ in sources), *weights, *held)
    return outs[0].reshape(-1, width), list(outs[1:])


def body(
    boundary,
    lengths,
    routes,
    attn_gain,
    query_weight,
    compress_weight,
    latent_gain,
    expand_weight,
    output_weight,
    ffn_gain,
    router_weight,
    shared_in,
    shared_out,
    expert_in,
    expert_out,
):
    attn_gain, latent_gain, ffn_gain = attn_gain[0], latent_gain[0], ffn_gain[0]
    query_weight, compress_weight = query_weight[0], compress_weight[0]
    expand_weight, output_weight = expand_weight[0], output_weight[0]
    router_weight, shared_out, expert_out = router_weight[0], shared_out[0], expert_out[0, 0]
    width = boundary.shape[3]
    rows = boundary.shape[2]
    half = shared_out.shape[0]
    units = expert_out.shape[0]
    experts_count = router_weight.shape[1]
    shared_in_t = jnp.transpose(shared_in[0], (1, 2, 0)).reshape(2 * half, width)
    joined_in = join(expert_in[0, 0], router_weight)

    packs, members = lax.axis_size(PACKS), lax.axis_size(MEMBERS)
    count = packs * members
    pack, member = lax.axis_index(PACKS), lax.axis_index(MEMBERS)
    me = pack * members + member
    is_first = lax.axis_index(SECTION) == 0
    pack_rows = members * rows
    all_rows = count * rows
    heads = output_weight.shape[0] // VD
    top = routes.shape[3]
    tiles = [Tiles(all_rows, pack_rows, pack, active) for active in range(2)]
    fusing = members == 4 and tiles[0].tile == 2 * rows

    def own_pack(value):
        size = value.shape[0] // packs
        return lax.dynamic_slice_in_dim(value, pack * size, size, 0)

    freqs = rope_base ** (-jnp.arange(HALF, dtype=jnp.float32) / HALF)
    angles = jnp.arange(rows, dtype=jnp.float32)[:, None] * freqs[None, :]
    turns = jnp.concatenate([jnp.cos(angles), jnp.sin(angles)], axis=1)

    def tables_of(block_lengths):
        segment, position = block_layout(block_lengths, rows)
        blocks = segment.shape[0]
        chosen = position.reshape(-1)[:, None] == jnp.arange(rows, dtype=jnp.int32)[None, :]
        found = jnp.dot(
            chosen.astype(jnp.float32),
            turns,
            precision=lax.Precision.HIGHEST,
            preferred_element_type=jnp.float32,
        )
        return (
            found[:, :HALF],
            found[:, HALF:],
            segment.reshape(blocks * rows, 1),
            segment.reshape(blocks, 1, rows),
        )

    own_lengths = lax.dynamic_index_in_dim(lengths[0, 0], member, 0, keepdims=False)
    layout = jnp.concatenate(
        [
            jnp.transpose(routes[0, 0]),
            jnp.pad(own_lengths, (0, rows - own_lengths.shape[0]))[None],
            jnp.zeros((-(top + 1) % 8, rows), jnp.int32),
        ],
        axis=0,
    )

    layout_all = lax.all_gather(layout.astype(jnp.float32), BOTH, axis=0, tiled=True)
    layout_all = layout_all.astype(jnp.int32).reshape(count, -1, rows)
    routed = jnp.any(layout_all[:, :top] == me, axis=1).astype(jnp.float32).reshape(all_rows, 1)

    tables_all = tables_of(layout_all[:, top, : lengths.shape[3]])
    tables_pack = tables_of(lengths[0, 0])
    tables_own = tables_of(own_lengths[None])
    own_cos, own_sin = tables_own[:2]
    own_column = (lax.broadcasted_iota(jnp.int32, (1, experts_count), 1) == me).astype(jnp.float32)

    def inputs_of(hidden):
        normed32, scale_attn = rms_forward(hidden, attn_gain)
        normed = bf16(normed32)
        compressed = dot(normed, compress_weight)
        latent32, scale_latent = rms_forward(compressed[:, :LAT], latent_gain)
        keyed = bf16(
            jnp.concatenate([latent32, rotate(compressed[:, LAT:], own_cos, own_sin)], axis=1)
        )
        return normed, keyed, (compressed, scale_attn, scale_latent)

    def run_experts(section, x, routed, gathered, into, number, full):
        at = tiles[section]
        results = [
            at.result(2 * units),
            at.result(units),
            at.result(experts_count, jnp.float32),
            at.pack_result(half),
        ]
        weights = [joined_in, shared_in_t]
        if full:
            results.append(at.result(width))
            weights += [expert_out, shared_out]
        if fusing:
            shapes = [(shape, index == 3) for index, (shape, _) in enumerate(results)]
            return fused_call(
                at, x, number, section, experts_body, own_column, [(routed, False)], weights, shapes, gathered, into
            )
        (x_all,) = gather_blocks([x], True, number, section, [gathered])
        return x_all, at.call(
            tiled(experts_body),
            "experts",
            [(x_all, at.source(width)), (own_column, at.small(own_column)), (routed, at.source(1))],
            weights,
            results,
            into[:4],
        )

    def run_experts_back(section, grad, routed, stored, gathered, into, number):
        at = tiles[section]
        pre, _, prob, shared_pre = stored
        weights = [joined_in, shared_in_t, expert_out, shared_out]
        results = [at.result(2 * units), at.result(1, jnp.float32), at.result(width)]
        scratch = [pltpu.VMEM((at.tile, joined_in.shape[1]), jnp.bfloat16)]
        if fusing and number is not None:
            shapes = [(shape, False) for shape, _ in results]
            sources = [(pre, False), (prob, False), (routed, False), (shared_pre, True)]
            return fused_call(
                at, grad, number, section, experts_back_body, own_column, sources, weights, shapes, gathered, into, scratch
            )
        grad_all = gathered
        if number is not None:
            (grad_all,) = gather_blocks([grad], True, number, section, [gathered])
        return grad_all, at.call(
            tiled(experts_back_body),
            "experts_back",
            [
                (grad_all, at.source(width)),
                (own_column, at.small(own_column)),
                (pre, at.source(2 * units)),
                (prob, at.source(experts_count)),
                (routed, at.source(1)),
                (shared_pre, at.pack_source(half)),
            ],
            weights,
            results,
            into,
            scratch,
            flops=6 * all_rows * width * units,
        )

    def prepare(section, normed_all, keyed_all, ffn_all, tables, into):
        at = tiles[section]
        cosine, sine, seg_col, seg_row = tables
        blocks = at.tile // rows
        row_spec = pl.BlockSpec((blocks, 1, rows), lambda i, control: (i * control[2], 0, 0))
        found = at.call(
            tiled(functools.partial(heads_body, rows)),
            "heads",
            [
                (normed_all, at.source(width)),
                (keyed_all, at.source(LAT + ROPE)),
                (cosine, at.source(HALF)),
                (sine, at.source(HALF)),
                (seg_col, at.source(1)),
                (seg_row, row_spec),
            ],
            [query_weight, expand_weight],
            [at.result(heads * VD), at.result(heads * QK), at.result(heads * KV)],
            into[:3],
            [pltpu.VMEM((at.tile, heads * QK), jnp.float32)],
            flops=4 * all_rows * width * heads * QK,
        )
        shared = at.call(
            tiled(shared_body),
            "shared",
            [(ffn_all, at.source(width))],
            [shared_in_t],
            [at.pair_result(half), at.result(half)],
            into[3:],
            flops=4 * all_rows * width * half,
        )
        return [*found, *shared]

    fresh = boundary[0, 0].astype(jnp.float32)

    normed, keyed, _ = inputs_of(fresh)
    normed_pack, keyed_pack = gather_blocks([normed, keyed], False, 0, 0)
    attended, _ = attend(
        dot(normed_pack, query_weight),
        bf16(dot(keyed_pack[:, :LAT], expand_weight)),
        keyed_pack,
        tables_pack,
    )
    mixed_first = fresh + scatter_blocks(bf16(dot(attended, output_weight)), rows, False, 1, 0)
    empty = [
        blank((all_rows, width), jnp.bfloat16),
        *(
            blank(shape, dtype)
            for shape, dtype in (
                ((all_rows + tiles[0].tile, 2 * units), jnp.bfloat16),
                ((all_rows + tiles[0].tile, units), jnp.bfloat16),
                ((all_rows + tiles[0].tile, experts_count), jnp.float32),
                ((2, pack_rows + tiles[0].tile, half), jnp.bfloat16),
            )
        ),
    ]
    ffn_all, (*stored, partial) = run_experts(
        0, bf16(rms_forward(mixed_first, ffn_gain)[0]), routed, empty[0], empty[1:], 2, True
    )
    result_first = mixed_first + scatter_blocks(partial, rows, True, 3, 0)
    heads_weights = spread_blocks([query_weight, expand_weight, output_weight], 4, 1)
    (target_all,) = gather_blocks([boundary[0, 0]], True, 5, 1, [blank((all_rows, width), jnp.bfloat16)])
    sent, target_all, heads_weights = lax.optimization_barrier((bf16(result_first), target_all, heads_weights))
    inbound = lax.ppermute(sent, SECTION, [(0, 1)])
    query_heads, expand_heads, output_heads = (
        value.reshape(members, -1, value.shape[1]) for value in heads_weights
    )

    hidden = jnp.where(is_first, fresh, inbound.astype(jnp.float32))
    normed, keyed, (compressed, scale_attn, scale_latent) = inputs_of(hidden)
    latent = bf16(jnp.einsum("rd,mdc->mrc", keyed[:, :LAT], expand_heads, preferred_element_type=jnp.float32))
    latent = latent.reshape(members * rows, -1)
    query_raw = jnp.einsum("rd,mdc->mrc", normed, query_heads, preferred_element_type=jnp.float32)
    attended, query = attend(query_raw.reshape(members * rows, -1), latent, keyed, tables_own, members)
    mixed = hidden + jnp.einsum(
        "mrc,mcd->rd", attended.reshape(members, rows, -1), output_heads, preferred_element_type=jnp.float32
    )
    mixed = jnp.where(is_first, mixed_first, mixed)
    ffn32, scale_ffn = rms_forward(mixed, ffn_gain)
    ffn_all, stored = run_experts(1, bf16(ffn32), routed, ffn_all, stored, 6, False)

    def latent_back(own):
        grad_latent, grad_latent_gain = rms_backward(
            compressed[:, :LAT], scale_latent, latent_gain, own[:, width : width + LAT]
        )
        grad_compressed = bf16(
            jnp.concatenate([grad_latent, rotate(own[:, width + LAT :], own_cos, -own_sin)], axis=1)
        )
        grad_normed = own[:, :width] + dot_t(grad_compressed, compress_weight)
        grad_hidden_norm, grad_attn_gain = rms_backward(hidden, scale_attn, attn_gain, grad_normed)
        return grad_compressed, grad_hidden_norm, grad_attn_gain, grad_latent_gain

    _, (*grad_units, partial) = run_experts_back(1, None, routed, stored, target_all, (), None)
    grad_ffn_second = scatter_blocks(partial, rows, True, 7, 1)
    grad_mixed = fresh + rms_backward(mixed, scale_ffn, ffn_gain, grad_ffn_second)[0]
    grad_attended = jnp.einsum(
        "rd,mcd->mrc", bf16(grad_mixed), output_heads, preferred_element_type=jnp.float32
    )
    grad_query, grad_latent_heads, grad_shared_key = attend_back(
        query, latent, keyed, bf16(grad_attended).reshape(members * rows, -1), tables_own, members
    )
    own_second = jnp.concatenate(
        [
            jnp.einsum(
                "mrc,mdc->rd",
                grad_query.reshape(members, rows, -1),
                query_heads,
                preferred_element_type=jnp.float32,
            ),
            jnp.einsum(
                "mrc,mdc->rd",
                grad_latent_heads.reshape(members, rows, -1),
                expand_heads,
                preferred_element_type=jnp.float32,
            ),
            jnp.sum(grad_shared_key.reshape(members, rows, -1), axis=0),
        ],
        axis=1,
    )
    grad_second = bf16(grad_mixed + latent_back(own_second)[1])

    all_inputs = gather_blocks([normed, keyed], True, 8, 0)
    prepared = prepare(0, *all_inputs, ffn_all, tables_all, ())
    grad_second, prepared, all_inputs = lax.optimization_barrier((grad_second, prepared, all_inputs))
    downbound = lax.ppermute(grad_second, SECTION, [(1, 0)]).astype(jnp.float32)

    normed_late, keyed_late, gated_late, _ = lax.optimization_barrier((normed, keyed, stored[1], grad_second))
    at = tiles[1]
    finished = at.call(
        tiled(finish_body),
        "finish",
        [(gated_late, at.source(units)), (stored[3], at.pack_source(half))],
        [expert_out, shared_out],
        [at.result(width)],
        flops=2 * all_rows * width * units,
    )
    upstream = jnp.where(is_first, downbound, fresh)
    upstream_all, (grad_pre, moved, partial) = run_experts_back(
        0, bf16(upstream), routed, stored, target_all, [*grad_units, *finished], 11
    )
    summed = scatter_blocks(partial, rows, True, 12)
    result = mixed + summed
    grad_ffn = jnp.where(is_first, summed, grad_ffn_second)
    normed_late, keyed_late, _ = lax.optimization_barrier((normed_late, keyed_late, summed))
    normed_all, keyed_all = gather_blocks([normed_late, keyed_late], True, 9, 1, all_inputs)
    prepared = prepare(1, normed_all, keyed_all, ffn_all, tables_all, prepared)
    attended_all, query_all, latent_all, shared_pre, shared_hid = prepared
    attended_all, shared_hid = attended_all[:all_rows], shared_hid[:all_rows]
    grad_mixed_norm, grad_ffn_gain = rms_backward(mixed, scale_ffn, ffn_gain, grad_ffn)
    grad_mixed = upstream + grad_mixed_norm
    grad_mixed_all = lax.all_gather(bf16(grad_mixed), BOTH, axis=0, tiled=True)
    grad_attended = bf16(dot_t(grad_mixed_all, output_weight))
    grad_query, grad_latent_heads, grad_shared_key = attend_back(
        query_all, latent_all, keyed_all, grad_attended, tables_all
    )
    own = lax.psum_scatter(
        bf16(
            jnp.concatenate(
                [
                    dot_t(own_pack(grad_query), query_weight),
                    dot_t(own_pack(grad_latent_heads), expand_weight),
                    own_pack(grad_shared_key),
                ],
                axis=1,
            )
        ),
        MEMBERS,
        scatter_dimension=0,
        tiled=True,
    ).astype(jnp.float32)
    grad_compressed, grad_hidden_norm, grad_attn_gain, grad_latent_gain = latent_back(own)
    grad_hidden = grad_mixed + grad_hidden_norm

    small = jnp.concatenate([grad_attn_gain, grad_latent_gain, grad_ffn_gain, moved[:all_rows, 0]])
    small = jnp.pad(small, (0, -small.shape[0] % 1024)).reshape(8, -1)
    grad_compressed_all, small_all = gather_blocks([grad_compressed, small], True, 13)
    small_all = small_all.reshape(count, -1)
    gains = jnp.sum(small_all[:, : 2 * width + LAT], axis=0)
    moved_all = small_all[:, 2 * width + LAT : 2 * width + LAT + all_rows].T
    prob = stored[2][:all_rows]
    grad_logits = bf16(moved_all - prob * jnp.sum(moved_all, axis=1, keepdims=True))
    left, right = gated_back(
        shared_pre[0, :all_rows].astype(jnp.float32),
        shared_pre[1, :all_rows].astype(jnp.float32),
        dot_t(upstream_all, shared_out),
    )
    grad_shared_in = lax.dot_general(
        jnp.stack([left, right]), ffn_all, (((1,), (0,)), ((), ())), preferred_element_type=jnp.float32
    )
    ends = jnp.where(is_first, grad_hidden, result)
    return (
        ends[None, None],
        gains[:width][None],
        t_dot(normed_all, grad_query)[None],
        t_dot(normed_all, grad_compressed_all)[None],
        gains[width : width + LAT][None],
        t_dot(keyed_all[:, :LAT], grad_latent_heads)[None],
        t_dot(attended_all, grad_mixed_all)[None],
        gains[width + LAT :][None],
        t_dot(ffn_all, grad_logits)[None],
        jnp.transpose(grad_shared_in, (2, 0, 1))[None],
        t_dot(shared_hid, upstream_all)[None],
        pair_grad(ffn_all, grad_pre)[None, None],
        t_dot(stored[1][:all_rows], upstream_all)[None, None],
    )


def solution(mesh):
    return jax.shard_map(
        body,
        mesh=mesh,
        in_specs=(
            P(SECTION, None, BOTH, None),
            P(None, PACKS, None, None),
            P(SECTION, None, BOTH, None),
            P(SECTION, None),
            P(SECTION, None, MEMBERS),
            P(SECTION, None, None),
            P(SECTION, None),
            P(SECTION, None, MEMBERS),
            P(SECTION, MEMBERS, None),
            P(SECTION, None),
            P(SECTION, None, None),
            P(SECTION, None, None, MEMBERS),
            P(SECTION, MEMBERS, None),
            P(SECTION, BOTH, None, None, None),
            P(SECTION, BOTH, None, None),
        ),
        out_specs=(
            P(SECTION, None, BOTH, None),
            P(SECTION, None),
            P(SECTION, None, MEMBERS),
            P(SECTION, None, None),
            P(SECTION, None),
            P(SECTION, None, MEMBERS),
            P(SECTION, MEMBERS, None),
            P(SECTION, None),
            P(SECTION, None, None),
            P(SECTION, None, None, MEMBERS),
            P(SECTION, MEMBERS, None),
            P(SECTION, BOTH, None, None, None),
            P(SECTION, BOTH, None, None),
        ),
        check_vma=False,
    )
```

```python
import functools

import jax
import jax.numpy as jnp
from jax import lax
from jax.experimental import pallas as pl
from jax.experimental.pallas import tpu as pltpu
from jax.sharding import PartitionSpec as P

NOPE = 128
ROPE = 64
VD = 128
LAT = 512

QK = NOPE + ROPE
KV = NOPE + VD
HALF = ROPE // 2
epsilon = 1e-06
rope_base = 10000.0
masked_score = -1e30
SECTION, PACKS, MEMBERS = "section", "dp", "expert"
BOTH = (PACKS, MEMBERS)
MESH = pl.DeviceIdType.MESH
def dot(left, right):
    return jnp.dot(left, right, preferred_element_type=jnp.float32)


def dot_t(left, right):
    return lax.dot_general(
        left, right, (((1,), (1,)), ((), ())), preferred_element_type=jnp.float32
    )


def t_dot(left, right):
    return lax.dot_general(
        left, right, (((0,), (0,)), ((), ())), preferred_element_type=jnp.float32
    )


def bf16(value):
    return value.astype(jnp.bfloat16)


def rms_forward(inputs, gain_vec):
    norm_scale = lax.rsqrt(jnp.mean(inputs * inputs, axis=-1, keepdims=True) + epsilon)
    return (inputs * norm_scale * gain_vec, norm_scale)


def rms_backward(inputs, norm_scale, gain_vec, upstream):
    weighted = upstream * gain_vec
    grad_gain = jnp.sum(upstream * inputs * norm_scale, axis=0)
    cubed = norm_scale * norm_scale * norm_scale
    grad_inputs = norm_scale * weighted - inputs * cubed * jnp.mean(
        weighted * inputs, axis=-1, keepdims=True
    )
    return (grad_inputs, grad_gain)


def rotate(inputs, cosine, sine):
    half = cosine.shape[-1]
    former = inputs[..., :half]
    latter = inputs[..., half:]
    return jnp.concatenate(
        [former * cosine - latter * sine, latter * cosine + former * sine], axis=-1
    )


def silu_parts(pre_gate):
    sigmoid = jax.nn.sigmoid(pre_gate)
    return (pre_gate * sigmoid, sigmoid * (1.0 + pre_gate * (1.0 - sigmoid)))


def block_layout(block_lengths, rows):
    starts = jnp.cumsum(block_lengths, axis=1) - block_lengths
    index = jnp.arange(rows, dtype=jnp.int32)
    begun = index[None, :, None] >= starts[:, None, :]
    segment = jnp.sum(begun.astype(jnp.int32), axis=2)
    opening = jnp.max(jnp.where(begun, starts[:, None, :], 0), axis=2)
    return segment, index[None, :] - opening


def places(spots):
    member = lax.axis_index(MEMBERS)
    spot = lax.axis_index(PACKS) if spots > 1 else 0
    return spot, member // 2, lax.rem(member, 2)


def to_partner(chip, core):
    return {MEMBERS: chip * 2 + 1 - core}


def to_other(chip, core):
    return {MEMBERS: (1 - chip) * 2 + core}


def when(condition, action):
    if condition is True:
        action()
    else:
        pl.when(condition)(action)


def greet(spots, spot, chip, core):
    barrier = pltpu.get_barrier_semaphore()

    def signal(target):
        pl.semaphore_signal(barrier, inc=1, device_id=target, device_id_type=MESH)

    signal(to_partner(chip, core))
    signal(to_other(chip, core))
    if spots > 1:
        pl.when(spot > 0)(lambda: signal({PACKS: spot - 1}))
        pl.when(spot < spots - 1)(lambda: signal({PACKS: spot + 1}))
        ends = jnp.where(spot > 0, 1, 0) + jnp.where(spot < spots - 1, 1, 0)
        pl.semaphore_wait(barrier, 2 + ends)
    else:
        pl.semaphore_wait(barrier, 2)


def remote(source, target_ref, target, out_sem, in_sem):
    return pltpu.make_async_remote_copy(
        src_ref=source,
        dst_ref=target_ref,
        send_sem=out_sem,
        recv_sem=in_sem,
        device_id=target,
        device_id_type=MESH,
    )


def slot(spot, chip, core):
    return spot * 4 + chip * 2 + core


def gather_kernel(spots, cuts, wide, active, *refs):
    arrays = len(cuts)
    x_refs, o_refs, sems = refs[:arrays], refs[-9 - arrays : -9], refs[-9:]
    own_sem, up_out, up_in, down_out, down_in, over_out, over_in, pair_out, pair_in = sems
    units = [
        (a, pl.ds(part * (x_refs[a].shape[0] // parts), x_refs[a].shape[0] // parts))
        for a, parts in enumerate(cuts)
        for part in range(parts)
    ]

    def run():
        spot, chip, core = places(spots)
        greet(spots, spot, chip, core)

        def piece(unit, index):
            array, cut = units[unit]
            return o_refs[array].at[index, cut]

        def first(unit):
            array, cut = units[unit]
            return x_refs[array].at[cut]

        def lane(unit):
            return wide[units[unit][0]]

        def spread(unit):
            return range(spots) if lane(unit) else [0]

        def up(source, at, unit, reach):
            return remote(
                source, piece(unit, slot(at, chip, core)), {PACKS: spot + 1}, up_out.at[reach, unit], up_in.at[reach, unit]
            )

        def down(source, at, unit, reach):
            return remote(
                source,
                piece(unit, slot(at, chip, core)),
                {PACKS: spot - 1},
                down_out.at[reach, unit],
                down_in.at[reach, unit],
            )

        def over(source, at, unit):
            return remote(
                source, piece(unit, slot(at, chip, core)), to_other(chip, core), over_out.at[at, unit], over_in.at[at, unit]
            )

        def pair(source, at, c, unit):
            return remote(
                source,
                piece(unit, slot(at, c, core)),
                to_partner(chip, core),
                pair_out.at[c, at, unit],
                pair_in.at[c, at, unit],
            )

        home = lambda unit: spot if lane(unit) else 0
        for unit in range(len(units)):
            source = first(unit)
            over(source, home(unit), unit).start()
            if spots > 1 and lane(unit):
                pl.when(spot < spots - 1)(lambda: up(source, spot, unit, 0).start())
                pl.when(spot > 0)(lambda: down(source, spot, unit, 0).start())
            pair(source, home(unit), chip, unit).start()
        own = [
            pltpu.make_async_copy(
                x_refs[a], o_refs[a].at[slot(spot if wide[a] else 0, chip, core)], own_sem.at[a]
            )
            for a in range(arrays)
        ]
        for copy in own:
            copy.start()
        for reach in range(1, spots):
            for unit in range(len(units)):
                if not lane(unit):
                    continue

                def below(reach=reach, unit=unit):
                    at = spot - reach
                    source = piece(unit, slot(at, chip, core))
                    up(source, at, unit, reach - 1).wait_recv()
                    pl.when(spot < spots - 1)(lambda: up(source, at, unit, reach).start())
                    over(source, at, unit).start()
                    pair(source, at, chip, unit).start()

                def above(reach=reach, unit=unit):
                    at = spot + reach
                    source = piece(unit, slot(at, chip, core))
                    down(source, at, unit, reach - 1).wait_recv()
                    pl.when(spot > 0)(lambda: down(source, at, unit, reach).start())
                    over(source, at, unit).start()
                    pair(source, at, chip, unit).start()

                pl.when(spot >= reach)(below)
                pl.when(spot + reach < spots)(above)
        for reach in range(spots):
            sides = [(True, spot)]
            if reach > 0:
                sides = [(spot >= reach, spot - reach), (spot + reach < spots, spot + reach)]
            for unit in range(len(units)):
                if not lane(unit) and reach > 0:
                    continue
                for there, at in sides:
                    at = at if lane(unit) else 0

                    def hand_on(at=at, unit=unit):
                        source = piece(unit, slot(at, 1 - chip, core))
                        over(source, at, unit).wait_recv()
                        pair(source, at, 1 - chip, unit).start()

                    when(there, hand_on)
        for copy in own:
            copy.wait()
        for unit in range(len(units)):
            source = first(unit)
            for at in spread(unit):
                over(source, at, unit).wait_send()
                for c in range(2):
                    pair(source, at, c, unit).wait()
            for reach in range(spots - 1 if lane(unit) else 0):
                pl.when((spot >= reach) & (spot < spots - 1))(lambda: up(source, spot, unit, reach).wait_send())
                pl.when((spot + reach < spots) & (spot > 0))(lambda: down(source, spot, unit, reach).wait_send())

    if active is None:
        run()
    else:
        pl.when(lax.axis_index(SECTION) == active)(run)


def gather_blocks(values, across, number, active=None, into=None, parts=4, wide=None):
    wide = [across] * len(values) if wide is None else wide
    if lax.axis_size(MEMBERS) != 4:
        found = [
            lax.all_gather(value, BOTH if far else MEMBERS, axis=0, tiled=True) for value, far in zip(values, wide)
        ]
        if into is None:
            return found
        chosen = lax.axis_index(SECTION) == active
        return [jnp.where(chosen, new, old) for new, old in zip(found, into)]
    spots = lax.axis_size(PACKS) if across else 1
    cuts = [parts if value.shape[0] % (16 * parts) == 0 else 1 for value in values]
    units = sum(cuts)
    dma = pltpu.SemaphoreType.DMA
    hops = max(spots - 1, 1)
    shapes = [
        jax.ShapeDtypeStruct(((spots if far else 1) * 4, *value.shape), value.dtype)
        for value, far in zip(values, wide)
    ]
    held = [] if into is None else [old.reshape(shape.shape) for old, shape in zip(into, shapes)]
    outs = pl.pallas_call(
        functools.partial(gather_kernel, spots, cuts, wide, active),
        out_shape=shapes,
        in_specs=[pl.BlockSpec(memory_space=pltpu.VMEM)] * len(values)
        + [pl.BlockSpec(memory_space=pl.ANY)] * len(held),
        out_specs=[pl.BlockSpec(memory_space=pl.ANY)] * len(values),
        input_output_aliases={len(values) + index: index for index in range(len(held))},
        scratch_shapes=[
            dma((len(values),)),
            dma((hops, units)),
            dma((hops, units)),
            dma((hops, units)),
            dma((hops, units)),
            dma((spots, units)),
            dma((spots, units)),
            dma((2, spots, units)),
            dma((2, spots, units)),
        ],
        compiler_params=pltpu.CompilerParams(collective_id=number, has_side_effects=True),
        name=f"gather{number}",
    )(*values, *held)
    return [out.reshape(-1, out.shape[2]) for out in outs]


def spread_kernel(cuts, active, *refs):
    arrays = len(cuts)
    x_refs, o_refs = refs[:arrays], refs[arrays : 2 * arrays]
    own_sem, over_out, over_in, side_out, side_in, pair_out, pair_in = refs[2 * arrays :]
    units = [
        (a, pl.ds(part * (x_refs[a].shape[0] // parts), x_refs[a].shape[0] // parts))
        for a, parts in enumerate(cuts)
        for part in range(parts)
    ]

    def run():
        member, spot = lax.axis_index(MEMBERS), lax.axis_index(PACKS)
        chip, core, odd = member // 2, lax.rem(member, 2), lax.rem(spot, 2)
        beside = {PACKS: spot + 1 - 2 * odd}
        barrier = pltpu.get_barrier_semaphore()
        for target in (to_partner(chip, core), to_other(chip, core), beside):
            pl.semaphore_signal(barrier, inc=1, device_id=target, device_id_type=MESH)
        pl.semaphore_wait(barrier, 3)

        def piece(unit, c):
            array, cut = units[unit]
            return o_refs[array].at[c * 2 + core, cut]

        def first(unit):
            array, cut = units[unit]
            return x_refs[array].at[cut]

        def over(unit):
            return remote(first(unit), piece(unit, chip), to_other(chip, core), over_out.at[unit], over_in.at[unit])

        def side(unit):
            source = piece(unit, 1 - chip)
            return remote(source, source, beside, side_out.at[unit], side_in.at[unit])

        def pair(source, unit, c, index):
            return remote(
                source, piece(unit, c), to_partner(chip, core), pair_out.at[index, unit], pair_in.at[index, unit]
            )

        for unit in range(len(units)):
            pl.when(odd == unit % 2)(lambda: over(unit).start())
        for unit in range(len(units)):
            pair(first(unit), unit, chip, 0).start()
        own = [
            pltpu.make_async_copy(x_refs[a], o_refs[a].at[member], own_sem.at[a]) for a in range(arrays)
        ]
        for copy in own:
            copy.start()
        for unit in range(len(units)):

            def taken(unit=unit):
                over(unit).wait_recv()
                side(unit).start()
                pair(piece(unit, 1 - chip), unit, 1 - chip, 1).start()

            pl.when(odd == unit % 2)(taken)
        for unit in range(len(units)):

            def handed(unit=unit):
                side(unit).wait_recv()
                pair(piece(unit, 1 - chip), unit, 1 - chip, 1).start()

            pl.when(odd != unit % 2)(handed)
        for copy in own:
            copy.wait()
        for unit in range(len(units)):

            def sent(unit=unit):
                over(unit).wait_send()
                side(unit).wait_send()

            pl.when(odd == unit % 2)(sent)
            pair(first(unit), unit, chip, 0).wait()
            pair(first(unit), unit, 1 - chip, 1).wait()

    pl.when(lax.axis_index(SECTION) == active)(run)


def spread_blocks(values, number, active, parts=8):
    if lax.axis_size(MEMBERS) != 4 or lax.axis_size(PACKS) % 2:
        return gather_blocks(values, False, number, active)
    units = parts * len(values)
    dma = pltpu.SemaphoreType.DMA
    outs = pl.pallas_call(
        functools.partial(spread_kernel, [parts] * len(values), active),
        out_shape=[jax.ShapeDtypeStruct((4, *value.shape), value.dtype) for value in values],
        in_specs=[pl.BlockSpec(memory_space=pltpu.VMEM)] * len(values),
        out_specs=[pl.BlockSpec(memory_space=pl.ANY)] * len(values),
        scratch_shapes=[
            dma((len(values),)),
            dma((units,)),
            dma((units,)),
            dma((units,)),
            dma((units,)),
            dma((2, units)),
            dma((2, units)),
        ],
        compiler_params=pltpu.CompilerParams(collective_id=number, has_side_effects=True),
        name=f"spread{number}",
    )(*values)
    return [out.reshape(-1, out.shape[2]) for out in outs]


def add_into(target, sources, rows, step=16):
    def some(index, carry):
        at = pl.ds(pl.multiple_of(index * step, step), step)
        total = sources[0][at, :].astype(jnp.float32)
        for source in sources[1:]:
            total = total + source[at, :].astype(jnp.float32)
        target[at, :] = total.astype(target.dtype)
        return carry

    lax.fori_loop(0, rows // step, some, 0)


def scatter_kernel(
    spots,
    parts,
    active,
    x_ref,
    o_ref,
    own_buf,
    pair_buf,
    over_src,
    over_buf,
    line_src,
    up_buf,
    down_buf,
    own_in,
    pair_out,
    pair_in,
    over_out,
    over_in,
    line_out,
    up_in,
    down_in,
):
    rows = x_ref.shape[1] // parts
    cut = lambda part: pl.ds(part * rows, rows)

    def run():
        spot, chip, core = places(spots)
        greet(spots, spot, chip, core)

        def order(step):
            if step == spots - 1:
                return spot
            fall = spots - 1 - step
            fall = jnp.where(fall <= spot, fall - 1, fall)
            rise = jnp.where(step >= spot, step + 1, step)
            return jnp.where(2 * spot < spots - 1, fall, rise)

        def pair(at, c, part):
            return remote(
                x_ref.at[slot(at, c, 1 - core), cut(part)],
                pair_buf.at[at, c, cut(part)],
                to_partner(chip, core),
                pair_out.at[at, c, part],
                pair_in.at[at, c, part],
            )

        def over(at, part):
            return remote(
                over_src.at[at, cut(part)],
                over_buf.at[at, cut(part)],
                to_other(chip, core),
                over_out.at[at, part],
                over_in.at[at, part],
            )

        def up(at, part):
            return remote(
                line_src.at[at, cut(part)],
                up_buf.at[at, cut(part)],
                {PACKS: spot + 1},
                line_out.at[at, part],
                up_in.at[at, part],
            )

        def down(at, part):
            return remote(
                line_src.at[at, cut(part)],
                down_buf.at[at, cut(part)],
                {PACKS: spot - 1},
                line_out.at[at, part],
                down_in.at[at, part],
            )

        def own(at, c):
            return pltpu.make_async_copy(x_ref.at[slot(at, c, core)], own_buf.at[at, c], own_in.at[at, c])

        for c in (1 - chip, chip):
            for step in range(spots):
                own(order(step), c).start()
                for part in range(parts):
                    pair(order(step), c, part).start()
        for step in range(spots):
            at = order(step)
            own(at, 1 - chip).wait()
            for part in range(parts):
                pair(at, 1 - chip, part).wait_recv()
                add_into(
                    over_src.at[at, cut(part)],
                    [own_buf.at[at, 1 - chip, cut(part)], pair_buf.at[at, 1 - chip, cut(part)]],
                    rows,
                )
                over(at, part).start()
        for step in range(spots):
            at = order(step)
            own(at, chip).wait()
            for part in range(parts):
                pair(at, chip, part).wait_recv()
                over(at, part).wait_recv()
                base = [
                    own_buf.at[at, chip, cut(part)],
                    pair_buf.at[at, chip, cut(part)],
                    over_buf.at[at, cut(part)],
                ]
                ups, downs = up_buf.at[at, cut(part)], down_buf.at[at, cut(part)]
                if step < spots - 1:
                    target = line_src.at[at, cut(part)]

                    def rising(first):
                        if not first:
                            up(at, part).wait_recv()
                        add_into(target, base if first else base + [ups], rows)
                        up(at, part).start()

                    def falling(first):
                        if not first:
                            down(at, part).wait_recv()
                        add_into(target, base if first else base + [downs], rows)
                        down(at, part).start()

                    pl.when((at > spot) & (spot == 0))(lambda: rising(True))
                    pl.when((at > spot) & (spot > 0))(lambda: rising(False))
                    pl.when((at < spot) & (spot == spots - 1))(lambda: falling(True))
                    pl.when((at < spot) & (spot < spots - 1))(lambda: falling(False))
                elif spots == 1:
                    add_into(o_ref.at[cut(part)], base, rows)
                else:

                    def finish(ends):
                        if ends < 1:
                            up(at, part).wait_recv()
                        if ends > -1:
                            down(at, part).wait_recv()
                        extra = ([ups] if ends < 1 else []) + ([downs] if ends > -1 else [])
                        add_into(o_ref.at[cut(part)], base + extra, rows)

                    pl.when(spot == 0)(lambda: finish(1))
                    pl.when(spot == spots - 1)(lambda: finish(-1))
                    pl.when((spot > 0) & (spot < spots - 1))(lambda: finish(0))
        for part in range(parts):
            for step in range(spots):
                at = order(step)
                pair(at, 0, part).wait_send()
                pair(at, 1, part).wait_send()
                over(at, part).wait_send()
                if step < spots - 1:
                    up(at, part).wait_send()

    if active is None:
        run()
    else:
        pl.when(lax.axis_index(SECTION) == active)(run)


def scatter_blocks(partial, rows, across, number, active=None, parts=4):
    if lax.axis_size(MEMBERS) != 4:
        axes = BOTH if across else MEMBERS
        taken = partial[: rows * lax.axis_size(axes)]
        return lax.psum_scatter(taken, axes, scatter_dimension=0, tiled=True).astype(jnp.float32)
    spots = lax.axis_size(PACKS) if across else 1
    width = partial.shape[1]
    dma = pltpu.SemaphoreType.DMA
    hold = lambda *lead: pltpu.VMEM((*lead, rows, width), partial.dtype)
    return pl.pallas_call(
        functools.partial(scatter_kernel, spots, parts, active),
        out_shape=jax.ShapeDtypeStruct((rows, width), jnp.float32),
        in_specs=[pl.BlockSpec(memory_space=pl.ANY)],
        out_specs=pl.BlockSpec(memory_space=pltpu.VMEM),
        scratch_shapes=[
            hold(spots, 2),
            hold(spots, 2),
            hold(spots),
            hold(spots),
            hold(spots),
            hold(spots),
            hold(spots),
            dma((spots, 2)),
            dma((spots, 2, parts)),
            dma((spots, 2, parts)),
            dma((spots, parts)),
            dma((spots, parts)),
            dma((spots, parts)),
            dma((spots, parts)),
            dma((spots, parts)),
        ],
        compiler_params=pltpu.CompilerParams(collective_id=number, has_side_effects=True),
        name=f"scatter{number}",
    )(partial.reshape(-1, rows, width))


def allowed_pairs(seg_col, seg_row):
    rows = seg_col.shape[0]
    later = lax.broadcasted_iota(jnp.int32, (rows, rows), 0)
    earlier = lax.broadcasted_iota(jnp.int32, (rows, rows), 1)
    return (seg_col == seg_row) & (earlier <= later)


def attend_kernel(heads, q_ref, lat_ref, key_ref, cos_ref, sin_ref, col_ref, row_ref, out_ref, rot_ref):
    factor = QK**-0.5
    allowed = allowed_pairs(col_ref[...], row_ref[0])
    cosine, sine = cos_ref[...], sin_ref[...]
    shared = key_ref[:, LAT:]
    for head in range(heads):
        raw = q_ref[:, head * QK : (head + 1) * QK]
        query = bf16(
            jnp.concatenate([raw[:, :NOPE], rotate(raw[:, NOPE:], cosine, sine)], axis=1)
        )
        rot_ref[:, head * QK : (head + 1) * QK] = query
        key = jnp.concatenate([lat_ref[:, head * KV : head * KV + NOPE], shared], axis=1)
        value = lat_ref[:, head * KV + NOPE : (head + 1) * KV]
        scores = jnp.where(allowed, dot_t(query, key) * factor, masked_score)
        top = jnp.max(scores, axis=1, keepdims=True)
        powers = jnp.exp(scores - top)
        probs = powers / jnp.sum(powers, axis=1, keepdims=True)
        out_ref[:, head * VD : (head + 1) * VD] = bf16(dot(bf16(probs), value))


def attend(query_raw, latent, keyed, tables, groups=1):
    cosine, sine, seg_col, seg_row = tables
    count, _, rows = seg_row.shape
    heads = query_raw.shape[1] // QK
    block = lambda width: pl.BlockSpec((rows, width), lambda i: (i, 0))
    same = lambda width: pl.BlockSpec((rows, width), lambda i: (0, 0) if groups > 1 else (i, 0))
    count = count * groups
    return pl.pallas_call(
        functools.partial(attend_kernel, heads),
        grid=(count,),
        in_specs=[
            block(heads * QK),
            block(heads * KV),
            same(LAT + ROPE),
            same(HALF),
            same(HALF),
            same(1),
            pl.BlockSpec((1, 1, rows), lambda i: (0, 0, 0) if groups > 1 else (i, 0, 0)),
        ],
        out_specs=[block(heads * VD), block(heads * QK)],
        out_shape=[
            jax.ShapeDtypeStruct((count * rows, heads * VD), jnp.bfloat16),
            jax.ShapeDtypeStruct((count * rows, heads * QK), jnp.bfloat16),
        ],
        name="attend",
        cost_estimate=pl.CostEstimate(
            flops=2 * count * heads * rows * rows * (QK + VD),
            bytes_accessed=count * rows * heads * (QK * 6 + KV * 2 + VD * 2),
            transcendentals=count * heads * rows * rows,
        ),
    )(query_raw, latent, keyed, cosine, sine, seg_col, seg_row)


def attend_back_kernel(
    heads, q_ref, lat_ref, key_ref, grad_ref, cos_ref, sin_ref, col_ref, row_ref, dq_ref, dlat_ref, dkey_ref
):
    factor = QK**-0.5
    allowed = allowed_pairs(col_ref[...], row_ref[0])
    cosine, sine = cos_ref[...], sin_ref[...]
    shared = key_ref[:, LAT:]
    total = None
    for head in range(heads):
        query = q_ref[:, head * QK : (head + 1) * QK]
        key = jnp.concatenate([lat_ref[:, head * KV : head * KV + NOPE], shared], axis=1)
        value = lat_ref[:, head * KV + NOPE : (head + 1) * KV]
        grad = grad_ref[:, head * VD : (head + 1) * VD]
        scores = jnp.where(allowed, dot_t(query, key) * factor, masked_score)
        top = jnp.max(scores, axis=1, keepdims=True)
        powers = jnp.exp(scores - top)
        probs = powers / jnp.sum(powers, axis=1, keepdims=True)
        grad_value = t_dot(bf16(probs), grad)
        grad_probs = dot_t(grad, value)
        centre = jnp.sum(probs * grad_probs, axis=1, keepdims=True)
        grad_scores = bf16(probs * (grad_probs - centre) * factor)
        grad_query = dot(grad_scores, key)
        grad_key = t_dot(grad_scores, query)
        dq_ref[:, head * QK : (head + 1) * QK] = bf16(
            jnp.concatenate(
                [grad_query[:, :NOPE], rotate(grad_query[:, NOPE:], cosine, -sine)], axis=1
            )
        )
        dlat_ref[:, head * KV : head * KV + NOPE] = bf16(grad_key[:, :NOPE])
        dlat_ref[:, head * KV + NOPE : (head + 1) * KV] = bf16(grad_value)
        part = grad_key[:, NOPE:]
        total = part if total is None else total + part
    dkey_ref[...] = total


def attend_back(query, latent, keyed, grad, tables, groups=1):
    cosine, sine, seg_col, seg_row = tables
    count, _, rows = seg_row.shape
    heads = query.shape[1] // QK
    block = lambda width: pl.BlockSpec((rows, width), lambda i: (i, 0))
    same = lambda width: pl.BlockSpec((rows, width), lambda i: (0, 0) if groups > 1 else (i, 0))
    count = count * groups
    return pl.pallas_call(
        functools.partial(attend_back_kernel, heads),
        grid=(count,),
        in_specs=[
            block(heads * QK),
            block(heads * KV),
            same(LAT + ROPE),
            block(heads * VD),
            same(HALF),
            same(HALF),
            same(1),
            pl.BlockSpec((1, 1, rows), lambda i: (0, 0, 0) if groups > 1 else (i, 0, 0)),
        ],
        out_specs=[block(heads * QK), block(heads * KV), block(ROPE)],
        out_shape=[
            jax.ShapeDtypeStruct((count * rows, heads * QK), jnp.bfloat16),
            jax.ShapeDtypeStruct((count * rows, heads * KV), jnp.bfloat16),
            jax.ShapeDtypeStruct((count * rows, ROPE), jnp.float32),
        ],
        name="attend_back",
        cost_estimate=pl.CostEstimate(
            flops=2 * count * heads * rows * rows * (3 * QK + 2 * VD),
            bytes_accessed=count * rows * heads * (QK * 4 + KV * 4 + VD * 2),
            transcendentals=count * heads * rows * rows,
        ),
    )(query, latent, keyed, grad, cosine, sine, seg_col, seg_row)


def gated_hidden(gate, up):
    return silu_parts(gate)[0] * up


def gated_back(gate, up, grad_hidden):
    act, slope = silu_parts(gate)
    return bf16(grad_hidden * up * slope), bf16(grad_hidden * act)


def columns(pieces):
    start = 0
    for piece in pieces:
        yield start, piece.shape[1]
        start += piece.shape[1]


def hold_weight(pieces):
    return pltpu.VMEM((pieces[0].shape[0], sum(piece.shape[1] for piece in pieces)), pieces[0].dtype)


def loads_of(counts, sources, targets, sems):
    copies = []
    for pieces, target in zip(counts, targets):
        group, sources = sources[:pieces], sources[pieces:]
        for source, (start, size) in zip(group, columns(group)):
            place = target if pieces == 1 else target.at[:, pl.ds(start, size)]
            copies.append(pltpu.make_async_copy(source, place, sems.at[len(copies)]))
    return copies


def load(*args):
    copies = loads_of(*args)
    for copy in copies:
        copy.start()
    for copy in copies:
        copy.wait()


class Tiles:
    def __init__(self, rows, pack_rows, pack, active):
        self.rows, self.pack_rows = rows, pack_rows
        self.tile = min(256, pack_rows)
        self.count = rows // self.tile
        inner = pack_rows // self.tile
        runs = (lax.axis_index(SECTION) == active).astype(jnp.int32)
        self.control = jnp.stack([pack * inner, (pack + 1) * inner, runs]).astype(jnp.int32)

    def source(self, width):
        return pl.BlockSpec((self.tile, width), lambda i, control: (i * control[2], 0))

    def small(self, array):
        return pl.BlockSpec(array.shape, lambda i, control: (0,) * array.ndim)

    def pack_source(self, width):
        def index(i, control):
            return (0, jnp.clip(i - control[0], 0, control[1] - control[0] - 1), 0)

        return pl.BlockSpec((2, self.tile, width), index)

    def result(self, width, dtype=jnp.bfloat16):
        def index(i, control):
            return (jnp.where(control[2] == 1, i, self.count), 0)

        shape = jax.ShapeDtypeStruct((self.rows + self.tile, width), dtype)
        return shape, pl.BlockSpec((self.tile, width), index)

    def pair_result(self, width):
        def index(i, control):
            return (0, jnp.where(control[2] == 1, i, self.count), 0)

        shape = jax.ShapeDtypeStruct((2, self.rows + self.tile, width), jnp.bfloat16)
        return shape, pl.BlockSpec((2, self.tile, width), index)

    def pack_result(self, width):
        def index(i, control):
            spot = jnp.clip(i - control[0], 0, control[1] - control[0] - 1)
            return (0, jnp.where(control[2] == 1, spot, control[1] - control[0]), 0)

        shape = jax.ShapeDtypeStruct((2, self.pack_rows + self.tile, width), jnp.bfloat16)
        return shape, pl.BlockSpec((2, self.tile, width), index)

    def call(self, kernel, name, sources, weights, results, into=(), scratch=(), flops=0):
        arrays, specs = zip(*sources)
        shapes, out_specs = zip(*results)
        anywhere = pl.BlockSpec(memory_space=pl.ANY)
        pieces = [piece for weight in weights for piece in weight]
        counts = [len(weight) for weight in weights]
        first = 1 + len(arrays) + len(pieces)
        return pl.pallas_call(
            functools.partial(kernel, len(arrays), counts, len(into), len(results)),
            grid_spec=pltpu.PrefetchScalarGridSpec(
                num_scalar_prefetch=1,
                grid=(self.count,),
                in_specs=[*specs, *([anywhere] * (len(pieces) + len(into)))],
                out_specs=list(out_specs),
                scratch_shapes=[
                    *[hold_weight(weight) for weight in weights],
                    pltpu.SemaphoreType.DMA((len(pieces),)),
                    *scratch,
                ],
            ),
            out_shape=list(shapes),
            input_output_aliases={first + index: index for index in range(len(into))},
            name=name,
            cost_estimate=pl.CostEstimate(flops=flops, bytes_accessed=self.rows * 16384, transcendentals=0),
        )(self.control, *arrays, *pieces, *into)


def tiled(body):
    def kernel(n_sources, counts, n_into, n_results, control, *refs):
        n_weights, n_pieces = len(counts), sum(counts)
        sources, refs = refs[:n_sources], refs[n_sources:]
        stored, refs = refs[:n_pieces], refs[n_pieces + n_into :]
        results, refs = refs[:n_results], refs[n_results:]
        weights, sems, scratch = refs[:n_weights], refs[n_weights], refs[n_weights + 1 :]

        def run():
            pl.when(pl.program_id(0) == 0)(lambda: load(counts, stored, weights, sems))
            body(inside_pack(control), [sources[0][...], *sources[1:]], weights, results, scratch)

        pl.when(control[2] == 1)(run)

    return kernel


def inside_pack(control):
    tile = pl.program_id(0)
    return (tile >= control[0]) & (tile < control[1])


def shared_units(x, shared_in):
    half = shared_in.shape[0] // 2
    return dot_t(x, shared_in[:half]), dot_t(x, shared_in[half:])


def experts_body(inside, sources, weights, results, scratch):
    x, own_ref, routed_ref = sources
    in_ref, shared_in_ref = weights[:2]
    pre_ref, gated_ref, prob_ref, shared_pre_ref = results[:4]
    units = gated_ref.shape[1]
    pre = dot(x, in_ref[...])
    logits = pre[:, 2 * units : 2 * units + own_ref.shape[1]]
    powers = jnp.exp(logits - jnp.max(logits, axis=1, keepdims=True))
    prob = powers / jnp.sum(powers, axis=1, keepdims=True)
    prob_ref[...] = prob
    gate = jnp.sum(prob * own_ref[...], axis=1, keepdims=True) * routed_ref[...]
    pre_ref[...] = bf16(pre[:, : 2 * units])
    gated = bf16(gate * gated_hidden(pre[:, :units], pre[:, units : 2 * units]))
    gated_ref[...] = gated

    def shared():
        left, right = shared_units(x, shared_in_ref)
        shared_pre_ref[0] = bf16(left)
        shared_pre_ref[1] = bf16(right)
        return left, right

    if len(weights) == 2:
        pl.when(inside)(lambda: shared() and None)
        return
    out_ref, shared_out_ref = weights[2:]
    partial_ref = results[4]

    def with_shared():
        hidden = bf16(gated_hidden(*shared()))
        partial_ref[...] = bf16(dot(gated, out_ref[...]) + dot(hidden, shared_out_ref[...]))

    def without():
        partial_ref[...] = bf16(dot(gated, out_ref[...]))

    pl.when(inside)(with_shared)
    pl.when(jnp.logical_not(inside))(without)


def finish_body(inside, sources, weights, results, scratch):
    gated, shared_pre_ref = sources
    out_ref, shared_out_ref = weights
    (partial_ref,) = results

    def with_shared():
        hidden = bf16(gated_hidden(shared_pre_ref[0].astype(jnp.float32), shared_pre_ref[1].astype(jnp.float32)))
        partial_ref[...] = bf16(dot(gated, out_ref[...]) + dot(hidden, shared_out_ref[...]))

    def without():
        partial_ref[...] = bf16(dot(gated, out_ref[...]))

    pl.when(inside)(with_shared)
    pl.when(jnp.logical_not(inside))(without)


def experts_back_body(inside, sources, weights, results, scratch):
    grad, own_ref, pre_ref, prob_ref, routed_ref, shared_pre_ref = sources
    in_ref, shared_in_ref, out_ref, shared_out_ref = weights
    grad_pre_ref, moved_ref, partial_ref = results
    (joined_ref,) = scratch
    units = out_ref.shape[0]
    prob = prob_ref[...]
    own_prob = jnp.sum(prob * own_ref[...], axis=1, keepdims=True) * routed_ref[...]
    gate, up = pre_ref[:, :units].astype(jnp.float32), pre_ref[:, units:].astype(jnp.float32)
    grad_units = dot_t(grad, out_ref[...])
    act, slope = silu_parts(gate)
    moved = own_prob * jnp.sum(grad_units * act * up, axis=1, keepdims=True)
    moved_ref[...] = moved
    scaled = own_prob * grad_units
    joined_ref[:, :units] = bf16(scaled * up * slope)
    joined_ref[:, units : 2 * units] = bf16(scaled * act)
    joined_ref[:, 2 * units :] = jnp.zeros_like(joined_ref[:, 2 * units :])
    joined_ref[:, 2 * units : 2 * units + own_ref.shape[1]] = bf16(moved * (own_ref[...] - prob))
    grad_pre_ref[...] = joined_ref[:, : 2 * units]
    base = dot_t(joined_ref[...], in_ref[...])
    half = shared_out_ref.shape[0]

    def with_shared():
        left, right = gated_back(
            shared_pre_ref[0].astype(jnp.float32),
            shared_pre_ref[1].astype(jnp.float32),
            dot_t(grad, shared_out_ref[...]),
        )
        partial_ref[...] = bf16(base + dot(left, shared_in_ref[:half]) + dot(right, shared_in_ref[half:]))

    def without():
        partial_ref[...] = bf16(base)

    pl.when(inside)(with_shared)
    pl.when(jnp.logical_not(inside))(without)


def shared_body(inside, sources, weights, results, scratch):
    pre_ref, hid_ref = results
    left, right = shared_units(sources[0], weights[0])
    pre_ref[0] = bf16(left)
    pre_ref[1] = bf16(right)
    hid_ref[...] = bf16(gated_hidden(left, right))


def heads_body(block, inside, sources, weights, results, scratch):
    x, key_ref, cos_ref, sin_ref, col_ref, row_ref = sources
    query_w_ref, expand_ref = weights
    out_ref, rot_ref, lat_ref = results
    (q_ref,) = scratch
    heads = q_ref.shape[1] // QK
    q_ref[...] = dot(x, query_w_ref[...])
    lat_ref[...] = bf16(dot(key_ref[:, :LAT], expand_ref[...]))
    for start in range(0, x.shape[0], block):
        at = pl.ds(start, block)
        attend_kernel(
            heads,
            q_ref.at[at],
            lat_ref.at[at],
            key_ref.at[at],
            cos_ref.at[at],
            sin_ref.at[at],
            col_ref.at[at],
            row_ref.at[pl.ds(start // block, 1)],
            out_ref.at[at],
            rot_ref.at[at],
        )


def pair_grad_kernel(x_ref, grad_ref, out_ref):
    units = out_ref.shape[2]
    x = x_ref[...]
    out_ref[:, 0, :] = t_dot(x, grad_ref[:, :units])
    out_ref[:, 1, :] = t_dot(x, grad_ref[:, units:])


def pair_grad(x, grad):
    rows, width = x.shape
    units = grad.shape[1] // 2
    if rows > 4096:
        return t_dot(x, grad[:rows]).reshape(width, 2, units)
    tile = 256
    return pl.pallas_call(
        pair_grad_kernel,
        grid=(width // tile,),
        in_specs=[
            pl.BlockSpec((rows, tile), lambda i: (0, i)),
            pl.BlockSpec((rows, 2 * units), lambda i: (0, 0), pipeline_mode=pl.Buffered(1)),
        ],
        out_specs=pl.BlockSpec((tile, 2, units), lambda i: (i, 0, 0)),
        out_shape=jax.ShapeDtypeStruct((width, 2, units), jnp.float32),
        name="pair_grad",
        cost_estimate=pl.CostEstimate(
            flops=4 * rows * width * units, bytes_accessed=rows * (width + 2 * units) * 2 + width * units * 8, transcendentals=0
        ),
    )(x, grad)


def blank(shape, dtype):
    return pl.pallas_call(
        lambda out_ref: None,
        out_shape=jax.ShapeDtypeStruct(shape, dtype),
        out_specs=pl.BlockSpec(memory_space=pl.ANY),
        compiler_params=pltpu.CompilerParams(has_side_effects=True),
        name="blank",
    )()


def arrival_order(spots):
    tiles = [(rank + 1.1 * over, rank, over) for rank in range(spots) for over in (0, 1)]
    return [(rank, over == 1) for _, rank, over in sorted(tiles)]


def ranked_spots(spots, spot):
    ranks = []
    for rank in range(spots):
        value = 0
        for own in range(spots):
            nearest = sorted(range(spots), key=lambda other: (abs(other - own), other))
            value = value + jnp.where(spot == own, nearest[rank], 0)
        ranks.append(value)
    return ranks


def pick(index, values):
    total = 0
    for position, value in enumerate(values):
        total = total + jnp.where(index == position, value, 0)
    return total


def fused_kernel(spots, parts, active, body, pack_kinds, counts, n_into, *refs):
    source_kinds, result_kinds = pack_kinds
    n_sources, n_results = len(source_kinds), len(result_kinds)
    n_weights, n_pieces = len(counts), sum(counts)
    x_ref, small_ref, refs = refs[0], refs[1], refs[2:]
    sources, refs = refs[:n_sources], refs[n_sources:]
    stored, refs = refs[:n_pieces], refs[n_pieces + n_into :]
    o_ref, refs = refs[0], refs[1:]
    results, refs = refs[:n_results], refs[n_results:]
    x_tile, refs = refs[0], refs[1:]
    source_tiles, refs = refs[:n_sources], refs[n_sources:]
    result_tiles, refs = refs[:n_results], refs[n_results:]
    weights, refs = refs[:n_weights], refs[n_weights:]
    sems, scratch = refs[:12], refs[12:]
    own_sem, weight_sem, tile_sem, out_sem = sems[:4]
    up_out, up_in, down_out, down_in, over_out, over_in, pair_out, pair_in = sems[4:]
    block = x_ref.shape[0]
    rows = block // parts
    tile = 2 * block

    def run():
        loads = loads_of(counts, stored, weights, weight_sem)
        for copy in loads:
            copy.start()
        spot, chip, core = places(spots)
        greet(spots, spot, chip, core)
        piece = lambda index, part: o_ref.at[index, pl.ds(part * rows, rows)]
        first = lambda part: x_ref.at[pl.ds(part * rows, rows)]

        def up(source, at, part, reach):
            return remote(
                source, piece(slot(at, chip, core), part), {PACKS: spot + 1}, up_out.at[reach, part], up_in.at[reach, part]
            )

        def down(source, at, part, reach):
            return remote(
                source,
                piece(slot(at, chip, core), part),
                {PACKS: spot - 1},
                down_out.at[reach, part],
                down_in.at[reach, part],
            )

        def over(source, at, part):
            return remote(
                source, piece(slot(at, chip, core), part), to_other(chip, core), over_out.at[at, part], over_in.at[at, part]
            )

        def pair(source, at, c, part):
            return remote(
                source,
                piece(slot(at, c, core), part),
                to_partner(chip, core),
                pair_out.at[c, at, part],
                pair_in.at[c, at, part],
            )

        mine = slot(spot, chip, core)
        for part in range(parts):
            source = first(part)
            pair(source, spot, chip, part).start()
            over(source, spot, part).start()
            pl.when(spot < spots - 1)(lambda: up(source, spot, part, 0).start())
            pl.when(spot > 0)(lambda: down(source, spot, part, 0).start())
        own = pltpu.make_async_copy(x_ref, o_ref.at[mine], own_sem.at[0])
        own.start()
        own.wait()
        ranks = ranked_spots(spots, spot)
        order = arrival_order(spots)

        def hand_on(reach):
            for part in range(parts):

                def below(part=part):
                    at = spot - reach
                    source = piece(slot(at, chip, core), part)
                    up(source, at, part, reach - 1).wait_recv()
                    pl.when(spot < spots - 1)(lambda: up(source, at, part, reach).start())
                    over(source, at, part).start()
                    pair(source, at, chip, part).start()

                def above(part=part):
                    at = spot + reach
                    source = piece(slot(at, chip, core), part)
                    down(source, at, part, reach - 1).wait_recv()
                    pl.when(spot > 0)(lambda: down(source, at, part, reach).start())
                    over(source, at, part).start()
                    pair(source, at, chip, part).start()

                pl.when(spot >= reach)(below)
                pl.when(spot + reach < spots)(above)

        def arrive(rank, across):
            at = ranks[rank]
            if across:
                for part in range(parts):
                    source = piece(slot(at, 1 - chip, core), part)
                    over(source, at, part).wait_recv()
                    pair(source, at, 1 - chip, part).start()
                for part in range(parts):
                    pair(first(part), at, 1 - chip, part).wait_recv()
                return
            if rank > 0:
                hand_on(rank)
            for part in range(parts):
                pair(first(part), at, chip, part).wait_recv()

        def window(ref, kind, at, c):
            if kind:
                return ref.at[:, pl.ds(pl.multiple_of(c * tile, tile), tile)]
            return ref.at[pl.ds(pl.multiple_of((at * 2 + c) * tile, tile), tile)]

        def outward(index, which, at, c):
            return pltpu.make_async_copy(
                result_tiles[index].at[which], window(results[index], result_kinds[index], at, c), out_sem.at[which, index]
            )

        def step(number, carry):
            for position, (rank, across) in enumerate(order):
                pl.when(number == position)(functools.partial(arrive, rank, across))
            at = pick(number, [ranks[rank] for rank, _ in order])
            c = pick(number, [1 - chip if across else chip for _, across in order])
            inside = at == spot
            inputs = [pltpu.make_async_copy(o_ref.at[pl.ds(slot(at, c, 0), 2)], x_tile, tile_sem.at[0])]
            for index, kind in enumerate(source_kinds):
                if not kind:
                    inputs.append(
                        pltpu.make_async_copy(
                            window(sources[index], kind, at, c), source_tiles[index], tile_sem.at[1 + index]
                        )
                    )
            for copy in inputs:
                copy.start()
            for index, kind in enumerate(source_kinds):
                if kind:

                    def fetch(index=index, kind=kind):
                        copy = pltpu.make_async_copy(
                            window(sources[index], kind, at, c), source_tiles[index], tile_sem.at[1 + index]
                        )
                        copy.start()
                        copy.wait()

                    pl.when(inside)(fetch)

            @pl.when(number == 0)
            def _():
                for copy in loads:
                    copy.wait()

            which = lax.rem(number, 2)

            @pl.when(number >= 2)
            def _():
                for index, kind in enumerate(result_kinds):
                    if not kind:
                        outward(index, which, at, c).wait()

            for copy in inputs:
                copy.wait()
            body(
                inside,
                [x_tile[...].reshape(tile, x_tile.shape[2]), small_ref, *source_tiles],
                weights,
                [target.at[which] for target in result_tiles],
                scratch,
            )
            for index, kind in enumerate(result_kinds):
                if kind:

                    def put(index=index):
                        copy = outward(index, which, at, c)
                        copy.start()
                        copy.wait()

                    pl.when(inside)(put)
                else:
                    outward(index, which, at, c).start()
            return carry

        lax.fori_loop(0, 2 * spots, step, 0)
        for which in range(2):
            for index, kind in enumerate(result_kinds):
                if not kind:
                    outward(index, which, spot, chip).wait()
        for part in range(parts):
            for at in range(spots):
                over(first(part), at, part).wait_send()
                for c in range(2):
                    pair(first(part), at, c, part).wait_send()
            for reach in range(spots - 1):
                pl.when((spot >= reach) & (spot < spots - 1))(lambda: up(first(part), spot, part, reach).wait_send())
                pl.when((spot + reach < spots) & (spot > 0))(lambda: down(first(part), spot, part, reach).wait_send())

    pl.when(lax.axis_index(SECTION) == active)(run)


def fused_call(tiles, rows_in, number, active, body, small, sources, weights, results, gathered, into, scratch=(), parts=4):
    spots = lax.axis_size(PACKS)
    block, width = rows_in.shape
    tile = 2 * block
    dma = pltpu.SemaphoreType.DMA
    hops = max(spots - 1, 1)
    anywhere = pl.BlockSpec(memory_space=pl.ANY)
    inside = pl.BlockSpec(memory_space=pltpu.VMEM)
    shapes = [jax.ShapeDtypeStruct((spots * 4, block, width), rows_in.dtype), *(shape for shape, _ in results)]
    held = [gathered.reshape(shapes[0].shape), *into]
    pieces = [piece for weight in weights for piece in weight]
    first = 2 + len(sources) + len(pieces)

    def hold(array, kind, *lead):
        shape = (2, tile, array.shape[2]) if kind else (tile, array.shape[1])
        return pltpu.VMEM((*lead, *shape), array.dtype)

    outs = pl.pallas_call(
        functools.partial(
            fused_kernel,
            spots,
            parts,
            active,
            body,
            ([kind for _, kind in sources], [kind for _, kind in results]),
            [len(weight) for weight in weights],
            len(held),
        ),
        out_shape=shapes,
        in_specs=[inside, inside, *([anywhere] * (len(sources) + len(pieces) + len(held)))],
        out_specs=[anywhere] * len(shapes),
        input_output_aliases={first + index: index for index in range(len(held))},
        scratch_shapes=[
            pltpu.VMEM((2, block, width), rows_in.dtype),
            *(hold(array, kind) for array, kind in sources),
            *(hold(shape, kind, 2) for shape, kind in results),
            *(hold_weight(weight) for weight in weights),
            dma((1,)),
            dma((len(pieces),)),
            dma((1 + len(sources),)),
            dma((2, len(results))),
            dma((hops, parts)),
            dma((hops, parts)),
            dma((hops, parts)),
            dma((hops, parts)),
            dma((spots, parts)),
            dma((spots, parts)),
            dma((2, spots, parts)),
            dma((2, spots, parts)),
            *scratch,
        ],
        compiler_params=pltpu.CompilerParams(collective_id=number, has_side_effects=True),
        name=f"fused{number}",
    )(rows_in, small, *(array for array, _ in sources), *pieces, *held)
    return outs[0].reshape(-1, width), list(outs[1:])


def body(
    boundary,
    lengths,
    routes,
    attn_gain,
    query_weight,
    compress_weight,
    latent_gain,
    expand_weight,
    output_weight,
    ffn_gain,
    router_weight,
    shared_in,
    shared_out,
    expert_in,
    expert_out,
):
    attn_gain, latent_gain, ffn_gain = attn_gain[0], latent_gain[0], ffn_gain[0]
    query_weight, compress_weight = query_weight[0], compress_weight[0]
    expand_weight, output_weight = expand_weight[0], output_weight[0]
    router_weight, shared_out, expert_out = router_weight[0], shared_out[0], expert_out[0, 0]
    width = boundary.shape[3]
    rows = boundary.shape[2]
    half = shared_out.shape[0]
    units = expert_out.shape[0]
    experts_count = router_weight.shape[1]
    shared_in_t = jnp.transpose(shared_in[0], (1, 2, 0)).reshape(2 * half, width)
    joined_in = (
        expert_in.reshape(width, 2 * units),
        jnp.pad(router_weight, ((0, 0), (0, -experts_count % 128))),
    )
    joined_width = sum(piece.shape[1] for piece in joined_in)

    packs, members = lax.axis_size(PACKS), lax.axis_size(MEMBERS)
    count = packs * members
    pack, member = lax.axis_index(PACKS), lax.axis_index(MEMBERS)
    me = pack * members + member
    is_first = lax.axis_index(SECTION) == 0
    pack_rows = members * rows
    all_rows = count * rows
    heads = output_weight.shape[0] // VD
    top = routes.shape[3]
    tiles = [Tiles(all_rows, pack_rows, pack, active) for active in range(2)]
    fusing = members == 4 and tiles[0].tile == 2 * rows

    def own_pack(value):
        size = value.shape[0] // packs
        return lax.dynamic_slice_in_dim(value, pack * size, size, 0)

    freqs = rope_base ** (-jnp.arange(HALF, dtype=jnp.float32) / HALF)
    angles = jnp.arange(rows, dtype=jnp.float32)[:, None] * freqs[None, :]
    turns = jnp.concatenate([jnp.cos(angles), jnp.sin(angles)], axis=1)

    def tables_of(block_lengths):
        segment, position = block_layout(block_lengths, rows)
        blocks = segment.shape[0]
        chosen = position.reshape(-1)[:, None] == jnp.arange(rows, dtype=jnp.int32)[None, :]
        found = jnp.dot(
            chosen.astype(jnp.float32),
            turns,
            precision=lax.Precision.HIGHEST,
            preferred_element_type=jnp.float32,
        )
        return (
            found[:, :HALF],
            found[:, HALF:],
            segment.reshape(blocks * rows, 1),
            segment.reshape(blocks, 1, rows),
        )

    own_lengths = lax.dynamic_index_in_dim(lengths[0, 0], member, 0, keepdims=False)
    layout = jnp.concatenate(
        [
            jnp.transpose(routes[0, 0]),
            jnp.pad(own_lengths, (0, rows - own_lengths.shape[0]))[None],
            jnp.zeros((-(top + 1) % 8, rows), jnp.int32),
        ],
        axis=0,
    )


    def routed_of(layout_all):
        named = layout_all.reshape(count, -1, rows)[:, :top] == me
        return jnp.any(named, axis=1).astype(jnp.float32).reshape(all_rows, 1)

    tables_pack = tables_of(lengths[0, 0])
    tables_own = tables_of(own_lengths[None])
    own_cos, own_sin = tables_own[:2]
    own_column = (lax.broadcasted_iota(jnp.int32, (1, experts_count), 1) == me).astype(jnp.float32)

    def inputs_of(hidden):
        normed32, scale_attn = rms_forward(hidden, attn_gain)
        normed = bf16(normed32)
        compressed = dot(normed, compress_weight)
        latent32, scale_latent = rms_forward(compressed[:, :LAT], latent_gain)
        keyed = bf16(
            jnp.concatenate([latent32, rotate(compressed[:, LAT:], own_cos, own_sin)], axis=1)
        )
        return normed, keyed, (compressed, scale_attn, scale_latent)

    def run_experts(section, x, routed, gathered, into, number, full):
        at = tiles[section]
        results = [
            at.result(2 * units),
            at.result(units),
            at.result(experts_count, jnp.float32),
            at.pack_result(half),
        ]
        weights = [joined_in, (shared_in_t,)]
        if full:
            results.append(at.result(width))
            weights += [(expert_out,), (shared_out,)]
        if fusing:
            shapes = [(shape, index == 3) for index, (shape, _) in enumerate(results)]
            return fused_call(
                at, x, number, section, experts_body, own_column, [(routed, False)], weights, shapes, gathered, into
            )
        (x_all,) = gather_blocks([x], True, number, section, [gathered])
        return x_all, at.call(
            tiled(experts_body),
            "experts",
            [(x_all, at.source(width)), (own_column, at.small(own_column)), (routed, at.source(1))],
            weights,
            results,
            into[:4],
        )

    def run_experts_back(section, grad, routed, stored, gathered, into, number):
        at = tiles[section]
        pre, _, prob, shared_pre = stored
        weights = [joined_in, (shared_in_t,), (expert_out,), (shared_out,)]
        results = [at.result(2 * units), at.result(1, jnp.float32), at.result(width)]
        scratch = [pltpu.VMEM((at.tile, joined_width), jnp.bfloat16)]
        if fusing and number is not None:
            shapes = [(shape, False) for shape, _ in results]
            sources = [(pre, False), (prob, False), (routed, False), (shared_pre, True)]
            return fused_call(
                at, grad, number, section, experts_back_body, own_column, sources, weights, shapes, gathered, into, scratch
            )
        grad_all = gathered
        if number is not None:
            (grad_all,) = gather_blocks([grad], True, number, section, [gathered])
        return grad_all, at.call(
            tiled(experts_back_body),
            "experts_back",
            [
                (grad_all, at.source(width)),
                (own_column, at.small(own_column)),
                (pre, at.source(2 * units)),
                (prob, at.source(experts_count)),
                (routed, at.source(1)),
                (shared_pre, at.pack_source(half)),
            ],
            weights,
            results,
            into,
            scratch,
            flops=6 * all_rows * width * units,
        )

    def prepare(section, normed_all, keyed_all, ffn_all, tables, into):
        at = tiles[section]
        cosine, sine, seg_col, seg_row = tables
        blocks = at.tile // rows
        row_spec = pl.BlockSpec((blocks, 1, rows), lambda i, control: (i * control[2], 0, 0))
        found = at.call(
            tiled(functools.partial(heads_body, rows)),
            "heads",
            [
                (normed_all, at.source(width)),
                (keyed_all, at.source(LAT + ROPE)),
                (cosine, at.source(HALF)),
                (sine, at.source(HALF)),
                (seg_col, at.source(1)),
                (seg_row, row_spec),
            ],
            [(query_weight,), (expand_weight,)],
            [at.result(heads * VD), at.result(heads * QK), at.result(heads * KV)],
            into[:3],
            [pltpu.VMEM((at.tile, heads * QK), jnp.float32)],
            flops=4 * all_rows * width * heads * QK,
        )
        shared = at.call(
            tiled(shared_body),
            "shared",
            [(ffn_all, at.source(width))],
            [(shared_in_t,)],
            [at.pair_result(half), at.result(half)],
            into[3:],
            flops=4 * all_rows * width * half,
        )
        return [*found, *shared]

    fresh = boundary[0, 0].astype(jnp.float32)

    normed, keyed, _ = inputs_of(fresh)
    normed_pack, keyed_pack, layout_all = gather_blocks(
        [normed, keyed, layout], True, 0, 0, wide=[False, False, True]
    )
    attended, _ = attend(
        dot(normed_pack, query_weight),
        bf16(dot(keyed_pack[:, :LAT], expand_weight)),
        keyed_pack,
        tables_pack,
    )
    mixed_first = fresh + scatter_blocks(bf16(dot(attended, output_weight)), rows, False, 1, 0)
    empty = [
        blank((all_rows, width), jnp.bfloat16),
        *(
            blank(shape, dtype)
            for shape, dtype in (
                ((all_rows + tiles[0].tile, 2 * units), jnp.bfloat16),
                ((all_rows + tiles[0].tile, units), jnp.bfloat16),
                ((all_rows + tiles[0].tile, experts_count), jnp.float32),
                ((2, pack_rows + tiles[0].tile, half), jnp.bfloat16),
            )
        ),
    ]
    ffn_all, (*stored, partial) = run_experts(
        0, bf16(rms_forward(mixed_first, ffn_gain)[0]), routed_of(layout_all), empty[0], empty[1:], 2, True
    )
    result_first = mixed_first + scatter_blocks(partial, rows, True, 3, 0)
    heads_weights = spread_blocks([query_weight, expand_weight, output_weight], 4, 1)
    target_all, layout_all = gather_blocks(
        [boundary[0, 0], layout], True, 5, 1, [blank((all_rows, width), jnp.bfloat16), layout_all]
    )
    sent, target_all, layout_all, heads_weights = lax.optimization_barrier(
        (bf16(result_first), target_all, layout_all, heads_weights)
    )
    inbound = lax.ppermute(sent, SECTION, [(0, 1)])
    routed = routed_of(layout_all)
    tables_all = tables_of(layout_all.reshape(count, -1, rows)[:, top, : lengths.shape[3]])
    query_heads, expand_heads, output_heads = (
        value.reshape(members, -1, value.shape[1]) for value in heads_weights
    )

    hidden = jnp.where(is_first, fresh, inbound.astype(jnp.float32))
    normed, keyed, (compressed, scale_attn, scale_latent) = inputs_of(hidden)
    latent = bf16(jnp.einsum("rd,mdc->mrc", keyed[:, :LAT], expand_heads, preferred_element_type=jnp.float32))
    latent = latent.reshape(members * rows, -1)
    query_raw = jnp.einsum("rd,mdc->mrc", normed, query_heads, preferred_element_type=jnp.float32)
    attended, query = attend(query_raw.reshape(members * rows, -1), latent, keyed, tables_own, members)
    mixed = hidden + jnp.einsum(
        "mrc,mcd->rd", attended.reshape(members, rows, -1), output_heads, preferred_element_type=jnp.float32
    )
    mixed = jnp.where(is_first, mixed_first, mixed)
    ffn32, scale_ffn = rms_forward(mixed, ffn_gain)
    ffn_all, stored = run_experts(1, bf16(ffn32), routed, ffn_all, stored, 6, False)

    def latent_back(own):
        grad_latent, grad_latent_gain = rms_backward(
            compressed[:, :LAT], scale_latent, latent_gain, own[:, width : width + LAT]
        )
        grad_compressed = bf16(
            jnp.concatenate([grad_latent, rotate(own[:, width + LAT :], own_cos, -own_sin)], axis=1)
        )
        grad_normed = own[:, :width] + dot_t(grad_compressed, compress_weight)
        grad_hidden_norm, grad_attn_gain = rms_backward(hidden, scale_attn, attn_gain, grad_normed)
        return grad_compressed, grad_hidden_norm, grad_attn_gain, grad_latent_gain

    _, (*grad_units, partial) = run_experts_back(1, None, routed, stored, target_all, (), None)
    grad_ffn_second = scatter_blocks(partial, rows, True, 7, 1)
    grad_mixed = fresh + rms_backward(mixed, scale_ffn, ffn_gain, grad_ffn_second)[0]
    grad_attended = jnp.einsum(
        "rd,mcd->mrc", bf16(grad_mixed), output_heads, preferred_element_type=jnp.float32
    )
    grad_query, grad_latent_heads, grad_shared_key = attend_back(
        query, latent, keyed, bf16(grad_attended).reshape(members * rows, -1), tables_own, members
    )
    own_second = jnp.concatenate(
        [
            jnp.einsum(
                "mrc,mdc->rd",
                grad_query.reshape(members, rows, -1),
                query_heads,
                preferred_element_type=jnp.float32,
            ),
            jnp.einsum(
                "mrc,mdc->rd",
                grad_latent_heads.reshape(members, rows, -1),
                expand_heads,
                preferred_element_type=jnp.float32,
            ),
            jnp.sum(grad_shared_key.reshape(members, rows, -1), axis=0),
        ],
        axis=1,
    )
    grad_second = bf16(grad_mixed + latent_back(own_second)[1])

    all_inputs = gather_blocks([normed, keyed], True, 8, 0)
    prepared = prepare(0, *all_inputs, ffn_all, tables_all, ())
    grad_second, prepared, all_inputs = lax.optimization_barrier((grad_second, prepared, all_inputs))
    downbound = lax.ppermute(grad_second, SECTION, [(1, 0)]).astype(jnp.float32)

    normed_late, keyed_late, gated_late, _ = lax.optimization_barrier((normed, keyed, stored[1], grad_second))
    at = tiles[1]
    finished = at.call(
        tiled(finish_body),
        "finish",
        [(gated_late, at.source(units)), (stored[3], at.pack_source(half))],
        [(expert_out,), (shared_out,)],
        [at.result(width)],
        flops=2 * all_rows * width * units,
    )
    upstream = jnp.where(is_first, downbound, fresh)
    upstream_all, (grad_pre, moved, partial) = run_experts_back(
        0, bf16(upstream), routed, stored, target_all, [*grad_units, *finished], 11
    )
    summed = scatter_blocks(partial, rows, True, 12)
    result = mixed + summed
    grad_ffn = jnp.where(is_first, summed, grad_ffn_second)
    normed_late, keyed_late, _ = lax.optimization_barrier((normed_late, keyed_late, summed))
    normed_all, keyed_all = gather_blocks([normed_late, keyed_late], True, 9, 1, all_inputs)
    prepared = prepare(1, normed_all, keyed_all, ffn_all, tables_all, prepared)
    attended_all, query_all, latent_all, shared_pre, shared_hid = prepared
    attended_all, shared_hid = attended_all[:all_rows], shared_hid[:all_rows]
    grad_mixed_norm, grad_ffn_gain = rms_backward(mixed, scale_ffn, ffn_gain, grad_ffn)
    grad_mixed = upstream + grad_mixed_norm
    grad_mixed_all = lax.all_gather(bf16(grad_mixed), BOTH, axis=0, tiled=True)
    grad_attended = bf16(dot_t(grad_mixed_all, output_weight))
    grad_query, grad_latent_heads, grad_shared_key = attend_back(
        query_all, latent_all, keyed_all, grad_attended, tables_all
    )
    own = lax.psum_scatter(
        bf16(
            jnp.concatenate(
                [
                    dot_t(own_pack(grad_query), query_weight),
                    dot_t(own_pack(grad_latent_heads), expand_weight),
                    own_pack(grad_shared_key),
                ],
                axis=1,
            )
        ),
        MEMBERS,
        scatter_dimension=0,
        tiled=True,
    ).astype(jnp.float32)
    grad_compressed, grad_hidden_norm, grad_attn_gain, grad_latent_gain = latent_back(own)
    grad_hidden = grad_mixed + grad_hidden_norm

    small = jnp.concatenate([grad_attn_gain, grad_latent_gain, grad_ffn_gain, moved[:all_rows, 0]])
    small = jnp.pad(small, (0, -small.shape[0] % 1024)).reshape(8, -1)
    grad_compressed_all, small_all = gather_blocks([grad_compressed, small], True, 13)
    small_all = small_all.reshape(count, -1)
    gains = jnp.sum(small_all[:, : 2 * width + LAT], axis=0)
    moved_all = small_all[:, 2 * width + LAT : 2 * width + LAT + all_rows].T
    prob = stored[2][:all_rows]
    grad_logits = bf16(moved_all - prob * jnp.sum(moved_all, axis=1, keepdims=True))
    left, right = gated_back(
        shared_pre[0, :all_rows].astype(jnp.float32),
        shared_pre[1, :all_rows].astype(jnp.float32),
        dot_t(upstream_all, shared_out),
    )
    grad_shared_in = lax.dot_general(
        jnp.stack([left, right]), ffn_all, (((1,), (0,)), ((), ())), preferred_element_type=jnp.float32
    )
    ends = jnp.where(is_first, grad_hidden, result)
    return (
        ends[None, None],
        gains[:width][None],
        t_dot(normed_all, grad_query)[None],
        t_dot(normed_all, grad_compressed_all)[None],
        gains[width : width + LAT][None],
        t_dot(keyed_all[:, :LAT], grad_latent_heads)[None],
        t_dot(attended_all, grad_mixed_all)[None],
        gains[width + LAT :][None],
        t_dot(ffn_all, grad_logits)[None],
        jnp.transpose(grad_shared_in, (2, 0, 1))[None],
        t_dot(shared_hid, upstream_all)[None],
        pair_grad(ffn_all, grad_pre)[None, None],
        t_dot(stored[1][:all_rows], upstream_all)[None, None],
    )


def solution(mesh):
    return jax.shard_map(
        body,
        mesh=mesh,
        in_specs=(
            P(SECTION, None, BOTH, None),
            P(None, PACKS, None, None),
            P(SECTION, None, BOTH, None),
            P(SECTION, None),
            P(SECTION, None, MEMBERS),
            P(SECTION, None, None),
            P(SECTION, None),
            P(SECTION, None, MEMBERS),
            P(SECTION, MEMBERS, None),
            P(SECTION, None),
            P(SECTION, None, None),
            P(SECTION, None, None, MEMBERS),
            P(SECTION, MEMBERS, None),
            P(SECTION, BOTH, None, None, None),
            P(SECTION, BOTH, None, None),
        ),
        out_specs=(
            P(SECTION, None, BOTH, None),
            P(SECTION, None),
            P(SECTION, None, MEMBERS),
            P(SECTION, None, None),
            P(SECTION, None),
            P(SECTION, None, MEMBERS),
            P(SECTION, MEMBERS, None),
            P(SECTION, None),
            P(SECTION, None, None),
            P(SECTION, None, None, MEMBERS),
            P(SECTION, MEMBERS, None),
            P(SECTION, BOTH, None, None, None),
            P(SECTION, BOTH, None, None),
        ),
        check_vma=False,
    )
```

```python
import functools

import jax
import jax.numpy as jnp
from jax import lax
from jax.experimental import pallas as pl
from jax.experimental.pallas import tpu as pltpu
from jax.sharding import PartitionSpec as P

NOPE = 128
ROPE = 64
VD = 128
LAT = 512

QK = NOPE + ROPE
KV = NOPE + VD
HALF = ROPE // 2
epsilon = 1e-06
rope_base = 10000.0
masked_score = -1e30
SECTION, PACKS, MEMBERS = "section", "dp", "expert"
BOTH = (PACKS, MEMBERS)
MESH = pl.DeviceIdType.MESH
def dot(left, right):
    return jnp.dot(left, right, preferred_element_type=jnp.float32)


def dot_t(left, right):
    return lax.dot_general(
        left, right, (((1,), (1,)), ((), ())), preferred_element_type=jnp.float32
    )


def t_dot(left, right):
    return lax.dot_general(
        left, right, (((0,), (0,)), ((), ())), preferred_element_type=jnp.float32
    )


def bf16(value):
    return value.astype(jnp.bfloat16)


def rms_forward(inputs, gain_vec):
    norm_scale = lax.rsqrt(jnp.mean(inputs * inputs, axis=-1, keepdims=True) + epsilon)
    return (inputs * norm_scale * gain_vec, norm_scale)


def rms_backward(inputs, norm_scale, gain_vec, upstream):
    weighted = upstream * gain_vec
    grad_gain = jnp.sum(upstream * inputs * norm_scale, axis=0)
    cubed = norm_scale * norm_scale * norm_scale
    grad_inputs = norm_scale * weighted - inputs * cubed * jnp.mean(
        weighted * inputs, axis=-1, keepdims=True
    )
    return (grad_inputs, grad_gain)


def rotate(inputs, cosine, sine):
    half = cosine.shape[-1]
    former = inputs[..., :half]
    latter = inputs[..., half:]
    return jnp.concatenate(
        [former * cosine - latter * sine, latter * cosine + former * sine], axis=-1
    )


def silu_parts(pre_gate):
    sigmoid = jax.nn.sigmoid(pre_gate)
    return (pre_gate * sigmoid, sigmoid * (1.0 + pre_gate * (1.0 - sigmoid)))


def block_layout(block_lengths, rows):
    index = lax.broadcasted_iota(jnp.int32, (block_lengths.shape[0], rows), 1)
    start, segment, opening = 0, 0, 0
    for sequence in range(block_lengths.shape[1]):
        begun = index >= start
        segment = segment + begun.astype(jnp.int32)
        opening = jnp.where(begun, start, opening)
        start = start + block_lengths[:, sequence : sequence + 1]
    return segment, index - opening


def places(spots):
    member = lax.axis_index(MEMBERS)
    spot = lax.axis_index(PACKS) if spots > 1 else 0
    return spot, member // 2, lax.rem(member, 2)


def to_partner(chip, core):
    return {MEMBERS: chip * 2 + 1 - core}


def to_other(chip, core):
    return {MEMBERS: (1 - chip) * 2 + core}


def when(condition, action):
    if condition is True:
        action()
    else:
        pl.when(condition)(action)


def greet(spots, spot, chip, core):
    barrier = pltpu.get_barrier_semaphore()

    def signal(target):
        pl.semaphore_signal(barrier, inc=1, device_id=target, device_id_type=MESH)

    signal(to_partner(chip, core))
    signal(to_other(chip, core))
    if spots > 1:
        pl.when(spot > 0)(lambda: signal({PACKS: spot - 1}))
        pl.when(spot < spots - 1)(lambda: signal({PACKS: spot + 1}))
        ends = jnp.where(spot > 0, 1, 0) + jnp.where(spot < spots - 1, 1, 0)
        pl.semaphore_wait(barrier, 2 + ends)
    else:
        pl.semaphore_wait(barrier, 2)


def remote(source, target_ref, target, out_sem, in_sem):
    return pltpu.make_async_remote_copy(
        src_ref=source,
        dst_ref=target_ref,
        send_sem=out_sem,
        recv_sem=in_sem,
        device_id=target,
        device_id_type=MESH,
    )


def slot(spot, chip, core):
    return spot * 4 + chip * 2 + core


def gather_kernel(spots, cuts, wide, active, *refs):
    arrays = len(cuts)
    x_refs, o_refs, sems = refs[:arrays], refs[-9 - arrays : -9], refs[-9:]
    own_sem, up_out, up_in, down_out, down_in, over_out, over_in, pair_out, pair_in = sems
    units = [
        (a, pl.ds(part * (x_refs[a].shape[0] // parts), x_refs[a].shape[0] // parts))
        for a, parts in enumerate(cuts)
        for part in range(parts)
    ]

    def run():
        spot, chip, core = places(spots)
        greet(spots, spot, chip, core)

        def piece(unit, index):
            array, cut = units[unit]
            return o_refs[array].at[index, cut]

        def first(unit):
            array, cut = units[unit]
            return x_refs[array].at[cut]

        def lane(unit):
            return wide[units[unit][0]]

        def spread(unit):
            return range(spots) if lane(unit) else [0]

        def up(source, at, unit, reach):
            return remote(
                source, piece(unit, slot(at, chip, core)), {PACKS: spot + 1}, up_out.at[reach, unit], up_in.at[reach, unit]
            )

        def down(source, at, unit, reach):
            return remote(
                source,
                piece(unit, slot(at, chip, core)),
                {PACKS: spot - 1},
                down_out.at[reach, unit],
                down_in.at[reach, unit],
            )

        def over(source, at, unit):
            return remote(
                source, piece(unit, slot(at, chip, core)), to_other(chip, core), over_out.at[at, unit], over_in.at[at, unit]
            )

        def pair(source, at, c, unit):
            return remote(
                source,
                piece(unit, slot(at, c, core)),
                to_partner(chip, core),
                pair_out.at[c, at, unit],
                pair_in.at[c, at, unit],
            )

        home = lambda unit: spot if lane(unit) else 0
        for unit in range(len(units)):
            source = first(unit)
            over(source, home(unit), unit).start()
            if spots > 1 and lane(unit):
                pl.when(spot < spots - 1)(lambda: up(source, spot, unit, 0).start())
                pl.when(spot > 0)(lambda: down(source, spot, unit, 0).start())
            pair(source, home(unit), chip, unit).start()
        own = [
            pltpu.make_async_copy(
                x_refs[a], o_refs[a].at[slot(spot if wide[a] else 0, chip, core)], own_sem.at[a]
            )
            for a in range(arrays)
        ]
        for copy in own:
            copy.start()
        for reach in range(1, spots):
            for unit in range(len(units)):
                if not lane(unit):
                    continue

                def below(reach=reach, unit=unit):
                    at = spot - reach
                    source = piece(unit, slot(at, chip, core))
                    up(source, at, unit, reach - 1).wait_recv()
                    pl.when(spot < spots - 1)(lambda: up(source, at, unit, reach).start())
                    over(source, at, unit).start()
                    pair(source, at, chip, unit).start()

                def above(reach=reach, unit=unit):
                    at = spot + reach
                    source = piece(unit, slot(at, chip, core))
                    down(source, at, unit, reach - 1).wait_recv()
                    pl.when(spot > 0)(lambda: down(source, at, unit, reach).start())
                    over(source, at, unit).start()
                    pair(source, at, chip, unit).start()

                pl.when(spot >= reach)(below)
                pl.when(spot + reach < spots)(above)
        for reach in range(spots):
            sides = [(True, spot)]
            if reach > 0:
                sides = [(spot >= reach, spot - reach), (spot + reach < spots, spot + reach)]
            for unit in range(len(units)):
                if not lane(unit) and reach > 0:
                    continue
                for there, at in sides:
                    at = at if lane(unit) else 0

                    def hand_on(at=at, unit=unit):
                        source = piece(unit, slot(at, 1 - chip, core))
                        over(source, at, unit).wait_recv()
                        pair(source, at, 1 - chip, unit).start()

                    when(there, hand_on)
        for copy in own:
            copy.wait()
        for unit in range(len(units)):
            source = first(unit)
            for at in spread(unit):
                over(source, at, unit).wait_send()
                for c in range(2):
                    pair(source, at, c, unit).wait()
            for reach in range(spots - 1 if lane(unit) else 0):
                pl.when((spot >= reach) & (spot < spots - 1))(lambda: up(source, spot, unit, reach).wait_send())
                pl.when((spot + reach < spots) & (spot > 0))(lambda: down(source, spot, unit, reach).wait_send())

    if active is None:
        run()
    else:
        pl.when(lax.axis_index(SECTION) == active)(run)


def gather_blocks(values, across, number, active=None, into=None, parts=4, wide=None):
    wide = [across] * len(values) if wide is None else wide
    if lax.axis_size(MEMBERS) != 4:
        found = [
            lax.all_gather(value, BOTH if far else MEMBERS, axis=0, tiled=True) for value, far in zip(values, wide)
        ]
        if into is None:
            return found
        chosen = lax.axis_index(SECTION) == active
        return [jnp.where(chosen, new, old) for new, old in zip(found, into)]
    spots = lax.axis_size(PACKS) if across else 1
    cuts = [parts if value.shape[0] % (16 * parts) == 0 else 1 for value in values]
    units = sum(cuts)
    dma = pltpu.SemaphoreType.DMA
    hops = max(spots - 1, 1)
    shapes = [
        jax.ShapeDtypeStruct(((spots if far else 1) * 4, *value.shape), value.dtype)
        for value, far in zip(values, wide)
    ]
    held = [] if into is None else [old.reshape(shape.shape) for old, shape in zip(into, shapes)]
    outs = pl.pallas_call(
        functools.partial(gather_kernel, spots, cuts, wide, active),
        out_shape=shapes,
        in_specs=[pl.BlockSpec(memory_space=pltpu.VMEM)] * len(values)
        + [pl.BlockSpec(memory_space=pl.ANY)] * len(held),
        out_specs=[pl.BlockSpec(memory_space=pl.ANY)] * len(values),
        input_output_aliases={len(values) + index: index for index in range(len(held))},
        scratch_shapes=[
            dma((len(values),)),
            dma((hops, units)),
            dma((hops, units)),
            dma((hops, units)),
            dma((hops, units)),
            dma((spots, units)),
            dma((spots, units)),
            dma((2, spots, units)),
            dma((2, spots, units)),
        ],
        compiler_params=pltpu.CompilerParams(collective_id=number, has_side_effects=True),
        name=f"gather{number}",
    )(*values, *held)
    return [out.reshape(-1, out.shape[2]) for out in outs]


def spread_kernel(cuts, active, *refs):
    arrays = len(cuts)
    x_refs, o_refs = refs[:arrays], refs[arrays : 2 * arrays]
    own_sem, over_out, over_in, side_out, side_in, pair_out, pair_in = refs[2 * arrays :]
    units = [
        (a, pl.ds(part * (x_refs[a].shape[0] // parts), x_refs[a].shape[0] // parts))
        for a, parts in enumerate(cuts)
        for part in range(parts)
    ]

    def run():
        member, spot = lax.axis_index(MEMBERS), lax.axis_index(PACKS)
        chip, core, odd = member // 2, lax.rem(member, 2), lax.rem(spot, 2)
        beside = {PACKS: spot + 1 - 2 * odd}
        barrier = pltpu.get_barrier_semaphore()
        for target in (to_partner(chip, core), to_other(chip, core), beside):
            pl.semaphore_signal(barrier, inc=1, device_id=target, device_id_type=MESH)
        pl.semaphore_wait(barrier, 3)

        def piece(unit, c):
            array, cut = units[unit]
            return o_refs[array].at[c * 2 + core, cut]

        def first(unit):
            array, cut = units[unit]
            return x_refs[array].at[cut]

        def over(unit):
            return remote(first(unit), piece(unit, chip), to_other(chip, core), over_out.at[unit], over_in.at[unit])

        def side(unit):
            source = piece(unit, 1 - chip)
            return remote(source, source, beside, side_out.at[unit], side_in.at[unit])

        def pair(source, unit, c, index):
            return remote(
                source, piece(unit, c), to_partner(chip, core), pair_out.at[index, unit], pair_in.at[index, unit]
            )

        for unit in range(len(units)):
            pl.when(odd == unit % 2)(lambda: over(unit).start())
        for unit in range(len(units)):
            pair(first(unit), unit, chip, 0).start()
        own = [
            pltpu.make_async_copy(x_refs[a], o_refs[a].at[member], own_sem.at[a]) for a in range(arrays)
        ]
        for copy in own:
            copy.start()
        for unit in range(len(units)):

            def taken(unit=unit):
                over(unit).wait_recv()
                side(unit).start()
                pair(piece(unit, 1 - chip), unit, 1 - chip, 1).start()

            pl.when(odd == unit % 2)(taken)
        for unit in range(len(units)):

            def handed(unit=unit):
                side(unit).wait_recv()
                pair(piece(unit, 1 - chip), unit, 1 - chip, 1).start()

            pl.when(odd != unit % 2)(handed)
        for copy in own:
            copy.wait()
        for unit in range(len(units)):

            def sent(unit=unit):
                over(unit).wait_send()
                side(unit).wait_send()

            pl.when(odd == unit % 2)(sent)
            pair(first(unit), unit, chip, 0).wait()
            pair(first(unit), unit, 1 - chip, 1).wait()

    pl.when(lax.axis_index(SECTION) == active)(run)


def spread_blocks(values, number, active, parts=8):
    if lax.axis_size(MEMBERS) != 4 or lax.axis_size(PACKS) % 2:
        return gather_blocks(values, False, number, active)
    units = parts * len(values)
    dma = pltpu.SemaphoreType.DMA
    outs = pl.pallas_call(
        functools.partial(spread_kernel, [parts] * len(values), active),
        out_shape=[jax.ShapeDtypeStruct((4, *value.shape), value.dtype) for value in values],
        in_specs=[pl.BlockSpec(memory_space=pltpu.VMEM)] * len(values),
        out_specs=[pl.BlockSpec(memory_space=pl.ANY)] * len(values),
        scratch_shapes=[
            dma((len(values),)),
            dma((units,)),
            dma((units,)),
            dma((units,)),
            dma((units,)),
            dma((2, units)),
            dma((2, units)),
        ],
        compiler_params=pltpu.CompilerParams(collective_id=number, has_side_effects=True),
        name=f"spread{number}",
    )(*values)
    return [out.reshape(-1, out.shape[2]) for out in outs]


def add_into(target, sources, rows, step=16):
    def some(index, carry):
        at = pl.ds(pl.multiple_of(index * step, step), step)
        total = sources[0][at, :].astype(jnp.float32)
        for source in sources[1:]:
            total = total + source[at, :].astype(jnp.float32)
        target[at, :] = total.astype(target.dtype)
        return carry

    lax.fori_loop(0, rows // step, some, 0)


def scatter_kernel(
    spots,
    parts,
    active,
    x_ref,
    o_ref,
    own_buf,
    pair_buf,
    over_src,
    over_buf,
    line_src,
    up_buf,
    down_buf,
    own_in,
    pair_out,
    pair_in,
    over_out,
    over_in,
    line_out,
    up_in,
    down_in,
):
    rows = x_ref.shape[1] // parts
    cut = lambda part: pl.ds(part * rows, rows)

    def run():
        spot, chip, core = places(spots)
        greet(spots, spot, chip, core)

        def order(step):
            if step == spots - 1:
                return spot
            fall = spots - 1 - step
            fall = jnp.where(fall <= spot, fall - 1, fall)
            rise = jnp.where(step >= spot, step + 1, step)
            return jnp.where(2 * spot < spots - 1, fall, rise)

        def pair(at, c, part):
            return remote(
                x_ref.at[slot(at, c, 1 - core), cut(part)],
                pair_buf.at[at, c, cut(part)],
                to_partner(chip, core),
                pair_out.at[at, c, part],
                pair_in.at[at, c, part],
            )

        def over(at, part):
            return remote(
                over_src.at[at, cut(part)],
                over_buf.at[at, cut(part)],
                to_other(chip, core),
                over_out.at[at, part],
                over_in.at[at, part],
            )

        def up(at, part):
            return remote(
                line_src.at[at, cut(part)],
                up_buf.at[at, cut(part)],
                {PACKS: spot + 1},
                line_out.at[at, part],
                up_in.at[at, part],
            )

        def down(at, part):
            return remote(
                line_src.at[at, cut(part)],
                down_buf.at[at, cut(part)],
                {PACKS: spot - 1},
                line_out.at[at, part],
                down_in.at[at, part],
            )

        def own(at, c):
            return pltpu.make_async_copy(x_ref.at[slot(at, c, core)], own_buf.at[at, c], own_in.at[at, c])

        for c in (1 - chip, chip):
            for step in range(spots):
                own(order(step), c).start()
                for part in range(parts):
                    pair(order(step), c, part).start()
        for step in range(spots):
            at = order(step)
            own(at, 1 - chip).wait()
            for part in range(parts):
                pair(at, 1 - chip, part).wait_recv()
                add_into(
                    over_src.at[at, cut(part)],
                    [own_buf.at[at, 1 - chip, cut(part)], pair_buf.at[at, 1 - chip, cut(part)]],
                    rows,
                )
                over(at, part).start()
        for step in range(spots):
            at = order(step)
            own(at, chip).wait()
            for part in range(parts):
                pair(at, chip, part).wait_recv()
                over(at, part).wait_recv()
                base = [
                    own_buf.at[at, chip, cut(part)],
                    pair_buf.at[at, chip, cut(part)],
                    over_buf.at[at, cut(part)],
                ]
                ups, downs = up_buf.at[at, cut(part)], down_buf.at[at, cut(part)]
                if step < spots - 1:
                    target = line_src.at[at, cut(part)]

                    def rising(first):
                        if not first:
                            up(at, part).wait_recv()
                        add_into(target, base if first else base + [ups], rows)
                        up(at, part).start()

                    def falling(first):
                        if not first:
                            down(at, part).wait_recv()
                        add_into(target, base if first else base + [downs], rows)
                        down(at, part).start()

                    pl.when((at > spot) & (spot == 0))(lambda: rising(True))
                    pl.when((at > spot) & (spot > 0))(lambda: rising(False))
                    pl.when((at < spot) & (spot == spots - 1))(lambda: falling(True))
                    pl.when((at < spot) & (spot < spots - 1))(lambda: falling(False))
                elif spots == 1:
                    add_into(o_ref.at[cut(part)], base, rows)
                else:

                    def finish(ends):
                        if ends < 1:
                            up(at, part).wait_recv()
                        if ends > -1:
                            down(at, part).wait_recv()
                        extra = ([ups] if ends < 1 else []) + ([downs] if ends > -1 else [])
                        add_into(o_ref.at[cut(part)], base + extra, rows)

                    pl.when(spot == 0)(lambda: finish(1))
                    pl.when(spot == spots - 1)(lambda: finish(-1))
                    pl.when((spot > 0) & (spot < spots - 1))(lambda: finish(0))
        for part in range(parts):
            for step in range(spots):
                at = order(step)
                pair(at, 0, part).wait_send()
                pair(at, 1, part).wait_send()
                over(at, part).wait_send()
                if step < spots - 1:
                    up(at, part).wait_send()

    if active is None:
        run()
    else:
        pl.when(lax.axis_index(SECTION) == active)(run)


def scatter_blocks(partial, rows, across, number, active=None, parts=4):
    if lax.axis_size(MEMBERS) != 4:
        axes = BOTH if across else MEMBERS
        taken = partial[: rows * lax.axis_size(axes)]
        return lax.psum_scatter(taken, axes, scatter_dimension=0, tiled=True).astype(jnp.float32)
    spots = lax.axis_size(PACKS) if across else 1
    width = partial.shape[1]
    dma = pltpu.SemaphoreType.DMA
    hold = lambda *lead: pltpu.VMEM((*lead, rows, width), partial.dtype)
    return pl.pallas_call(
        functools.partial(scatter_kernel, spots, parts, active),
        out_shape=jax.ShapeDtypeStruct((rows, width), jnp.float32),
        in_specs=[pl.BlockSpec(memory_space=pl.ANY)],
        out_specs=pl.BlockSpec(memory_space=pltpu.VMEM),
        scratch_shapes=[
            hold(spots, 2),
            hold(spots, 2),
            hold(spots),
            hold(spots),
            hold(spots),
            hold(spots),
            hold(spots),
            dma((spots, 2)),
            dma((spots, 2, parts)),
            dma((spots, 2, parts)),
            dma((spots, parts)),
            dma((spots, parts)),
            dma((spots, parts)),
            dma((spots, parts)),
            dma((spots, parts)),
        ],
        compiler_params=pltpu.CompilerParams(collective_id=number, has_side_effects=True),
        name=f"scatter{number}",
    )(partial.reshape(-1, rows, width))


def allowed_pairs(seg_col, seg_row):
    rows = seg_col.shape[0]
    later = lax.broadcasted_iota(jnp.int32, (rows, rows), 0)
    earlier = lax.broadcasted_iota(jnp.int32, (rows, rows), 1)
    return (seg_col == seg_row) & (earlier <= later)


def attend_kernel(heads, q_ref, lat_ref, key_ref, cos_ref, sin_ref, col_ref, row_ref, out_ref, rot_ref):
    factor = QK**-0.5
    allowed = allowed_pairs(col_ref[...], row_ref[0])
    cosine, sine = cos_ref[...], sin_ref[...]
    shared = key_ref[:, LAT:]
    for head in range(heads):
        raw = q_ref[:, head * QK : (head + 1) * QK]
        query = bf16(
            jnp.concatenate([raw[:, :NOPE], rotate(raw[:, NOPE:], cosine, sine)], axis=1)
        )
        rot_ref[:, head * QK : (head + 1) * QK] = query
        key = jnp.concatenate([lat_ref[:, head * KV : head * KV + NOPE], shared], axis=1)
        value = lat_ref[:, head * KV + NOPE : (head + 1) * KV]
        scores = jnp.where(allowed, dot_t(query, key) * factor, masked_score)
        top = jnp.max(scores, axis=1, keepdims=True)
        powers = jnp.exp(scores - top)
        probs = powers / jnp.sum(powers, axis=1, keepdims=True)
        out_ref[:, head * VD : (head + 1) * VD] = bf16(dot(bf16(probs), value))


def attend(query_raw, latent, keyed, tables, groups=1):
    cosine, sine, seg_col, seg_row = tables
    count, _, rows = seg_row.shape
    heads = query_raw.shape[1] // QK
    block = lambda width: pl.BlockSpec((rows, width), lambda i: (i, 0))
    same = lambda width: pl.BlockSpec((rows, width), lambda i: (0, 0) if groups > 1 else (i, 0))
    count = count * groups
    return pl.pallas_call(
        functools.partial(attend_kernel, heads),
        grid=(count,),
        in_specs=[
            block(heads * QK),
            block(heads * KV),
            same(LAT + ROPE),
            same(HALF),
            same(HALF),
            same(1),
            pl.BlockSpec((1, 1, rows), lambda i: (0, 0, 0) if groups > 1 else (i, 0, 0)),
        ],
        out_specs=[block(heads * VD), block(heads * QK)],
        out_shape=[
            jax.ShapeDtypeStruct((count * rows, heads * VD), jnp.bfloat16),
            jax.ShapeDtypeStruct((count * rows, heads * QK), jnp.bfloat16),
        ],
        name="attend",
        cost_estimate=pl.CostEstimate(
            flops=2 * count * heads * rows * rows * (QK + VD),
            bytes_accessed=count * rows * heads * (QK * 6 + KV * 2 + VD * 2),
            transcendentals=count * heads * rows * rows,
        ),
    )(query_raw, latent, keyed, cosine, sine, seg_col, seg_row)


def attend_back_kernel(
    heads, q_ref, lat_ref, key_ref, grad_ref, cos_ref, sin_ref, col_ref, row_ref, dq_ref, dlat_ref, dkey_ref
):
    factor = QK**-0.5
    allowed = allowed_pairs(col_ref[...], row_ref[0])
    cosine, sine = cos_ref[...], sin_ref[...]
    shared = key_ref[:, LAT:]
    total = None
    for head in range(heads):
        query = q_ref[:, head * QK : (head + 1) * QK]
        key = jnp.concatenate([lat_ref[:, head * KV : head * KV + NOPE], shared], axis=1)
        value = lat_ref[:, head * KV + NOPE : (head + 1) * KV]
        grad = grad_ref[:, head * VD : (head + 1) * VD]
        scores = jnp.where(allowed, dot_t(query, key) * factor, masked_score)
        top = jnp.max(scores, axis=1, keepdims=True)
        powers = jnp.exp(scores - top)
        probs = powers / jnp.sum(powers, axis=1, keepdims=True)
        grad_value = t_dot(bf16(probs), grad)
        grad_probs = dot_t(grad, value)
        centre = jnp.sum(probs * grad_probs, axis=1, keepdims=True)
        grad_scores = bf16(probs * (grad_probs - centre) * factor)
        grad_query = dot(grad_scores, key)
        grad_key = t_dot(grad_scores, query)
        dq_ref[:, head * QK : (head + 1) * QK] = bf16(
            jnp.concatenate(
                [grad_query[:, :NOPE], rotate(grad_query[:, NOPE:], cosine, -sine)], axis=1
            )
        )
        dlat_ref[:, head * KV : head * KV + NOPE] = bf16(grad_key[:, :NOPE])
        dlat_ref[:, head * KV + NOPE : (head + 1) * KV] = bf16(grad_value)
        part = grad_key[:, NOPE:]
        total = part if total is None else total + part
    dkey_ref[...] = total


def attend_back(query, latent, keyed, grad, tables, groups=1):
    cosine, sine, seg_col, seg_row = tables
    count, _, rows = seg_row.shape
    heads = query.shape[1] // QK
    block = lambda width: pl.BlockSpec((rows, width), lambda i: (i, 0))
    same = lambda width: pl.BlockSpec((rows, width), lambda i: (0, 0) if groups > 1 else (i, 0))
    count = count * groups
    return pl.pallas_call(
        functools.partial(attend_back_kernel, heads),
        grid=(count,),
        in_specs=[
            block(heads * QK),
            block(heads * KV),
            same(LAT + ROPE),
            block(heads * VD),
            same(HALF),
            same(HALF),
            same(1),
            pl.BlockSpec((1, 1, rows), lambda i: (0, 0, 0) if groups > 1 else (i, 0, 0)),
        ],
        out_specs=[block(heads * QK), block(heads * KV), block(ROPE)],
        out_shape=[
            jax.ShapeDtypeStruct((count * rows, heads * QK), jnp.bfloat16),
            jax.ShapeDtypeStruct((count * rows, heads * KV), jnp.bfloat16),
            jax.ShapeDtypeStruct((count * rows, ROPE), jnp.float32),
        ],
        name="attend_back",
        cost_estimate=pl.CostEstimate(
            flops=2 * count * heads * rows * rows * (3 * QK + 2 * VD),
            bytes_accessed=count * rows * heads * (QK * 4 + KV * 4 + VD * 2),
            transcendentals=count * heads * rows * rows,
        ),
    )(query, latent, keyed, grad, cosine, sine, seg_col, seg_row)


def gated_hidden(gate, up):
    return silu_parts(gate)[0] * up


def gated_back(gate, up, grad_hidden):
    act, slope = silu_parts(gate)
    return bf16(grad_hidden * up * slope), bf16(grad_hidden * act)


def columns(pieces):
    start = 0
    for piece in pieces:
        yield start, piece.shape[1]
        start += piece.shape[1]


def hold_weight(pieces):
    return pltpu.VMEM((pieces[0].shape[0], sum(piece.shape[1] for piece in pieces)), pieces[0].dtype)


def loads_of(counts, sources, targets, sems):
    copies = []
    for pieces, target in zip(counts, targets):
        group, sources = sources[:pieces], sources[pieces:]
        for source, (start, size) in zip(group, columns(group)):
            place = target if pieces == 1 else target.at[:, pl.ds(start, size)]
            copies.append(pltpu.make_async_copy(source, place, sems.at[len(copies)]))
    return copies


def load(*args):
    copies = loads_of(*args)
    for copy in copies:
        copy.start()
    for copy in copies:
        copy.wait()


class Tiles:
    def __init__(self, rows, pack_rows, pack, active):
        self.rows, self.pack_rows = rows, pack_rows
        self.tile = min(256, pack_rows)
        self.count = rows // self.tile
        inner = pack_rows // self.tile
        runs = (lax.axis_index(SECTION) == active).astype(jnp.int32)
        self.control = jnp.stack([pack * inner, (pack + 1) * inner, runs]).astype(jnp.int32)

    def source(self, width):
        return pl.BlockSpec((self.tile, width), lambda i, control: (i * control[2], 0))

    def small(self, array):
        return pl.BlockSpec(array.shape, lambda i, control: (0,) * array.ndim)

    def pack_source(self, width):
        def index(i, control):
            return (0, jnp.clip(i - control[0], 0, control[1] - control[0] - 1), 0)

        return pl.BlockSpec((2, self.tile, width), index)

    def result(self, width, dtype=jnp.bfloat16):
        def index(i, control):
            return (jnp.where(control[2] == 1, i, self.count), 0)

        shape = jax.ShapeDtypeStruct((self.rows + self.tile, width), dtype)
        return shape, pl.BlockSpec((self.tile, width), index)

    def pair_result(self, width):
        def index(i, control):
            return (0, jnp.where(control[2] == 1, i, self.count), 0)

        shape = jax.ShapeDtypeStruct((2, self.rows + self.tile, width), jnp.bfloat16)
        return shape, pl.BlockSpec((2, self.tile, width), index)

    def pack_result(self, width):
        def index(i, control):
            spot = jnp.clip(i - control[0], 0, control[1] - control[0] - 1)
            return (0, jnp.where(control[2] == 1, spot, control[1] - control[0]), 0)

        shape = jax.ShapeDtypeStruct((2, self.pack_rows + self.tile, width), jnp.bfloat16)
        return shape, pl.BlockSpec((2, self.tile, width), index)

    def call(self, kernel, name, sources, weights, results, into=(), scratch=(), flops=0):
        arrays, specs = zip(*sources)
        shapes, out_specs = zip(*results)
        anywhere = pl.BlockSpec(memory_space=pl.ANY)
        pieces = [piece for weight in weights for piece in weight]
        counts = [len(weight) for weight in weights]
        first = 1 + len(arrays) + len(pieces)
        return pl.pallas_call(
            functools.partial(kernel, len(arrays), counts, len(into), len(results)),
            grid_spec=pltpu.PrefetchScalarGridSpec(
                num_scalar_prefetch=1,
                grid=(self.count,),
                in_specs=[*specs, *([anywhere] * (len(pieces) + len(into)))],
                out_specs=list(out_specs),
                scratch_shapes=[
                    *[hold_weight(weight) for weight in weights],
                    pltpu.SemaphoreType.DMA((len(pieces),)),
                    *scratch,
                ],
            ),
            out_shape=list(shapes),
            input_output_aliases={first + index: index for index in range(len(into))},
            name=name,
            cost_estimate=pl.CostEstimate(flops=flops, bytes_accessed=self.rows * 16384, transcendentals=0),
        )(self.control, *arrays, *pieces, *into)


def tiled(body):
    def kernel(n_sources, counts, n_into, n_results, control, *refs):
        n_weights, n_pieces = len(counts), sum(counts)
        sources, refs = refs[:n_sources], refs[n_sources:]
        stored, refs = refs[:n_pieces], refs[n_pieces + n_into :]
        results, refs = refs[:n_results], refs[n_results:]
        weights, sems, scratch = refs[:n_weights], refs[n_weights], refs[n_weights + 1 :]

        def run():
            pl.when(pl.program_id(0) == 0)(lambda: load(counts, stored, weights, sems))
            body(inside_pack(control), [sources[0][...], *sources[1:]], weights, results, scratch)

        pl.when(control[2] == 1)(run)

    return kernel


def inside_pack(control):
    tile = pl.program_id(0)
    return (tile >= control[0]) & (tile < control[1])


def shared_units(x, shared_in):
    half = shared_in.shape[0] // 2
    return dot_t(x, shared_in[:half]), dot_t(x, shared_in[half:])


def experts_body(inside, sources, weights, results, scratch):
    x, own_ref, routed_ref = sources
    in_ref, shared_in_ref = weights[:2]
    pre_ref, gated_ref, prob_ref, shared_pre_ref = results[:4]
    units = gated_ref.shape[1]
    pre = dot(x, in_ref[...])
    logits = pre[:, 2 * units : 2 * units + own_ref.shape[1]]
    powers = jnp.exp(logits - jnp.max(logits, axis=1, keepdims=True))
    prob = powers / jnp.sum(powers, axis=1, keepdims=True)
    prob_ref[...] = prob
    gate = jnp.sum(prob * own_ref[...], axis=1, keepdims=True) * routed_ref[...]
    pre_ref[...] = bf16(pre[:, : 2 * units])
    gated = bf16(gate * gated_hidden(pre[:, :units], pre[:, units : 2 * units]))
    gated_ref[...] = gated

    def shared():
        left, right = shared_units(x, shared_in_ref)
        shared_pre_ref[0] = bf16(left)
        shared_pre_ref[1] = bf16(right)
        return left, right

    if len(weights) == 2:
        pl.when(inside)(lambda: shared() and None)
        return
    out_ref, shared_out_ref = weights[2:]
    partial_ref = results[4]

    def with_shared():
        hidden = bf16(gated_hidden(*shared()))
        partial_ref[...] = bf16(dot(gated, out_ref[...]) + dot(hidden, shared_out_ref[...]))

    def without():
        partial_ref[...] = bf16(dot(gated, out_ref[...]))

    pl.when(inside)(with_shared)
    pl.when(jnp.logical_not(inside))(without)


def finish_body(inside, sources, weights, results, scratch):
    gated, _, shared_pre_ref = sources
    out_ref, shared_out_ref = weights
    (partial_ref,) = results

    def with_shared():
        hidden = bf16(gated_hidden(shared_pre_ref[0].astype(jnp.float32), shared_pre_ref[1].astype(jnp.float32)))
        partial_ref[...] = bf16(dot(gated, out_ref[...]) + dot(hidden, shared_out_ref[...]))

    def without():
        partial_ref[...] = bf16(dot(gated, out_ref[...]))

    pl.when(inside)(with_shared)
    pl.when(jnp.logical_not(inside))(without)


def experts_back_body(inside, sources, weights, results, scratch):
    grad, own_ref, pre_ref, prob_ref, routed_ref, shared_pre_ref = sources
    in_ref, shared_in_ref, out_ref, shared_out_ref = weights
    grad_pre_ref, moved_ref, partial_ref = results
    (joined_ref,) = scratch
    units = out_ref.shape[0]
    prob = prob_ref[...]
    own_prob = jnp.sum(prob * own_ref[...], axis=1, keepdims=True) * routed_ref[...]
    gate, up = pre_ref[:, :units].astype(jnp.float32), pre_ref[:, units:].astype(jnp.float32)
    grad_units = dot_t(grad, out_ref[...])
    act, slope = silu_parts(gate)
    moved = own_prob * jnp.sum(grad_units * act * up, axis=1, keepdims=True)
    moved_ref[...] = moved
    scaled = own_prob * grad_units
    joined_ref[:, :units] = bf16(scaled * up * slope)
    joined_ref[:, units : 2 * units] = bf16(scaled * act)
    joined_ref[:, 2 * units :] = jnp.zeros_like(joined_ref[:, 2 * units :])
    joined_ref[:, 2 * units : 2 * units + own_ref.shape[1]] = bf16(moved * (own_ref[...] - prob))
    grad_pre_ref[...] = joined_ref[:, : 2 * units]
    base = dot_t(joined_ref[...], in_ref[...])
    half = shared_out_ref.shape[0]

    def with_shared():
        left, right = gated_back(
            shared_pre_ref[0].astype(jnp.float32),
            shared_pre_ref[1].astype(jnp.float32),
            dot_t(grad, shared_out_ref[...]),
        )
        partial_ref[...] = bf16(base + dot(left, shared_in_ref[:half]) + dot(right, shared_in_ref[half:]))

    def without():
        partial_ref[...] = bf16(base)

    pl.when(inside)(with_shared)
    pl.when(jnp.logical_not(inside))(without)


def shared_body(inside, sources, weights, results, scratch):
    pre_ref, hid_ref = results
    left, right = shared_units(sources[0], weights[0])
    pre_ref[0] = bf16(left)
    pre_ref[1] = bf16(right)
    hid_ref[...] = bf16(gated_hidden(left, right))


def heads_body(block, inside, sources, weights, results, scratch):
    x, key_ref, cos_ref, sin_ref, col_ref, row_ref = sources
    query_w_ref, expand_ref = weights
    out_ref, rot_ref, lat_ref = results
    (q_ref,) = scratch
    heads = q_ref.shape[1] // QK
    q_ref[...] = dot(x, query_w_ref[...])
    lat_ref[...] = bf16(dot(key_ref[:, :LAT], expand_ref[...]))
    for start in range(0, x.shape[0], block):
        at = pl.ds(start, block)
        attend_kernel(
            heads,
            q_ref.at[at],
            lat_ref.at[at],
            key_ref.at[at],
            cos_ref.at[at],
            sin_ref.at[at],
            col_ref.at[at],
            row_ref.at[pl.ds(start // block, 1)],
            out_ref.at[at],
            rot_ref.at[at],
        )


def pair_grad_kernel(x_ref, grad_ref, out_ref):
    units = out_ref.shape[2]
    x = x_ref[...]
    out_ref[:, 0, :] = t_dot(x, grad_ref[:, :units])
    out_ref[:, 1, :] = t_dot(x, grad_ref[:, units:])


def pair_grad(x, grad):
    rows, width = x.shape
    units = grad.shape[1] // 2
    if rows > 4096:
        return t_dot(x, grad[:rows]).reshape(width, 2, units)
    tile = 256
    return pl.pallas_call(
        pair_grad_kernel,
        grid=(width // tile,),
        in_specs=[
            pl.BlockSpec((rows, tile), lambda i: (0, i)),
            pl.BlockSpec((rows, 2 * units), lambda i: (0, 0), pipeline_mode=pl.Buffered(1)),
        ],
        out_specs=pl.BlockSpec((tile, 2, units), lambda i: (i, 0, 0)),
        out_shape=jax.ShapeDtypeStruct((width, 2, units), jnp.float32),
        name="pair_grad",
        cost_estimate=pl.CostEstimate(
            flops=4 * rows * width * units, bytes_accessed=rows * (width + 2 * units) * 2 + width * units * 8, transcendentals=0
        ),
    )(x, grad)


def blank(shape, dtype):
    return pl.pallas_call(
        lambda out_ref: None,
        out_shape=jax.ShapeDtypeStruct(shape, dtype),
        out_specs=pl.BlockSpec(memory_space=pl.ANY),
        compiler_params=pltpu.CompilerParams(has_side_effects=True),
        name="blank",
    )()


def arrival_order(spots):
    tiles = [(rank + 1.1 * over, rank, over) for rank in range(spots) for over in (0, 1)]
    return [(rank, over == 1) for _, rank, over in sorted(tiles)]


def ranked_spots(spots, spot):
    ranks = []
    for rank in range(spots):
        value = 0
        for own in range(spots):
            nearest = sorted(range(spots), key=lambda other: (abs(other - own), other))
            value = value + jnp.where(spot == own, nearest[rank], 0)
        ranks.append(value)
    return ranks


def pick(index, values):
    total = 0
    for position, value in enumerate(values):
        total = total + jnp.where(index == position, value, 0)
    return total


def fused_kernel(spots, parts, active, body, pack_kinds, counts, n_into, *refs):
    source_kinds, result_kinds = pack_kinds
    n_sources, n_results = len(source_kinds), len(result_kinds)
    n_weights, n_pieces = len(counts), sum(counts)
    x_ref, small_ref, refs = refs[0], refs[1], refs[2:]
    sources, refs = refs[:n_sources], refs[n_sources:]
    stored, refs = refs[:n_pieces], refs[n_pieces + n_into :]
    o_ref, refs = refs[0], refs[1:]
    results, refs = refs[:n_results], refs[n_results:]
    x_tile, refs = refs[0], refs[1:]
    source_tiles, refs = refs[:n_sources], refs[n_sources:]
    result_tiles, refs = refs[:n_results], refs[n_results:]
    weights, refs = refs[:n_weights], refs[n_weights:]
    sems, scratch = refs[:12], refs[12:]
    own_sem, weight_sem, tile_sem, out_sem = sems[:4]
    up_out, up_in, down_out, down_in, over_out, over_in, pair_out, pair_in = sems[4:]
    block = x_ref.shape[0]
    rows = block // parts
    tile = 2 * block

    def run():
        loads = loads_of(counts, stored, weights, weight_sem)
        for copy in loads:
            copy.start()
        spot, chip, core = places(spots)
        greet(spots, spot, chip, core)
        piece = lambda index, part: o_ref.at[index, pl.ds(part * rows, rows)]
        first = lambda part: x_ref.at[pl.ds(part * rows, rows)]

        def up(source, at, part, reach):
            return remote(
                source, piece(slot(at, chip, core), part), {PACKS: spot + 1}, up_out.at[reach, part], up_in.at[reach, part]
            )

        def down(source, at, part, reach):
            return remote(
                source,
                piece(slot(at, chip, core), part),
                {PACKS: spot - 1},
                down_out.at[reach, part],
                down_in.at[reach, part],
            )

        def over(source, at, part):
            return remote(
                source, piece(slot(at, chip, core), part), to_other(chip, core), over_out.at[at, part], over_in.at[at, part]
            )

        def pair(source, at, c, part):
            return remote(
                source,
                piece(slot(at, c, core), part),
                to_partner(chip, core),
                pair_out.at[c, at, part],
                pair_in.at[c, at, part],
            )

        mine = slot(spot, chip, core)
        for part in range(parts):
            source = first(part)
            pair(source, spot, chip, part).start()
            over(source, spot, part).start()
            pl.when(spot < spots - 1)(lambda: up(source, spot, part, 0).start())
            pl.when(spot > 0)(lambda: down(source, spot, part, 0).start())
        own = pltpu.make_async_copy(x_ref, o_ref.at[mine], own_sem.at[0])
        own.start()
        own.wait()
        ranks = ranked_spots(spots, spot)
        order = arrival_order(spots)

        def hand_on(reach):
            for part in range(parts):

                def below(part=part):
                    at = spot - reach
                    source = piece(slot(at, chip, core), part)
                    up(source, at, part, reach - 1).wait_recv()
                    pl.when(spot < spots - 1)(lambda: up(source, at, part, reach).start())
                    over(source, at, part).start()
                    pair(source, at, chip, part).start()

                def above(part=part):
                    at = spot + reach
                    source = piece(slot(at, chip, core), part)
                    down(source, at, part, reach - 1).wait_recv()
                    pl.when(spot > 0)(lambda: down(source, at, part, reach).start())
                    over(source, at, part).start()
                    pair(source, at, chip, part).start()

                pl.when(spot >= reach)(below)
                pl.when(spot + reach < spots)(above)

        def arrive(rank, across):
            at = ranks[rank]
            if across:
                for part in range(parts):
                    source = piece(slot(at, 1 - chip, core), part)
                    over(source, at, part).wait_recv()
                    pair(source, at, 1 - chip, part).start()
                for part in range(parts):
                    pair(first(part), at, 1 - chip, part).wait_recv()
                return
            if rank > 0:
                hand_on(rank)
            for part in range(parts):
                pair(first(part), at, chip, part).wait_recv()

        def window(ref, kind, at, c):
            if kind:
                return ref.at[:, pl.ds(pl.multiple_of(c * tile, tile), tile)]
            return ref.at[pl.ds(pl.multiple_of((at * 2 + c) * tile, tile), tile)]

        def outward(index, which, at, c):
            return pltpu.make_async_copy(
                result_tiles[index].at[which], window(results[index], result_kinds[index], at, c), out_sem.at[which, index]
            )

        def step(number, carry):
            for position, (rank, across) in enumerate(order):
                pl.when(number == position)(functools.partial(arrive, rank, across))
            at = pick(number, [ranks[rank] for rank, _ in order])
            c = pick(number, [1 - chip if across else chip for _, across in order])
            inside = at == spot
            inputs = [pltpu.make_async_copy(o_ref.at[pl.ds(slot(at, c, 0), 2)], x_tile, tile_sem.at[0])]
            for index, kind in enumerate(source_kinds):
                if not kind:
                    inputs.append(
                        pltpu.make_async_copy(
                            window(sources[index], kind, at, c), source_tiles[index], tile_sem.at[1 + index]
                        )
                    )
            for copy in inputs:
                copy.start()
            for index, kind in enumerate(source_kinds):
                if kind:

                    def fetch(index=index, kind=kind):
                        copy = pltpu.make_async_copy(
                            window(sources[index], kind, at, c), source_tiles[index], tile_sem.at[1 + index]
                        )
                        copy.start()
                        copy.wait()

                    pl.when(inside)(fetch)

            @pl.when(number == 0)
            def _():
                for copy in loads:
                    copy.wait()

            which = lax.rem(number, 2)

            @pl.when(number >= 2)
            def _():
                for index, kind in enumerate(result_kinds):
                    if not kind:
                        outward(index, which, at, c).wait()

            for copy in inputs:
                copy.wait()
            body(
                inside,
                [x_tile[...].reshape(tile, x_tile.shape[2]), small_ref, *source_tiles],
                weights,
                [target.at[which] for target in result_tiles],
                scratch,
            )
            for index, kind in enumerate(result_kinds):
                if kind:

                    def put(index=index):
                        copy = outward(index, which, at, c)
                        copy.start()
                        copy.wait()

                    pl.when(inside)(put)
                else:
                    outward(index, which, at, c).start()
            return carry

        lax.fori_loop(0, 2 * spots, step, 0)
        for which in range(2):
            for index, kind in enumerate(result_kinds):
                if not kind:
                    outward(index, which, spot, chip).wait()
        for part in range(parts):
            for at in range(spots):
                over(first(part), at, part).wait_send()
                for c in range(2):
                    pair(first(part), at, c, part).wait_send()
            for reach in range(spots - 1):
                pl.when((spot >= reach) & (spot < spots - 1))(lambda: up(first(part), spot, part, reach).wait_send())
                pl.when((spot + reach < spots) & (spot > 0))(lambda: down(first(part), spot, part, reach).wait_send())

    pl.when(lax.axis_index(SECTION) == active)(run)


def fused_call(tiles, rows_in, number, active, body, small, sources, weights, results, gathered, into, scratch=(), parts=4):
    spots = lax.axis_size(PACKS)
    block, width = rows_in.shape
    tile = 2 * block
    dma = pltpu.SemaphoreType.DMA
    hops = max(spots - 1, 1)
    anywhere = pl.BlockSpec(memory_space=pl.ANY)
    inside = pl.BlockSpec(memory_space=pltpu.VMEM)
    shapes = [jax.ShapeDtypeStruct((spots * 4, block, width), rows_in.dtype), *(shape for shape, _ in results)]
    held = [gathered.reshape(shapes[0].shape), *into]
    pieces = [piece for weight in weights for piece in weight]
    first = 2 + len(sources) + len(pieces)

    def hold(array, kind, *lead):
        shape = (2, tile, array.shape[2]) if kind else (tile, array.shape[1])
        return pltpu.VMEM((*lead, *shape), array.dtype)

    outs = pl.pallas_call(
        functools.partial(
            fused_kernel,
            spots,
            parts,
            active,
            body,
            ([kind for _, kind in sources], [kind for _, kind in results]),
            [len(weight) for weight in weights],
            len(held),
        ),
        out_shape=shapes,
        in_specs=[inside, inside, *([anywhere] * (len(sources) + len(pieces) + len(held)))],
        out_specs=[anywhere] * len(shapes),
        input_output_aliases={first + index: index for index in range(len(held))},
        scratch_shapes=[
            pltpu.VMEM((2, block, width), rows_in.dtype),
            *(hold(array, kind) for array, kind in sources),
            *(hold(shape, kind, 2) for shape, kind in results),
            *(hold_weight(weight) for weight in weights),
            dma((1,)),
            dma((len(pieces),)),
            dma((1 + len(sources),)),
            dma((2, len(results))),
            dma((hops, parts)),
            dma((hops, parts)),
            dma((hops, parts)),
            dma((hops, parts)),
            dma((spots, parts)),
            dma((spots, parts)),
            dma((2, spots, parts)),
            dma((2, spots, parts)),
            *scratch,
        ],
        compiler_params=pltpu.CompilerParams(collective_id=number, has_side_effects=True),
        name=f"fused{number}",
    )(rows_in, small, *(array for array, _ in sources), *pieces, *held)
    return outs[0].reshape(-1, width), list(outs[1:])


def sum_kernel(spots, parts, active, body, pack_kinds, counts, n_into, *refs):
    source_kinds, result_kinds = pack_kinds
    n_sources, n_results = len(source_kinds), len(result_kinds)
    n_weights, n_pieces = len(counts), sum(counts)
    small_ref, refs = refs[0], refs[1:]
    sources, refs = refs[:n_sources], refs[n_sources:]
    stored, refs = refs[:n_pieces], refs[n_pieces + n_into :]
    o_ref, refs = refs[0], refs[1:]
    results, refs = refs[:n_results], refs[n_results:]
    source_tiles, refs = refs[:n_sources], refs[n_sources:]
    result_tiles, refs = refs[:n_results], refs[n_results:]
    weights, refs = refs[:n_weights], refs[n_weights:]
    x_buf, pair_buf, over_src, over_buf, line_src, up_buf, down_buf = refs[:7]
    weight_sem, tile_sem, out_sem, pair_out, pair_in, over_out, over_in, line_out, up_in, down_in = refs[7:17]
    scratch = refs[17:]
    block = o_ref.shape[0]
    rows = block // parts
    tile = 2 * block
    cut = lambda part: pl.ds(part * rows, rows)

    def run():
        loads = loads_of(counts, stored, weights, weight_sem)
        for copy in loads:
            copy.start()
        spot, chip, core = places(spots)

        def order(step):
            if step == spots - 1:
                return spot
            fall = spots - 1 - step
            fall = jnp.where(fall <= spot, fall - 1, fall)
            rise = jnp.where(step >= spot, step + 1, step)
            return jnp.where(2 * spot < spots - 1, fall, rise)

        def place(number):
            at = pick(number // 2, [order(step) for step in range(spots)])
            return at, jnp.where(number % 2 == 0, 1 - chip, chip)

        def window(ref, kind, at, c):
            if kind:
                return ref.at[:, pl.ds(pl.multiple_of(c * tile, tile), tile)]
            return ref.at[pl.ds(pl.multiple_of((at * 2 + c) * tile, tile), tile)]

        def inputs(number):
            at, c = place(number)
            which = lax.rem(number, 2)
            return [
                pltpu.make_async_copy(
                    window(sources[index], kind, at, c), source_tiles[index].at[which], tile_sem.at[which, index]
                )
                for index, kind in enumerate(source_kinds)
                if not kind
            ]

        for copy in inputs(0):
            copy.start()
        greet(spots, spot, chip, core)

        def mine(at, c, k, part):
            return x_buf.at[at * 2 + c, pl.ds(pl.multiple_of(k * block + part * rows, rows), rows)]

        def pair(at, c, part):
            return remote(
                mine(at, c, 1 - core, part),
                pair_buf.at[at, c, cut(part)],
                to_partner(chip, core),
                pair_out.at[at, c, part],
                pair_in.at[at, c, part],
            )

        def over(at, part):
            return remote(
                over_src.at[at, cut(part)],
                over_buf.at[at, cut(part)],
                to_other(chip, core),
                over_out.at[at, part],
                over_in.at[at, part],
            )

        def up(at, part):
            return remote(
                line_src.at[at, cut(part)],
                up_buf.at[at, cut(part)],
                {PACKS: spot + 1},
                line_out.at[at, part],
                up_in.at[at, part],
            )

        def down(at, part):
            return remote(
                line_src.at[at, cut(part)],
                down_buf.at[at, cut(part)],
                {PACKS: spot - 1},
                line_out.at[at, part],
                down_in.at[at, part],
            )

        def across(step):
            at = order(step)
            for part in range(parts):
                pair(at, 1 - chip, part).wait_recv()
                add_into(
                    over_src.at[at, cut(part)],
                    [mine(at, 1 - chip, core, part), pair_buf.at[at, 1 - chip, cut(part)]],
                    rows,
                )
                over(at, part).start()

        def along(step):
            at = order(step)
            for part in range(parts):
                pair(at, chip, part).wait_recv()
                over(at, part).wait_recv()
                base = [mine(at, chip, core, part), pair_buf.at[at, chip, cut(part)], over_buf.at[at, cut(part)]]
                ups, downs = up_buf.at[at, cut(part)], down_buf.at[at, cut(part)]
                if step < spots - 1:
                    target = line_src.at[at, cut(part)]

                    def rising(first):
                        if not first:
                            up(at, part).wait_recv()
                        add_into(target, base if first else base + [ups], rows)
                        up(at, part).start()

                    def falling(first):
                        if not first:
                            down(at, part).wait_recv()
                        add_into(target, base if first else base + [downs], rows)
                        down(at, part).start()

                    pl.when((at > spot) & (spot == 0))(lambda: rising(True))
                    pl.when((at > spot) & (spot > 0))(lambda: rising(False))
                    pl.when((at < spot) & (spot == spots - 1))(lambda: falling(True))
                    pl.when((at < spot) & (spot < spots - 1))(lambda: falling(False))
                elif spots == 1:
                    add_into(o_ref.at[cut(part)], base, rows)
                else:

                    def finish(ends):
                        if ends < 1:
                            up(at, part).wait_recv()
                        if ends > -1:
                            down(at, part).wait_recv()
                        extra = ([ups] if ends < 1 else []) + ([downs] if ends > -1 else [])
                        add_into(o_ref.at[cut(part)], base + extra, rows)

                    pl.when(spot == 0)(lambda: finish(1))
                    pl.when(spot == spots - 1)(lambda: finish(-1))
                    pl.when((spot > 0) & (spot < spots - 1))(lambda: finish(0))

        late = 4 + jnp.where((spot > 0) & (spot < spots - 1), 1, 0)

        def outward(index, which, at, c):
            return pltpu.make_async_copy(
                result_tiles[index].at[which], window(results[index], result_kinds[index], at, c), out_sem.at[which, index]
            )

        def step(number, carry):
            at, c = place(number)
            inside = at == spot
            which = lax.rem(number, 2)
            for copy in inputs(number):
                copy.wait()

            @pl.when(number + 1 < 2 * spots)
            def _():
                for copy in inputs(number + 1):
                    copy.start()

            for index, kind in enumerate(source_kinds):
                if kind:

                    def fetch(index=index, kind=kind):
                        copy = pltpu.make_async_copy(
                            window(sources[index], kind, at, c), source_tiles[index], tile_sem.at[0, index]
                        )
                        copy.start()
                        copy.wait()

                    pl.when(inside)(fetch)

            @pl.when(number == 0)
            def _():
                for copy in loads:
                    copy.wait()

            @pl.when(number >= 2)
            def _():
                for index, kind in enumerate(result_kinds):
                    if not kind:
                        outward(index, which, at, c).wait()

            tiles = [
                target if kind else target.at[which] for target, kind in zip(source_tiles, source_kinds)
            ]
            body(
                inside,
                [tiles[0][...], small_ref, *tiles[1:]],
                weights,
                [*(target.at[which] for target in result_tiles), x_buf.at[at * 2 + c]],
                scratch,
            )
            for part in range(parts):
                pair(at, c, part).start()
            for index, kind in enumerate(result_kinds):
                if kind:

                    def put(index=index):
                        copy = outward(index, which, at, c)
                        copy.start()
                        copy.wait()

                    pl.when(inside)(put)
                else:
                    outward(index, which, at, c).start()
            for number_of in range(spots):
                pl.when(number == 2 * number_of + 1)(functools.partial(across, number_of))
                pl.when(number == 2 * number_of + late)(functools.partial(along, number_of))
            return carry

        lax.fori_loop(0, 2 * spots, step, 0)
        for number_of in range(spots):
            pl.when(2 * number_of + late >= 2 * spots)(functools.partial(along, number_of))
        for which in range(2):
            for index, kind in enumerate(result_kinds):
                if not kind:
                    outward(index, which, spot, chip).wait()
        for part in range(parts):
            for number_of in range(spots):
                at = order(number_of)
                pair(at, 0, part).wait_send()
                pair(at, 1, part).wait_send()
                over(at, part).wait_send()
                if number_of < spots - 1:
                    up(at, part).wait_send()

    pl.when(lax.axis_index(SECTION) == active)(run)


def sum_call(rows, number, active, body, small, sources, weights, results, into, scratch=(), parts=4):
    spots = lax.axis_size(PACKS)
    width = weights[-1][0].shape[1]
    tile = 2 * rows
    dma = pltpu.SemaphoreType.DMA
    anywhere = pl.BlockSpec(memory_space=pl.ANY)
    inside = pl.BlockSpec(memory_space=pltpu.VMEM)
    pieces = [piece for weight in weights for piece in weight]
    first = 1 + len(sources) + len(pieces)
    held = lambda *lead: pltpu.VMEM((*lead, rows, width), jnp.bfloat16)

    def hold(array, kind, *lead):
        if kind:
            return pltpu.VMEM((*lead, 2, tile, array.shape[2]), array.dtype)
        return pltpu.VMEM((2, tile, array.shape[1]), array.dtype)

    outs = pl.pallas_call(
        functools.partial(
            sum_kernel,
            spots,
            parts,
            active,
            body,
            ([kind for _, kind in sources], [kind for _, kind in results]),
            [len(weight) for weight in weights],
            len(into),
        ),
        out_shape=[jax.ShapeDtypeStruct((rows, width), jnp.float32), *(shape for shape, _ in results)],
        in_specs=[inside, *([anywhere] * (len(sources) + len(pieces) + len(into)))],
        out_specs=[inside, *([anywhere] * len(results))],
        input_output_aliases={first + index: 1 + index for index in range(len(into))},
        scratch_shapes=[
            *(hold(array, kind) for array, kind in sources),
            *(hold(shape, kind, 2) for shape, kind in results),
            *(hold_weight(weight) for weight in weights),
            pltpu.VMEM((2 * spots, tile, width), jnp.bfloat16),
            held(spots, 2),
            held(spots),
            held(spots),
            held(spots),
            held(spots),
            held(spots),
            dma((len(pieces),)),
            dma((2, len(sources))),
            dma((2, max(len(results), 1))),
            dma((spots, 2, parts)),
            dma((spots, 2, parts)),
            dma((spots, parts)),
            dma((spots, parts)),
            dma((spots, parts)),
            dma((spots, parts)),
            dma((spots, parts)),
            *scratch,
        ],
        compiler_params=pltpu.CompilerParams(collective_id=number, has_side_effects=True),
        name=f"sum{number}",
    )(small, *(array for array, _ in sources), *pieces, *into)
    return outs[0], list(outs[1:])


def body(
    boundary,
    lengths,
    routes,
    attn_gain,
    query_weight,
    compress_weight,
    latent_gain,
    expand_weight,
    output_weight,
    ffn_gain,
    router_weight,
    shared_in,
    shared_out,
    expert_in,
    expert_out,
):
    attn_gain, latent_gain, ffn_gain = attn_gain[0], latent_gain[0], ffn_gain[0]
    query_weight, compress_weight = query_weight[0], compress_weight[0]
    expand_weight, output_weight = expand_weight[0], output_weight[0]
    router_weight, shared_out, expert_out = router_weight[0], shared_out[0], expert_out[0, 0]
    width = boundary.shape[3]
    rows = boundary.shape[2]
    half = shared_out.shape[0]
    units = expert_out.shape[0]
    experts_count = router_weight.shape[1]
    shared_in_t = jnp.transpose(shared_in[0], (1, 2, 0)).reshape(2 * half, width)
    joined_in = (
        expert_in.reshape(width, 2 * units),
        jnp.pad(router_weight, ((0, 0), (0, -experts_count % 128))),
    )
    joined_width = sum(piece.shape[1] for piece in joined_in)

    packs, members = lax.axis_size(PACKS), lax.axis_size(MEMBERS)
    count = packs * members
    pack, member = lax.axis_index(PACKS), lax.axis_index(MEMBERS)
    me = pack * members + member
    is_first = lax.axis_index(SECTION) == 0
    pack_rows = members * rows
    all_rows = count * rows
    heads = output_weight.shape[0] // VD
    top = routes.shape[3]
    tiles = [Tiles(all_rows, pack_rows, pack, active) for active in range(2)]
    fusing = members == 4 and tiles[0].tile == 2 * rows

    def own_pack(value):
        size = value.shape[0] // packs
        return lax.dynamic_slice_in_dim(value, pack * size, size, 0)

    freqs = rope_base ** (-jnp.arange(HALF, dtype=jnp.float32) / HALF)
    angles = jnp.arange(rows, dtype=jnp.float32)[:, None] * freqs[None, :]
    turns = jnp.concatenate([jnp.cos(angles), jnp.sin(angles)], axis=1)

    def tables_of(block_lengths):
        segment, position = block_layout(block_lengths, rows)
        blocks = segment.shape[0]
        chosen = position.reshape(-1)[:, None] == jnp.arange(rows, dtype=jnp.int32)[None, :]
        found = jnp.dot(
            chosen.astype(jnp.float32),
            turns,
            precision=lax.Precision.HIGHEST,
            preferred_element_type=jnp.float32,
        )
        return (
            found[:, :HALF],
            found[:, HALF:],
            segment.reshape(blocks * rows, 1),
            segment.reshape(blocks, 1, rows),
        )

    own_lengths = lax.dynamic_index_in_dim(lengths[0, 0], member, 0, keepdims=False)
    layout = jnp.concatenate(
        [
            jnp.transpose(routes[0, 0]),
            jnp.pad(own_lengths, (0, rows - own_lengths.shape[0]))[None],
            jnp.zeros((-(top + 1) % 8, rows), jnp.int32),
        ],
        axis=0,
    )


    def routed_of(layout_all):
        named = layout_all.reshape(count, -1, rows)[:, :top] == me
        return jnp.any(named, axis=1).astype(jnp.float32).reshape(all_rows, 1)

    tables_pack = tables_of(lengths[0, 0])
    tables_own = tables_of(own_lengths[None])
    own_cos, own_sin = tables_own[:2]
    own_column = (lax.broadcasted_iota(jnp.int32, (1, experts_count), 1) == me).astype(jnp.float32)

    def inputs_of(hidden):
        normed32, scale_attn = rms_forward(hidden, attn_gain)
        normed = bf16(normed32)
        compressed = dot(normed, compress_weight)
        latent32, scale_latent = rms_forward(compressed[:, :LAT], latent_gain)
        keyed = bf16(
            jnp.concatenate([latent32, rotate(compressed[:, LAT:], own_cos, own_sin)], axis=1)
        )
        return normed, keyed, (compressed, scale_attn, scale_latent)

    def run_experts(section, x, routed, gathered, into, number, full):
        at = tiles[section]
        results = [
            at.result(2 * units),
            at.result(units),
            at.result(experts_count, jnp.float32),
            at.pack_result(half),
        ]
        weights = [joined_in, (shared_in_t,)]
        if full:
            results.append(at.result(width))
            weights += [(expert_out,), (shared_out,)]
        if fusing:
            shapes = [(shape, index == 3) for index, (shape, _) in enumerate(results)]
            return fused_call(
                at, x, number, section, experts_body, own_column, [(routed, False)], weights, shapes, gathered, into
            )
        (x_all,) = gather_blocks([x], True, number, section, [gathered])
        return x_all, at.call(
            tiled(experts_body),
            "experts",
            [(x_all, at.source(width)), (own_column, at.small(own_column)), (routed, at.source(1))],
            weights,
            results,
            into[:4],
        )

    def summed_over(section, number, body_of, name, sources, weights, results, into, scratch=()):
        at = tiles[section]
        if fusing:
            shapes = [(shape, shape.ndim == 3) for shape, _ in results]
            return sum_call(rows, number, section, body_of, own_column, sources, weights, shapes, into, scratch)
        specs = [(array, at.pack_source(half) if kind else at.source(array.shape[1])) for array, kind in sources]
        specs.insert(1, (own_column, at.small(own_column)))
        *found, partial = at.call(
            tiled(body_of), name, specs, weights, [*results, at.result(width)], into, scratch
        )
        return scatter_blocks(partial, rows, True, number, section), found

    def run_experts_back(section, number, grad_all, routed, stored, into):
        at = tiles[section]
        pre, _, prob, shared_pre = stored
        return summed_over(
            section,
            number,
            experts_back_body,
            "experts_back",
            [(grad_all, False), (pre, False), (prob, False), (routed, False), (shared_pre, True)],
            [joined_in, (shared_in_t,), (expert_out,), (shared_out,)],
            [at.result(2 * units), at.result(1, jnp.float32)],
            into,
            [pltpu.VMEM((at.tile, joined_width), jnp.bfloat16)],
        )

    def prepare(section, normed_all, keyed_all, ffn_all, tables, into):
        at = tiles[section]
        cosine, sine, seg_col, seg_row = tables
        blocks = at.tile // rows
        row_spec = pl.BlockSpec((blocks, 1, rows), lambda i, control: (i * control[2], 0, 0))
        found = at.call(
            tiled(functools.partial(heads_body, rows)),
            "heads",
            [
                (normed_all, at.source(width)),
                (keyed_all, at.source(LAT + ROPE)),
                (cosine, at.source(HALF)),
                (sine, at.source(HALF)),
                (seg_col, at.source(1)),
                (seg_row, row_spec),
            ],
            [(query_weight,), (expand_weight,)],
            [at.result(heads * VD), at.result(heads * QK), at.result(heads * KV)],
            into[:3],
            [pltpu.VMEM((at.tile, heads * QK), jnp.float32)],
            flops=4 * all_rows * width * heads * QK,
        )
        shared = at.call(
            tiled(shared_body),
            "shared",
            [(ffn_all, at.source(width))],
            [(shared_in_t,)],
            [at.pair_result(half), at.result(half)],
            into[3:],
            flops=4 * all_rows * width * half,
        )
        return [*found, *shared]

    fresh = boundary[0, 0].astype(jnp.float32)

    normed, keyed, _ = inputs_of(fresh)
    normed_pack, keyed_pack, layout_all = gather_blocks(
        [normed, keyed, layout], True, 0, 0, wide=[False, False, True]
    )
    attended, _ = attend(
        dot(normed_pack, query_weight),
        bf16(dot(keyed_pack[:, :LAT], expand_weight)),
        keyed_pack,
        tables_pack,
    )
    mixed_first = fresh + scatter_blocks(bf16(dot(attended, output_weight)), rows, False, 1, 0)
    empty = [
        blank((all_rows, width), jnp.bfloat16),
        *(
            blank(shape, dtype)
            for shape, dtype in (
                ((all_rows + tiles[0].tile, 2 * units), jnp.bfloat16),
                ((all_rows + tiles[0].tile, units), jnp.bfloat16),
                ((all_rows + tiles[0].tile, experts_count), jnp.float32),
                ((2, pack_rows + tiles[0].tile, half), jnp.bfloat16),
            )
        ),
    ]
    ffn_all, (*stored, partial) = run_experts(
        0, bf16(rms_forward(mixed_first, ffn_gain)[0]), routed_of(layout_all), empty[0], empty[1:], 2, True
    )
    result_first = mixed_first + scatter_blocks(partial, rows, True, 3, 0)
    heads_weights = spread_blocks([query_weight, expand_weight, output_weight], 4, 1)
    target_all, layout_all = gather_blocks(
        [boundary[0, 0], layout], True, 5, 1, [blank((all_rows, width), jnp.bfloat16), layout_all]
    )
    sent, target_all, layout_all, heads_weights = lax.optimization_barrier(
        (bf16(result_first), target_all, layout_all, heads_weights)
    )
    inbound = lax.ppermute(sent, SECTION, [(0, 1)])
    routed = routed_of(layout_all)
    tables_all = tables_of(layout_all.reshape(count, -1, rows)[:, top, : lengths.shape[3]])
    query_heads, expand_heads, output_heads = (
        value.reshape(members, -1, value.shape[1]) for value in heads_weights
    )

    hidden = jnp.where(is_first, fresh, inbound.astype(jnp.float32))
    normed, keyed, (compressed, scale_attn, scale_latent) = inputs_of(hidden)
    latent = bf16(jnp.einsum("rd,mdc->mrc", keyed[:, :LAT], expand_heads, preferred_element_type=jnp.float32))
    latent = latent.reshape(members * rows, -1)
    query_raw = jnp.einsum("rd,mdc->mrc", normed, query_heads, preferred_element_type=jnp.float32)
    attended, query = attend(query_raw.reshape(members * rows, -1), latent, keyed, tables_own, members)
    mixed = hidden + jnp.einsum(
        "mrc,mcd->rd", attended.reshape(members, rows, -1), output_heads, preferred_element_type=jnp.float32
    )
    mixed = jnp.where(is_first, mixed_first, mixed)
    ffn32, scale_ffn = rms_forward(mixed, ffn_gain)
    ffn_all, stored = run_experts(1, bf16(ffn32), routed, ffn_all, stored, 6, False)

    def latent_back(own):
        grad_latent, grad_latent_gain = rms_backward(
            compressed[:, :LAT], scale_latent, latent_gain, own[:, width : width + LAT]
        )
        grad_compressed = bf16(
            jnp.concatenate([grad_latent, rotate(own[:, width + LAT :], own_cos, -own_sin)], axis=1)
        )
        grad_normed = own[:, :width] + dot_t(grad_compressed, compress_weight)
        grad_hidden_norm, grad_attn_gain = rms_backward(hidden, scale_attn, attn_gain, grad_normed)
        return grad_compressed, grad_hidden_norm, grad_attn_gain, grad_latent_gain

    grad_ffn_second, grad_units = run_experts_back(1, 7, target_all, routed, stored, ())
    grad_mixed = fresh + rms_backward(mixed, scale_ffn, ffn_gain, grad_ffn_second)[0]
    grad_attended = jnp.einsum(
        "rd,mcd->mrc", bf16(grad_mixed), output_heads, preferred_element_type=jnp.float32
    )
    grad_query, grad_latent_heads, grad_shared_key = attend_back(
        query, latent, keyed, bf16(grad_attended).reshape(members * rows, -1), tables_own, members
    )
    own_second = jnp.concatenate(
        [
            jnp.einsum(
                "mrc,mdc->rd",
                grad_query.reshape(members, rows, -1),
                query_heads,
                preferred_element_type=jnp.float32,
            ),
            jnp.einsum(
                "mrc,mdc->rd",
                grad_latent_heads.reshape(members, rows, -1),
                expand_heads,
                preferred_element_type=jnp.float32,
            ),
            jnp.sum(grad_shared_key.reshape(members, rows, -1), axis=0),
        ],
        axis=1,
    )
    grad_second = bf16(grad_mixed + latent_back(own_second)[1])

    all_inputs = gather_blocks([normed, keyed], True, 8, 0)
    prepared = prepare(0, *all_inputs, ffn_all, tables_all, ())
    grad_second, prepared, all_inputs = lax.optimization_barrier((grad_second, prepared, all_inputs))
    downbound = lax.ppermute(grad_second, SECTION, [(1, 0)]).astype(jnp.float32)

    normed_late, keyed_late, gated_late, _ = lax.optimization_barrier((normed, keyed, stored[1], grad_second))
    finished, _ = summed_over(
        1,
        10,
        finish_body,
        "finish",
        [(gated_late, False), (stored[3], True)],
        [(expert_out,), (shared_out,)],
        [],
        (),
    )
    result = mixed + finished
    upstream = jnp.where(is_first, downbound, fresh)
    (upstream_all,) = gather_blocks([bf16(upstream)], True, 11, 0, [target_all])
    grad_ffn, (grad_pre, moved) = run_experts_back(0, 12, upstream_all, routed, stored, grad_units)
    grad_ffn = jnp.where(is_first, grad_ffn, grad_ffn_second)
    normed_late, keyed_late, _ = lax.optimization_barrier((normed_late, keyed_late, finished))
    normed_all, keyed_all = gather_blocks([normed_late, keyed_late], True, 9, 1, all_inputs)
    prepared = prepare(1, normed_all, keyed_all, ffn_all, tables_all, prepared)
    attended_all, query_all, latent_all, shared_pre, shared_hid = prepared
    attended_all, shared_hid = attended_all[:all_rows], shared_hid[:all_rows]
    grad_mixed_norm, grad_ffn_gain = rms_backward(mixed, scale_ffn, ffn_gain, grad_ffn)
    grad_mixed = upstream + grad_mixed_norm
    grad_mixed_all = lax.all_gather(bf16(grad_mixed), BOTH, axis=0, tiled=True)
    grad_attended = bf16(dot_t(grad_mixed_all, output_weight))
    grad_query, grad_latent_heads, grad_shared_key = attend_back(
        query_all, latent_all, keyed_all, grad_attended, tables_all
    )
    own = lax.psum_scatter(
        bf16(
            jnp.concatenate(
                [
                    dot_t(own_pack(grad_query), query_weight),
                    dot_t(own_pack(grad_latent_heads), expand_weight),
                    own_pack(grad_shared_key),
                ],
                axis=1,
            )
        ),
        MEMBERS,
        scatter_dimension=0,
        tiled=True,
    ).astype(jnp.float32)
    grad_compressed, grad_hidden_norm, grad_attn_gain, grad_latent_gain = latent_back(own)
    grad_hidden = grad_mixed + grad_hidden_norm

    small = jnp.concatenate([grad_attn_gain, grad_latent_gain, grad_ffn_gain, moved[:all_rows, 0]])
    small = jnp.pad(small, (0, -small.shape[0] % 1024)).reshape(8, -1)
    grad_compressed_all, small_all = gather_blocks([grad_compressed, small], True, 13)
    small_all = small_all.reshape(count, -1)
    gains = jnp.sum(small_all[:, : 2 * width + LAT], axis=0)
    moved_all = small_all[:, 2 * width + LAT : 2 * width + LAT + all_rows].T
    prob = stored[2][:all_rows]
    grad_logits = bf16(moved_all - prob * jnp.sum(moved_all, axis=1, keepdims=True))
    left, right = gated_back(
        shared_pre[0, :all_rows].astype(jnp.float32),
        shared_pre[1, :all_rows].astype(jnp.float32),
        dot_t(upstream_all, shared_out),
    )
    grad_shared_in = lax.dot_general(
        jnp.stack([left, right]), ffn_all, (((1,), (0,)), ((), ())), preferred_element_type=jnp.float32
    )
    ends = jnp.where(is_first, grad_hidden, result)
    return (
        ends[None, None],
        gains[:width][None],
        t_dot(normed_all, grad_query)[None],
        t_dot(normed_all, grad_compressed_all)[None],
        gains[width : width + LAT][None],
        t_dot(keyed_all[:, :LAT], grad_latent_heads)[None],
        t_dot(attended_all, grad_mixed_all)[None],
        gains[width + LAT :][None],
        t_dot(ffn_all, grad_logits)[None],
        jnp.transpose(grad_shared_in, (2, 0, 1))[None],
        t_dot(shared_hid, upstream_all)[None],
        pair_grad(ffn_all, grad_pre)[None, None],
        t_dot(stored[1][:all_rows], upstream_all)[None, None],
    )


def solution(mesh):
    return jax.shard_map(
        body,
        mesh=mesh,
        in_specs=(
            P(SECTION, None, BOTH, None),
            P(None, PACKS, None, None),
            P(SECTION, None, BOTH, None),
            P(SECTION, None),
            P(SECTION, None, MEMBERS),
            P(SECTION, None, None),
            P(SECTION, None),
            P(SECTION, None, MEMBERS),
            P(SECTION, MEMBERS, None),
            P(SECTION, None),
            P(SECTION, None, None),
            P(SECTION, None, None, MEMBERS),
            P(SECTION, MEMBERS, None),
            P(SECTION, BOTH, None, None, None),
            P(SECTION, BOTH, None, None),
        ),
        out_specs=(
            P(SECTION, None, BOTH, None),
            P(SECTION, None),
            P(SECTION, None, MEMBERS),
            P(SECTION, None, None),
            P(SECTION, None),
            P(SECTION, None, MEMBERS),
            P(SECTION, MEMBERS, None),
            P(SECTION, None),
            P(SECTION, None, None),
            P(SECTION, None, None, MEMBERS),
            P(SECTION, MEMBERS, None),
            P(SECTION, BOTH, None, None, None),
            P(SECTION, BOTH, None, None),
        ),
        check_vma=False,
    )
```

```python
import functools

import jax
import jax.numpy as jnp
from jax import lax
from jax.experimental import pallas as pl
from jax.experimental.pallas import tpu as pltpu
from jax.sharding import PartitionSpec as P

NOPE = 128
ROPE = 64
VD = 128
LAT = 512

QK = NOPE + ROPE
KV = NOPE + VD
HALF = ROPE // 2
epsilon = 1e-06
rope_base = 10000.0
masked_score = -1e30
SECTION, PACKS, MEMBERS = "section", "dp", "expert"
BOTH = (PACKS, MEMBERS)
MESH = pl.DeviceIdType.MESH
def dot(left, right):
    return jnp.dot(left, right, preferred_element_type=jnp.float32)


def dot_t(left, right):
    return lax.dot_general(
        left, right, (((1,), (1,)), ((), ())), preferred_element_type=jnp.float32
    )


def t_dot(left, right):
    return lax.dot_general(
        left, right, (((0,), (0,)), ((), ())), preferred_element_type=jnp.float32
    )


def bf16(value):
    return value.astype(jnp.bfloat16)


def rms_forward(inputs, gain_vec):
    norm_scale = lax.rsqrt(jnp.mean(inputs * inputs, axis=-1, keepdims=True) + epsilon)
    return (inputs * norm_scale * gain_vec, norm_scale)


def rms_backward(inputs, norm_scale, gain_vec, upstream):
    weighted = upstream * gain_vec
    grad_gain = jnp.sum(upstream * inputs * norm_scale, axis=0)
    cubed = norm_scale * norm_scale * norm_scale
    grad_inputs = norm_scale * weighted - inputs * cubed * jnp.mean(
        weighted * inputs, axis=-1, keepdims=True
    )
    return (grad_inputs, grad_gain)


def rotate(inputs, cosine, sine):
    half = cosine.shape[-1]
    former = inputs[..., :half]
    latter = inputs[..., half:]
    return jnp.concatenate(
        [former * cosine - latter * sine, latter * cosine + former * sine], axis=-1
    )


def silu_parts(pre_gate):
    sigmoid = jax.nn.sigmoid(pre_gate)
    return (pre_gate * sigmoid, sigmoid * (1.0 + pre_gate * (1.0 - sigmoid)))


def block_layout(block_lengths, rows):
    index = lax.broadcasted_iota(jnp.int32, (block_lengths.shape[0], rows), 1)
    start, segment, opening = 0, 0, 0
    for sequence in range(block_lengths.shape[1]):
        begun = index >= start
        segment = segment + begun.astype(jnp.int32)
        opening = jnp.where(begun, start, opening)
        start = start + block_lengths[:, sequence : sequence + 1]
    return segment, index - opening


def places(spots):
    member = lax.axis_index(MEMBERS)
    spot = lax.axis_index(PACKS) if spots > 1 else 0
    return spot, member // 2, lax.rem(member, 2)


def to_partner(chip, core):
    return {MEMBERS: chip * 2 + 1 - core}


def to_other(chip, core):
    return {MEMBERS: (1 - chip) * 2 + core}


def when(condition, action):
    if condition is True:
        action()
    else:
        pl.when(condition)(action)


def greet(spots, spot, chip, core):
    barrier = pltpu.get_barrier_semaphore()

    def signal(target):
        pl.semaphore_signal(barrier, inc=1, device_id=target, device_id_type=MESH)

    signal(to_partner(chip, core))
    signal(to_other(chip, core))
    if spots > 1:
        pl.when(spot > 0)(lambda: signal({PACKS: spot - 1}))
        pl.when(spot < spots - 1)(lambda: signal({PACKS: spot + 1}))
        ends = jnp.where(spot > 0, 1, 0) + jnp.where(spot < spots - 1, 1, 0)
        pl.semaphore_wait(barrier, 2 + ends)
    else:
        pl.semaphore_wait(barrier, 2)


def remote(source, target_ref, target, out_sem, in_sem):
    return pltpu.make_async_remote_copy(
        src_ref=source,
        dst_ref=target_ref,
        send_sem=out_sem,
        recv_sem=in_sem,
        device_id=target,
        device_id_type=MESH,
    )


def slot(spot, chip, core):
    return spot * 4 + chip * 2 + core


def gather_kernel(spots, cuts, wide, active, *refs):
    arrays = len(cuts)
    x_refs, o_refs, sems = refs[:arrays], refs[-9 - arrays : -9], refs[-9:]
    own_sem, up_out, up_in, down_out, down_in, over_out, over_in, pair_out, pair_in = sems
    units = [
        (a, pl.ds(part * (x_refs[a].shape[0] // parts), x_refs[a].shape[0] // parts))
        for a, parts in enumerate(cuts)
        for part in range(parts)
    ]

    def run():
        spot, chip, core = places(spots)
        greet(spots, spot, chip, core)

        def piece(unit, index):
            array, cut = units[unit]
            return o_refs[array].at[index, cut]

        def first(unit):
            array, cut = units[unit]
            return x_refs[array].at[cut]

        def lane(unit):
            return wide[units[unit][0]]

        def spread(unit):
            return range(spots) if lane(unit) else [0]

        def up(source, at, unit, reach):
            return remote(
                source, piece(unit, slot(at, chip, core)), {PACKS: spot + 1}, up_out.at[reach, unit], up_in.at[reach, unit]
            )

        def down(source, at, unit, reach):
            return remote(
                source,
                piece(unit, slot(at, chip, core)),
                {PACKS: spot - 1},
                down_out.at[reach, unit],
                down_in.at[reach, unit],
            )

        def over(source, at, unit):
            return remote(
                source, piece(unit, slot(at, chip, core)), to_other(chip, core), over_out.at[at, unit], over_in.at[at, unit]
            )

        def pair(source, at, c, unit):
            return remote(
                source,
                piece(unit, slot(at, c, core)),
                to_partner(chip, core),
                pair_out.at[c, at, unit],
                pair_in.at[c, at, unit],
            )

        home = lambda unit: spot if lane(unit) else 0
        for unit in range(len(units)):
            source = first(unit)
            over(source, home(unit), unit).start()
            if spots > 1 and lane(unit):
                pl.when(spot < spots - 1)(lambda: up(source, spot, unit, 0).start())
                pl.when(spot > 0)(lambda: down(source, spot, unit, 0).start())
            pair(source, home(unit), chip, unit).start()
        own = [
            pltpu.make_async_copy(
                x_refs[a], o_refs[a].at[slot(spot if wide[a] else 0, chip, core)], own_sem.at[a]
            )
            for a in range(arrays)
        ]
        for copy in own:
            copy.start()
        for reach in range(1, spots):
            for unit in range(len(units)):
                if not lane(unit):
                    continue

                def below(reach=reach, unit=unit):
                    at = spot - reach
                    source = piece(unit, slot(at, chip, core))
                    up(source, at, unit, reach - 1).wait_recv()
                    pl.when(spot < spots - 1)(lambda: up(source, at, unit, reach).start())
                    over(source, at, unit).start()
                    pair(source, at, chip, unit).start()

                def above(reach=reach, unit=unit):
                    at = spot + reach
                    source = piece(unit, slot(at, chip, core))
                    down(source, at, unit, reach - 1).wait_recv()
                    pl.when(spot > 0)(lambda: down(source, at, unit, reach).start())
                    over(source, at, unit).start()
                    pair(source, at, chip, unit).start()

                pl.when(spot >= reach)(below)
                pl.when(spot + reach < spots)(above)
        for reach in range(spots):
            sides = [(True, spot)]
            if reach > 0:
                sides = [(spot >= reach, spot - reach), (spot + reach < spots, spot + reach)]
            for unit in range(len(units)):
                if not lane(unit) and reach > 0:
                    continue
                for there, at in sides:
                    at = at if lane(unit) else 0

                    def hand_on(at=at, unit=unit):
                        source = piece(unit, slot(at, 1 - chip, core))
                        over(source, at, unit).wait_recv()
                        pair(source, at, 1 - chip, unit).start()

                    when(there, hand_on)
        for copy in own:
            copy.wait()
        for unit in range(len(units)):
            source = first(unit)
            for at in spread(unit):
                over(source, at, unit).wait_send()
                for c in range(2):
                    pair(source, at, c, unit).wait()
            for reach in range(spots - 1 if lane(unit) else 0):
                pl.when((spot >= reach) & (spot < spots - 1))(lambda: up(source, spot, unit, reach).wait_send())
                pl.when((spot + reach < spots) & (spot > 0))(lambda: down(source, spot, unit, reach).wait_send())

    if active is None:
        run()
    else:
        pl.when(lax.axis_index(SECTION) == active)(run)


def gather_blocks(values, across, number, active=None, into=None, parts=4, wide=None):
    wide = [across] * len(values) if wide is None else wide
    if lax.axis_size(MEMBERS) != 4:
        found = [
            lax.all_gather(value, BOTH if far else MEMBERS, axis=0, tiled=True) for value, far in zip(values, wide)
        ]
        if into is None:
            return found
        chosen = lax.axis_index(SECTION) == active
        return [jnp.where(chosen, new, old) for new, old in zip(found, into)]
    spots = lax.axis_size(PACKS) if across else 1
    cuts = [parts if value.shape[0] % (16 * parts) == 0 else 1 for value in values]
    units = sum(cuts)
    dma = pltpu.SemaphoreType.DMA
    hops = max(spots - 1, 1)
    shapes = [
        jax.ShapeDtypeStruct(((spots if far else 1) * 4, *value.shape), value.dtype)
        for value, far in zip(values, wide)
    ]
    held = [] if into is None else [old.reshape(shape.shape) for old, shape in zip(into, shapes)]
    outs = pl.pallas_call(
        functools.partial(gather_kernel, spots, cuts, wide, active),
        out_shape=shapes,
        in_specs=[pl.BlockSpec(memory_space=pltpu.VMEM)] * len(values)
        + [pl.BlockSpec(memory_space=pl.ANY)] * len(held),
        out_specs=[pl.BlockSpec(memory_space=pl.ANY)] * len(values),
        input_output_aliases={len(values) + index: index for index in range(len(held))},
        scratch_shapes=[
            dma((len(values),)),
            dma((hops, units)),
            dma((hops, units)),
            dma((hops, units)),
            dma((hops, units)),
            dma((spots, units)),
            dma((spots, units)),
            dma((2, spots, units)),
            dma((2, spots, units)),
        ],
        compiler_params=pltpu.CompilerParams(collective_id=number, has_side_effects=True),
        name=f"gather{number}",
    )(*values, *held)
    return [out.reshape(-1, out.shape[2]) for out in outs]


def spread_kernel(cuts, active, *refs):
    arrays = len(cuts)
    sources, o_refs, x_refs = refs[:arrays], refs[arrays : 2 * arrays], refs[2 * arrays : 3 * arrays]
    own_sem, over_out, over_in, side_out, side_in, pair_out, pair_in = refs[3 * arrays :]
    units = [
        (a, pl.ds(part * (x_refs[a].shape[0] // parts), x_refs[a].shape[0] // parts))
        for a, parts in enumerate(cuts)
        for part in range(parts)
    ]

    def run():
        taken_in = [pltpu.make_async_copy(sources[a], x_refs[a], own_sem.at[a]) for a in range(arrays)]
        for copy in taken_in:
            copy.start()
        for copy in taken_in:
            copy.wait()
        member, spot = lax.axis_index(MEMBERS), lax.axis_index(PACKS)
        chip, core, odd = member // 2, lax.rem(member, 2), lax.rem(spot, 2)
        beside = {PACKS: spot + 1 - 2 * odd}
        barrier = pltpu.get_barrier_semaphore()
        for target in (to_partner(chip, core), to_other(chip, core), beside):
            pl.semaphore_signal(barrier, inc=1, device_id=target, device_id_type=MESH)
        pl.semaphore_wait(barrier, 3)

        def piece(unit, c):
            array, cut = units[unit]
            return o_refs[array].at[c * 2 + core, cut]

        def first(unit):
            array, cut = units[unit]
            return x_refs[array].at[cut]

        def over(unit):
            return remote(first(unit), piece(unit, chip), to_other(chip, core), over_out.at[unit], over_in.at[unit])

        def side(unit):
            source = piece(unit, 1 - chip)
            return remote(source, source, beside, side_out.at[unit], side_in.at[unit])

        def pair(source, unit, c, index):
            return remote(
                source, piece(unit, c), to_partner(chip, core), pair_out.at[index, unit], pair_in.at[index, unit]
            )

        for unit in range(len(units)):
            pl.when(odd == unit % 2)(lambda: over(unit).start())
        for unit in range(len(units)):
            pair(first(unit), unit, chip, 0).start()
        own = [
            pltpu.make_async_copy(x_refs[a], o_refs[a].at[member], own_sem.at[a]) for a in range(arrays)
        ]
        for copy in own:
            copy.start()
        for unit in range(len(units)):

            def taken(unit=unit):
                over(unit).wait_recv()
                side(unit).start()
                pair(piece(unit, 1 - chip), unit, 1 - chip, 1).start()

            pl.when(odd == unit % 2)(taken)
        for unit in range(len(units)):

            def handed(unit=unit):
                side(unit).wait_recv()
                pair(piece(unit, 1 - chip), unit, 1 - chip, 1).start()

            pl.when(odd != unit % 2)(handed)
        for copy in own:
            copy.wait()
        for unit in range(len(units)):

            def sent(unit=unit):
                over(unit).wait_send()
                side(unit).wait_send()

            pl.when(odd == unit % 2)(sent)
            pair(first(unit), unit, chip, 0).wait()
            pair(first(unit), unit, 1 - chip, 1).wait()

    pl.when(lax.axis_index(SECTION) == active)(run)


def spread_blocks(values, number, active, parts=8):
    if lax.axis_size(MEMBERS) != 4 or lax.axis_size(PACKS) % 2:
        return gather_blocks(values, False, number, active)
    units = parts * len(values)
    dma = pltpu.SemaphoreType.DMA
    outs = pl.pallas_call(
        functools.partial(spread_kernel, [parts] * len(values), active),
        out_shape=[jax.ShapeDtypeStruct((4, *value.shape), value.dtype) for value in values],
        in_specs=[pl.BlockSpec(memory_space=pl.ANY)] * len(values),
        out_specs=[pl.BlockSpec(memory_space=pl.ANY)] * len(values),
        scratch_shapes=[
            *(pltpu.VMEM(value.shape, value.dtype) for value in values),
            dma((len(values),)),
            dma((units,)),
            dma((units,)),
            dma((units,)),
            dma((units,)),
            dma((2, units)),
            dma((2, units)),
        ],
        compiler_params=pltpu.CompilerParams(collective_id=number, has_side_effects=True),
        name=f"spread{number}",
    )(*values)
    return [out.reshape(-1, out.shape[2]) for out in outs]


def add_into(target, sources, rows, step=16):
    def some(index, carry):
        at = pl.ds(pl.multiple_of(index * step, step), step)
        total = sources[0][at, :].astype(jnp.float32)
        for source in sources[1:]:
            total = total + source[at, :].astype(jnp.float32)
        target[at, :] = total.astype(target.dtype)
        return carry

    lax.fori_loop(0, rows // step, some, 0)


def scatter_kernel(
    spots,
    parts,
    active,
    x_ref,
    o_ref,
    own_buf,
    pair_buf,
    over_src,
    over_buf,
    line_src,
    up_buf,
    down_buf,
    own_in,
    pair_out,
    pair_in,
    over_out,
    over_in,
    line_out,
    up_in,
    down_in,
):
    rows = x_ref.shape[1] // parts
    cut = lambda part: pl.ds(part * rows, rows)

    def run():
        spot, chip, core = places(spots)
        greet(spots, spot, chip, core)

        def order(step):
            if step == spots - 1:
                return spot
            fall = spots - 1 - step
            fall = jnp.where(fall <= spot, fall - 1, fall)
            rise = jnp.where(step >= spot, step + 1, step)
            return jnp.where(2 * spot < spots - 1, fall, rise)

        def pair(at, c, part):
            return remote(
                x_ref.at[slot(at, c, 1 - core), cut(part)],
                pair_buf.at[at, c, cut(part)],
                to_partner(chip, core),
                pair_out.at[at, c, part],
                pair_in.at[at, c, part],
            )

        def over(at, part):
            return remote(
                over_src.at[at, cut(part)],
                over_buf.at[at, cut(part)],
                to_other(chip, core),
                over_out.at[at, part],
                over_in.at[at, part],
            )

        def up(at, part):
            return remote(
                line_src.at[at, cut(part)],
                up_buf.at[at, cut(part)],
                {PACKS: spot + 1},
                line_out.at[at, part],
                up_in.at[at, part],
            )

        def down(at, part):
            return remote(
                line_src.at[at, cut(part)],
                down_buf.at[at, cut(part)],
                {PACKS: spot - 1},
                line_out.at[at, part],
                down_in.at[at, part],
            )

        def own(at, c):
            return pltpu.make_async_copy(x_ref.at[slot(at, c, core)], own_buf.at[at, c], own_in.at[at, c])

        for c in (1 - chip, chip):
            for step in range(spots):
                own(order(step), c).start()
                for part in range(parts):
                    pair(order(step), c, part).start()
        for step in range(spots):
            at = order(step)
            own(at, 1 - chip).wait()
            for part in range(parts):
                pair(at, 1 - chip, part).wait_recv()
                add_into(
                    over_src.at[at, cut(part)],
                    [own_buf.at[at, 1 - chip, cut(part)], pair_buf.at[at, 1 - chip, cut(part)]],
                    rows,
                )
                over(at, part).start()
        for step in range(spots):
            at = order(step)
            own(at, chip).wait()
            for part in range(parts):
                pair(at, chip, part).wait_recv()
                over(at, part).wait_recv()
                base = [
                    own_buf.at[at, chip, cut(part)],
                    pair_buf.at[at, chip, cut(part)],
                    over_buf.at[at, cut(part)],
                ]
                ups, downs = up_buf.at[at, cut(part)], down_buf.at[at, cut(part)]
                if step < spots - 1:
                    target = line_src.at[at, cut(part)]

                    def rising(first):
                        if not first:
                            up(at, part).wait_recv()
                        add_into(target, base if first else base + [ups], rows)
                        up(at, part).start()

                    def falling(first):
                        if not first:
                            down(at, part).wait_recv()
                        add_into(target, base if first else base + [downs], rows)
                        down(at, part).start()

                    pl.when((at > spot) & (spot == 0))(lambda: rising(True))
                    pl.when((at > spot) & (spot > 0))(lambda: rising(False))
                    pl.when((at < spot) & (spot == spots - 1))(lambda: falling(True))
                    pl.when((at < spot) & (spot < spots - 1))(lambda: falling(False))
                elif spots == 1:
                    add_into(o_ref.at[cut(part)], base, rows)
                else:

                    def finish(ends):
                        if ends < 1:
                            up(at, part).wait_recv()
                        if ends > -1:
                            down(at, part).wait_recv()
                        extra = ([ups] if ends < 1 else []) + ([downs] if ends > -1 else [])
                        add_into(o_ref.at[cut(part)], base + extra, rows)

                    pl.when(spot == 0)(lambda: finish(1))
                    pl.when(spot == spots - 1)(lambda: finish(-1))
                    pl.when((spot > 0) & (spot < spots - 1))(lambda: finish(0))
        for part in range(parts):
            for step in range(spots):
                at = order(step)
                pair(at, 0, part).wait_send()
                pair(at, 1, part).wait_send()
                over(at, part).wait_send()
                if step < spots - 1:
                    up(at, part).wait_send()

    if active is None:
        run()
    else:
        pl.when(lax.axis_index(SECTION) == active)(run)


def scatter_blocks(partial, rows, across, number, active=None, parts=4):
    if lax.axis_size(MEMBERS) != 4:
        axes = BOTH if across else MEMBERS
        taken = partial[: rows * lax.axis_size(axes)]
        return lax.psum_scatter(taken, axes, scatter_dimension=0, tiled=True).astype(jnp.float32)
    spots = lax.axis_size(PACKS) if across else 1
    width = partial.shape[1]
    dma = pltpu.SemaphoreType.DMA
    hold = lambda *lead: pltpu.VMEM((*lead, rows, width), partial.dtype)
    return pl.pallas_call(
        functools.partial(scatter_kernel, spots, parts, active),
        out_shape=jax.ShapeDtypeStruct((rows, width), jnp.float32),
        in_specs=[pl.BlockSpec(memory_space=pl.ANY)],
        out_specs=pl.BlockSpec(memory_space=pltpu.VMEM),
        scratch_shapes=[
            hold(spots, 2),
            hold(spots, 2),
            hold(spots),
            hold(spots),
            hold(spots),
            hold(spots),
            hold(spots),
            dma((spots, 2)),
            dma((spots, 2, parts)),
            dma((spots, 2, parts)),
            dma((spots, parts)),
            dma((spots, parts)),
            dma((spots, parts)),
            dma((spots, parts)),
            dma((spots, parts)),
        ],
        compiler_params=pltpu.CompilerParams(collective_id=number, has_side_effects=True),
        name=f"scatter{number}",
    )(partial.reshape(-1, rows, width))


def allowed_pairs(seg_col, seg_row):
    rows = seg_col.shape[0]
    later = lax.broadcasted_iota(jnp.int32, (rows, rows), 0)
    earlier = lax.broadcasted_iota(jnp.int32, (rows, rows), 1)
    return (seg_col == seg_row) & (earlier <= later)


def attend_kernel(heads, q_ref, lat_ref, key_ref, cos_ref, sin_ref, col_ref, row_ref, out_ref, rot_ref):
    factor = QK**-0.5
    allowed = allowed_pairs(col_ref[...], row_ref[0])
    cosine, sine = cos_ref[...], sin_ref[...]
    shared = key_ref[:, LAT:]
    for head in range(heads):
        raw = q_ref[:, head * QK : (head + 1) * QK]
        query = bf16(
            jnp.concatenate([raw[:, :NOPE], rotate(raw[:, NOPE:], cosine, sine)], axis=1)
        )
        rot_ref[:, head * QK : (head + 1) * QK] = query
        key = jnp.concatenate([lat_ref[:, head * KV : head * KV + NOPE], shared], axis=1)
        value = lat_ref[:, head * KV + NOPE : (head + 1) * KV]
        scores = jnp.where(allowed, dot_t(query, key) * factor, masked_score)
        top = jnp.max(scores, axis=1, keepdims=True)
        powers = jnp.exp(scores - top)
        probs = powers / jnp.sum(powers, axis=1, keepdims=True)
        out_ref[:, head * VD : (head + 1) * VD] = bf16(dot(bf16(probs), value))


def attend(query_raw, latent, keyed, tables, groups=1):
    cosine, sine, seg_col, seg_row = tables
    count, _, rows = seg_row.shape
    heads = query_raw.shape[1] // QK
    block = lambda width: pl.BlockSpec((rows, width), lambda i: (i, 0))
    same = lambda width: pl.BlockSpec((rows, width), lambda i: (0, 0) if groups > 1 else (i, 0))
    count = count * groups
    return pl.pallas_call(
        functools.partial(attend_kernel, heads),
        grid=(count,),
        in_specs=[
            block(heads * QK),
            block(heads * KV),
            same(LAT + ROPE),
            same(HALF),
            same(HALF),
            same(1),
            pl.BlockSpec((1, 1, rows), lambda i: (0, 0, 0) if groups > 1 else (i, 0, 0)),
        ],
        out_specs=[block(heads * VD), block(heads * QK)],
        out_shape=[
            jax.ShapeDtypeStruct((count * rows, heads * VD), jnp.bfloat16),
            jax.ShapeDtypeStruct((count * rows, heads * QK), jnp.bfloat16),
        ],
        name="attend",
        cost_estimate=pl.CostEstimate(
            flops=2 * count * heads * rows * rows * (QK + VD),
            bytes_accessed=count * rows * heads * (QK * 6 + KV * 2 + VD * 2),
            transcendentals=count * heads * rows * rows,
        ),
    )(query_raw, latent, keyed, cosine, sine, seg_col, seg_row)


def attend_back_kernel(
    heads, q_ref, lat_ref, key_ref, grad_ref, cos_ref, sin_ref, col_ref, row_ref, dq_ref, dlat_ref, dkey_ref
):
    factor = QK**-0.5
    allowed = allowed_pairs(col_ref[...], row_ref[0])
    cosine, sine = cos_ref[...], sin_ref[...]
    shared = key_ref[:, LAT:]
    total = None
    for head in range(heads):
        query = q_ref[:, head * QK : (head + 1) * QK]
        key = jnp.concatenate([lat_ref[:, head * KV : head * KV + NOPE], shared], axis=1)
        value = lat_ref[:, head * KV + NOPE : (head + 1) * KV]
        grad = grad_ref[:, head * VD : (head + 1) * VD]
        scores = jnp.where(allowed, dot_t(query, key) * factor, masked_score)
        top = jnp.max(scores, axis=1, keepdims=True)
        powers = jnp.exp(scores - top)
        probs = powers / jnp.sum(powers, axis=1, keepdims=True)
        grad_value = t_dot(bf16(probs), grad)
        grad_probs = dot_t(grad, value)
        centre = jnp.sum(probs * grad_probs, axis=1, keepdims=True)
        grad_scores = bf16(probs * (grad_probs - centre) * factor)
        grad_query = dot(grad_scores, key)
        grad_key = t_dot(grad_scores, query)
        dq_ref[:, head * QK : (head + 1) * QK] = bf16(
            jnp.concatenate(
                [grad_query[:, :NOPE], rotate(grad_query[:, NOPE:], cosine, -sine)], axis=1
            )
        )
        dlat_ref[:, head * KV : head * KV + NOPE] = bf16(grad_key[:, :NOPE])
        dlat_ref[:, head * KV + NOPE : (head + 1) * KV] = bf16(grad_value)
        part = grad_key[:, NOPE:]
        total = part if total is None else total + part
    dkey_ref[...] = total


def attend_back(query, latent, keyed, grad, tables, groups=1):
    cosine, sine, seg_col, seg_row = tables
    count, _, rows = seg_row.shape
    heads = query.shape[1] // QK
    block = lambda width: pl.BlockSpec((rows, width), lambda i: (i, 0))
    same = lambda width: pl.BlockSpec((rows, width), lambda i: (0, 0) if groups > 1 else (i, 0))
    count = count * groups
    return pl.pallas_call(
        functools.partial(attend_back_kernel, heads),
        grid=(count,),
        in_specs=[
            block(heads * QK),
            block(heads * KV),
            same(LAT + ROPE),
            block(heads * VD),
            same(HALF),
            same(HALF),
            same(1),
            pl.BlockSpec((1, 1, rows), lambda i: (0, 0, 0) if groups > 1 else (i, 0, 0)),
        ],
        out_specs=[block(heads * QK), block(heads * KV), block(ROPE)],
        out_shape=[
            jax.ShapeDtypeStruct((count * rows, heads * QK), jnp.bfloat16),
            jax.ShapeDtypeStruct((count * rows, heads * KV), jnp.bfloat16),
            jax.ShapeDtypeStruct((count * rows, ROPE), jnp.float32),
        ],
        name="attend_back",
        cost_estimate=pl.CostEstimate(
            flops=2 * count * heads * rows * rows * (3 * QK + 2 * VD),
            bytes_accessed=count * rows * heads * (QK * 4 + KV * 4 + VD * 2),
            transcendentals=count * heads * rows * rows,
        ),
    )(query, latent, keyed, grad, cosine, sine, seg_col, seg_row)


def gated_hidden(gate, up):
    return silu_parts(gate)[0] * up


def gated_back(gate, up, grad_hidden):
    act, slope = silu_parts(gate)
    return bf16(grad_hidden * up * slope), bf16(grad_hidden * act)


def columns(pieces):
    start = 0
    for piece in pieces:
        yield start, piece.shape[1]
        start += piece.shape[1]


def hold_weight(pieces):
    return pltpu.VMEM((pieces[0].shape[0], sum(piece.shape[1] for piece in pieces)), pieces[0].dtype)


def loads_of(counts, sources, targets, sems):
    copies = []
    for pieces, target in zip(counts, targets):
        group, sources = sources[:pieces], sources[pieces:]
        for source, (start, size) in zip(group, columns(group)):
            place = target if pieces == 1 else target.at[:, pl.ds(start, size)]
            copies.append(pltpu.make_async_copy(source, place, sems.at[len(copies)]))
    return copies


def load(*args):
    copies = loads_of(*args)
    for copy in copies:
        copy.start()
    for copy in copies:
        copy.wait()


class Tiles:
    def __init__(self, rows, pack_rows, pack, active):
        self.rows, self.pack_rows = rows, pack_rows
        self.tile = min(256, pack_rows)
        self.count = rows // self.tile
        inner = pack_rows // self.tile
        runs = (lax.axis_index(SECTION) == active).astype(jnp.int32)
        self.control = jnp.stack([pack * inner, (pack + 1) * inner, runs]).astype(jnp.int32)

    def source(self, width):
        return pl.BlockSpec((self.tile, width), lambda i, control: (i * control[2], 0))

    def small(self, array):
        return pl.BlockSpec(array.shape, lambda i, control: (0,) * array.ndim)

    def pack_source(self, width):
        def index(i, control):
            return (0, jnp.clip(i - control[0], 0, control[1] - control[0] - 1), 0)

        return pl.BlockSpec((2, self.tile, width), index)

    def result(self, width, dtype=jnp.bfloat16):
        def index(i, control):
            return (jnp.where(control[2] == 1, i, self.count), 0)

        shape = jax.ShapeDtypeStruct((self.rows + self.tile, width), dtype)
        return shape, pl.BlockSpec((self.tile, width), index)

    def pair_result(self, width):
        def index(i, control):
            return (0, jnp.where(control[2] == 1, i, self.count), 0)

        shape = jax.ShapeDtypeStruct((2, self.rows + self.tile, width), jnp.bfloat16)
        return shape, pl.BlockSpec((2, self.tile, width), index)

    def pack_result(self, width):
        def index(i, control):
            spot = jnp.clip(i - control[0], 0, control[1] - control[0] - 1)
            return (0, jnp.where(control[2] == 1, spot, control[1] - control[0]), 0)

        shape = jax.ShapeDtypeStruct((2, self.pack_rows + self.tile, width), jnp.bfloat16)
        return shape, pl.BlockSpec((2, self.tile, width), index)

    def call(self, kernel, name, sources, weights, results, into=(), scratch=(), flops=0):
        arrays, specs = zip(*sources)
        shapes, out_specs = zip(*results)
        anywhere = pl.BlockSpec(memory_space=pl.ANY)
        pieces = [piece for weight in weights for piece in weight]
        counts = [len(weight) for weight in weights]
        first = 1 + len(arrays) + len(pieces)
        return pl.pallas_call(
            functools.partial(kernel, len(arrays), counts, len(into), len(results)),
            grid_spec=pltpu.PrefetchScalarGridSpec(
                num_scalar_prefetch=1,
                grid=(self.count,),
                in_specs=[*specs, *([anywhere] * (len(pieces) + len(into)))],
                out_specs=list(out_specs),
                scratch_shapes=[
                    *[hold_weight(weight) for weight in weights],
                    pltpu.SemaphoreType.DMA((len(pieces),)),
                    *scratch,
                ],
            ),
            out_shape=list(shapes),
            input_output_aliases={first + index: index for index in range(len(into))},
            name=name,
            cost_estimate=pl.CostEstimate(flops=flops, bytes_accessed=self.rows * 16384, transcendentals=0),
        )(self.control, *arrays, *pieces, *into)


def tiled(body):
    def kernel(n_sources, counts, n_into, n_results, control, *refs):
        n_weights, n_pieces = len(counts), sum(counts)
        sources, refs = refs[:n_sources], refs[n_sources:]
        stored, refs = refs[:n_pieces], refs[n_pieces + n_into :]
        results, refs = refs[:n_results], refs[n_results:]
        weights, sems, scratch = refs[:n_weights], refs[n_weights], refs[n_weights + 1 :]

        def run():
            pl.when(pl.program_id(0) == 0)(lambda: load(counts, stored, weights, sems))
            body(inside_pack(control), [sources[0][...], *sources[1:]], weights, results, scratch)

        pl.when(control[2] == 1)(run)

    return kernel


def inside_pack(control):
    tile = pl.program_id(0)
    return (tile >= control[0]) & (tile < control[1])


def shared_units(x, shared_in):
    half = shared_in.shape[0] // 2
    return dot_t(x, shared_in[:half]), dot_t(x, shared_in[half:])


def experts_body(inside, sources, weights, results, scratch):
    x, own_ref, routed_ref = sources
    in_ref, shared_in_ref = weights[:2]
    pre_ref, gated_ref, prob_ref, shared_pre_ref = results[:4]
    units = gated_ref.shape[1]
    pre = dot(x, in_ref[...])
    logits = pre[:, 2 * units : 2 * units + own_ref.shape[1]]
    powers = jnp.exp(logits - jnp.max(logits, axis=1, keepdims=True))
    prob = powers / jnp.sum(powers, axis=1, keepdims=True)
    prob_ref[...] = prob
    gate = jnp.sum(prob * own_ref[...], axis=1, keepdims=True) * routed_ref[...]
    pre_ref[...] = bf16(pre[:, : 2 * units])
    gated = bf16(gate * gated_hidden(pre[:, :units], pre[:, units : 2 * units]))
    gated_ref[...] = gated

    def shared():
        left, right = shared_units(x, shared_in_ref)
        shared_pre_ref[0] = bf16(left)
        shared_pre_ref[1] = bf16(right)
        return left, right

    if len(weights) == 2:
        pl.when(inside)(lambda: shared() and None)
        return
    out_ref, shared_out_ref = weights[2:]
    partial_ref = results[4]

    def with_shared():
        hidden = bf16(gated_hidden(*shared()))
        partial_ref[...] = bf16(dot(gated, out_ref[...]) + dot(hidden, shared_out_ref[...]))

    def without():
        partial_ref[...] = bf16(dot(gated, out_ref[...]))

    pl.when(inside)(with_shared)
    pl.when(jnp.logical_not(inside))(without)


def finish_body(inside, sources, weights, results, scratch):
    gated, _, shared_pre_ref = sources
    out_ref, shared_out_ref = weights
    (partial_ref,) = results

    def with_shared():
        hidden = bf16(gated_hidden(shared_pre_ref[0].astype(jnp.float32), shared_pre_ref[1].astype(jnp.float32)))
        partial_ref[...] = bf16(dot(gated, out_ref[...]) + dot(hidden, shared_out_ref[...]))

    def without():
        partial_ref[...] = bf16(dot(gated, out_ref[...]))

    pl.when(inside)(with_shared)
    pl.when(jnp.logical_not(inside))(without)


def experts_back_body(inside, sources, weights, results, scratch):
    grad, own_ref, pre_ref, prob_ref, routed_ref, shared_pre_ref = sources
    in_ref, shared_in_ref, out_ref, shared_out_ref = weights
    grad_pre_ref, moved_ref, partial_ref = results
    (joined_ref,) = scratch
    units = out_ref.shape[0]
    prob = prob_ref[...]
    own_prob = jnp.sum(prob * own_ref[...], axis=1, keepdims=True) * routed_ref[...]
    gate, up = pre_ref[:, :units].astype(jnp.float32), pre_ref[:, units:].astype(jnp.float32)
    grad_units = dot_t(grad, out_ref[...])
    act, slope = silu_parts(gate)
    moved = own_prob * jnp.sum(grad_units * act * up, axis=1, keepdims=True)
    moved_ref[...] = moved
    scaled = own_prob * grad_units
    joined_ref[:, :units] = bf16(scaled * up * slope)
    joined_ref[:, units : 2 * units] = bf16(scaled * act)
    joined_ref[:, 2 * units :] = jnp.zeros_like(joined_ref[:, 2 * units :])
    joined_ref[:, 2 * units : 2 * units + own_ref.shape[1]] = bf16(moved * (own_ref[...] - prob))
    grad_pre_ref[...] = joined_ref[:, : 2 * units]
    base = dot_t(joined_ref[...], in_ref[...])
    half = shared_out_ref.shape[0]

    def with_shared():
        left, right = gated_back(
            shared_pre_ref[0].astype(jnp.float32),
            shared_pre_ref[1].astype(jnp.float32),
            dot_t(grad, shared_out_ref[...]),
        )
        partial_ref[...] = bf16(base + dot(left, shared_in_ref[:half]) + dot(right, shared_in_ref[half:]))

    def without():
        partial_ref[...] = bf16(base)

    pl.when(inside)(with_shared)
    pl.when(jnp.logical_not(inside))(without)


def shared_body(inside, sources, weights, results, scratch):
    pre_ref, hid_ref = results
    left, right = shared_units(sources[0], weights[0])
    pre_ref[0] = bf16(left)
    pre_ref[1] = bf16(right)
    hid_ref[...] = bf16(gated_hidden(left, right))


def heads_body(block, inside, sources, weights, results, scratch):
    x, key_ref, cos_ref, sin_ref, col_ref, row_ref = sources
    query_w_ref, expand_ref = weights
    out_ref, rot_ref, lat_ref = results
    (q_ref,) = scratch
    heads = q_ref.shape[1] // QK
    q_ref[...] = dot(x, query_w_ref[...])
    lat_ref[...] = bf16(dot(key_ref[:, :LAT], expand_ref[...]))
    for start in range(0, x.shape[0], block):
        at = pl.ds(start, block)
        attend_kernel(
            heads,
            q_ref.at[at],
            lat_ref.at[at],
            key_ref.at[at],
            cos_ref.at[at],
            sin_ref.at[at],
            col_ref.at[at],
            row_ref.at[pl.ds(start // block, 1)],
            out_ref.at[at],
            rot_ref.at[at],
        )


def pair_grad_kernel(x_ref, grad_ref, out_ref):
    units = out_ref.shape[2]
    x = x_ref[...]
    out_ref[:, 0, :] = t_dot(x, grad_ref[:, :units])
    out_ref[:, 1, :] = t_dot(x, grad_ref[:, units:])


def pair_grad(x, grad):
    rows, width = x.shape
    units = grad.shape[1] // 2
    if rows > 4096:
        return t_dot(x, grad[:rows]).reshape(width, 2, units)
    tile = 256
    return pl.pallas_call(
        pair_grad_kernel,
        grid=(width // tile,),
        in_specs=[
            pl.BlockSpec((rows, tile), lambda i: (0, i)),
            pl.BlockSpec((rows, 2 * units), lambda i: (0, 0), pipeline_mode=pl.Buffered(1)),
        ],
        out_specs=pl.BlockSpec((tile, 2, units), lambda i: (i, 0, 0)),
        out_shape=jax.ShapeDtypeStruct((width, 2, units), jnp.float32),
        name="pair_grad",
        cost_estimate=pl.CostEstimate(
            flops=4 * rows * width * units, bytes_accessed=rows * (width + 2 * units) * 2 + width * units * 8, transcendentals=0
        ),
    )(x, grad)


def blank(shape, dtype):
    return pl.pallas_call(
        lambda out_ref: None,
        out_shape=jax.ShapeDtypeStruct(shape, dtype),
        out_specs=pl.BlockSpec(memory_space=pl.ANY),
        compiler_params=pltpu.CompilerParams(has_side_effects=True),
        name="blank",
    )()


def arrival_order(spots):
    tiles = [(rank + 1.1 * over, rank, over) for rank in range(spots) for over in (0, 1)]
    return [(rank, over == 1) for _, rank, over in sorted(tiles)]


def ranked_spots(spots, spot):
    ranks = []
    for rank in range(spots):
        value = 0
        for own in range(spots):
            nearest = sorted(range(spots), key=lambda other: (abs(other - own), other))
            value = value + jnp.where(spot == own, nearest[rank], 0)
        ranks.append(value)
    return ranks


def pick(index, values):
    total = 0
    for position, value in enumerate(values):
        total = total + jnp.where(index == position, value, 0)
    return total


def fused_kernel(spots, parts, active, body, pack_kinds, counts, n_into, *refs):
    source_kinds, result_kinds = pack_kinds
    n_sources, n_results = len(source_kinds), len(result_kinds)
    n_weights, n_pieces = len(counts), sum(counts)
    x_ref, small_ref, refs = refs[0], refs[1], refs[2:]
    sources, refs = refs[:n_sources], refs[n_sources:]
    stored, refs = refs[:n_pieces], refs[n_pieces + n_into :]
    o_ref, refs = refs[0], refs[1:]
    results, refs = refs[:n_results], refs[n_results:]
    x_tile, refs = refs[0], refs[1:]
    source_tiles, refs = refs[:n_sources], refs[n_sources:]
    result_tiles, refs = refs[:n_results], refs[n_results:]
    weights, refs = refs[:n_weights], refs[n_weights:]
    sems, scratch = refs[:12], refs[12:]
    own_sem, weight_sem, tile_sem, out_sem = sems[:4]
    up_out, up_in, down_out, down_in, over_out, over_in, pair_out, pair_in = sems[4:]
    block = x_ref.shape[0]
    rows = block // parts
    tile = 2 * block

    def run():
        loads = loads_of(counts, stored, weights, weight_sem)
        for copy in loads:
            copy.start()
        spot, chip, core = places(spots)
        greet(spots, spot, chip, core)
        piece = lambda index, part: o_ref.at[index, pl.ds(part * rows, rows)]
        first = lambda part: x_ref.at[pl.ds(part * rows, rows)]

        def up(source, at, part, reach):
            return remote(
                source, piece(slot(at, chip, core), part), {PACKS: spot + 1}, up_out.at[reach, part], up_in.at[reach, part]
            )

        def down(source, at, part, reach):
            return remote(
                source,
                piece(slot(at, chip, core), part),
                {PACKS: spot - 1},
                down_out.at[reach, part],
                down_in.at[reach, part],
            )

        def over(source, at, part):
            return remote(
                source, piece(slot(at, chip, core), part), to_other(chip, core), over_out.at[at, part], over_in.at[at, part]
            )

        def pair(source, at, c, part):
            return remote(
                source,
                piece(slot(at, c, core), part),
                to_partner(chip, core),
                pair_out.at[c, at, part],
                pair_in.at[c, at, part],
            )

        mine = slot(spot, chip, core)
        for part in range(parts):
            source = first(part)
            pair(source, spot, chip, part).start()
            over(source, spot, part).start()
            pl.when(spot < spots - 1)(lambda: up(source, spot, part, 0).start())
            pl.when(spot > 0)(lambda: down(source, spot, part, 0).start())
        own = pltpu.make_async_copy(x_ref, o_ref.at[mine], own_sem.at[0])
        own.start()
        own.wait()
        ranks = ranked_spots(spots, spot)
        order = arrival_order(spots)

        def hand_on(reach):
            for part in range(parts):

                def below(part=part):
                    at = spot - reach
                    source = piece(slot(at, chip, core), part)
                    up(source, at, part, reach - 1).wait_recv()
                    pl.when(spot < spots - 1)(lambda: up(source, at, part, reach).start())
                    over(source, at, part).start()
                    pair(source, at, chip, part).start()

                def above(part=part):
                    at = spot + reach
                    source = piece(slot(at, chip, core), part)
                    down(source, at, part, reach - 1).wait_recv()
                    pl.when(spot > 0)(lambda: down(source, at, part, reach).start())
                    over(source, at, part).start()
                    pair(source, at, chip, part).start()

                pl.when(spot >= reach)(below)
                pl.when(spot + reach < spots)(above)

        def arrive(rank, across):
            at = ranks[rank]
            if across:
                for part in range(parts):
                    source = piece(slot(at, 1 - chip, core), part)
                    over(source, at, part).wait_recv()
                    pair(source, at, 1 - chip, part).start()
                for part in range(parts):
                    pair(first(part), at, 1 - chip, part).wait_recv()
                return
            if rank > 0:
                hand_on(rank)
            for part in range(parts):
                pair(first(part), at, chip, part).wait_recv()

        def window(ref, kind, at, c):
            if kind:
                return ref.at[:, pl.ds(pl.multiple_of(c * tile, tile), tile)]
            return ref.at[pl.ds(pl.multiple_of((at * 2 + c) * tile, tile), tile)]

        def outward(index, which, at, c):
            return pltpu.make_async_copy(
                result_tiles[index].at[which], window(results[index], result_kinds[index], at, c), out_sem.at[which, index]
            )

        def step(number, carry):
            for position, (rank, across) in enumerate(order):
                pl.when(number == position)(functools.partial(arrive, rank, across))
            at = pick(number, [ranks[rank] for rank, _ in order])
            c = pick(number, [1 - chip if across else chip for _, across in order])
            inside = at == spot
            inputs = [pltpu.make_async_copy(o_ref.at[pl.ds(slot(at, c, 0), 2)], x_tile, tile_sem.at[0])]
            for index, kind in enumerate(source_kinds):
                if not kind:
                    inputs.append(
                        pltpu.make_async_copy(
                            window(sources[index], kind, at, c), source_tiles[index], tile_sem.at[1 + index]
                        )
                    )
            for copy in inputs:
                copy.start()
            for index, kind in enumerate(source_kinds):
                if kind:

                    def fetch(index=index, kind=kind):
                        copy = pltpu.make_async_copy(
                            window(sources[index], kind, at, c), source_tiles[index], tile_sem.at[1 + index]
                        )
                        copy.start()
                        copy.wait()

                    pl.when(inside)(fetch)

            @pl.when(number == 0)
            def _():
                for copy in loads:
                    copy.wait()

            which = lax.rem(number, 2)

            @pl.when(number >= 2)
            def _():
                for index, kind in enumerate(result_kinds):
                    if not kind:
                        outward(index, which, at, c).wait()

            for copy in inputs:
                copy.wait()
            body(
                inside,
                [x_tile[...].reshape(tile, x_tile.shape[2]), small_ref, *source_tiles],
                weights,
                [target.at[which] for target in result_tiles],
                scratch,
            )
            for index, kind in enumerate(result_kinds):
                if kind:

                    def put(index=index):
                        copy = outward(index, which, at, c)
                        copy.start()
                        copy.wait()

                    pl.when(inside)(put)
                else:
                    outward(index, which, at, c).start()
            return carry

        lax.fori_loop(0, 2 * spots, step, 0)
        for which in range(2):
            for index, kind in enumerate(result_kinds):
                if not kind:
                    outward(index, which, spot, chip).wait()
        for part in range(parts):
            for at in range(spots):
                over(first(part), at, part).wait_send()
                for c in range(2):
                    pair(first(part), at, c, part).wait_send()
            for reach in range(spots - 1):
                pl.when((spot >= reach) & (spot < spots - 1))(lambda: up(first(part), spot, part, reach).wait_send())
                pl.when((spot + reach < spots) & (spot > 0))(lambda: down(first(part), spot, part, reach).wait_send())

    pl.when(lax.axis_index(SECTION) == active)(run)


def fused_call(tiles, rows_in, number, active, body, small, sources, weights, results, gathered, into, scratch=(), parts=4):
    spots = lax.axis_size(PACKS)
    block, width = rows_in.shape
    tile = 2 * block
    dma = pltpu.SemaphoreType.DMA
    hops = max(spots - 1, 1)
    anywhere = pl.BlockSpec(memory_space=pl.ANY)
    inside = pl.BlockSpec(memory_space=pltpu.VMEM)
    shapes = [jax.ShapeDtypeStruct((spots * 4, block, width), rows_in.dtype), *(shape for shape, _ in results)]
    held = [gathered.reshape(shapes[0].shape), *into]
    pieces = [piece for weight in weights for piece in weight]
    first = 2 + len(sources) + len(pieces)

    def hold(array, kind, *lead):
        shape = (2, tile, array.shape[2]) if kind else (tile, array.shape[1])
        return pltpu.VMEM((*lead, *shape), array.dtype)

    outs = pl.pallas_call(
        functools.partial(
            fused_kernel,
            spots,
            parts,
            active,
            body,
            ([kind for _, kind in sources], [kind for _, kind in results]),
            [len(weight) for weight in weights],
            len(held),
        ),
        out_shape=shapes,
        in_specs=[inside, inside, *([anywhere] * (len(sources) + len(pieces) + len(held)))],
        out_specs=[anywhere] * len(shapes),
        input_output_aliases={first + index: index for index in range(len(held))},
        scratch_shapes=[
            pltpu.VMEM((2, block, width), rows_in.dtype),
            *(hold(array, kind) for array, kind in sources),
            *(hold(shape, kind, 2) for shape, kind in results),
            *(hold_weight(weight) for weight in weights),
            dma((1,)),
            dma((len(pieces),)),
            dma((1 + len(sources),)),
            dma((2, len(results))),
            dma((hops, parts)),
            dma((hops, parts)),
            dma((hops, parts)),
            dma((hops, parts)),
            dma((spots, parts)),
            dma((spots, parts)),
            dma((2, spots, parts)),
            dma((2, spots, parts)),
            *scratch,
        ],
        compiler_params=pltpu.CompilerParams(collective_id=number, has_side_effects=True),
        name=f"fused{number}",
    )(rows_in, small, *(array for array, _ in sources), *pieces, *held)
    return outs[0].reshape(-1, width), list(outs[1:])


def sum_kernel(spots, parts, active, body, pack_kinds, counts, n_into, *refs):
    source_kinds, result_kinds = pack_kinds
    n_sources, n_results = len(source_kinds), len(result_kinds)
    n_weights, n_pieces = len(counts), sum(counts)
    small_ref, refs = refs[0], refs[1:]
    sources, refs = refs[:n_sources], refs[n_sources:]
    stored, refs = refs[:n_pieces], refs[n_pieces + n_into :]
    o_ref, refs = refs[0], refs[1:]
    results, refs = refs[:n_results], refs[n_results:]
    source_tiles, refs = refs[:n_sources], refs[n_sources:]
    result_tiles, refs = refs[:n_results], refs[n_results:]
    weights, refs = refs[:n_weights], refs[n_weights:]
    x_buf, pair_buf, over_src, over_buf, line_src, up_buf, down_buf = refs[:7]
    weight_sem, tile_sem, out_sem, pair_out, pair_in, over_out, over_in, line_out, up_in, down_in = refs[7:17]
    scratch = refs[17:]
    block = o_ref.shape[0]
    rows = block // parts
    tile = 2 * block
    cut = lambda part: pl.ds(part * rows, rows)

    def run():
        loads = loads_of(counts, stored, weights, weight_sem)
        for copy in loads:
            copy.start()
        spot, chip, core = places(spots)

        def order(step):
            if step == spots - 1:
                return spot
            fall = spots - 1 - step
            fall = jnp.where(fall <= spot, fall - 1, fall)
            rise = jnp.where(step >= spot, step + 1, step)
            return jnp.where(2 * spot < spots - 1, fall, rise)

        turns = [(0, True)]
        for ahead in range(1, spots):
            turns += [(ahead, True), (ahead - 1, False)]
        turns.append((spots - 1, False))

        def place(number):
            at = pick(number, [order(turn) for turn, _ in turns])
            return at, pick(number, [1 - chip if far else chip for _, far in turns])

        def window(ref, kind, at, c):
            if kind:
                return ref.at[:, pl.ds(pl.multiple_of(c * tile, tile), tile)]
            return ref.at[pl.ds(pl.multiple_of((at * 2 + c) * tile, tile), tile)]

        def inputs(number):
            at, c = place(number)
            which = lax.rem(number, 2)
            return [
                pltpu.make_async_copy(
                    window(sources[index], kind, at, c), source_tiles[index].at[which], tile_sem.at[which, index]
                )
                for index, kind in enumerate(source_kinds)
                if not kind
            ]

        for copy in inputs(0):
            copy.start()
        greet(spots, spot, chip, core)

        def mine(at, c, k, part):
            return x_buf.at[at * 2 + c, pl.ds(pl.multiple_of(k * block + part * rows, rows), rows)]

        def pair(at, c, part):
            return remote(
                mine(at, c, 1 - core, part),
                pair_buf.at[at, c, cut(part)],
                to_partner(chip, core),
                pair_out.at[at, c, part],
                pair_in.at[at, c, part],
            )

        def over(at, part):
            return remote(
                over_src.at[at, cut(part)],
                over_buf.at[at, cut(part)],
                to_other(chip, core),
                over_out.at[at, part],
                over_in.at[at, part],
            )

        def up(at, part):
            return remote(
                line_src.at[at, cut(part)],
                up_buf.at[at, cut(part)],
                {PACKS: spot + 1},
                line_out.at[at, part],
                up_in.at[at, part],
            )

        def down(at, part):
            return remote(
                line_src.at[at, cut(part)],
                down_buf.at[at, cut(part)],
                {PACKS: spot - 1},
                line_out.at[at, part],
                down_in.at[at, part],
            )

        def across(step):
            at = order(step)
            for part in range(parts):
                pair(at, 1 - chip, part).wait_recv()
                add_into(
                    over_src.at[at, cut(part)],
                    [mine(at, 1 - chip, core, part), pair_buf.at[at, 1 - chip, cut(part)]],
                    rows,
                )
                over(at, part).start()

        def along(step):
            at = order(step)
            for part in range(parts):
                pair(at, chip, part).wait_recv()
                over(at, part).wait_recv()
                base = [mine(at, chip, core, part), pair_buf.at[at, chip, cut(part)], over_buf.at[at, cut(part)]]
                ups, downs = up_buf.at[at, cut(part)], down_buf.at[at, cut(part)]
                if step < spots - 1:
                    target = line_src.at[at, cut(part)]

                    def rising(first):
                        if not first:
                            up(at, part).wait_recv()
                        add_into(target, base if first else base + [ups], rows)
                        up(at, part).start()

                    def falling(first):
                        if not first:
                            down(at, part).wait_recv()
                        add_into(target, base if first else base + [downs], rows)
                        down(at, part).start()

                    pl.when((at > spot) & (spot == 0))(lambda: rising(True))
                    pl.when((at > spot) & (spot > 0))(lambda: rising(False))
                    pl.when((at < spot) & (spot == spots - 1))(lambda: falling(True))
                    pl.when((at < spot) & (spot < spots - 1))(lambda: falling(False))
                elif spots == 1:
                    add_into(o_ref.at[cut(part)], base, rows)
                else:

                    def finish(ends):
                        if ends < 1:
                            up(at, part).wait_recv()
                        if ends > -1:
                            down(at, part).wait_recv()
                        extra = ([ups] if ends < 1 else []) + ([downs] if ends > -1 else [])
                        add_into(o_ref.at[cut(part)], base + extra, rows)

                    pl.when(spot == 0)(lambda: finish(1))
                    pl.when(spot == spots - 1)(lambda: finish(-1))
                    pl.when((spot > 0) & (spot < spots - 1))(lambda: finish(0))

        late = 3 + jnp.where((spot > 0) & (spot < spots - 1), 2, 0)

        def outward(index, which, at, c):
            return pltpu.make_async_copy(
                result_tiles[index].at[which], window(results[index], result_kinds[index], at, c), out_sem.at[which, index]
            )

        def step(number, carry):
            at, c = place(number)
            inside = at == spot
            which = lax.rem(number, 2)
            for copy in inputs(number):
                copy.wait()

            @pl.when(number + 1 < 2 * spots)
            def _():
                for copy in inputs(number + 1):
                    copy.start()

            for index, kind in enumerate(source_kinds):
                if kind:

                    def fetch(index=index, kind=kind):
                        copy = pltpu.make_async_copy(
                            window(sources[index], kind, at, c), source_tiles[index], tile_sem.at[0, index]
                        )
                        copy.start()
                        copy.wait()

                    pl.when(inside)(fetch)

            @pl.when(number == 0)
            def _():
                for copy in loads:
                    copy.wait()

            @pl.when(number >= 2)
            def _():
                for index, kind in enumerate(result_kinds):
                    if not kind:
                        outward(index, which, at, c).wait()

            tiles = [
                target if kind else target.at[which] for target, kind in zip(source_tiles, source_kinds)
            ]
            body(
                inside,
                [tiles[0][...], small_ref, *tiles[1:]],
                weights,
                [*(target.at[which] for target in result_tiles), x_buf.at[at * 2 + c]],
                scratch,
            )
            for part in range(parts):
                pair(at, c, part).start()
            for index, kind in enumerate(result_kinds):
                if kind:

                    def put(index=index):
                        copy = outward(index, which, at, c)
                        copy.start()
                        copy.wait()

                    pl.when(inside)(put)
                else:
                    outward(index, which, at, c).start()
            for number_of in range(spots):
                pl.when(number == 2 * number_of)(functools.partial(across, number_of))
                pl.when(number == 2 * number_of + late)(functools.partial(along, number_of))
            return carry

        lax.fori_loop(0, 2 * spots, step, 0)
        for number_of in range(spots):
            pl.when(2 * number_of + late >= 2 * spots)(functools.partial(along, number_of))
        for which in range(2):
            for index, kind in enumerate(result_kinds):
                if not kind:
                    outward(index, which, spot, chip).wait()
        for part in range(parts):
            for number_of in range(spots):
                at = order(number_of)
                pair(at, 0, part).wait_send()
                pair(at, 1, part).wait_send()
                over(at, part).wait_send()
                if number_of < spots - 1:
                    up(at, part).wait_send()

    pl.when(lax.axis_index(SECTION) == active)(run)


def sum_call(rows, number, active, body, small, sources, weights, results, into, scratch=(), parts=4):
    spots = lax.axis_size(PACKS)
    width = weights[-1][0].shape[1]
    tile = 2 * rows
    dma = pltpu.SemaphoreType.DMA
    anywhere = pl.BlockSpec(memory_space=pl.ANY)
    inside = pl.BlockSpec(memory_space=pltpu.VMEM)
    pieces = [piece for weight in weights for piece in weight]
    first = 1 + len(sources) + len(pieces)
    held = lambda *lead: pltpu.VMEM((*lead, rows, width), jnp.bfloat16)

    def hold(array, kind, *lead):
        if kind:
            return pltpu.VMEM((*lead, 2, tile, array.shape[2]), array.dtype)
        return pltpu.VMEM((2, tile, array.shape[1]), array.dtype)

    outs = pl.pallas_call(
        functools.partial(
            sum_kernel,
            spots,
            parts,
            active,
            body,
            ([kind for _, kind in sources], [kind for _, kind in results]),
            [len(weight) for weight in weights],
            len(into),
        ),
        out_shape=[jax.ShapeDtypeStruct((rows, width), jnp.float32), *(shape for shape, _ in results)],
        in_specs=[inside, *([anywhere] * (len(sources) + len(pieces) + len(into)))],
        out_specs=[inside, *([anywhere] * len(results))],
        input_output_aliases={first + index: 1 + index for index in range(len(into))},
        scratch_shapes=[
            *(hold(array, kind) for array, kind in sources),
            *(hold(shape, kind, 2) for shape, kind in results),
            *(hold_weight(weight) for weight in weights),
            pltpu.VMEM((2 * spots, tile, width), jnp.bfloat16),
            held(spots, 2),
            held(spots),
            held(spots),
            held(spots),
            held(spots),
            held(spots),
            dma((len(pieces),)),
            dma((2, len(sources))),
            dma((2, max(len(results), 1))),
            dma((spots, 2, parts)),
            dma((spots, 2, parts)),
            dma((spots, parts)),
            dma((spots, parts)),
            dma((spots, parts)),
            dma((spots, parts)),
            dma((spots, parts)),
            *scratch,
        ],
        compiler_params=pltpu.CompilerParams(collective_id=number, has_side_effects=True),
        name=f"sum{number}",
    )(small, *(array for array, _ in sources), *pieces, *into)
    return outs[0], list(outs[1:])


def body(
    boundary,
    lengths,
    routes,
    attn_gain,
    query_weight,
    compress_weight,
    latent_gain,
    expand_weight,
    output_weight,
    ffn_gain,
    router_weight,
    shared_in,
    shared_out,
    expert_in,
    expert_out,
):
    attn_gain, latent_gain, ffn_gain = attn_gain[0], latent_gain[0], ffn_gain[0]
    query_weight, compress_weight = query_weight[0], compress_weight[0]
    expand_weight, output_weight = expand_weight[0], output_weight[0]
    router_weight, shared_out, expert_out = router_weight[0], shared_out[0], expert_out[0, 0]
    width = boundary.shape[3]
    rows = boundary.shape[2]
    half = shared_out.shape[0]
    units = expert_out.shape[0]
    experts_count = router_weight.shape[1]
    shared_in_t = jnp.transpose(shared_in[0], (1, 2, 0)).reshape(2 * half, width)
    joined_in = (
        expert_in.reshape(width, 2 * units),
        jnp.pad(router_weight, ((0, 0), (0, -experts_count % 128))),
    )
    joined_width = sum(piece.shape[1] for piece in joined_in)

    packs, members = lax.axis_size(PACKS), lax.axis_size(MEMBERS)
    count = packs * members
    pack, member = lax.axis_index(PACKS), lax.axis_index(MEMBERS)
    me = pack * members + member
    is_first = lax.axis_index(SECTION) == 0
    pack_rows = members * rows
    all_rows = count * rows
    heads = output_weight.shape[0] // VD
    top = routes.shape[3]
    tiles = [Tiles(all_rows, pack_rows, pack, active) for active in range(2)]
    fusing = members == 4 and tiles[0].tile == 2 * rows

    def own_pack(value):
        size = value.shape[0] // packs
        return lax.dynamic_slice_in_dim(value, pack * size, size, 0)

    freqs = rope_base ** (-jnp.arange(HALF, dtype=jnp.float32) / HALF)
    angles = jnp.arange(rows, dtype=jnp.float32)[:, None] * freqs[None, :]
    turns = jnp.concatenate([jnp.cos(angles), jnp.sin(angles)], axis=1)

    def tables_of(block_lengths):
        segment, position = block_layout(block_lengths, rows)
        blocks = segment.shape[0]
        chosen = position.reshape(-1)[:, None] == jnp.arange(rows, dtype=jnp.int32)[None, :]
        found = jnp.dot(
            chosen.astype(jnp.float32),
            turns,
            precision=lax.Precision.HIGHEST,
            preferred_element_type=jnp.float32,
        )
        return (
            found[:, :HALF],
            found[:, HALF:],
            segment.reshape(blocks * rows, 1),
            segment.reshape(blocks, 1, rows),
        )

    own_lengths = lax.dynamic_index_in_dim(lengths[0, 0], member, 0, keepdims=False)
    layout = jnp.concatenate(
        [
            jnp.transpose(routes[0, 0]),
            jnp.pad(own_lengths, (0, rows - own_lengths.shape[0]))[None],
            jnp.zeros((-(top + 1) % 8, rows), jnp.int32),
        ],
        axis=0,
    )


    def routed_of(layout_all):
        named = layout_all.reshape(count, -1, rows)[:, :top] == me
        return jnp.any(named, axis=1).astype(jnp.float32).reshape(all_rows, 1)

    tables_pack = tables_of(lengths[0, 0])
    tables_own = tables_of(own_lengths[None])
    own_cos, own_sin = tables_own[:2]
    own_column = (lax.broadcasted_iota(jnp.int32, (1, experts_count), 1) == me).astype(jnp.float32)

    def inputs_of(hidden):
        normed32, scale_attn = rms_forward(hidden, attn_gain)
        normed = bf16(normed32)
        compressed = dot(normed, compress_weight)
        latent32, scale_latent = rms_forward(compressed[:, :LAT], latent_gain)
        keyed = bf16(
            jnp.concatenate([latent32, rotate(compressed[:, LAT:], own_cos, own_sin)], axis=1)
        )
        return normed, keyed, (compressed, scale_attn, scale_latent)

    def run_experts(section, x, routed, gathered, into, number, full):
        at = tiles[section]
        results = [
            at.result(2 * units),
            at.result(units),
            at.result(experts_count, jnp.float32),
            at.pack_result(half),
        ]
        weights = [joined_in, (shared_in_t,)]
        if full:
            results.append(at.result(width))
            weights += [(expert_out,), (shared_out,)]
        if fusing:
            shapes = [(shape, index == 3) for index, (shape, _) in enumerate(results)]
            return fused_call(
                at, x, number, section, experts_body, own_column, [(routed, False)], weights, shapes, gathered, into
            )
        (x_all,) = gather_blocks([x], True, number, section, [gathered])
        return x_all, at.call(
            tiled(experts_body),
            "experts",
            [(x_all, at.source(width)), (own_column, at.small(own_column)), (routed, at.source(1))],
            weights,
            results,
            into[:4],
        )

    def summed_over(section, number, body_of, name, sources, weights, results, into, scratch=()):
        at = tiles[section]
        if fusing:
            shapes = [(shape, shape.ndim == 3) for shape, _ in results]
            return sum_call(rows, number, section, body_of, own_column, sources, weights, shapes, into, scratch)
        specs = [(array, at.pack_source(half) if kind else at.source(array.shape[1])) for array, kind in sources]
        specs.insert(1, (own_column, at.small(own_column)))
        *found, partial = at.call(
            tiled(body_of), name, specs, weights, [*results, at.result(width)], into, scratch
        )
        return scatter_blocks(partial, rows, True, number, section), found

    def run_experts_back(section, number, grad_all, routed, stored, into):
        at = tiles[section]
        pre, _, prob, shared_pre = stored
        return summed_over(
            section,
            number,
            experts_back_body,
            "experts_back",
            [(grad_all, False), (pre, False), (prob, False), (routed, False), (shared_pre, True)],
            [joined_in, (shared_in_t,), (expert_out,), (shared_out,)],
            [at.result(2 * units), at.result(1, jnp.float32)],
            into,
            [pltpu.VMEM((at.tile, joined_width), jnp.bfloat16)],
        )

    def prepare(section, normed_all, keyed_all, ffn_all, tables, into):
        at = tiles[section]
        cosine, sine, seg_col, seg_row = tables
        blocks = at.tile // rows
        row_spec = pl.BlockSpec((blocks, 1, rows), lambda i, control: (i * control[2], 0, 0))
        found = at.call(
            tiled(functools.partial(heads_body, rows)),
            "heads",
            [
                (normed_all, at.source(width)),
                (keyed_all, at.source(LAT + ROPE)),
                (cosine, at.source(HALF)),
                (sine, at.source(HALF)),
                (seg_col, at.source(1)),
                (seg_row, row_spec),
            ],
            [(query_weight,), (expand_weight,)],
            [at.result(heads * VD), at.result(heads * QK), at.result(heads * KV)],
            into[:3],
            [pltpu.VMEM((at.tile, heads * QK), jnp.float32)],
            flops=4 * all_rows * width * heads * QK,
        )
        shared = at.call(
            tiled(shared_body),
            "shared",
            [(ffn_all, at.source(width))],
            [(shared_in_t,)],
            [at.pair_result(half), at.result(half)],
            into[3:],
            flops=4 * all_rows * width * half,
        )
        return [*found, *shared]

    fresh = boundary[0, 0].astype(jnp.float32)

    normed, keyed, _ = inputs_of(fresh)
    normed_pack, keyed_pack, layout_all = gather_blocks(
        [normed, keyed, layout], True, 0, 0, wide=[False, False, True]
    )
    attended, _ = attend(
        dot(normed_pack, query_weight),
        bf16(dot(keyed_pack[:, :LAT], expand_weight)),
        keyed_pack,
        tables_pack,
    )
    mixed_first = fresh + scatter_blocks(bf16(dot(attended, output_weight)), rows, False, 1, 0)
    empty = [
        blank((all_rows, width), jnp.bfloat16),
        *(
            blank(shape, dtype)
            for shape, dtype in (
                ((all_rows + tiles[0].tile, 2 * units), jnp.bfloat16),
                ((all_rows + tiles[0].tile, units), jnp.bfloat16),
                ((all_rows + tiles[0].tile, experts_count), jnp.float32),
                ((2, pack_rows + tiles[0].tile, half), jnp.bfloat16),
            )
        ),
    ]
    ffn_all, (*stored, partial) = run_experts(
        0, bf16(rms_forward(mixed_first, ffn_gain)[0]), routed_of(layout_all), empty[0], empty[1:], 2, True
    )
    result_first = mixed_first + scatter_blocks(partial, rows, True, 3, 0)
    heads_weights = spread_blocks([query_weight, expand_weight, output_weight], 4, 1)
    target_all, layout_all = gather_blocks(
        [boundary[0, 0], layout], True, 5, 1, [blank((all_rows, width), jnp.bfloat16), layout_all]
    )
    sent, target_all, layout_all, heads_weights = lax.optimization_barrier(
        (bf16(result_first), target_all, layout_all, heads_weights)
    )
    inbound = lax.ppermute(sent, SECTION, [(0, 1)])
    routed = routed_of(layout_all)
    tables_all = tables_of(layout_all.reshape(count, -1, rows)[:, top, : lengths.shape[3]])
    query_heads, expand_heads, output_heads = (
        value.reshape(members, -1, value.shape[1]) for value in heads_weights
    )

    hidden = jnp.where(is_first, fresh, inbound.astype(jnp.float32))
    normed, keyed, (compressed, scale_attn, scale_latent) = inputs_of(hidden)
    latent = bf16(jnp.einsum("rd,mdc->mrc", keyed[:, :LAT], expand_heads, preferred_element_type=jnp.float32))
    latent = latent.reshape(members * rows, -1)
    query_raw = jnp.einsum("rd,mdc->mrc", normed, query_heads, preferred_element_type=jnp.float32)
    attended, query = attend(query_raw.reshape(members * rows, -1), latent, keyed, tables_own, members)
    mixed = hidden + jnp.einsum(
        "mrc,mcd->rd", attended.reshape(members, rows, -1), output_heads, preferred_element_type=jnp.float32
    )
    mixed = jnp.where(is_first, mixed_first, mixed)
    ffn32, scale_ffn = rms_forward(mixed, ffn_gain)
    ffn_all, stored = run_experts(1, bf16(ffn32), routed, ffn_all, stored, 6, False)

    def latent_back(own):
        grad_latent, grad_latent_gain = rms_backward(
            compressed[:, :LAT], scale_latent, latent_gain, own[:, width : width + LAT]
        )
        grad_compressed = bf16(
            jnp.concatenate([grad_latent, rotate(own[:, width + LAT :], own_cos, -own_sin)], axis=1)
        )
        grad_normed = own[:, :width] + dot_t(grad_compressed, compress_weight)
        grad_hidden_norm, grad_attn_gain = rms_backward(hidden, scale_attn, attn_gain, grad_normed)
        return grad_compressed, grad_hidden_norm, grad_attn_gain, grad_latent_gain

    grad_ffn_second, grad_units = run_experts_back(1, 7, target_all, routed, stored, ())
    grad_mixed = fresh + rms_backward(mixed, scale_ffn, ffn_gain, grad_ffn_second)[0]
    grad_attended = jnp.einsum(
        "rd,mcd->mrc", bf16(grad_mixed), output_heads, preferred_element_type=jnp.float32
    )
    grad_query, grad_latent_heads, grad_shared_key = attend_back(
        query, latent, keyed, bf16(grad_attended).reshape(members * rows, -1), tables_own, members
    )
    own_second = jnp.concatenate(
        [
            jnp.einsum(
                "mrc,mdc->rd",
                grad_query.reshape(members, rows, -1),
                query_heads,
                preferred_element_type=jnp.float32,
            ),
            jnp.einsum(
                "mrc,mdc->rd",
                grad_latent_heads.reshape(members, rows, -1),
                expand_heads,
                preferred_element_type=jnp.float32,
            ),
            jnp.sum(grad_shared_key.reshape(members, rows, -1), axis=0),
        ],
        axis=1,
    )
    grad_second = bf16(grad_mixed + latent_back(own_second)[1])

    all_inputs = gather_blocks([normed, keyed], True, 8, 0)
    prepared = prepare(0, *all_inputs, ffn_all, tables_all, ())
    grad_second, prepared, all_inputs = lax.optimization_barrier((grad_second, prepared, all_inputs))
    downbound = lax.ppermute(grad_second, SECTION, [(1, 0)]).astype(jnp.float32)

    normed_late, keyed_late, gated_late, _ = lax.optimization_barrier((normed, keyed, stored[1], grad_second))
    finished, _ = summed_over(
        1,
        10,
        finish_body,
        "finish",
        [(gated_late, False), (stored[3], True)],
        [(expert_out,), (shared_out,)],
        [],
        (),
    )
    result = mixed + finished
    upstream = jnp.where(is_first, downbound, fresh)
    (upstream_all,) = gather_blocks([bf16(upstream)], True, 11, 0, [target_all])
    grad_ffn, (grad_pre, moved) = run_experts_back(0, 12, upstream_all, routed, stored, grad_units)
    grad_ffn = jnp.where(is_first, grad_ffn, grad_ffn_second)
    normed_late, keyed_late, _ = lax.optimization_barrier((normed_late, keyed_late, finished))
    normed_all, keyed_all = gather_blocks([normed_late, keyed_late], True, 9, 1, all_inputs)
    prepared = prepare(1, normed_all, keyed_all, ffn_all, tables_all, prepared)
    attended_all, query_all, latent_all, shared_pre, shared_hid = prepared
    attended_all, shared_hid = attended_all[:all_rows], shared_hid[:all_rows]
    grad_mixed_norm, grad_ffn_gain = rms_backward(mixed, scale_ffn, ffn_gain, grad_ffn)
    grad_mixed = upstream + grad_mixed_norm
    grad_mixed_all = lax.all_gather(bf16(grad_mixed), BOTH, axis=0, tiled=True)
    grad_attended = bf16(dot_t(grad_mixed_all, output_weight))
    grad_query, grad_latent_heads, grad_shared_key = attend_back(
        query_all, latent_all, keyed_all, grad_attended, tables_all
    )
    own = lax.psum_scatter(
        bf16(
            jnp.concatenate(
                [
                    dot_t(own_pack(grad_query), query_weight),
                    dot_t(own_pack(grad_latent_heads), expand_weight),
                    own_pack(grad_shared_key),
                ],
                axis=1,
            )
        ),
        MEMBERS,
        scatter_dimension=0,
        tiled=True,
    ).astype(jnp.float32)
    grad_compressed, grad_hidden_norm, grad_attn_gain, grad_latent_gain = latent_back(own)
    grad_hidden = grad_mixed + grad_hidden_norm

    gains = jnp.concatenate([grad_attn_gain, grad_latent_gain, grad_ffn_gain])
    rounded = lax.reduce_precision(gains, 8, 7)
    small = jnp.concatenate([bf16(rounded), bf16(gains - rounded), bf16(moved[:all_rows, 0])])
    small = jnp.pad(small, (0, -small.shape[0] % rows)).reshape(rows, -1)
    last = lax.all_gather(jnp.concatenate([grad_compressed, small], axis=1), BOTH, axis=0, tiled=True)
    grad_compressed_all = last[:, : LAT + ROPE]
    small_all = last[:, LAT + ROPE :].reshape(count, -1).astype(jnp.float32)
    many = 2 * width + LAT
    gains = jnp.sum(small_all[:, :many] + small_all[:, many : 2 * many], axis=0)
    moved_all = small_all[:, 2 * many : 2 * many + all_rows].T
    prob = stored[2][:all_rows]
    grad_logits = bf16(moved_all - prob * jnp.sum(moved_all, axis=1, keepdims=True))
    left, right = gated_back(
        shared_pre[0, :all_rows].astype(jnp.float32),
        shared_pre[1, :all_rows].astype(jnp.float32),
        dot_t(upstream_all, shared_out),
    )
    grad_shared_in = lax.dot_general(
        jnp.stack([left, right]), ffn_all, (((1,), (0,)), ((), ())), preferred_element_type=jnp.float32
    )
    ends = jnp.where(is_first, grad_hidden, result)
    return (
        ends[None, None],
        gains[:width][None],
        t_dot(normed_all, grad_query)[None],
        t_dot(normed_all, grad_compressed_all)[None],
        gains[width : width + LAT][None],
        t_dot(keyed_all[:, :LAT], grad_latent_heads)[None],
        t_dot(attended_all, grad_mixed_all)[None],
        gains[width + LAT :][None],
        t_dot(ffn_all, grad_logits)[None],
        jnp.transpose(grad_shared_in, (2, 0, 1))[None],
        t_dot(shared_hid, upstream_all)[None],
        pair_grad(ffn_all, grad_pre)[None, None],
        t_dot(stored[1][:all_rows], upstream_all)[None, None],
    )


def solution(mesh):
    return jax.shard_map(
        body,
        mesh=mesh,
        in_specs=(
            P(SECTION, None, BOTH, None),
            P(None, PACKS, None, None),
            P(SECTION, None, BOTH, None),
            P(SECTION, None),
            P(SECTION, None, MEMBERS),
            P(SECTION, None, None),
            P(SECTION, None),
            P(SECTION, None, MEMBERS),
            P(SECTION, MEMBERS, None),
            P(SECTION, None),
            P(SECTION, None, None),
            P(SECTION, None, None, MEMBERS),
            P(SECTION, MEMBERS, None),
            P(SECTION, BOTH, None, None, None),
            P(SECTION, BOTH, None, None),
        ),
        out_specs=(
            P(SECTION, None, BOTH, None),
            P(SECTION, None),
            P(SECTION, None, MEMBERS),
            P(SECTION, None, None),
            P(SECTION, None),
            P(SECTION, None, MEMBERS),
            P(SECTION, MEMBERS, None),
            P(SECTION, None),
            P(SECTION, None, None),
            P(SECTION, None, None, MEMBERS),
            P(SECTION, MEMBERS, None),
            P(SECTION, BOTH, None, None, None),
            P(SECTION, BOTH, None, None),
        ),
        check_vma=False,
    )
```

```python
import functools

import jax
import jax.numpy as jnp
from jax import lax
from jax.experimental import pallas as pl
from jax.experimental.pallas import tpu as pltpu
from jax.sharding import PartitionSpec as P

NOPE = 128
ROPE = 64
VD = 128
LAT = 512

QK = NOPE + ROPE
KV = NOPE + VD
HALF = ROPE // 2
epsilon = 1e-06
rope_base = 10000.0
masked_score = -1e30
SECTION, PACKS, MEMBERS = "section", "dp", "expert"
BOTH = (PACKS, MEMBERS)
MESH = pl.DeviceIdType.MESH
def dot(left, right):
    return jnp.dot(left, right, preferred_element_type=jnp.float32)


def dot_t(left, right):
    return lax.dot_general(
        left, right, (((1,), (1,)), ((), ())), preferred_element_type=jnp.float32
    )


def t_dot(left, right):
    return lax.dot_general(
        left, right, (((0,), (0,)), ((), ())), preferred_element_type=jnp.float32
    )


def bf16(value):
    return value.astype(jnp.bfloat16)


def rms_forward(inputs, gain_vec):
    norm_scale = lax.rsqrt(jnp.mean(inputs * inputs, axis=-1, keepdims=True) + epsilon)
    return (inputs * norm_scale * gain_vec, norm_scale)


def rms_backward(inputs, norm_scale, gain_vec, upstream):
    weighted = upstream * gain_vec
    grad_gain = jnp.sum(upstream * inputs * norm_scale, axis=0)
    cubed = norm_scale * norm_scale * norm_scale
    grad_inputs = norm_scale * weighted - inputs * cubed * jnp.mean(
        weighted * inputs, axis=-1, keepdims=True
    )
    return (grad_inputs, grad_gain)


def rotate(inputs, cosine, sine):
    half = cosine.shape[-1]
    former = inputs[..., :half]
    latter = inputs[..., half:]
    return jnp.concatenate(
        [former * cosine - latter * sine, latter * cosine + former * sine], axis=-1
    )


def silu_parts(pre_gate):
    sigmoid = jax.nn.sigmoid(pre_gate)
    return (pre_gate * sigmoid, sigmoid * (1.0 + pre_gate * (1.0 - sigmoid)))


def block_layout(block_lengths, rows):
    index = lax.broadcasted_iota(jnp.int32, (block_lengths.shape[0], rows), 1)
    start, segment, opening = 0, 0, 0
    for sequence in range(block_lengths.shape[1]):
        begun = index >= start
        segment = segment + begun.astype(jnp.int32)
        opening = jnp.where(begun, start, opening)
        start = start + block_lengths[:, sequence : sequence + 1]
    return segment, index - opening


def places(spots):
    member = lax.axis_index(MEMBERS)
    spot = lax.axis_index(PACKS) if spots > 1 else 0
    return spot, member // 2, lax.rem(member, 2)


def to_partner(chip, core):
    return {MEMBERS: chip * 2 + 1 - core}


def to_other(chip, core):
    return {MEMBERS: (1 - chip) * 2 + core}


def when(condition, action):
    if condition is True:
        action()
    else:
        pl.when(condition)(action)


def greet(spots, spot, chip, core):
    barrier = pltpu.get_barrier_semaphore()

    def signal(target):
        pl.semaphore_signal(barrier, inc=1, device_id=target, device_id_type=MESH)

    signal(to_partner(chip, core))
    signal(to_other(chip, core))
    if spots > 1:
        pl.when(spot > 0)(lambda: signal({PACKS: spot - 1}))
        pl.when(spot < spots - 1)(lambda: signal({PACKS: spot + 1}))
        ends = jnp.where(spot > 0, 1, 0) + jnp.where(spot < spots - 1, 1, 0)
        pl.semaphore_wait(barrier, 2 + ends)
    else:
        pl.semaphore_wait(barrier, 2)


def remote(source, target_ref, target, out_sem, in_sem):
    return pltpu.make_async_remote_copy(
        src_ref=source,
        dst_ref=target_ref,
        send_sem=out_sem,
        recv_sem=in_sem,
        device_id=target,
        device_id_type=MESH,
    )


def slot(spot, chip, core):
    return spot * 4 + chip * 2 + core


def gather_kernel(spots, cuts, wide, active, *refs):
    arrays = len(cuts)
    x_refs, o_refs, sems = refs[:arrays], refs[-9 - arrays : -9], refs[-9:]
    own_sem, up_out, up_in, down_out, down_in, over_out, over_in, pair_out, pair_in = sems
    units = [
        (a, pl.ds(part * (x_refs[a].shape[0] // parts), x_refs[a].shape[0] // parts))
        for a, parts in enumerate(cuts)
        for part in range(parts)
    ]

    def run():
        spot, chip, core = places(spots)
        greet(spots, spot, chip, core)

        def piece(unit, index):
            array, cut = units[unit]
            return o_refs[array].at[index, cut]

        def first(unit):
            array, cut = units[unit]
            return x_refs[array].at[cut]

        def lane(unit):
            return wide[units[unit][0]]

        def spread(unit):
            return range(spots) if lane(unit) else [0]

        def up(source, at, unit, reach):
            return remote(
                source, piece(unit, slot(at, chip, core)), {PACKS: spot + 1}, up_out.at[reach, unit], up_in.at[reach, unit]
            )

        def down(source, at, unit, reach):
            return remote(
                source,
                piece(unit, slot(at, chip, core)),
                {PACKS: spot - 1},
                down_out.at[reach, unit],
                down_in.at[reach, unit],
            )

        def over(source, at, unit):
            return remote(
                source, piece(unit, slot(at, chip, core)), to_other(chip, core), over_out.at[at, unit], over_in.at[at, unit]
            )

        def pair(source, at, c, unit):
            return remote(
                source,
                piece(unit, slot(at, c, core)),
                to_partner(chip, core),
                pair_out.at[c, at, unit],
                pair_in.at[c, at, unit],
            )

        home = lambda unit: spot if lane(unit) else 0
        for unit in range(len(units)):
            source = first(unit)
            over(source, home(unit), unit).start()
            if spots > 1 and lane(unit):
                pl.when(spot < spots - 1)(lambda: up(source, spot, unit, 0).start())
                pl.when(spot > 0)(lambda: down(source, spot, unit, 0).start())
            pair(source, home(unit), chip, unit).start()
        own = [
            pltpu.make_async_copy(
                x_refs[a], o_refs[a].at[slot(spot if wide[a] else 0, chip, core)], own_sem.at[a]
            )
            for a in range(arrays)
        ]
        for copy in own:
            copy.start()
        for reach in range(1, spots):
            for unit in range(len(units)):
                if not lane(unit):
                    continue

                def below(reach=reach, unit=unit):
                    at = spot - reach
                    source = piece(unit, slot(at, chip, core))
                    up(source, at, unit, reach - 1).wait_recv()
                    pl.when(spot < spots - 1)(lambda: up(source, at, unit, reach).start())
                    over(source, at, unit).start()
                    pair(source, at, chip, unit).start()

                def above(reach=reach, unit=unit):
                    at = spot + reach
                    source = piece(unit, slot(at, chip, core))
                    down(source, at, unit, reach - 1).wait_recv()
                    pl.when(spot > 0)(lambda: down(source, at, unit, reach).start())
                    over(source, at, unit).start()
                    pair(source, at, chip, unit).start()

                pl.when(spot >= reach)(below)
                pl.when(spot + reach < spots)(above)
        for reach in range(spots):
            sides = [(True, spot)]
            if reach > 0:
                sides = [(spot >= reach, spot - reach), (spot + reach < spots, spot + reach)]
            for unit in range(len(units)):
                if not lane(unit) and reach > 0:
                    continue
                for there, at in sides:
                    at = at if lane(unit) else 0

                    def hand_on(at=at, unit=unit):
                        source = piece(unit, slot(at, 1 - chip, core))
                        over(source, at, unit).wait_recv()
                        pair(source, at, 1 - chip, unit).start()

                    when(there, hand_on)
        for copy in own:
            copy.wait()
        for unit in range(len(units)):
            source = first(unit)
            for at in spread(unit):
                over(source, at, unit).wait_send()
                for c in range(2):
                    pair(source, at, c, unit).wait()
            for reach in range(spots - 1 if lane(unit) else 0):
                pl.when((spot >= reach) & (spot < spots - 1))(lambda: up(source, spot, unit, reach).wait_send())
                pl.when((spot + reach < spots) & (spot > 0))(lambda: down(source, spot, unit, reach).wait_send())

    if active is None:
        run()
    else:
        pl.when(lax.axis_index(SECTION) == active)(run)


def gather_blocks(values, across, number, active=None, into=None, parts=4, wide=None):
    wide = [across] * len(values) if wide is None else wide
    if lax.axis_size(MEMBERS) != 4:
        found = [
            lax.all_gather(value, BOTH if far else MEMBERS, axis=0, tiled=True) for value, far in zip(values, wide)
        ]
        if into is None:
            return found
        chosen = lax.axis_index(SECTION) == active
        return [jnp.where(chosen, new, old) for new, old in zip(found, into)]
    spots = lax.axis_size(PACKS) if across else 1
    cuts = [parts if value.shape[0] % (16 * parts) == 0 else 1 for value in values]
    units = sum(cuts)
    dma = pltpu.SemaphoreType.DMA
    hops = max(spots - 1, 1)
    shapes = [
        jax.ShapeDtypeStruct(((spots if far else 1) * 4, *value.shape), value.dtype)
        for value, far in zip(values, wide)
    ]
    held = [] if into is None else [old.reshape(shape.shape) for old, shape in zip(into, shapes)]
    outs = pl.pallas_call(
        functools.partial(gather_kernel, spots, cuts, wide, active),
        out_shape=shapes,
        in_specs=[pl.BlockSpec(memory_space=pltpu.VMEM)] * len(values)
        + [pl.BlockSpec(memory_space=pl.ANY)] * len(held),
        out_specs=[pl.BlockSpec(memory_space=pl.ANY)] * len(values),
        input_output_aliases={len(values) + index: index for index in range(len(held))},
        scratch_shapes=[
            dma((len(values),)),
            dma((hops, units)),
            dma((hops, units)),
            dma((hops, units)),
            dma((hops, units)),
            dma((spots, units)),
            dma((spots, units)),
            dma((2, spots, units)),
            dma((2, spots, units)),
        ],
        compiler_params=pltpu.CompilerParams(collective_id=number, has_side_effects=True),
        name=f"gather{number}",
    )(*values, *held)
    return [out.reshape(-1, out.shape[2]) for out in outs]


def spread_kernel(cuts, active, *refs):
    arrays = len(cuts)
    sources, o_refs, x_refs = refs[:arrays], refs[arrays : 2 * arrays], refs[2 * arrays : 3 * arrays]
    own_sem, over_out, over_in, side_out, side_in, pair_out, pair_in = refs[3 * arrays :]
    units = [
        (a, pl.ds(part * (x_refs[a].shape[0] // parts), x_refs[a].shape[0] // parts))
        for a, parts in enumerate(cuts)
        for part in range(parts)
    ]

    def run():
        taken_in = [pltpu.make_async_copy(sources[a], x_refs[a], own_sem.at[a]) for a in range(arrays)]
        for copy in taken_in:
            copy.start()
        for copy in taken_in:
            copy.wait()
        member, spot = lax.axis_index(MEMBERS), lax.axis_index(PACKS)
        chip, core, odd = member // 2, lax.rem(member, 2), lax.rem(spot, 2)
        beside = {PACKS: spot + 1 - 2 * odd}
        barrier = pltpu.get_barrier_semaphore()
        for target in (to_partner(chip, core), to_other(chip, core), beside):
            pl.semaphore_signal(barrier, inc=1, device_id=target, device_id_type=MESH)
        pl.semaphore_wait(barrier, 3)

        def piece(unit, c):
            array, cut = units[unit]
            return o_refs[array].at[c * 2 + core, cut]

        def first(unit):
            array, cut = units[unit]
            return x_refs[array].at[cut]

        def over(unit):
            return remote(first(unit), piece(unit, chip), to_other(chip, core), over_out.at[unit], over_in.at[unit])

        def side(unit):
            source = piece(unit, 1 - chip)
            return remote(source, source, beside, side_out.at[unit], side_in.at[unit])

        def pair(source, unit, c, index):
            return remote(
                source, piece(unit, c), to_partner(chip, core), pair_out.at[index, unit], pair_in.at[index, unit]
            )

        for unit in range(len(units)):
            pl.when(odd == unit % 2)(lambda: over(unit).start())
        for unit in range(len(units)):
            pair(first(unit), unit, chip, 0).start()
        own = [
            pltpu.make_async_copy(x_refs[a], o_refs[a].at[member], own_sem.at[a]) for a in range(arrays)
        ]
        for copy in own:
            copy.start()
        for unit in range(len(units)):

            def taken(unit=unit):
                over(unit).wait_recv()
                side(unit).start()
                pair(piece(unit, 1 - chip), unit, 1 - chip, 1).start()

            pl.when(odd == unit % 2)(taken)
        for unit in range(len(units)):

            def handed(unit=unit):
                side(unit).wait_recv()
                pair(piece(unit, 1 - chip), unit, 1 - chip, 1).start()

            pl.when(odd != unit % 2)(handed)
        for copy in own:
            copy.wait()
        for unit in range(len(units)):

            def sent(unit=unit):
                over(unit).wait_send()
                side(unit).wait_send()

            pl.when(odd == unit % 2)(sent)
            pair(first(unit), unit, chip, 0).wait()
            pair(first(unit), unit, 1 - chip, 1).wait()

    pl.when(lax.axis_index(SECTION) == active)(run)


def spread_blocks(values, number, active, parts=8):
    if lax.axis_size(MEMBERS) != 4 or lax.axis_size(PACKS) % 2:
        return gather_blocks(values, False, number, active)
    units = parts * len(values)
    dma = pltpu.SemaphoreType.DMA
    outs = pl.pallas_call(
        functools.partial(spread_kernel, [parts] * len(values), active),
        out_shape=[jax.ShapeDtypeStruct((4, *value.shape), value.dtype) for value in values],
        in_specs=[pl.BlockSpec(memory_space=pl.ANY)] * len(values),
        out_specs=[pl.BlockSpec(memory_space=pl.ANY)] * len(values),
        scratch_shapes=[
            *(pltpu.VMEM(value.shape, value.dtype) for value in values),
            dma((len(values),)),
            dma((units,)),
            dma((units,)),
            dma((units,)),
            dma((units,)),
            dma((2, units)),
            dma((2, units)),
        ],
        compiler_params=pltpu.CompilerParams(collective_id=number, has_side_effects=True),
        name=f"spread{number}",
    )(*values)
    return [out.reshape(-1, out.shape[2]) for out in outs]


def add_into(target, sources, rows, step=16):
    def some(index, carry):
        at = pl.ds(pl.multiple_of(index * step, step), step)
        total = sources[0][at, :].astype(jnp.float32)
        for source in sources[1:]:
            total = total + source[at, :].astype(jnp.float32)
        target[at, :] = total.astype(target.dtype)
        return carry

    lax.fori_loop(0, rows // step, some, 0)


def scatter_kernel(
    spots,
    parts,
    active,
    x_ref,
    o_ref,
    own_buf,
    pair_buf,
    over_src,
    over_buf,
    line_src,
    up_buf,
    down_buf,
    own_in,
    pair_out,
    pair_in,
    over_out,
    over_in,
    line_out,
    up_in,
    down_in,
):
    rows = x_ref.shape[1] // parts
    cut = lambda part: pl.ds(part * rows, rows)

    def run():
        spot, chip, core = places(spots)
        greet(spots, spot, chip, core)

        def order(step):
            if step == spots - 1:
                return spot
            fall = spots - 1 - step
            fall = jnp.where(fall <= spot, fall - 1, fall)
            rise = jnp.where(step >= spot, step + 1, step)
            return jnp.where(2 * spot < spots - 1, fall, rise)

        def pair(at, c, part):
            return remote(
                x_ref.at[slot(at, c, 1 - core), cut(part)],
                pair_buf.at[at, c, cut(part)],
                to_partner(chip, core),
                pair_out.at[at, c, part],
                pair_in.at[at, c, part],
            )

        def over(at, part):
            return remote(
                over_src.at[at, cut(part)],
                over_buf.at[at, cut(part)],
                to_other(chip, core),
                over_out.at[at, part],
                over_in.at[at, part],
            )

        def up(at, part):
            return remote(
                line_src.at[at, cut(part)],
                up_buf.at[at, cut(part)],
                {PACKS: spot + 1},
                line_out.at[at, part],
                up_in.at[at, part],
            )

        def down(at, part):
            return remote(
                line_src.at[at, cut(part)],
                down_buf.at[at, cut(part)],
                {PACKS: spot - 1},
                line_out.at[at, part],
                down_in.at[at, part],
            )

        def own(at, c):
            return pltpu.make_async_copy(x_ref.at[slot(at, c, core)], own_buf.at[at, c], own_in.at[at, c])

        for c in (1 - chip, chip):
            for step in range(spots):
                own(order(step), c).start()
                for part in range(parts):
                    pair(order(step), c, part).start()
        for step in range(spots):
            at = order(step)
            own(at, 1 - chip).wait()
            for part in range(parts):
                pair(at, 1 - chip, part).wait_recv()
                add_into(
                    over_src.at[at, cut(part)],
                    [own_buf.at[at, 1 - chip, cut(part)], pair_buf.at[at, 1 - chip, cut(part)]],
                    rows,
                )
                over(at, part).start()
        for step in range(spots):
            at = order(step)
            own(at, chip).wait()
            for part in range(parts):
                pair(at, chip, part).wait_recv()
                over(at, part).wait_recv()
                base = [
                    own_buf.at[at, chip, cut(part)],
                    pair_buf.at[at, chip, cut(part)],
                    over_buf.at[at, cut(part)],
                ]
                ups, downs = up_buf.at[at, cut(part)], down_buf.at[at, cut(part)]
                if step < spots - 1:
                    target = line_src.at[at, cut(part)]

                    def rising(first):
                        if not first:
                            up(at, part).wait_recv()
                        add_into(target, base if first else base + [ups], rows)
                        up(at, part).start()

                    def falling(first):
                        if not first:
                            down(at, part).wait_recv()
                        add_into(target, base if first else base + [downs], rows)
                        down(at, part).start()

                    pl.when((at > spot) & (spot == 0))(lambda: rising(True))
                    pl.when((at > spot) & (spot > 0))(lambda: rising(False))
                    pl.when((at < spot) & (spot == spots - 1))(lambda: falling(True))
                    pl.when((at < spot) & (spot < spots - 1))(lambda: falling(False))
                elif spots == 1:
                    add_into(o_ref.at[cut(part)], base, rows)
                else:

                    def finish(ends):
                        if ends < 1:
                            up(at, part).wait_recv()
                        if ends > -1:
                            down(at, part).wait_recv()
                        extra = ([ups] if ends < 1 else []) + ([downs] if ends > -1 else [])
                        add_into(o_ref.at[cut(part)], base + extra, rows)

                    pl.when(spot == 0)(lambda: finish(1))
                    pl.when(spot == spots - 1)(lambda: finish(-1))
                    pl.when((spot > 0) & (spot < spots - 1))(lambda: finish(0))
        for part in range(parts):
            for step in range(spots):
                at = order(step)
                pair(at, 0, part).wait_send()
                pair(at, 1, part).wait_send()
                over(at, part).wait_send()
                if step < spots - 1:
                    up(at, part).wait_send()

    if active is None:
        run()
    else:
        pl.when(lax.axis_index(SECTION) == active)(run)


def scatter_blocks(partial, rows, across, number, active=None, parts=4):
    if lax.axis_size(MEMBERS) != 4:
        axes = BOTH if across else MEMBERS
        taken = partial[: rows * lax.axis_size(axes)]
        return lax.psum_scatter(taken, axes, scatter_dimension=0, tiled=True).astype(jnp.float32)
    spots = lax.axis_size(PACKS) if across else 1
    width = partial.shape[1]
    dma = pltpu.SemaphoreType.DMA
    hold = lambda *lead: pltpu.VMEM((*lead, rows, width), partial.dtype)
    return pl.pallas_call(
        functools.partial(scatter_kernel, spots, parts, active),
        out_shape=jax.ShapeDtypeStruct((rows, width), jnp.float32),
        in_specs=[pl.BlockSpec(memory_space=pl.ANY)],
        out_specs=pl.BlockSpec(memory_space=pltpu.VMEM),
        scratch_shapes=[
            hold(spots, 2),
            hold(spots, 2),
            hold(spots),
            hold(spots),
            hold(spots),
            hold(spots),
            hold(spots),
            dma((spots, 2)),
            dma((spots, 2, parts)),
            dma((spots, 2, parts)),
            dma((spots, parts)),
            dma((spots, parts)),
            dma((spots, parts)),
            dma((spots, parts)),
            dma((spots, parts)),
        ],
        compiler_params=pltpu.CompilerParams(collective_id=number, has_side_effects=True),
        name=f"scatter{number}",
    )(partial.reshape(-1, rows, width))


def allowed_pairs(seg_col, seg_row):
    rows = seg_col.shape[0]
    later = lax.broadcasted_iota(jnp.int32, (rows, rows), 0)
    earlier = lax.broadcasted_iota(jnp.int32, (rows, rows), 1)
    return (seg_col == seg_row) & (earlier <= later)


def attend_kernel(heads, q_ref, lat_ref, key_ref, cos_ref, sin_ref, col_ref, row_ref, out_ref, rot_ref):
    factor = QK**-0.5
    allowed = allowed_pairs(col_ref[...], row_ref[0])
    cosine, sine = cos_ref[...], sin_ref[...]
    shared = key_ref[:, LAT:]
    for head in range(heads):
        raw = q_ref[:, head * QK : (head + 1) * QK]
        query = bf16(
            jnp.concatenate([raw[:, :NOPE], rotate(raw[:, NOPE:], cosine, sine)], axis=1)
        )
        rot_ref[:, head * QK : (head + 1) * QK] = query
        key = jnp.concatenate([lat_ref[:, head * KV : head * KV + NOPE], shared], axis=1)
        value = lat_ref[:, head * KV + NOPE : (head + 1) * KV]
        scores = jnp.where(allowed, dot_t(query, key) * factor, masked_score)
        top = jnp.max(scores, axis=1, keepdims=True)
        powers = jnp.exp(scores - top)
        probs = powers / jnp.sum(powers, axis=1, keepdims=True)
        out_ref[:, head * VD : (head + 1) * VD] = bf16(dot(bf16(probs), value))


def attend(query_raw, latent, keyed, tables, groups=1):
    cosine, sine, seg_col, seg_row = tables
    count, _, rows = seg_row.shape
    heads = query_raw.shape[1] // QK
    block = lambda width: pl.BlockSpec((rows, width), lambda i: (i, 0))
    same = lambda width: pl.BlockSpec((rows, width), lambda i: (0, 0) if groups > 1 else (i, 0))
    count = count * groups
    return pl.pallas_call(
        functools.partial(attend_kernel, heads),
        grid=(count,),
        in_specs=[
            block(heads * QK),
            block(heads * KV),
            same(LAT + ROPE),
            same(HALF),
            same(HALF),
            same(1),
            pl.BlockSpec((1, 1, rows), lambda i: (0, 0, 0) if groups > 1 else (i, 0, 0)),
        ],
        out_specs=[block(heads * VD), block(heads * QK)],
        out_shape=[
            jax.ShapeDtypeStruct((count * rows, heads * VD), jnp.bfloat16),
            jax.ShapeDtypeStruct((count * rows, heads * QK), jnp.bfloat16),
        ],
        name="attend",
        cost_estimate=pl.CostEstimate(
            flops=2 * count * heads * rows * rows * (QK + VD),
            bytes_accessed=count * rows * heads * (QK * 6 + KV * 2 + VD * 2),
            transcendentals=count * heads * rows * rows,
        ),
    )(query_raw, latent, keyed, cosine, sine, seg_col, seg_row)


def attend_back_kernel(
    heads, q_ref, lat_ref, key_ref, grad_ref, cos_ref, sin_ref, col_ref, row_ref, dq_ref, dlat_ref, dkey_ref
):
    factor = QK**-0.5
    allowed = allowed_pairs(col_ref[...], row_ref[0])
    cosine, sine = cos_ref[...], sin_ref[...]
    shared = key_ref[:, LAT:]
    total = None
    for head in range(heads):
        query = q_ref[:, head * QK : (head + 1) * QK]
        key = jnp.concatenate([lat_ref[:, head * KV : head * KV + NOPE], shared], axis=1)
        value = lat_ref[:, head * KV + NOPE : (head + 1) * KV]
        grad = grad_ref[:, head * VD : (head + 1) * VD]
        scores = jnp.where(allowed, dot_t(query, key) * factor, masked_score)
        top = jnp.max(scores, axis=1, keepdims=True)
        powers = jnp.exp(scores - top)
        probs = powers / jnp.sum(powers, axis=1, keepdims=True)
        grad_value = t_dot(bf16(probs), grad)
        grad_probs = dot_t(grad, value)
        centre = jnp.sum(probs * grad_probs, axis=1, keepdims=True)
        grad_scores = bf16(probs * (grad_probs - centre) * factor)
        grad_query = dot(grad_scores, key)
        grad_key = t_dot(grad_scores, query)
        dq_ref[:, head * QK : (head + 1) * QK] = bf16(
            jnp.concatenate(
                [grad_query[:, :NOPE], rotate(grad_query[:, NOPE:], cosine, -sine)], axis=1
            )
        )
        dlat_ref[:, head * KV : head * KV + NOPE] = bf16(grad_key[:, :NOPE])
        dlat_ref[:, head * KV + NOPE : (head + 1) * KV] = bf16(grad_value)
        part = grad_key[:, NOPE:]
        total = part if total is None else total + part
    dkey_ref[...] = total


def attend_back(query, latent, keyed, grad, tables, groups=1):
    cosine, sine, seg_col, seg_row = tables
    count, _, rows = seg_row.shape
    heads = query.shape[1] // QK
    block = lambda width: pl.BlockSpec((rows, width), lambda i: (i, 0))
    same = lambda width: pl.BlockSpec((rows, width), lambda i: (0, 0) if groups > 1 else (i, 0))
    count = count * groups
    return pl.pallas_call(
        functools.partial(attend_back_kernel, heads),
        grid=(count,),
        in_specs=[
            block(heads * QK),
            block(heads * KV),
            same(LAT + ROPE),
            block(heads * VD),
            same(HALF),
            same(HALF),
            same(1),
            pl.BlockSpec((1, 1, rows), lambda i: (0, 0, 0) if groups > 1 else (i, 0, 0)),
        ],
        out_specs=[block(heads * QK), block(heads * KV), block(ROPE)],
        out_shape=[
            jax.ShapeDtypeStruct((count * rows, heads * QK), jnp.bfloat16),
            jax.ShapeDtypeStruct((count * rows, heads * KV), jnp.bfloat16),
            jax.ShapeDtypeStruct((count * rows, ROPE), jnp.float32),
        ],
        name="attend_back",
        cost_estimate=pl.CostEstimate(
            flops=2 * count * heads * rows * rows * (3 * QK + 2 * VD),
            bytes_accessed=count * rows * heads * (QK * 4 + KV * 4 + VD * 2),
            transcendentals=count * heads * rows * rows,
        ),
    )(query, latent, keyed, grad, cosine, sine, seg_col, seg_row)


def gated_hidden(gate, up):
    return silu_parts(gate)[0] * up


def gated_back(gate, up, grad_hidden):
    act, slope = silu_parts(gate)
    return bf16(grad_hidden * up * slope), bf16(grad_hidden * act)


def columns(pieces):
    start = 0
    for piece in pieces:
        yield start, piece.shape[1]
        start += piece.shape[1]


def hold_weight(pieces):
    return pltpu.VMEM((pieces[0].shape[0], sum(piece.shape[1] for piece in pieces)), pieces[0].dtype)


def loads_of(counts, sources, targets, sems):
    copies = []
    for pieces, target in zip(counts, targets):
        group, sources = sources[:pieces], sources[pieces:]
        for source, (start, size) in zip(group, columns(group)):
            place = target if pieces == 1 else target.at[:, pl.ds(start, size)]
            copies.append(pltpu.make_async_copy(source, place, sems.at[len(copies)]))
    return copies


def load(*args):
    copies = loads_of(*args)
    for copy in copies:
        copy.start()
    for copy in copies:
        copy.wait()


class Tiles:
    def __init__(self, rows, pack_rows, pack, active):
        self.rows, self.pack_rows = rows, pack_rows
        self.tile = min(256, pack_rows)
        self.count = rows // self.tile
        inner = pack_rows // self.tile
        runs = (lax.axis_index(SECTION) == active).astype(jnp.int32)
        self.control = jnp.stack([pack * inner, (pack + 1) * inner, runs]).astype(jnp.int32)

    def source(self, width):
        return pl.BlockSpec((self.tile, width), lambda i, control: (i * control[2], 0))

    def small(self, array):
        return pl.BlockSpec(array.shape, lambda i, control: (0,) * array.ndim)

    def pair_source(self, width):
        return pl.BlockSpec((2, self.tile, width), lambda i, control: (0, i * control[2], 0))

    def result(self, width, dtype=jnp.bfloat16):
        def index(i, control):
            return (jnp.where(control[2] == 1, i, self.count), 0)

        shape = jax.ShapeDtypeStruct((self.rows + self.tile, width), dtype)
        return shape, pl.BlockSpec((self.tile, width), index)

    def pair_result(self, width):
        def index(i, control):
            return (0, jnp.where(control[2] == 1, i, self.count), 0)

        shape = jax.ShapeDtypeStruct((2, self.rows + self.tile, width), jnp.bfloat16)
        return shape, pl.BlockSpec((2, self.tile, width), index)

    def call(self, kernel, name, sources, weights, results, into=(), scratch=(), flops=0):
        arrays, specs = zip(*sources)
        shapes, out_specs = zip(*results)
        anywhere = pl.BlockSpec(memory_space=pl.ANY)
        pieces = [piece for weight in weights for piece in weight]
        counts = [len(weight) for weight in weights]
        first = 1 + len(arrays) + len(pieces)
        return pl.pallas_call(
            functools.partial(kernel, len(arrays), counts, len(into), len(results)),
            grid_spec=pltpu.PrefetchScalarGridSpec(
                num_scalar_prefetch=1,
                grid=(self.count,),
                in_specs=[*specs, *([anywhere] * (len(pieces) + len(into)))],
                out_specs=list(out_specs),
                scratch_shapes=[
                    *[hold_weight(weight) for weight in weights],
                    pltpu.SemaphoreType.DMA((len(pieces),)),
                    *scratch,
                ],
            ),
            out_shape=list(shapes),
            input_output_aliases={first + index: index for index in range(len(into))},
            name=name,
            cost_estimate=pl.CostEstimate(flops=flops, bytes_accessed=self.rows * 16384, transcendentals=0),
        )(self.control, *arrays, *pieces, *into)


def tiled(body):
    def kernel(n_sources, counts, n_into, n_results, control, *refs):
        n_weights, n_pieces = len(counts), sum(counts)
        sources, refs = refs[:n_sources], refs[n_sources:]
        stored, refs = refs[:n_pieces], refs[n_pieces + n_into :]
        results, refs = refs[:n_results], refs[n_results:]
        weights, sems, scratch = refs[:n_weights], refs[n_weights], refs[n_weights + 1 :]

        def run():
            pl.when(pl.program_id(0) == 0)(lambda: load(counts, stored, weights, sems))
            body(inside_pack(control), [sources[0][...], *sources[1:]], weights, results, scratch)

        pl.when(control[2] == 1)(run)

    return kernel


def inside_pack(control):
    tile = pl.program_id(0)
    return (tile >= control[0]) & (tile < control[1])


def shared_units(x, shared_in):
    half = shared_in.shape[0] // 2
    return dot_t(x, shared_in[:half]), dot_t(x, shared_in[half:])


def experts_body(inside, sources, weights, results, scratch):
    x, own_ref, routed_ref = sources
    in_ref, shared_in_ref = weights[:2]
    pre_ref, gated_ref, prob_ref, shared_pre_ref, hid_ref = results[:5]
    units = gated_ref.shape[1]
    pre = dot(x, in_ref[...])
    logits = pre[:, 2 * units : 2 * units + own_ref.shape[1]]
    powers = jnp.exp(logits - jnp.max(logits, axis=1, keepdims=True))
    prob = powers / jnp.sum(powers, axis=1, keepdims=True)
    prob_ref[...] = prob
    gate = jnp.sum(prob * own_ref[...], axis=1, keepdims=True) * routed_ref[...]
    pre_ref[...] = bf16(pre[:, : 2 * units])
    gated = bf16(gate * gated_hidden(pre[:, :units], pre[:, units : 2 * units]))
    gated_ref[...] = gated

    def shared():
        left, right = shared_units(x, shared_in_ref)
        hidden = bf16(gated_hidden(left, right))
        shared_pre_ref[0] = bf16(left)
        shared_pre_ref[1] = bf16(right)
        hid_ref[...] = hidden
        return hidden

    if len(weights) == 2:
        shared()
        return
    out_ref, shared_out_ref = weights[2:]
    partial_ref = results[5]

    def with_shared():
        hidden = shared()
        partial_ref[...] = bf16(dot(gated, out_ref[...]) + dot(hidden, shared_out_ref[...]))

    def without():
        partial_ref[...] = bf16(dot(gated, out_ref[...]))

    pl.when(inside)(with_shared)
    pl.when(jnp.logical_not(inside))(without)


def finish_body(inside, sources, weights, results, scratch):
    gated, _, shared_pre_ref = sources
    out_ref, shared_out_ref = weights
    (partial_ref,) = results

    def with_shared():
        hidden = bf16(gated_hidden(shared_pre_ref[0].astype(jnp.float32), shared_pre_ref[1].astype(jnp.float32)))
        partial_ref[...] = bf16(dot(gated, out_ref[...]) + dot(hidden, shared_out_ref[...]))

    def without():
        partial_ref[...] = bf16(dot(gated, out_ref[...]))

    pl.when(inside)(with_shared)
    pl.when(jnp.logical_not(inside))(without)


def experts_back_body(inside, sources, weights, results, scratch):
    grad, own_ref, pre_ref, prob_ref, routed_ref, shared_pre_ref = sources
    in_ref, shared_in_ref, out_ref, shared_out_ref = weights
    grad_pre_ref, moved_ref, partial_ref = results
    (joined_ref,) = scratch
    units = out_ref.shape[0]
    prob = prob_ref[...]
    own_prob = jnp.sum(prob * own_ref[...], axis=1, keepdims=True) * routed_ref[...]
    gate, up = pre_ref[:, :units].astype(jnp.float32), pre_ref[:, units:].astype(jnp.float32)
    grad_units = dot_t(grad, out_ref[...])
    act, slope = silu_parts(gate)
    moved = own_prob * jnp.sum(grad_units * act * up, axis=1, keepdims=True)
    moved_ref[...] = moved
    scaled = own_prob * grad_units
    joined_ref[:, :units] = bf16(scaled * up * slope)
    joined_ref[:, units : 2 * units] = bf16(scaled * act)
    joined_ref[:, 2 * units :] = jnp.zeros_like(joined_ref[:, 2 * units :])
    joined_ref[:, 2 * units : 2 * units + own_ref.shape[1]] = bf16(moved * (own_ref[...] - prob))
    grad_pre_ref[...] = joined_ref[:, : 2 * units]
    base = dot_t(joined_ref[...], in_ref[...])
    half = shared_out_ref.shape[0]

    def with_shared():
        left, right = gated_back(
            shared_pre_ref[0].astype(jnp.float32),
            shared_pre_ref[1].astype(jnp.float32),
            dot_t(grad, shared_out_ref[...]),
        )
        partial_ref[...] = bf16(base + dot(left, shared_in_ref[:half]) + dot(right, shared_in_ref[half:]))

    def without():
        partial_ref[...] = bf16(base)

    pl.when(inside)(with_shared)
    pl.when(jnp.logical_not(inside))(without)


def shared_body(inside, sources, weights, results, scratch):
    pre_ref, hid_ref = results
    left, right = shared_units(sources[0], weights[0])
    pre_ref[0] = bf16(left)
    pre_ref[1] = bf16(right)
    hid_ref[...] = bf16(gated_hidden(left, right))


def heads_body(block, inside, sources, weights, results, scratch):
    x, key_ref, cos_ref, sin_ref, col_ref, row_ref = sources
    query_w_ref, expand_ref = weights
    out_ref, rot_ref, lat_ref = results
    (q_ref,) = scratch
    heads = q_ref.shape[1] // QK
    q_ref[...] = dot(x, query_w_ref[...])
    lat_ref[...] = bf16(dot(key_ref[:, :LAT], expand_ref[...]))
    for start in range(0, x.shape[0], block):
        at = pl.ds(start, block)
        attend_kernel(
            heads,
            q_ref.at[at],
            lat_ref.at[at],
            key_ref.at[at],
            cos_ref.at[at],
            sin_ref.at[at],
            col_ref.at[at],
            row_ref.at[pl.ds(start // block, 1)],
            out_ref.at[at],
            rot_ref.at[at],
        )


def pair_grad_kernel(x_ref, grad_ref, out_ref):
    units = out_ref.shape[2]
    x = x_ref[...]
    out_ref[:, 0, :] = t_dot(x, grad_ref[:, :units])
    out_ref[:, 1, :] = t_dot(x, grad_ref[:, units:])


def pair_grad(x, grad):
    rows, width = x.shape
    units = grad.shape[1] // 2
    if rows > 4096:
        return t_dot(x, grad[:rows]).reshape(width, 2, units)
    tile = 256
    return pl.pallas_call(
        pair_grad_kernel,
        grid=(width // tile,),
        in_specs=[
            pl.BlockSpec((rows, tile), lambda i: (0, i)),
            pl.BlockSpec((rows, 2 * units), lambda i: (0, 0), pipeline_mode=pl.Buffered(1)),
        ],
        out_specs=pl.BlockSpec((tile, 2, units), lambda i: (i, 0, 0)),
        out_shape=jax.ShapeDtypeStruct((width, 2, units), jnp.float32),
        name="pair_grad",
        cost_estimate=pl.CostEstimate(
            flops=4 * rows * width * units, bytes_accessed=rows * (width + 2 * units) * 2 + width * units * 8, transcendentals=0
        ),
    )(x, grad)


def blank(shape, dtype):
    return pl.pallas_call(
        lambda out_ref: None,
        out_shape=jax.ShapeDtypeStruct(shape, dtype),
        out_specs=pl.BlockSpec(memory_space=pl.ANY),
        compiler_params=pltpu.CompilerParams(has_side_effects=True),
        name="blank",
    )()


def arrival_order(spots):
    tiles = [(rank + 1.1 * over, rank, over) for rank in range(spots) for over in (0, 1)]
    return [(rank, over == 1) for _, rank, over in sorted(tiles)]


def ranked_spots(spots, spot):
    ranks = []
    for rank in range(spots):
        value = 0
        for own in range(spots):
            nearest = sorted(range(spots), key=lambda other: (abs(other - own), other))
            value = value + jnp.where(spot == own, nearest[rank], 0)
        ranks.append(value)
    return ranks


def pick(index, values):
    total = 0
    for position, value in enumerate(values):
        total = total + jnp.where(index == position, value, 0)
    return total


def fused_kernel(spots, parts, active, body, pack_kinds, counts, n_into, *refs):
    source_kinds, result_kinds = pack_kinds
    n_sources, n_results = len(source_kinds), len(result_kinds)
    n_weights, n_pieces = len(counts), sum(counts)
    x_ref, small_ref, refs = refs[0], refs[1], refs[2:]
    sources, refs = refs[:n_sources], refs[n_sources:]
    stored, refs = refs[:n_pieces], refs[n_pieces + n_into :]
    o_ref, refs = refs[0], refs[1:]
    results, refs = refs[:n_results], refs[n_results:]
    x_tile, refs = refs[0], refs[1:]
    source_tiles, refs = refs[:n_sources], refs[n_sources:]
    result_tiles, refs = refs[:n_results], refs[n_results:]
    weights, refs = refs[:n_weights], refs[n_weights:]
    sems, scratch = refs[:12], refs[12:]
    own_sem, weight_sem, tile_sem, out_sem = sems[:4]
    up_out, up_in, down_out, down_in, over_out, over_in, pair_out, pair_in = sems[4:]
    block = x_ref.shape[0]
    rows = block // parts
    tile = 2 * block

    def run():
        loads = loads_of(counts, stored, weights, weight_sem)
        for copy in loads:
            copy.start()
        spot, chip, core = places(spots)
        greet(spots, spot, chip, core)
        piece = lambda index, part: o_ref.at[index, pl.ds(part * rows, rows)]
        first = lambda part: x_ref.at[pl.ds(part * rows, rows)]

        def up(source, at, part, reach):
            return remote(
                source, piece(slot(at, chip, core), part), {PACKS: spot + 1}, up_out.at[reach, part], up_in.at[reach, part]
            )

        def down(source, at, part, reach):
            return remote(
                source,
                piece(slot(at, chip, core), part),
                {PACKS: spot - 1},
                down_out.at[reach, part],
                down_in.at[reach, part],
            )

        def over(source, at, part):
            return remote(
                source, piece(slot(at, chip, core), part), to_other(chip, core), over_out.at[at, part], over_in.at[at, part]
            )

        def pair(source, at, c, part):
            return remote(
                source,
                piece(slot(at, c, core), part),
                to_partner(chip, core),
                pair_out.at[c, at, part],
                pair_in.at[c, at, part],
            )

        mine = slot(spot, chip, core)
        for part in range(parts):
            source = first(part)
            pair(source, spot, chip, part).start()
            over(source, spot, part).start()
            pl.when(spot < spots - 1)(lambda: up(source, spot, part, 0).start())
            pl.when(spot > 0)(lambda: down(source, spot, part, 0).start())
        own = pltpu.make_async_copy(x_ref, o_ref.at[mine], own_sem.at[0])
        own.start()
        own.wait()
        ranks = ranked_spots(spots, spot)
        order = arrival_order(spots)

        def hand_on(reach):
            for part in range(parts):

                def below(part=part):
                    at = spot - reach
                    source = piece(slot(at, chip, core), part)
                    up(source, at, part, reach - 1).wait_recv()
                    pl.when(spot < spots - 1)(lambda: up(source, at, part, reach).start())
                    over(source, at, part).start()
                    pair(source, at, chip, part).start()

                def above(part=part):
                    at = spot + reach
                    source = piece(slot(at, chip, core), part)
                    down(source, at, part, reach - 1).wait_recv()
                    pl.when(spot > 0)(lambda: down(source, at, part, reach).start())
                    over(source, at, part).start()
                    pair(source, at, chip, part).start()

                pl.when(spot >= reach)(below)
                pl.when(spot + reach < spots)(above)

        def arrive(rank, across):
            at = ranks[rank]
            if across:
                for part in range(parts):
                    source = piece(slot(at, 1 - chip, core), part)
                    over(source, at, part).wait_recv()
                    pair(source, at, 1 - chip, part).start()
                for part in range(parts):
                    pair(first(part), at, 1 - chip, part).wait_recv()
                return
            if rank > 0:
                hand_on(rank)
            for part in range(parts):
                pair(first(part), at, chip, part).wait_recv()

        def window(ref, kind, at, c):
            if kind:
                return ref.at[:, pl.ds(pl.multiple_of((at * 2 + c) * tile, tile), tile)]
            return ref.at[pl.ds(pl.multiple_of((at * 2 + c) * tile, tile), tile)]

        def outward(index, which, at, c):
            return pltpu.make_async_copy(
                result_tiles[index].at[which], window(results[index], result_kinds[index], at, c), out_sem.at[which, index]
            )

        def step(number, carry):
            for position, (rank, across) in enumerate(order):
                pl.when(number == position)(functools.partial(arrive, rank, across))
            at = pick(number, [ranks[rank] for rank, _ in order])
            c = pick(number, [1 - chip if across else chip for _, across in order])
            inside = at == spot
            inputs = [pltpu.make_async_copy(o_ref.at[pl.ds(slot(at, c, 0), 2)], x_tile, tile_sem.at[0])]
            for index, kind in enumerate(source_kinds):
                if not kind:
                    inputs.append(
                        pltpu.make_async_copy(
                            window(sources[index], kind, at, c), source_tiles[index], tile_sem.at[1 + index]
                        )
                    )
            for copy in inputs:
                copy.start()
            for index, kind in enumerate(source_kinds):
                if kind:

                    def fetch(index=index, kind=kind):
                        copy = pltpu.make_async_copy(
                            window(sources[index], kind, at, c), source_tiles[index], tile_sem.at[1 + index]
                        )
                        copy.start()
                        copy.wait()

                    pl.when(inside)(fetch)

            @pl.when(number == 0)
            def _():
                for copy in loads:
                    copy.wait()

            which = lax.rem(number, 2)

            @pl.when(number >= 2)
            def _():
                for index in range(n_results):
                    outward(index, which, at, c).wait()

            for copy in inputs:
                copy.wait()
            body(
                inside,
                [x_tile[...].reshape(tile, x_tile.shape[2]), small_ref, *source_tiles],
                weights,
                [target.at[which] for target in result_tiles],
                scratch,
            )
            for index in range(n_results):
                outward(index, which, at, c).start()
            return carry

        lax.fori_loop(0, 2 * spots, step, 0)
        for which in range(2):
            for index in range(n_results):
                outward(index, which, spot, chip).wait()
        for part in range(parts):
            for at in range(spots):
                over(first(part), at, part).wait_send()
                for c in range(2):
                    pair(first(part), at, c, part).wait_send()
            for reach in range(spots - 1):
                pl.when((spot >= reach) & (spot < spots - 1))(lambda: up(first(part), spot, part, reach).wait_send())
                pl.when((spot + reach < spots) & (spot > 0))(lambda: down(first(part), spot, part, reach).wait_send())

    pl.when(lax.axis_index(SECTION) == active)(run)


def fused_call(tiles, rows_in, number, active, body, small, sources, weights, results, gathered, into, scratch=(), parts=4):
    spots = lax.axis_size(PACKS)
    block, width = rows_in.shape
    tile = 2 * block
    dma = pltpu.SemaphoreType.DMA
    hops = max(spots - 1, 1)
    anywhere = pl.BlockSpec(memory_space=pl.ANY)
    inside = pl.BlockSpec(memory_space=pltpu.VMEM)
    shapes = [jax.ShapeDtypeStruct((spots * 4, block, width), rows_in.dtype), *(shape for shape, _ in results)]
    held = [gathered.reshape(shapes[0].shape), *into]
    pieces = [piece for weight in weights for piece in weight]
    first = 2 + len(sources) + len(pieces)

    def hold(array, kind, *lead):
        shape = (2, tile, array.shape[2]) if kind else (tile, array.shape[1])
        return pltpu.VMEM((*lead, *shape), array.dtype)

    outs = pl.pallas_call(
        functools.partial(
            fused_kernel,
            spots,
            parts,
            active,
            body,
            ([kind for _, kind in sources], [kind for _, kind in results]),
            [len(weight) for weight in weights],
            len(held),
        ),
        out_shape=shapes,
        in_specs=[inside, inside, *([anywhere] * (len(sources) + len(pieces) + len(held)))],
        out_specs=[anywhere] * len(shapes),
        input_output_aliases={first + index: index for index in range(len(held))},
        scratch_shapes=[
            pltpu.VMEM((2, block, width), rows_in.dtype),
            *(hold(array, kind) for array, kind in sources),
            *(hold(shape, kind, 2) for shape, kind in results),
            *(hold_weight(weight) for weight in weights),
            dma((1,)),
            dma((len(pieces),)),
            dma((1 + len(sources),)),
            dma((2, len(results))),
            dma((hops, parts)),
            dma((hops, parts)),
            dma((hops, parts)),
            dma((hops, parts)),
            dma((spots, parts)),
            dma((spots, parts)),
            dma((2, spots, parts)),
            dma((2, spots, parts)),
            *scratch,
        ],
        compiler_params=pltpu.CompilerParams(collective_id=number, has_side_effects=True),
        name=f"fused{number}",
    )(rows_in, small, *(array for array, _ in sources), *pieces, *held)
    return outs[0].reshape(-1, width), list(outs[1:])


def sum_kernel(spots, parts, active, body, pack_kinds, counts, n_into, *refs):
    source_kinds, result_kinds = pack_kinds
    n_sources, n_results = len(source_kinds), len(result_kinds)
    n_weights, n_pieces = len(counts), sum(counts)
    small_ref, refs = refs[0], refs[1:]
    sources, refs = refs[:n_sources], refs[n_sources:]
    stored, refs = refs[:n_pieces], refs[n_pieces + n_into :]
    o_ref, refs = refs[0], refs[1:]
    results, refs = refs[:n_results], refs[n_results:]
    source_tiles, refs = refs[:n_sources], refs[n_sources:]
    result_tiles, refs = refs[:n_results], refs[n_results:]
    weights, refs = refs[:n_weights], refs[n_weights:]
    x_buf, pair_buf, over_src, over_buf, line_src, up_buf, down_buf = refs[:7]
    weight_sem, tile_sem, out_sem, pair_out, pair_in, over_out, over_in, line_out, up_in, down_in = refs[7:17]
    scratch = refs[17:]
    block = o_ref.shape[0]
    rows = block // parts
    tile = 2 * block
    cut = lambda part: pl.ds(part * rows, rows)

    def run():
        loads = loads_of(counts, stored, weights, weight_sem)
        for copy in loads:
            copy.start()
        spot, chip, core = places(spots)

        def order(step):
            if step == spots - 1:
                return spot
            fall = spots - 1 - step
            fall = jnp.where(fall <= spot, fall - 1, fall)
            rise = jnp.where(step >= spot, step + 1, step)
            return jnp.where(2 * spot < spots - 1, fall, rise)

        turns = [(0, True)]
        for ahead in range(1, spots):
            turns += [(ahead, True), (ahead - 1, False)]
        turns.append((spots - 1, False))

        def place(number):
            at = pick(number, [order(turn) for turn, _ in turns])
            return at, pick(number, [1 - chip if far else chip for _, far in turns])

        def window(ref, kind, at, c):
            if kind:
                return ref.at[:, pl.ds(pl.multiple_of((at * 2 + c) * tile, tile), tile)]
            return ref.at[pl.ds(pl.multiple_of((at * 2 + c) * tile, tile), tile)]

        def inputs(number):
            at, c = place(number)
            which = lax.rem(number, 2)
            return [
                pltpu.make_async_copy(
                    window(sources[index], kind, at, c), source_tiles[index].at[which], tile_sem.at[which, index]
                )
                for index, kind in enumerate(source_kinds)
                if not kind
            ]

        for copy in inputs(0):
            copy.start()
        greet(spots, spot, chip, core)

        def mine(at, c, k, part):
            return x_buf.at[at * 2 + c, pl.ds(pl.multiple_of(k * block + part * rows, rows), rows)]

        def pair(at, c, part):
            return remote(
                mine(at, c, 1 - core, part),
                pair_buf.at[at, c, cut(part)],
                to_partner(chip, core),
                pair_out.at[at, c, part],
                pair_in.at[at, c, part],
            )

        def over(at, part):
            return remote(
                over_src.at[at, cut(part)],
                over_buf.at[at, cut(part)],
                to_other(chip, core),
                over_out.at[at, part],
                over_in.at[at, part],
            )

        def up(at, part):
            return remote(
                line_src.at[at, cut(part)],
                up_buf.at[at, cut(part)],
                {PACKS: spot + 1},
                line_out.at[at, part],
                up_in.at[at, part],
            )

        def down(at, part):
            return remote(
                line_src.at[at, cut(part)],
                down_buf.at[at, cut(part)],
                {PACKS: spot - 1},
                line_out.at[at, part],
                down_in.at[at, part],
            )

        def across(step):
            at = order(step)
            for part in range(parts):
                pair(at, 1 - chip, part).wait_recv()
                add_into(
                    over_src.at[at, cut(part)],
                    [mine(at, 1 - chip, core, part), pair_buf.at[at, 1 - chip, cut(part)]],
                    rows,
                )
                over(at, part).start()

        def along(step):
            at = order(step)
            for part in range(parts):
                pair(at, chip, part).wait_recv()
                over(at, part).wait_recv()
                base = [mine(at, chip, core, part), pair_buf.at[at, chip, cut(part)], over_buf.at[at, cut(part)]]
                ups, downs = up_buf.at[at, cut(part)], down_buf.at[at, cut(part)]
                if step < spots - 1:
                    target = line_src.at[at, cut(part)]

                    def rising(first):
                        if not first:
                            up(at, part).wait_recv()
                        add_into(target, base if first else base + [ups], rows)
                        up(at, part).start()

                    def falling(first):
                        if not first:
                            down(at, part).wait_recv()
                        add_into(target, base if first else base + [downs], rows)
                        down(at, part).start()

                    pl.when((at > spot) & (spot == 0))(lambda: rising(True))
                    pl.when((at > spot) & (spot > 0))(lambda: rising(False))
                    pl.when((at < spot) & (spot == spots - 1))(lambda: falling(True))
                    pl.when((at < spot) & (spot < spots - 1))(lambda: falling(False))
                elif spots == 1:
                    add_into(o_ref.at[cut(part)], base, rows)
                else:

                    def finish(ends):
                        if ends < 1:
                            up(at, part).wait_recv()
                        if ends > -1:
                            down(at, part).wait_recv()
                        extra = ([ups] if ends < 1 else []) + ([downs] if ends > -1 else [])
                        add_into(o_ref.at[cut(part)], base + extra, rows)

                    pl.when(spot == 0)(lambda: finish(1))
                    pl.when(spot == spots - 1)(lambda: finish(-1))
                    pl.when((spot > 0) & (spot < spots - 1))(lambda: finish(0))

        late = 3 + jnp.where((spot > 0) & (spot < spots - 1), 2, 0)

        def outward(index, which, at, c):
            return pltpu.make_async_copy(
                result_tiles[index].at[which], window(results[index], result_kinds[index], at, c), out_sem.at[which, index]
            )

        def step(number, carry):
            at, c = place(number)
            inside = at == spot
            which = lax.rem(number, 2)
            for copy in inputs(number):
                copy.wait()

            @pl.when(number + 1 < 2 * spots)
            def _():
                for copy in inputs(number + 1):
                    copy.start()

            for index, kind in enumerate(source_kinds):
                if kind:

                    def fetch(index=index, kind=kind):
                        copy = pltpu.make_async_copy(
                            window(sources[index], kind, at, c), source_tiles[index], tile_sem.at[0, index]
                        )
                        copy.start()
                        copy.wait()

                    pl.when(inside)(fetch)

            @pl.when(number == 0)
            def _():
                for copy in loads:
                    copy.wait()

            @pl.when(number >= 2)
            def _():
                for index, kind in enumerate(result_kinds):
                    if not kind:
                        outward(index, which, at, c).wait()

            tiles = [
                target if kind else target.at[which] for target, kind in zip(source_tiles, source_kinds)
            ]
            body(
                inside,
                [tiles[0][...], small_ref, *tiles[1:]],
                weights,
                [*(target.at[which] for target in result_tiles), x_buf.at[at * 2 + c]],
                scratch,
            )
            for part in range(parts):
                pair(at, c, part).start()
            for index, kind in enumerate(result_kinds):
                if kind:

                    def put(index=index):
                        copy = outward(index, which, at, c)
                        copy.start()
                        copy.wait()

                    pl.when(inside)(put)
                else:
                    outward(index, which, at, c).start()
            for number_of in range(spots):
                pl.when(number == 2 * number_of)(functools.partial(across, number_of))
                pl.when(number == 2 * number_of + late)(functools.partial(along, number_of))
            return carry

        lax.fori_loop(0, 2 * spots, step, 0)
        for number_of in range(spots):
            pl.when(2 * number_of + late >= 2 * spots)(functools.partial(along, number_of))
        for which in range(2):
            for index, kind in enumerate(result_kinds):
                if not kind:
                    outward(index, which, spot, chip).wait()
        for part in range(parts):
            for number_of in range(spots):
                at = order(number_of)
                pair(at, 0, part).wait_send()
                pair(at, 1, part).wait_send()
                over(at, part).wait_send()
                if number_of < spots - 1:
                    up(at, part).wait_send()

    pl.when(lax.axis_index(SECTION) == active)(run)


def sum_call(rows, number, active, body, small, sources, weights, results, into, scratch=(), parts=4):
    spots = lax.axis_size(PACKS)
    width = weights[-1][0].shape[1]
    tile = 2 * rows
    dma = pltpu.SemaphoreType.DMA
    anywhere = pl.BlockSpec(memory_space=pl.ANY)
    inside = pl.BlockSpec(memory_space=pltpu.VMEM)
    pieces = [piece for weight in weights for piece in weight]
    first = 1 + len(sources) + len(pieces)
    held = lambda *lead: pltpu.VMEM((*lead, rows, width), jnp.bfloat16)

    def hold(array, kind, *lead):
        if kind:
            return pltpu.VMEM((*lead, 2, tile, array.shape[2]), array.dtype)
        return pltpu.VMEM((2, tile, array.shape[1]), array.dtype)

    outs = pl.pallas_call(
        functools.partial(
            sum_kernel,
            spots,
            parts,
            active,
            body,
            ([kind for _, kind in sources], [kind for _, kind in results]),
            [len(weight) for weight in weights],
            len(into),
        ),
        out_shape=[jax.ShapeDtypeStruct((rows, width), jnp.float32), *(shape for shape, _ in results)],
        in_specs=[inside, *([anywhere] * (len(sources) + len(pieces) + len(into)))],
        out_specs=[inside, *([anywhere] * len(results))],
        input_output_aliases={first + index: 1 + index for index in range(len(into))},
        scratch_shapes=[
            *(hold(array, kind) for array, kind in sources),
            *(hold(shape, kind, 2) for shape, kind in results),
            *(hold_weight(weight) for weight in weights),
            pltpu.VMEM((2 * spots, tile, width), jnp.bfloat16),
            held(spots, 2),
            held(spots),
            held(spots),
            held(spots),
            held(spots),
            held(spots),
            dma((len(pieces),)),
            dma((2, len(sources))),
            dma((2, max(len(results), 1))),
            dma((spots, 2, parts)),
            dma((spots, 2, parts)),
            dma((spots, parts)),
            dma((spots, parts)),
            dma((spots, parts)),
            dma((spots, parts)),
            dma((spots, parts)),
            *scratch,
        ],
        compiler_params=pltpu.CompilerParams(collective_id=number, has_side_effects=True),
        name=f"sum{number}",
    )(small, *(array for array, _ in sources), *pieces, *into)
    return outs[0], list(outs[1:])


def body(
    boundary,
    lengths,
    routes,
    attn_gain,
    query_weight,
    compress_weight,
    latent_gain,
    expand_weight,
    output_weight,
    ffn_gain,
    router_weight,
    shared_in,
    shared_out,
    expert_in,
    expert_out,
):
    attn_gain, latent_gain, ffn_gain = attn_gain[0], latent_gain[0], ffn_gain[0]
    query_weight, compress_weight = query_weight[0], compress_weight[0]
    expand_weight, output_weight = expand_weight[0], output_weight[0]
    router_weight, shared_out, expert_out = router_weight[0], shared_out[0], expert_out[0, 0]
    width = boundary.shape[3]
    rows = boundary.shape[2]
    half = shared_out.shape[0]
    units = expert_out.shape[0]
    experts_count = router_weight.shape[1]
    shared_in_t = jnp.transpose(shared_in[0], (1, 2, 0)).reshape(2 * half, width)
    joined_in = (
        expert_in.reshape(width, 2 * units),
        jnp.pad(router_weight, ((0, 0), (0, -experts_count % 128))),
    )
    joined_width = sum(piece.shape[1] for piece in joined_in)

    packs, members = lax.axis_size(PACKS), lax.axis_size(MEMBERS)
    count = packs * members
    pack, member = lax.axis_index(PACKS), lax.axis_index(MEMBERS)
    me = pack * members + member
    is_first = lax.axis_index(SECTION) == 0
    pack_rows = members * rows
    all_rows = count * rows
    heads = output_weight.shape[0] // VD
    top = routes.shape[3]
    tiles = [Tiles(all_rows, pack_rows, pack, active) for active in range(2)]
    fusing = members == 4 and tiles[0].tile == 2 * rows

    def own_pack(value):
        size = value.shape[0] // packs
        return lax.dynamic_slice_in_dim(value, pack * size, size, 0)

    freqs = rope_base ** (-jnp.arange(HALF, dtype=jnp.float32) / HALF)
    angles = jnp.arange(rows, dtype=jnp.float32)[:, None] * freqs[None, :]
    turns = jnp.concatenate([jnp.cos(angles), jnp.sin(angles)], axis=1)

    def tables_of(block_lengths):
        segment, position = block_layout(block_lengths, rows)
        blocks = segment.shape[0]
        chosen = position.reshape(-1)[:, None] == jnp.arange(rows, dtype=jnp.int32)[None, :]
        found = jnp.dot(
            chosen.astype(jnp.float32),
            turns,
            precision=lax.Precision.HIGHEST,
            preferred_element_type=jnp.float32,
        )
        return (
            found[:, :HALF],
            found[:, HALF:],
            segment.reshape(blocks * rows, 1),
            segment.reshape(blocks, 1, rows),
        )

    own_lengths = lax.dynamic_index_in_dim(lengths[0, 0], member, 0, keepdims=False)
    layout = jnp.concatenate(
        [
            jnp.transpose(routes[0, 0]),
            jnp.pad(own_lengths, (0, rows - own_lengths.shape[0]))[None],
            jnp.zeros((-(top + 1) % 8, rows), jnp.int32),
        ],
        axis=0,
    )


    def routed_of(layout_all):
        named = layout_all.reshape(count, -1, rows)[:, :top] == me
        return jnp.any(named, axis=1).astype(jnp.float32).reshape(all_rows, 1)

    tables_pack = tables_of(lengths[0, 0])
    tables_own = tables_of(own_lengths[None])
    own_cos, own_sin = tables_own[:2]
    own_column = (lax.broadcasted_iota(jnp.int32, (1, experts_count), 1) == me).astype(jnp.float32)

    def inputs_of(hidden):
        normed32, scale_attn = rms_forward(hidden, attn_gain)
        normed = bf16(normed32)
        compressed = dot(normed, compress_weight)
        latent32, scale_latent = rms_forward(compressed[:, :LAT], latent_gain)
        keyed = bf16(
            jnp.concatenate([latent32, rotate(compressed[:, LAT:], own_cos, own_sin)], axis=1)
        )
        return normed, keyed, (compressed, scale_attn, scale_latent)

    def run_experts(section, x, routed, gathered, into, number, full):
        at = tiles[section]
        results = [
            at.result(2 * units),
            at.result(units),
            at.result(experts_count, jnp.float32),
            at.pair_result(half),
            at.result(half),
        ]
        weights = [joined_in, (shared_in_t,)]
        if full:
            results.append(at.result(width))
            weights += [(expert_out,), (shared_out,)]
        if fusing:
            shapes = [(shape, index == 3) for index, (shape, _) in enumerate(results)]
            return fused_call(
                at, x, number, section, experts_body, own_column, [(routed, False)], weights, shapes, gathered, into
            )
        (x_all,) = gather_blocks([x], True, number, section, [gathered])
        return x_all, at.call(
            tiled(experts_body),
            "experts",
            [(x_all, at.source(width)), (own_column, at.small(own_column)), (routed, at.source(1))],
            weights,
            results,
            into[:5],
        )

    def summed_over(section, number, body_of, name, sources, weights, results, into, scratch=()):
        at = tiles[section]
        if fusing:
            shapes = [(shape, shape.ndim == 3) for shape, _ in results]
            return sum_call(rows, number, section, body_of, own_column, sources, weights, shapes, into, scratch)
        specs = [(array, at.pair_source(half) if kind else at.source(array.shape[1])) for array, kind in sources]
        specs.insert(1, (own_column, at.small(own_column)))
        *found, partial = at.call(
            tiled(body_of), name, specs, weights, [*results, at.result(width)], into, scratch
        )
        return scatter_blocks(partial, rows, True, number, section), found

    def run_experts_back(section, number, grad_all, routed, stored, into):
        at = tiles[section]
        pre, _, prob, shared_pre, _ = stored
        return summed_over(
            section,
            number,
            experts_back_body,
            "experts_back",
            [(grad_all, False), (pre, False), (prob, False), (routed, False), (shared_pre, True)],
            [joined_in, (shared_in_t,), (expert_out,), (shared_out,)],
            [at.result(2 * units), at.result(1, jnp.float32)],
            into,
            [pltpu.VMEM((at.tile, joined_width), jnp.bfloat16)],
        )

    def run_heads(section, normed_all, keyed_all, tables, into):
        at = tiles[section]
        cosine, sine, seg_col, seg_row = tables
        blocks = at.tile // rows
        row_spec = pl.BlockSpec((blocks, 1, rows), lambda i, control: (i * control[2], 0, 0))
        return at.call(
            tiled(functools.partial(heads_body, rows)),
            "heads",
            [
                (normed_all, at.source(width)),
                (keyed_all, at.source(LAT + ROPE)),
                (cosine, at.source(HALF)),
                (sine, at.source(HALF)),
                (seg_col, at.source(1)),
                (seg_row, row_spec),
            ],
            [(query_weight,), (expand_weight,)],
            [at.result(heads * VD), at.result(heads * QK), at.result(heads * KV)],
            into,
            [pltpu.VMEM((at.tile, heads * QK), jnp.float32)],
            flops=4 * all_rows * width * heads * QK,
        )

    def run_shared(section, ffn_all, into):
        at = tiles[section]
        return at.call(
            tiled(shared_body),
            "shared",
            [(ffn_all, at.source(width))],
            [(shared_in_t,)],
            [at.pair_result(half), at.result(half)],
            into,
            flops=4 * all_rows * width * half,
        )

    fresh = boundary[0, 0].astype(jnp.float32)

    normed, keyed, _ = inputs_of(fresh)
    normed_pack, keyed_pack, layout_all = gather_blocks(
        [normed, keyed, layout], True, 0, 0, wide=[False, False, True]
    )
    attended, _ = attend(
        dot(normed_pack, query_weight),
        bf16(dot(keyed_pack[:, :LAT], expand_weight)),
        keyed_pack,
        tables_pack,
    )
    mixed_first = fresh + scatter_blocks(bf16(dot(attended, output_weight)), rows, False, 1, 0)
    empty = [
        blank((all_rows, width), jnp.bfloat16),
        *(
            blank(shape, dtype)
            for shape, dtype in (
                ((all_rows + tiles[0].tile, 2 * units), jnp.bfloat16),
                ((all_rows + tiles[0].tile, units), jnp.bfloat16),
                ((all_rows + tiles[0].tile, experts_count), jnp.float32),
                ((2, all_rows + tiles[0].tile, half), jnp.bfloat16),
                ((all_rows + tiles[0].tile, half), jnp.bfloat16),
            )
        ),
    ]
    ffn_all, (*stored, partial) = run_experts(
        0, bf16(rms_forward(mixed_first, ffn_gain)[0]), routed_of(layout_all), empty[0], empty[1:], 2, True
    )
    result_first = mixed_first + scatter_blocks(partial, rows, True, 3, 0)
    heads_weights = spread_blocks([query_weight, expand_weight, output_weight], 4, 1)
    target_all, layout_all = gather_blocks(
        [boundary[0, 0], layout], True, 5, 1, [blank((all_rows, width), jnp.bfloat16), layout_all]
    )
    sent, target_all, layout_all, heads_weights = lax.optimization_barrier(
        (bf16(result_first), target_all, layout_all, heads_weights)
    )
    inbound = lax.ppermute(sent, SECTION, [(0, 1)])
    routed = routed_of(layout_all)
    tables_all = tables_of(layout_all.reshape(count, -1, rows)[:, top, : lengths.shape[3]])

    normed, keyed, ffn_all, _ = lax.optimization_barrier((normed, keyed, ffn_all, sent))
    all_inputs = gather_blocks([normed, keyed], True, 8, 0)
    prepared = run_heads(0, *all_inputs, tables_all, ())
    stored[3:] = run_shared(0, ffn_all, stored[3:])
    inbound, prepared, all_inputs, stored = lax.optimization_barrier((inbound, prepared, all_inputs, stored))
    query_heads, expand_heads, output_heads = (
        value.reshape(members, -1, value.shape[1]) for value in heads_weights
    )

    hidden = jnp.where(is_first, fresh, inbound.astype(jnp.float32))
    normed, keyed, (compressed, scale_attn, scale_latent) = inputs_of(hidden)
    latent = bf16(jnp.einsum("rd,mdc->mrc", keyed[:, :LAT], expand_heads, preferred_element_type=jnp.float32))
    latent = latent.reshape(members * rows, -1)
    query_raw = jnp.einsum("rd,mdc->mrc", normed, query_heads, preferred_element_type=jnp.float32)
    attended, query = attend(query_raw.reshape(members * rows, -1), latent, keyed, tables_own, members)
    mixed = hidden + jnp.einsum(
        "mrc,mcd->rd", attended.reshape(members, rows, -1), output_heads, preferred_element_type=jnp.float32
    )
    mixed = jnp.where(is_first, mixed_first, mixed)
    ffn32, scale_ffn = rms_forward(mixed, ffn_gain)
    ffn_all, stored = run_experts(1, bf16(ffn32), routed, ffn_all, stored, 6, False)

    def latent_back(own):
        grad_latent, grad_latent_gain = rms_backward(
            compressed[:, :LAT], scale_latent, latent_gain, own[:, width : width + LAT]
        )
        grad_compressed = bf16(
            jnp.concatenate([grad_latent, rotate(own[:, width + LAT :], own_cos, -own_sin)], axis=1)
        )
        grad_normed = own[:, :width] + dot_t(grad_compressed, compress_weight)
        grad_hidden_norm, grad_attn_gain = rms_backward(hidden, scale_attn, attn_gain, grad_normed)
        return grad_compressed, grad_hidden_norm, grad_attn_gain, grad_latent_gain

    grad_ffn_second, grad_units = run_experts_back(1, 7, target_all, routed, stored, ())
    grad_mixed = fresh + rms_backward(mixed, scale_ffn, ffn_gain, grad_ffn_second)[0]
    grad_attended = jnp.einsum(
        "rd,mcd->mrc", bf16(grad_mixed), output_heads, preferred_element_type=jnp.float32
    )
    grad_query, grad_latent_heads, grad_shared_key = attend_back(
        query, latent, keyed, bf16(grad_attended).reshape(members * rows, -1), tables_own, members
    )
    own_second = jnp.concatenate(
        [
            jnp.einsum(
                "mrc,mdc->rd",
                grad_query.reshape(members, rows, -1),
                query_heads,
                preferred_element_type=jnp.float32,
            ),
            jnp.einsum(
                "mrc,mdc->rd",
                grad_latent_heads.reshape(members, rows, -1),
                expand_heads,
                preferred_element_type=jnp.float32,
            ),
            jnp.sum(grad_shared_key.reshape(members, rows, -1), axis=0),
        ],
        axis=1,
    )
    grad_second = bf16(grad_mixed + latent_back(own_second)[1])

    downbound = lax.ppermute(grad_second, SECTION, [(1, 0)]).astype(jnp.float32)

    normed_late, keyed_late, gated_late, _ = lax.optimization_barrier((normed, keyed, stored[1], grad_second))
    finished, _ = summed_over(
        1,
        10,
        finish_body,
        "finish",
        [(gated_late, False), (stored[3], True)],
        [(expert_out,), (shared_out,)],
        [],
        (),
    )
    result = mixed + finished
    upstream = jnp.where(is_first, downbound, fresh)
    (upstream_all,) = gather_blocks([bf16(upstream)], True, 11, 0, [target_all])
    grad_ffn, (grad_pre, moved) = run_experts_back(0, 12, upstream_all, routed, stored, grad_units)
    grad_ffn = jnp.where(is_first, grad_ffn, grad_ffn_second)
    normed_late, keyed_late, _ = lax.optimization_barrier((normed_late, keyed_late, finished))
    normed_all, keyed_all = gather_blocks([normed_late, keyed_late], True, 9, 1, all_inputs)
    attended_all, query_all, latent_all = run_heads(1, normed_all, keyed_all, tables_all, prepared)
    shared_pre, shared_hid = stored[3:]
    attended_all, shared_hid = attended_all[:all_rows], shared_hid[:all_rows]
    grad_mixed_norm, grad_ffn_gain = rms_backward(mixed, scale_ffn, ffn_gain, grad_ffn)
    grad_mixed = upstream + grad_mixed_norm
    grad_mixed_all = lax.all_gather(bf16(grad_mixed), BOTH, axis=0, tiled=True)
    grad_attended = bf16(dot_t(grad_mixed_all, output_weight))
    grad_query, grad_latent_heads, grad_shared_key = attend_back(
        query_all, latent_all, keyed_all, grad_attended, tables_all
    )
    own = lax.psum_scatter(
        bf16(
            jnp.concatenate(
                [
                    dot_t(own_pack(grad_query), query_weight),
                    dot_t(own_pack(grad_latent_heads), expand_weight),
                    own_pack(grad_shared_key),
                ],
                axis=1,
            )
        ),
        MEMBERS,
        scatter_dimension=0,
        tiled=True,
    ).astype(jnp.float32)
    grad_compressed, grad_hidden_norm, grad_attn_gain, grad_latent_gain = latent_back(own)
    grad_hidden = grad_mixed + grad_hidden_norm

    gains = jnp.concatenate([grad_attn_gain, grad_latent_gain, grad_ffn_gain])
    rounded = lax.reduce_precision(gains, 8, 7)
    small = jnp.concatenate([bf16(rounded), bf16(gains - rounded), bf16(moved[:all_rows, 0])])
    small = jnp.pad(small, (0, -small.shape[0] % rows)).reshape(rows, -1)
    last = lax.all_gather(jnp.concatenate([grad_compressed, small], axis=1), BOTH, axis=0, tiled=True)
    grad_compressed_all = last[:, : LAT + ROPE]
    small_all = last[:, LAT + ROPE :].reshape(count, -1).astype(jnp.float32)
    many = 2 * width + LAT
    gains = jnp.sum(small_all[:, :many] + small_all[:, many : 2 * many], axis=0)
    moved_all = small_all[:, 2 * many : 2 * many + all_rows].T
    prob = stored[2][:all_rows]
    grad_logits = bf16(moved_all - prob * jnp.sum(moved_all, axis=1, keepdims=True))
    left, right = gated_back(
        shared_pre[0, :all_rows].astype(jnp.float32),
        shared_pre[1, :all_rows].astype(jnp.float32),
        dot_t(upstream_all, shared_out),
    )
    grad_shared_in = lax.dot_general(
        jnp.stack([left, right]), ffn_all, (((1,), (0,)), ((), ())), preferred_element_type=jnp.float32
    )
    ends = jnp.where(is_first, grad_hidden, result)
    return (
        ends[None, None],
        gains[:width][None],
        t_dot(normed_all, grad_query)[None],
        t_dot(normed_all, grad_compressed_all)[None],
        gains[width : width + LAT][None],
        t_dot(keyed_all[:, :LAT], grad_latent_heads)[None],
        t_dot(attended_all, grad_mixed_all)[None],
        gains[width + LAT :][None],
        t_dot(ffn_all, grad_logits)[None],
        jnp.transpose(grad_shared_in, (2, 0, 1))[None],
        t_dot(shared_hid, upstream_all)[None],
        pair_grad(ffn_all, grad_pre)[None, None],
        t_dot(stored[1][:all_rows], upstream_all)[None, None],
    )


def solution(mesh):
    return jax.shard_map(
        body,
        mesh=mesh,
        in_specs=(
            P(SECTION, None, BOTH, None),
            P(None, PACKS, None, None),
            P(SECTION, None, BOTH, None),
            P(SECTION, None),
            P(SECTION, None, MEMBERS),
            P(SECTION, None, None),
            P(SECTION, None),
            P(SECTION, None, MEMBERS),
            P(SECTION, MEMBERS, None),
            P(SECTION, None),
            P(SECTION, None, None),
            P(SECTION, None, None, MEMBERS),
            P(SECTION, MEMBERS, None),
            P(SECTION, BOTH, None, None, None),
            P(SECTION, BOTH, None, None),
        ),
        out_specs=(
            P(SECTION, None, BOTH, None),
            P(SECTION, None),
            P(SECTION, None, MEMBERS),
            P(SECTION, None, None),
            P(SECTION, None),
            P(SECTION, None, MEMBERS),
            P(SECTION, MEMBERS, None),
            P(SECTION, None),
            P(SECTION, None, None),
            P(SECTION, None, None, MEMBERS),
            P(SECTION, MEMBERS, None),
            P(SECTION, BOTH, None, None, None),
            P(SECTION, BOTH, None, None),
        ),
        check_vma=False,
    )
```

```python
import functools

import jax
import jax.numpy as jnp
from jax import lax
from jax.experimental import pallas as pl
from jax.experimental.pallas import tpu as pltpu
from jax.sharding import PartitionSpec as P

NOPE = 128
ROPE = 64
VD = 128
LAT = 512

QK = NOPE + ROPE
KV = NOPE + VD
HALF = ROPE // 2
epsilon = 1e-06
rope_base = 10000.0
masked_score = -1e30
SECTION, PACKS, MEMBERS = "section", "dp", "expert"
BOTH = (PACKS, MEMBERS)
MESH = pl.DeviceIdType.MESH
def dot(left, right):
    return jnp.dot(left, right, preferred_element_type=jnp.float32)


def dot_t(left, right):
    return lax.dot_general(
        left, right, (((1,), (1,)), ((), ())), preferred_element_type=jnp.float32
    )


def t_dot(left, right):
    return lax.dot_general(
        left, right, (((0,), (0,)), ((), ())), preferred_element_type=jnp.float32
    )


def bf16(value):
    return value.astype(jnp.bfloat16)


def rms_forward(inputs, gain_vec):
    norm_scale = lax.rsqrt(jnp.mean(inputs * inputs, axis=-1, keepdims=True) + epsilon)
    return (inputs * norm_scale * gain_vec, norm_scale)


def rms_backward(inputs, norm_scale, gain_vec, upstream):
    weighted = upstream * gain_vec
    grad_gain = jnp.sum(upstream * inputs * norm_scale, axis=0)
    cubed = norm_scale * norm_scale * norm_scale
    grad_inputs = norm_scale * weighted - inputs * cubed * jnp.mean(
        weighted * inputs, axis=-1, keepdims=True
    )
    return (grad_inputs, grad_gain)


def rotate(inputs, cosine, sine):
    half = cosine.shape[-1]
    former = inputs[..., :half]
    latter = inputs[..., half:]
    return jnp.concatenate(
        [former * cosine - latter * sine, latter * cosine + former * sine], axis=-1
    )


def silu_parts(pre_gate):
    sigmoid = jax.nn.sigmoid(pre_gate)
    return (pre_gate * sigmoid, sigmoid * (1.0 + pre_gate * (1.0 - sigmoid)))


def block_layout(block_lengths, rows):
    index = lax.broadcasted_iota(jnp.int32, (block_lengths.shape[0], rows), 1)
    start, segment, opening = 0, 0, 0
    for sequence in range(block_lengths.shape[1]):
        begun = index >= start
        segment = segment + begun.astype(jnp.int32)
        opening = jnp.where(begun, start, opening)
        start = start + block_lengths[:, sequence : sequence + 1]
    return segment, index - opening


def places(spots):
    member = lax.axis_index(MEMBERS)
    spot = lax.axis_index(PACKS) if spots > 1 else 0
    return spot, member // 2, lax.rem(member, 2)


def to_partner(chip, core):
    return {MEMBERS: chip * 2 + 1 - core}


def to_other(chip, core):
    return {MEMBERS: (1 - chip) * 2 + core}


def when(condition, action):
    if condition is True:
        action()
    else:
        pl.when(condition)(action)


def greet(spots, spot, chip, core):
    barrier = pltpu.get_barrier_semaphore()

    def signal(target):
        pl.semaphore_signal(barrier, inc=1, device_id=target, device_id_type=MESH)

    signal(to_partner(chip, core))
    signal(to_other(chip, core))
    if spots > 1:
        pl.when(spot > 0)(lambda: signal({PACKS: spot - 1}))
        pl.when(spot < spots - 1)(lambda: signal({PACKS: spot + 1}))
        ends = jnp.where(spot > 0, 1, 0) + jnp.where(spot < spots - 1, 1, 0)
        pl.semaphore_wait(barrier, 2 + ends)
    else:
        pl.semaphore_wait(barrier, 2)


def remote(source, target_ref, target, out_sem, in_sem):
    return pltpu.make_async_remote_copy(
        src_ref=source,
        dst_ref=target_ref,
        send_sem=out_sem,
        recv_sem=in_sem,
        device_id=target,
        device_id_type=MESH,
    )


def slot(spot, chip, core):
    return spot * 4 + chip * 2 + core


def gather_kernel(spots, cuts, wide, active, *refs):
    arrays = len(cuts)
    x_refs, o_refs, sems = refs[:arrays], refs[-9 - arrays : -9], refs[-9:]
    own_sem, up_out, up_in, down_out, down_in, over_out, over_in, pair_out, pair_in = sems
    units = [
        (a, pl.ds(part * (x_refs[a].shape[0] // parts), x_refs[a].shape[0] // parts))
        for a, parts in enumerate(cuts)
        for part in range(parts)
    ]

    def run():
        spot, chip, core = places(spots)
        greet(spots, spot, chip, core)

        def piece(unit, index):
            array, cut = units[unit]
            return o_refs[array].at[index, cut]

        def first(unit):
            array, cut = units[unit]
            return x_refs[array].at[cut]

        def lane(unit):
            return wide[units[unit][0]]

        def spread(unit):
            return range(spots) if lane(unit) else [0]

        def up(source, at, unit, reach):
            return remote(
                source, piece(unit, slot(at, chip, core)), {PACKS: spot + 1}, up_out.at[reach, unit], up_in.at[reach, unit]
            )

        def down(source, at, unit, reach):
            return remote(
                source,
                piece(unit, slot(at, chip, core)),
                {PACKS: spot - 1},
                down_out.at[reach, unit],
                down_in.at[reach, unit],
            )

        def over(source, at, unit):
            return remote(
                source, piece(unit, slot(at, chip, core)), to_other(chip, core), over_out.at[at, unit], over_in.at[at, unit]
            )

        def pair(source, at, c, unit):
            return remote(
                source,
                piece(unit, slot(at, c, core)),
                to_partner(chip, core),
                pair_out.at[c, at, unit],
                pair_in.at[c, at, unit],
            )

        home = lambda unit: spot if lane(unit) else 0
        for unit in range(len(units)):
            source = first(unit)
            over(source, home(unit), unit).start()
            if spots > 1 and lane(unit):
                pl.when(spot < spots - 1)(lambda: up(source, spot, unit, 0).start())
                pl.when(spot > 0)(lambda: down(source, spot, unit, 0).start())
            pair(source, home(unit), chip, unit).start()
        own = [
            pltpu.make_async_copy(
                x_refs[a], o_refs[a].at[slot(spot if wide[a] else 0, chip, core)], own_sem.at[a]
            )
            for a in range(arrays)
        ]
        for copy in own:
            copy.start()
        for reach in range(1, spots):
            for unit in range(len(units)):
                if not lane(unit):
                    continue

                def below(reach=reach, unit=unit):
                    at = spot - reach
                    source = piece(unit, slot(at, chip, core))
                    up(source, at, unit, reach - 1).wait_recv()
                    pl.when(spot < spots - 1)(lambda: up(source, at, unit, reach).start())
                    over(source, at, unit).start()
                    pair(source, at, chip, unit).start()

                def above(reach=reach, unit=unit):
                    at = spot + reach
                    source = piece(unit, slot(at, chip, core))
                    down(source, at, unit, reach - 1).wait_recv()
                    pl.when(spot > 0)(lambda: down(source, at, unit, reach).start())
                    over(source, at, unit).start()
                    pair(source, at, chip, unit).start()

                pl.when(spot >= reach)(below)
                pl.when(spot + reach < spots)(above)
        for reach in range(spots):
            sides = [(True, spot)]
            if reach > 0:
                sides = [(spot >= reach, spot - reach), (spot + reach < spots, spot + reach)]
            for unit in range(len(units)):
                if not lane(unit) and reach > 0:
                    continue
                for there, at in sides:
                    at = at if lane(unit) else 0

                    def hand_on(at=at, unit=unit):
                        source = piece(unit, slot(at, 1 - chip, core))
                        over(source, at, unit).wait_recv()
                        pair(source, at, 1 - chip, unit).start()

                    when(there, hand_on)
        for copy in own:
            copy.wait()
        for unit in range(len(units)):
            source = first(unit)
            for at in spread(unit):
                over(source, at, unit).wait_send()
                for c in range(2):
                    pair(source, at, c, unit).wait()
            for reach in range(spots - 1 if lane(unit) else 0):
                pl.when((spot >= reach) & (spot < spots - 1))(lambda: up(source, spot, unit, reach).wait_send())
                pl.when((spot + reach < spots) & (spot > 0))(lambda: down(source, spot, unit, reach).wait_send())

    if active is None:
        run()
    else:
        pl.when(lax.axis_index(SECTION) == active)(run)


def gather_blocks(values, across, number, active=None, into=None, parts=4, wide=None):
    wide = [across] * len(values) if wide is None else wide
    if lax.axis_size(MEMBERS) != 4:
        found = [
            lax.all_gather(value, BOTH if far else MEMBERS, axis=0, tiled=True) for value, far in zip(values, wide)
        ]
        if into is None:
            return found
        chosen = lax.axis_index(SECTION) == active
        return [jnp.where(chosen, new, old) for new, old in zip(found, into)]
    spots = lax.axis_size(PACKS) if across else 1
    cuts = [parts if value.shape[0] % (16 * parts) == 0 else 1 for value in values]
    units = sum(cuts)
    dma = pltpu.SemaphoreType.DMA
    hops = max(spots - 1, 1)
    shapes = [
        jax.ShapeDtypeStruct(((spots if far else 1) * 4, *value.shape), value.dtype)
        for value, far in zip(values, wide)
    ]
    held = [] if into is None else [old.reshape(shape.shape) for old, shape in zip(into, shapes)]
    outs = pl.pallas_call(
        functools.partial(gather_kernel, spots, cuts, wide, active),
        out_shape=shapes,
        in_specs=[pl.BlockSpec(memory_space=pltpu.VMEM)] * len(values)
        + [pl.BlockSpec(memory_space=pl.ANY)] * len(held),
        out_specs=[pl.BlockSpec(memory_space=pl.ANY)] * len(values),
        input_output_aliases={len(values) + index: index for index in range(len(held))},
        scratch_shapes=[
            dma((len(values),)),
            dma((hops, units)),
            dma((hops, units)),
            dma((hops, units)),
            dma((hops, units)),
            dma((spots, units)),
            dma((spots, units)),
            dma((2, spots, units)),
            dma((2, spots, units)),
        ],
        compiler_params=pltpu.CompilerParams(collective_id=number, has_side_effects=True),
        name=f"gather{number}",
    )(*values, *held)
    return [out.reshape(-1, out.shape[2]) for out in outs]


def spread_kernel(cuts, active, *refs):
    arrays = len(cuts)
    sources, o_refs, x_refs = refs[:arrays], refs[arrays : 2 * arrays], refs[2 * arrays : 3 * arrays]
    own_sem, over_out, over_in, side_out, side_in, pair_out, pair_in = refs[3 * arrays :]
    units = [
        (a, pl.ds(part * (x_refs[a].shape[0] // parts), x_refs[a].shape[0] // parts))
        for a, parts in enumerate(cuts)
        for part in range(parts)
    ]

    def run():
        taken_in = [pltpu.make_async_copy(sources[a], x_refs[a], own_sem.at[a]) for a in range(arrays)]
        for copy in taken_in:
            copy.start()
        for copy in taken_in:
            copy.wait()
        member, spot = lax.axis_index(MEMBERS), lax.axis_index(PACKS)
        chip, core, odd = member // 2, lax.rem(member, 2), lax.rem(spot, 2)
        beside = {PACKS: spot + 1 - 2 * odd}
        barrier = pltpu.get_barrier_semaphore()
        for target in (to_partner(chip, core), to_other(chip, core), beside):
            pl.semaphore_signal(barrier, inc=1, device_id=target, device_id_type=MESH)
        pl.semaphore_wait(barrier, 3)

        def piece(unit, c):
            array, cut = units[unit]
            return o_refs[array].at[c * 2 + core, cut]

        def first(unit):
            array, cut = units[unit]
            return x_refs[array].at[cut]

        def over(unit):
            return remote(first(unit), piece(unit, chip), to_other(chip, core), over_out.at[unit], over_in.at[unit])

        def side(unit):
            source = piece(unit, 1 - chip)
            return remote(source, source, beside, side_out.at[unit], side_in.at[unit])

        def pair(source, unit, c, index):
            return remote(
                source, piece(unit, c), to_partner(chip, core), pair_out.at[index, unit], pair_in.at[index, unit]
            )

        for unit in range(len(units)):
            pl.when(odd == unit % 2)(lambda: over(unit).start())
        for unit in range(len(units)):
            pair(first(unit), unit, chip, 0).start()
        own = [
            pltpu.make_async_copy(x_refs[a], o_refs[a].at[member], own_sem.at[a]) for a in range(arrays)
        ]
        for copy in own:
            copy.start()
        for unit in range(len(units)):

            def taken(unit=unit):
                over(unit).wait_recv()
                side(unit).start()
                pair(piece(unit, 1 - chip), unit, 1 - chip, 1).start()

            pl.when(odd == unit % 2)(taken)
        for unit in range(len(units)):

            def handed(unit=unit):
                side(unit).wait_recv()
                pair(piece(unit, 1 - chip), unit, 1 - chip, 1).start()

            pl.when(odd != unit % 2)(handed)
        for copy in own:
            copy.wait()
        for unit in range(len(units)):

            def sent(unit=unit):
                over(unit).wait_send()
                side(unit).wait_send()

            pl.when(odd == unit % 2)(sent)
            pair(first(unit), unit, chip, 0).wait()
            pair(first(unit), unit, 1 - chip, 1).wait()

    pl.when(lax.axis_index(SECTION) == active)(run)


def spread_blocks(values, number, active, parts=8):
    if lax.axis_size(MEMBERS) != 4 or lax.axis_size(PACKS) % 2:
        return gather_blocks(values, False, number, active)
    units = parts * len(values)
    dma = pltpu.SemaphoreType.DMA
    outs = pl.pallas_call(
        functools.partial(spread_kernel, [parts] * len(values), active),
        out_shape=[jax.ShapeDtypeStruct((4, *value.shape), value.dtype) for value in values],
        in_specs=[pl.BlockSpec(memory_space=pl.ANY)] * len(values),
        out_specs=[pl.BlockSpec(memory_space=pl.ANY)] * len(values),
        scratch_shapes=[
            *(pltpu.VMEM(value.shape, value.dtype) for value in values),
            dma((len(values),)),
            dma((units,)),
            dma((units,)),
            dma((units,)),
            dma((units,)),
            dma((2, units)),
            dma((2, units)),
        ],
        compiler_params=pltpu.CompilerParams(collective_id=number, has_side_effects=True),
        name=f"spread{number}",
    )(*values)
    return [out.reshape(-1, out.shape[2]) for out in outs]


def add_into(target, sources, rows, step=16):
    def some(index, carry):
        at = pl.ds(pl.multiple_of(index * step, step), step)
        total = sources[0][at, :].astype(jnp.float32)
        for source in sources[1:]:
            total = total + source[at, :].astype(jnp.float32)
        target[at, :] = total.astype(target.dtype)
        return carry

    lax.fori_loop(0, rows // step, some, 0)


def scatter_kernel(
    spots,
    parts,
    active,
    x_ref,
    o_ref,
    own_buf,
    pair_buf,
    over_src,
    over_buf,
    line_src,
    up_buf,
    down_buf,
    own_in,
    pair_out,
    pair_in,
    over_out,
    over_in,
    line_out,
    up_in,
    down_in,
):
    rows = x_ref.shape[1] // parts
    cut = lambda part: pl.ds(part * rows, rows)

    def run():
        spot, chip, core = places(spots)
        greet(spots, spot, chip, core)

        def order(step):
            if step == spots - 1:
                return spot
            fall = spots - 1 - step
            fall = jnp.where(fall <= spot, fall - 1, fall)
            rise = jnp.where(step >= spot, step + 1, step)
            return jnp.where(2 * spot < spots - 1, fall, rise)

        def pair(at, c, part):
            return remote(
                x_ref.at[slot(at, c, 1 - core), cut(part)],
                pair_buf.at[at, c, cut(part)],
                to_partner(chip, core),
                pair_out.at[at, c, part],
                pair_in.at[at, c, part],
            )

        def over(at, part):
            return remote(
                over_src.at[at, cut(part)],
                over_buf.at[at, cut(part)],
                to_other(chip, core),
                over_out.at[at, part],
                over_in.at[at, part],
            )

        def up(at, part):
            return remote(
                line_src.at[at, cut(part)],
                up_buf.at[at, cut(part)],
                {PACKS: spot + 1},
                line_out.at[at, part],
                up_in.at[at, part],
            )

        def down(at, part):
            return remote(
                line_src.at[at, cut(part)],
                down_buf.at[at, cut(part)],
                {PACKS: spot - 1},
                line_out.at[at, part],
                down_in.at[at, part],
            )

        def own(at, c):
            return pltpu.make_async_copy(x_ref.at[slot(at, c, core)], own_buf.at[at, c], own_in.at[at, c])

        for c in (1 - chip, chip):
            for step in range(spots):
                own(order(step), c).start()
                for part in range(parts):
                    pair(order(step), c, part).start()
        for step in range(spots):
            at = order(step)
            own(at, 1 - chip).wait()
            for part in range(parts):
                pair(at, 1 - chip, part).wait_recv()
                add_into(
                    over_src.at[at, cut(part)],
                    [own_buf.at[at, 1 - chip, cut(part)], pair_buf.at[at, 1 - chip, cut(part)]],
                    rows,
                )
                over(at, part).start()
        for step in range(spots):
            at = order(step)
            own(at, chip).wait()
            for part in range(parts):
                pair(at, chip, part).wait_recv()
                over(at, part).wait_recv()
                base = [
                    own_buf.at[at, chip, cut(part)],
                    pair_buf.at[at, chip, cut(part)],
                    over_buf.at[at, cut(part)],
                ]
                ups, downs = up_buf.at[at, cut(part)], down_buf.at[at, cut(part)]
                if step < spots - 1:
                    target = line_src.at[at, cut(part)]

                    def rising(first):
                        if not first:
                            up(at, part).wait_recv()
                        add_into(target, base if first else base + [ups], rows)
                        up(at, part).start()

                    def falling(first):
                        if not first:
                            down(at, part).wait_recv()
                        add_into(target, base if first else base + [downs], rows)
                        down(at, part).start()

                    pl.when((at > spot) & (spot == 0))(lambda: rising(True))
                    pl.when((at > spot) & (spot > 0))(lambda: rising(False))
                    pl.when((at < spot) & (spot == spots - 1))(lambda: falling(True))
                    pl.when((at < spot) & (spot < spots - 1))(lambda: falling(False))
                elif spots == 1:
                    add_into(o_ref.at[cut(part)], base, rows)
                else:

                    def finish(ends):
                        if ends < 1:
                            up(at, part).wait_recv()
                        if ends > -1:
                            down(at, part).wait_recv()
                        extra = ([ups] if ends < 1 else []) + ([downs] if ends > -1 else [])
                        add_into(o_ref.at[cut(part)], base + extra, rows)

                    pl.when(spot == 0)(lambda: finish(1))
                    pl.when(spot == spots - 1)(lambda: finish(-1))
                    pl.when((spot > 0) & (spot < spots - 1))(lambda: finish(0))
        for part in range(parts):
            for step in range(spots):
                at = order(step)
                pair(at, 0, part).wait_send()
                pair(at, 1, part).wait_send()
                over(at, part).wait_send()
                if step < spots - 1:
                    up(at, part).wait_send()

    if active is None:
        run()
    else:
        pl.when(lax.axis_index(SECTION) == active)(run)


def scatter_blocks(partial, rows, across, number, active=None, parts=4):
    if lax.axis_size(MEMBERS) != 4:
        axes = BOTH if across else MEMBERS
        taken = partial[: rows * lax.axis_size(axes)]
        return lax.psum_scatter(taken, axes, scatter_dimension=0, tiled=True).astype(jnp.float32)
    spots = lax.axis_size(PACKS) if across else 1
    width = partial.shape[1]
    dma = pltpu.SemaphoreType.DMA
    hold = lambda *lead: pltpu.VMEM((*lead, rows, width), partial.dtype)
    return pl.pallas_call(
        functools.partial(scatter_kernel, spots, parts, active),
        out_shape=jax.ShapeDtypeStruct((rows, width), jnp.float32),
        in_specs=[pl.BlockSpec(memory_space=pl.ANY)],
        out_specs=pl.BlockSpec(memory_space=pltpu.VMEM),
        scratch_shapes=[
            hold(spots, 2),
            hold(spots, 2),
            hold(spots),
            hold(spots),
            hold(spots),
            hold(spots),
            hold(spots),
            dma((spots, 2)),
            dma((spots, 2, parts)),
            dma((spots, 2, parts)),
            dma((spots, parts)),
            dma((spots, parts)),
            dma((spots, parts)),
            dma((spots, parts)),
            dma((spots, parts)),
        ],
        compiler_params=pltpu.CompilerParams(collective_id=number, has_side_effects=True),
        name=f"scatter{number}",
    )(partial.reshape(-1, rows, width))


def allowed_pairs(seg_col, seg_row):
    rows = seg_col.shape[0]
    later = lax.broadcasted_iota(jnp.int32, (rows, rows), 0)
    earlier = lax.broadcasted_iota(jnp.int32, (rows, rows), 1)
    return (seg_col == seg_row) & (earlier <= later)


def attend_kernel(heads, q_ref, lat_ref, key_ref, cos_ref, sin_ref, col_ref, row_ref, out_ref, rot_ref):
    factor = QK**-0.5
    allowed = allowed_pairs(col_ref[...], row_ref[0])
    cosine, sine = cos_ref[...], sin_ref[...]
    shared = key_ref[:, LAT:]
    for head in range(heads):
        raw = q_ref[:, head * QK : (head + 1) * QK]
        query = bf16(
            jnp.concatenate([raw[:, :NOPE], rotate(raw[:, NOPE:], cosine, sine)], axis=1)
        )
        rot_ref[:, head * QK : (head + 1) * QK] = query
        key = jnp.concatenate([lat_ref[:, head * KV : head * KV + NOPE], shared], axis=1)
        value = lat_ref[:, head * KV + NOPE : (head + 1) * KV]
        scores = jnp.where(allowed, dot_t(query, key) * factor, masked_score)
        top = jnp.max(scores, axis=1, keepdims=True)
        powers = jnp.exp(scores - top)
        probs = powers * (1.0 / jnp.sum(powers, axis=1, keepdims=True))
        out_ref[:, head * VD : (head + 1) * VD] = bf16(dot(bf16(probs), value))


def attend(query_raw, latent, keyed, tables, groups=1):
    cosine, sine, seg_col, seg_row = tables
    count, _, rows = seg_row.shape
    heads = query_raw.shape[1] // QK
    block = lambda width: pl.BlockSpec((rows, width), lambda i: (i, 0))
    same = lambda width: pl.BlockSpec((rows, width), lambda i: (0, 0) if groups > 1 else (i, 0))
    count = count * groups
    return pl.pallas_call(
        functools.partial(attend_kernel, heads),
        grid=(count,),
        in_specs=[
            block(heads * QK),
            block(heads * KV),
            same(LAT + ROPE),
            same(HALF),
            same(HALF),
            same(1),
            pl.BlockSpec((1, 1, rows), lambda i: (0, 0, 0) if groups > 1 else (i, 0, 0)),
        ],
        out_specs=[block(heads * VD), block(heads * QK)],
        out_shape=[
            jax.ShapeDtypeStruct((count * rows, heads * VD), jnp.bfloat16),
            jax.ShapeDtypeStruct((count * rows, heads * QK), jnp.bfloat16),
        ],
        name="attend",
        cost_estimate=pl.CostEstimate(
            flops=2 * count * heads * rows * rows * (QK + VD),
            bytes_accessed=count * rows * heads * (QK * 6 + KV * 2 + VD * 2),
            transcendentals=count * heads * rows * rows,
        ),
    )(query_raw, latent, keyed, cosine, sine, seg_col, seg_row)


def attend_back_kernel(
    heads, q_ref, lat_ref, key_ref, grad_ref, cos_ref, sin_ref, col_ref, row_ref, dq_ref, dlat_ref, dkey_ref
):
    factor = QK**-0.5
    allowed = allowed_pairs(col_ref[...], row_ref[0])
    cosine, sine = cos_ref[...], sin_ref[...]
    shared = key_ref[:, LAT:]
    total = None
    for head in range(heads):
        query = q_ref[:, head * QK : (head + 1) * QK]
        key = jnp.concatenate([lat_ref[:, head * KV : head * KV + NOPE], shared], axis=1)
        value = lat_ref[:, head * KV + NOPE : (head + 1) * KV]
        grad = grad_ref[:, head * VD : (head + 1) * VD]
        scores = jnp.where(allowed, dot_t(query, key) * factor, masked_score)
        top = jnp.max(scores, axis=1, keepdims=True)
        powers = jnp.exp(scores - top)
        probs = powers * (1.0 / jnp.sum(powers, axis=1, keepdims=True))
        grad_value = t_dot(bf16(probs), grad)
        grad_probs = dot_t(grad, value)
        centre = jnp.sum(probs * grad_probs, axis=1, keepdims=True)
        grad_scores = bf16(probs * (grad_probs - centre) * factor)
        grad_query = dot(grad_scores, key)
        grad_key = t_dot(grad_scores, query)
        dq_ref[:, head * QK : (head + 1) * QK] = bf16(
            jnp.concatenate(
                [grad_query[:, :NOPE], rotate(grad_query[:, NOPE:], cosine, -sine)], axis=1
            )
        )
        dlat_ref[:, head * KV : head * KV + NOPE] = bf16(grad_key[:, :NOPE])
        dlat_ref[:, head * KV + NOPE : (head + 1) * KV] = bf16(grad_value)
        part = grad_key[:, NOPE:]
        total = part if total is None else total + part
    dkey_ref[...] = total


def attend_back(query, latent, keyed, grad, tables, groups=1):
    cosine, sine, seg_col, seg_row = tables
    count, _, rows = seg_row.shape
    heads = query.shape[1] // QK
    block = lambda width: pl.BlockSpec((rows, width), lambda i: (i, 0))
    same = lambda width: pl.BlockSpec((rows, width), lambda i: (0, 0) if groups > 1 else (i, 0))
    count = count * groups
    return pl.pallas_call(
        functools.partial(attend_back_kernel, heads),
        grid=(count,),
        in_specs=[
            block(heads * QK),
            block(heads * KV),
            same(LAT + ROPE),
            block(heads * VD),
            same(HALF),
            same(HALF),
            same(1),
            pl.BlockSpec((1, 1, rows), lambda i: (0, 0, 0) if groups > 1 else (i, 0, 0)),
        ],
        out_specs=[block(heads * QK), block(heads * KV), block(ROPE)],
        out_shape=[
            jax.ShapeDtypeStruct((count * rows, heads * QK), jnp.bfloat16),
            jax.ShapeDtypeStruct((count * rows, heads * KV), jnp.bfloat16),
            jax.ShapeDtypeStruct((count * rows, ROPE), jnp.float32),
        ],
        name="attend_back",
        cost_estimate=pl.CostEstimate(
            flops=2 * count * heads * rows * rows * (3 * QK + 2 * VD),
            bytes_accessed=count * rows * heads * (QK * 4 + KV * 4 + VD * 2),
            transcendentals=count * heads * rows * rows,
        ),
    )(query, latent, keyed, grad, cosine, sine, seg_col, seg_row)


def gated_hidden(gate, up):
    return silu_parts(gate)[0] * up


def gated_back(gate, up, grad_hidden):
    act, slope = silu_parts(gate)
    return bf16(grad_hidden * up * slope), bf16(grad_hidden * act)


def columns(pieces):
    start = 0
    for piece in pieces:
        yield start, piece.shape[1]
        start += piece.shape[1]


def hold_weight(pieces):
    return pltpu.VMEM((pieces[0].shape[0], sum(piece.shape[1] for piece in pieces)), pieces[0].dtype)


def loads_of(counts, sources, targets, sems):
    copies = []
    for pieces, target in zip(counts, targets):
        group, sources = sources[:pieces], sources[pieces:]
        for source, (start, size) in zip(group, columns(group)):
            place = target if pieces == 1 else target.at[:, pl.ds(start, size)]
            copies.append(pltpu.make_async_copy(source, place, sems.at[len(copies)]))
    return copies


def load(*args):
    copies = loads_of(*args)
    for copy in copies:
        copy.start()
    for copy in copies:
        copy.wait()


class Tiles:
    def __init__(self, rows, pack_rows, pack, active):
        self.rows, self.pack_rows = rows, pack_rows
        self.tile = min(256, pack_rows)
        self.count = rows // self.tile
        inner = pack_rows // self.tile
        runs = (lax.axis_index(SECTION) == active).astype(jnp.int32)
        self.control = jnp.stack([pack * inner, (pack + 1) * inner, runs]).astype(jnp.int32)

    def source(self, width):
        return pl.BlockSpec((self.tile, width), lambda i, control: (i * control[2], 0))

    def small(self, array):
        return pl.BlockSpec(array.shape, lambda i, control: (0,) * array.ndim)

    def pair_source(self, width):
        return pl.BlockSpec((2, self.tile, width), lambda i, control: (0, i * control[2], 0))

    def result(self, width, dtype=jnp.bfloat16):
        def index(i, control):
            return (jnp.where(control[2] == 1, i, self.count), 0)

        shape = jax.ShapeDtypeStruct((self.rows + self.tile, width), dtype)
        return shape, pl.BlockSpec((self.tile, width), index)

    def pair_result(self, width):
        def index(i, control):
            return (0, jnp.where(control[2] == 1, i, self.count), 0)

        shape = jax.ShapeDtypeStruct((2, self.rows + self.tile, width), jnp.bfloat16)
        return shape, pl.BlockSpec((2, self.tile, width), index)

    def call(self, kernel, name, sources, weights, results, into=(), scratch=(), flops=0):
        arrays, specs = zip(*sources)
        shapes, out_specs = zip(*results)
        anywhere = pl.BlockSpec(memory_space=pl.ANY)
        pieces = [piece for weight in weights for piece in weight]
        counts = [len(weight) for weight in weights]
        first = 1 + len(arrays) + len(pieces)
        return pl.pallas_call(
            functools.partial(kernel, len(arrays), counts, len(into), len(results)),
            grid_spec=pltpu.PrefetchScalarGridSpec(
                num_scalar_prefetch=1,
                grid=(self.count,),
                in_specs=[*specs, *([anywhere] * (len(pieces) + len(into)))],
                out_specs=list(out_specs),
                scratch_shapes=[
                    *[hold_weight(weight) for weight in weights],
                    pltpu.SemaphoreType.DMA((len(pieces),)),
                    *scratch,
                ],
            ),
            out_shape=list(shapes),
            input_output_aliases={first + index: index for index in range(len(into))},
            name=name,
            cost_estimate=pl.CostEstimate(flops=flops, bytes_accessed=self.rows * 16384, transcendentals=0),
        )(self.control, *arrays, *pieces, *into)


def tiled(body):
    def kernel(n_sources, counts, n_into, n_results, control, *refs):
        n_weights, n_pieces = len(counts), sum(counts)
        sources, refs = refs[:n_sources], refs[n_sources:]
        stored, refs = refs[:n_pieces], refs[n_pieces + n_into :]
        results, refs = refs[:n_results], refs[n_results:]
        weights, sems, scratch = refs[:n_weights], refs[n_weights], refs[n_weights + 1 :]

        def run():
            pl.when(pl.program_id(0) == 0)(lambda: load(counts, stored, weights, sems))
            body(inside_pack(control), [sources[0][...], *sources[1:]], weights, results, scratch)

        pl.when(control[2] == 1)(run)

    return kernel


def inside_pack(control):
    tile = pl.program_id(0)
    return (tile >= control[0]) & (tile < control[1])


def shared_units(x, shared_in):
    half = shared_in.shape[0] // 2
    return dot_t(x, shared_in[:half]), dot_t(x, shared_in[half:])


def experts_body(inside, sources, weights, results, scratch):
    x, own_ref, routed_ref = sources
    in_ref, shared_in_ref = weights[:2]
    pre_ref, gated_ref, prob_ref, shared_pre_ref, hid_ref = results[:5]
    units = gated_ref.shape[1]
    pre = dot(x, in_ref[...])
    logits = pre[:, 2 * units : 2 * units + own_ref.shape[1]]
    powers = jnp.exp(logits - jnp.max(logits, axis=1, keepdims=True))
    prob = powers / jnp.sum(powers, axis=1, keepdims=True)
    prob_ref[...] = prob
    gate = jnp.sum(prob * own_ref[...], axis=1, keepdims=True) * routed_ref[...]
    pre_ref[...] = bf16(pre[:, : 2 * units])
    gated = bf16(gate * gated_hidden(pre[:, :units], pre[:, units : 2 * units]))
    gated_ref[...] = gated

    def shared():
        left, right = shared_units(x, shared_in_ref)
        hidden = bf16(gated_hidden(left, right))
        shared_pre_ref[0] = bf16(left)
        shared_pre_ref[1] = bf16(right)
        hid_ref[...] = hidden
        return hidden

    if len(weights) == 2:
        shared()
        return
    out_ref, shared_out_ref = weights[2:]
    partial_ref = results[5]

    def with_shared():
        hidden = shared()
        partial_ref[...] = bf16(dot(gated, out_ref[...]) + dot(hidden, shared_out_ref[...]))

    def without():
        partial_ref[...] = bf16(dot(gated, out_ref[...]))

    pl.when(inside)(with_shared)
    pl.when(jnp.logical_not(inside))(without)


def finish_body(inside, sources, weights, results, scratch):
    gated, _, shared_pre_ref = sources
    out_ref, shared_out_ref = weights
    (partial_ref,) = results

    def with_shared():
        hidden = bf16(gated_hidden(shared_pre_ref[0].astype(jnp.float32), shared_pre_ref[1].astype(jnp.float32)))
        partial_ref[...] = bf16(dot(gated, out_ref[...]) + dot(hidden, shared_out_ref[...]))

    def without():
        partial_ref[...] = bf16(dot(gated, out_ref[...]))

    pl.when(inside)(with_shared)
    pl.when(jnp.logical_not(inside))(without)


def experts_back_body(inside, sources, weights, results, scratch):
    grad, own_ref, pre_ref, prob_ref, routed_ref, shared_pre_ref = sources
    in_ref, shared_in_ref, out_ref, shared_out_ref = weights
    grad_pre_ref, moved_ref, partial_ref = results
    (joined_ref,) = scratch
    units = out_ref.shape[0]
    prob = prob_ref[...]
    own_prob = jnp.sum(prob * own_ref[...], axis=1, keepdims=True) * routed_ref[...]
    gate, up = pre_ref[:, :units].astype(jnp.float32), pre_ref[:, units:].astype(jnp.float32)
    grad_units = dot_t(grad, out_ref[...])
    act, slope = silu_parts(gate)
    moved = own_prob * jnp.sum(grad_units * act * up, axis=1, keepdims=True)
    moved_ref[...] = moved
    scaled = own_prob * grad_units
    joined_ref[:, :units] = bf16(scaled * up * slope)
    joined_ref[:, units : 2 * units] = bf16(scaled * act)
    joined_ref[:, 2 * units :] = jnp.zeros_like(joined_ref[:, 2 * units :])
    joined_ref[:, 2 * units : 2 * units + own_ref.shape[1]] = bf16(moved * (own_ref[...] - prob))
    grad_pre_ref[...] = joined_ref[:, : 2 * units]
    base = dot_t(joined_ref[...], in_ref[...])
    half = shared_out_ref.shape[0]

    def with_shared():
        left, right = gated_back(
            shared_pre_ref[0].astype(jnp.float32),
            shared_pre_ref[1].astype(jnp.float32),
            dot_t(grad, shared_out_ref[...]),
        )
        partial_ref[...] = bf16(base + dot(left, shared_in_ref[:half]) + dot(right, shared_in_ref[half:]))

    def without():
        partial_ref[...] = bf16(base)

    pl.when(inside)(with_shared)
    pl.when(jnp.logical_not(inside))(without)


def shared_body(inside, sources, weights, results, scratch):
    pre_ref, hid_ref = results
    left, right = shared_units(sources[0], weights[0])
    pre_ref[0] = bf16(left)
    pre_ref[1] = bf16(right)
    hid_ref[...] = bf16(gated_hidden(left, right))


def heads_body(block, inside, sources, weights, results, scratch):
    x, key_ref, cos_ref, sin_ref, col_ref, row_ref = sources
    query_w_ref, expand_ref = weights
    out_ref, rot_ref, lat_ref = results
    (q_ref,) = scratch
    heads = q_ref.shape[1] // QK
    q_ref[...] = dot(x, query_w_ref[...])
    lat_ref[...] = bf16(dot(key_ref[:, :LAT], expand_ref[...]))
    for start in range(0, x.shape[0], block):
        at = pl.ds(start, block)
        attend_kernel(
            heads,
            q_ref.at[at],
            lat_ref.at[at],
            key_ref.at[at],
            cos_ref.at[at],
            sin_ref.at[at],
            col_ref.at[at],
            row_ref.at[pl.ds(start // block, 1)],
            out_ref.at[at],
            rot_ref.at[at],
        )


def pair_grad_kernel(x_ref, grad_ref, out_ref):
    units = out_ref.shape[2]
    x = x_ref[...]
    out_ref[:, 0, :] = t_dot(x, grad_ref[:, :units])
    out_ref[:, 1, :] = t_dot(x, grad_ref[:, units:])


def pair_grad(x, grad):
    rows, width = x.shape
    units = grad.shape[1] // 2
    if rows > 4096:
        return t_dot(x, grad[:rows]).reshape(width, 2, units)
    tile = 256
    return pl.pallas_call(
        pair_grad_kernel,
        grid=(width // tile,),
        in_specs=[
            pl.BlockSpec((rows, tile), lambda i: (0, i)),
            pl.BlockSpec((rows, 2 * units), lambda i: (0, 0), pipeline_mode=pl.Buffered(1)),
        ],
        out_specs=pl.BlockSpec((tile, 2, units), lambda i: (i, 0, 0)),
        out_shape=jax.ShapeDtypeStruct((width, 2, units), jnp.float32),
        name="pair_grad",
        cost_estimate=pl.CostEstimate(
            flops=4 * rows * width * units, bytes_accessed=rows * (width + 2 * units) * 2 + width * units * 8, transcendentals=0
        ),
    )(x, grad)


def blank(shape, dtype):
    return pl.pallas_call(
        lambda out_ref: None,
        out_shape=jax.ShapeDtypeStruct(shape, dtype),
        out_specs=pl.BlockSpec(memory_space=pl.ANY),
        compiler_params=pltpu.CompilerParams(has_side_effects=True),
        name="blank",
    )()


def arrival_order(spots):
    tiles = [(rank + 1.1 * over, rank, over) for rank in range(spots) for over in (0, 1)]
    return [(rank, over == 1) for _, rank, over in sorted(tiles)]


def ranked_spots(spots, spot):
    ranks = []
    for rank in range(spots):
        value = 0
        for own in range(spots):
            nearest = sorted(range(spots), key=lambda other: (abs(other - own), other))
            value = value + jnp.where(spot == own, nearest[rank], 0)
        ranks.append(value)
    return ranks


def pick(index, values):
    total = 0
    for position, value in enumerate(values):
        total = total + jnp.where(index == position, value, 0)
    return total


def fused_kernel(spots, parts, active, body, pack_kinds, counts, n_into, *refs):
    source_kinds, result_kinds = pack_kinds
    n_sources, n_results = len(source_kinds), len(result_kinds)
    n_weights, n_pieces = len(counts), sum(counts)
    x_ref, small_ref, refs = refs[0], refs[1], refs[2:]
    sources, refs = refs[:n_sources], refs[n_sources:]
    stored, refs = refs[:n_pieces], refs[n_pieces + n_into :]
    o_ref, refs = refs[0], refs[1:]
    results, refs = refs[:n_results], refs[n_results:]
    x_tile, refs = refs[0], refs[1:]
    source_tiles, refs = refs[:n_sources], refs[n_sources:]
    result_tiles, refs = refs[:n_results], refs[n_results:]
    weights, refs = refs[:n_weights], refs[n_weights:]
    sems, scratch = refs[:12], refs[12:]
    own_sem, weight_sem, tile_sem, out_sem = sems[:4]
    up_out, up_in, down_out, down_in, over_out, over_in, pair_out, pair_in = sems[4:]
    block = x_ref.shape[0]
    rows = block // parts
    tile = 2 * block

    def run():
        loads = loads_of(counts, stored, weights, weight_sem)
        for copy in loads:
            copy.start()
        spot, chip, core = places(spots)
        greet(spots, spot, chip, core)
        piece = lambda index, part: o_ref.at[index, pl.ds(part * rows, rows)]
        first = lambda part: x_ref.at[pl.ds(part * rows, rows)]

        def up(source, at, part, reach):
            return remote(
                source, piece(slot(at, chip, core), part), {PACKS: spot + 1}, up_out.at[reach, part], up_in.at[reach, part]
            )

        def down(source, at, part, reach):
            return remote(
                source,
                piece(slot(at, chip, core), part),
                {PACKS: spot - 1},
                down_out.at[reach, part],
                down_in.at[reach, part],
            )

        def over(source, at, part):
            return remote(
                source, piece(slot(at, chip, core), part), to_other(chip, core), over_out.at[at, part], over_in.at[at, part]
            )

        def pair(source, at, c, part):
            return remote(
                source,
                piece(slot(at, c, core), part),
                to_partner(chip, core),
                pair_out.at[c, at, part],
                pair_in.at[c, at, part],
            )

        mine = slot(spot, chip, core)
        for part in range(parts):
            source = first(part)
            pair(source, spot, chip, part).start()
            over(source, spot, part).start()
            pl.when(spot < spots - 1)(lambda: up(source, spot, part, 0).start())
            pl.when(spot > 0)(lambda: down(source, spot, part, 0).start())
        own = pltpu.make_async_copy(x_ref, o_ref.at[mine], own_sem.at[0])
        own.start()
        own.wait()
        ranks = ranked_spots(spots, spot)
        order = arrival_order(spots)

        def hand_on(reach):
            for part in range(parts):

                def below(part=part):
                    at = spot - reach
                    source = piece(slot(at, chip, core), part)
                    up(source, at, part, reach - 1).wait_recv()
                    pl.when(spot < spots - 1)(lambda: up(source, at, part, reach).start())
                    over(source, at, part).start()
                    pair(source, at, chip, part).start()

                def above(part=part):
                    at = spot + reach
                    source = piece(slot(at, chip, core), part)
                    down(source, at, part, reach - 1).wait_recv()
                    pl.when(spot > 0)(lambda: down(source, at, part, reach).start())
                    over(source, at, part).start()
                    pair(source, at, chip, part).start()

                pl.when(spot >= reach)(below)
                pl.when(spot + reach < spots)(above)

        def arrive(rank, across):
            at = ranks[rank]
            if across:
                for part in range(parts):
                    source = piece(slot(at, 1 - chip, core), part)
                    over(source, at, part).wait_recv()
                    pair(source, at, 1 - chip, part).start()
                for part in range(parts):
                    pair(first(part), at, 1 - chip, part).wait_recv()
                return
            if rank > 0:
                hand_on(rank)
            for part in range(parts):
                pair(first(part), at, chip, part).wait_recv()

        def window(ref, kind, at, c):
            if kind:
                return ref.at[:, pl.ds(pl.multiple_of((at * 2 + c) * tile, tile), tile)]
            return ref.at[pl.ds(pl.multiple_of((at * 2 + c) * tile, tile), tile)]

        def outward(index, which, at, c):
            return pltpu.make_async_copy(
                result_tiles[index].at[which], window(results[index], result_kinds[index], at, c), out_sem.at[which, index]
            )

        def step(number, carry):
            for position, (rank, across) in enumerate(order):
                pl.when(number == position)(functools.partial(arrive, rank, across))
            at = pick(number, [ranks[rank] for rank, _ in order])
            c = pick(number, [1 - chip if across else chip for _, across in order])
            inside = at == spot
            inputs = [pltpu.make_async_copy(o_ref.at[pl.ds(slot(at, c, 0), 2)], x_tile, tile_sem.at[0])]
            for index, kind in enumerate(source_kinds):
                if not kind:
                    inputs.append(
                        pltpu.make_async_copy(
                            window(sources[index], kind, at, c), source_tiles[index], tile_sem.at[1 + index]
                        )
                    )
            for copy in inputs:
                copy.start()
            for index, kind in enumerate(source_kinds):
                if kind:

                    def fetch(index=index, kind=kind):
                        copy = pltpu.make_async_copy(
                            window(sources[index], kind, at, c), source_tiles[index], tile_sem.at[1 + index]
                        )
                        copy.start()
                        copy.wait()

                    pl.when(inside)(fetch)

            @pl.when(number == 0)
            def _():
                for copy in loads:
                    copy.wait()

            which = lax.rem(number, 2)

            @pl.when(number >= 2)
            def _():
                for index in range(n_results):
                    outward(index, which, at, c).wait()

            for copy in inputs:
                copy.wait()
            body(
                inside,
                [x_tile[...].reshape(tile, x_tile.shape[2]), small_ref, *source_tiles],
                weights,
                [target.at[which] for target in result_tiles],
                scratch,
            )
            for index in range(n_results):
                outward(index, which, at, c).start()
            return carry

        lax.fori_loop(0, 2 * spots, step, 0)
        for which in range(2):
            for index in range(n_results):
                outward(index, which, spot, chip).wait()
        for part in range(parts):
            for at in range(spots):
                over(first(part), at, part).wait_send()
                for c in range(2):
                    pair(first(part), at, c, part).wait_send()
            for reach in range(spots - 1):
                pl.when((spot >= reach) & (spot < spots - 1))(lambda: up(first(part), spot, part, reach).wait_send())
                pl.when((spot + reach < spots) & (spot > 0))(lambda: down(first(part), spot, part, reach).wait_send())

    pl.when(lax.axis_index(SECTION) == active)(run)


def fused_call(tiles, rows_in, number, active, body, small, sources, weights, results, gathered, into, scratch=(), parts=4):
    spots = lax.axis_size(PACKS)
    block, width = rows_in.shape
    tile = 2 * block
    dma = pltpu.SemaphoreType.DMA
    hops = max(spots - 1, 1)
    anywhere = pl.BlockSpec(memory_space=pl.ANY)
    inside = pl.BlockSpec(memory_space=pltpu.VMEM)
    shapes = [jax.ShapeDtypeStruct((spots * 4, block, width), rows_in.dtype), *(shape for shape, _ in results)]
    held = [gathered.reshape(shapes[0].shape), *into]
    pieces = [piece for weight in weights for piece in weight]
    first = 2 + len(sources) + len(pieces)

    def hold(array, kind, *lead):
        shape = (2, tile, array.shape[2]) if kind else (tile, array.shape[1])
        return pltpu.VMEM((*lead, *shape), array.dtype)

    outs = pl.pallas_call(
        functools.partial(
            fused_kernel,
            spots,
            parts,
            active,
            body,
            ([kind for _, kind in sources], [kind for _, kind in results]),
            [len(weight) for weight in weights],
            len(held),
        ),
        out_shape=shapes,
        in_specs=[inside, inside, *([anywhere] * (len(sources) + len(pieces) + len(held)))],
        out_specs=[anywhere] * len(shapes),
        input_output_aliases={first + index: index for index in range(len(held))},
        scratch_shapes=[
            pltpu.VMEM((2, block, width), rows_in.dtype),
            *(hold(array, kind) for array, kind in sources),
            *(hold(shape, kind, 2) for shape, kind in results),
            *(hold_weight(weight) for weight in weights),
            dma((1,)),
            dma((len(pieces),)),
            dma((1 + len(sources),)),
            dma((2, len(results))),
            dma((hops, parts)),
            dma((hops, parts)),
            dma((hops, parts)),
            dma((hops, parts)),
            dma((spots, parts)),
            dma((spots, parts)),
            dma((2, spots, parts)),
            dma((2, spots, parts)),
            *scratch,
        ],
        compiler_params=pltpu.CompilerParams(collective_id=number, has_side_effects=True),
        name=f"fused{number}",
    )(rows_in, small, *(array for array, _ in sources), *pieces, *held)
    return outs[0].reshape(-1, width), list(outs[1:])


def sum_kernel(spots, parts, active, body, pack_kinds, counts, later, n_into, *refs):
    source_kinds, result_kinds = pack_kinds
    n_sources, n_results = len(source_kinds), len(result_kinds)
    n_weights, n_pieces = len(counts), sum(counts)
    small_ref, refs = refs[0], refs[1:]
    sources, refs = refs[:n_sources], refs[n_sources:]
    stored, refs = refs[:n_pieces], refs[n_pieces + n_into :]
    o_ref, refs = refs[0], refs[1:]
    results, refs = refs[:n_results], refs[n_results:]
    source_tiles, refs = refs[:n_sources], refs[n_sources:]
    result_tiles, refs = refs[:n_results], refs[n_results:]
    weights, refs = refs[:n_weights], refs[n_weights:]
    x_buf, pair_buf, over_src, over_buf, line_src, up_buf, down_buf = refs[:7]
    weight_sem, tile_sem, out_sem, pair_out, pair_in, over_out, over_in, line_out, up_in, down_in = refs[7:17]
    scratch = refs[17:]
    block = o_ref.shape[0]
    rows = block // parts
    tile = 2 * block
    cut = lambda part: pl.ds(part * rows, rows)

    def run():
        loads = loads_of(counts, stored, weights, weight_sem)
        early = [copy for index, copy in enumerate(loads) if index not in later]
        for copy in early:
            copy.start()
        spot, chip, core = places(spots)

        def order(step):
            if step == spots - 1:
                return spot
            fall = spots - 1 - step
            fall = jnp.where(fall <= spot, fall - 1, fall)
            rise = jnp.where(step >= spot, step + 1, step)
            return jnp.where(2 * spot < spots - 1, fall, rise)

        turns = [(0, True)]
        for ahead in range(1, spots):
            turns += [(ahead, True), (ahead - 1, False)]
        turns.append((spots - 1, False))

        def place(number):
            at = pick(number, [order(turn) for turn, _ in turns])
            return at, pick(number, [1 - chip if far else chip for _, far in turns])

        def window(ref, kind, at, c):
            if kind:
                return ref.at[:, pl.ds(pl.multiple_of((at * 2 + c) * tile, tile), tile)]
            return ref.at[pl.ds(pl.multiple_of((at * 2 + c) * tile, tile), tile)]

        def inputs(number):
            at, c = place(number)
            which = lax.rem(number, 2)
            return [
                pltpu.make_async_copy(
                    window(sources[index], kind, at, c), source_tiles[index].at[which], tile_sem.at[which, index]
                )
                for index, kind in enumerate(source_kinds)
                if not kind
            ]

        for copy in inputs(0):
            copy.start()
        greet(spots, spot, chip, core)

        def mine(at, c, k, part):
            return x_buf.at[at * 2 + c, pl.ds(pl.multiple_of(k * block + part * rows, rows), rows)]

        def pair(at, c, part):
            return remote(
                mine(at, c, 1 - core, part),
                pair_buf.at[at, c, cut(part)],
                to_partner(chip, core),
                pair_out.at[at, c, part],
                pair_in.at[at, c, part],
            )

        def over(at, part):
            return remote(
                over_src.at[at, cut(part)],
                over_buf.at[at, cut(part)],
                to_other(chip, core),
                over_out.at[at, part],
                over_in.at[at, part],
            )

        def up(at, part):
            return remote(
                line_src.at[at, cut(part)],
                up_buf.at[at, cut(part)],
                {PACKS: spot + 1},
                line_out.at[at, part],
                up_in.at[at, part],
            )

        def down(at, part):
            return remote(
                line_src.at[at, cut(part)],
                down_buf.at[at, cut(part)],
                {PACKS: spot - 1},
                line_out.at[at, part],
                down_in.at[at, part],
            )

        def across(step):
            at = order(step)
            for part in range(parts):
                pair(at, 1 - chip, part).wait_recv()
                add_into(
                    over_src.at[at, cut(part)],
                    [mine(at, 1 - chip, core, part), pair_buf.at[at, 1 - chip, cut(part)]],
                    rows,
                )
                over(at, part).start()

        def along(step):
            at = order(step)
            for part in range(parts):
                pair(at, chip, part).wait_recv()
                over(at, part).wait_recv()
                base = [mine(at, chip, core, part), pair_buf.at[at, chip, cut(part)], over_buf.at[at, cut(part)]]
                ups, downs = up_buf.at[at, cut(part)], down_buf.at[at, cut(part)]
                if step < spots - 1:
                    target = line_src.at[at, cut(part)]

                    def rising(first):
                        if not first:
                            up(at, part).wait_recv()
                        add_into(target, base if first else base + [ups], rows)
                        up(at, part).start()

                    def falling(first):
                        if not first:
                            down(at, part).wait_recv()
                        add_into(target, base if first else base + [downs], rows)
                        down(at, part).start()

                    pl.when((at > spot) & (spot == 0))(lambda: rising(True))
                    pl.when((at > spot) & (spot > 0))(lambda: rising(False))
                    pl.when((at < spot) & (spot == spots - 1))(lambda: falling(True))
                    pl.when((at < spot) & (spot < spots - 1))(lambda: falling(False))
                elif spots == 1:
                    add_into(o_ref.at[cut(part)], base, rows)
                else:

                    def finish(ends):
                        if ends < 1:
                            up(at, part).wait_recv()
                        if ends > -1:
                            down(at, part).wait_recv()
                        extra = ([ups] if ends < 1 else []) + ([downs] if ends > -1 else [])
                        add_into(o_ref.at[cut(part)], base + extra, rows)

                    pl.when(spot == 0)(lambda: finish(1))
                    pl.when(spot == spots - 1)(lambda: finish(-1))
                    pl.when((spot > 0) & (spot < spots - 1))(lambda: finish(0))

        late = 3 + jnp.where((spot > 0) & (spot < spots - 1), 2, 0)

        def outward(index, which, at, c):
            return pltpu.make_async_copy(
                result_tiles[index].at[which], window(results[index], result_kinds[index], at, c), out_sem.at[which, index]
            )

        def step(number, carry):
            at, c = place(number)
            inside = at == spot
            which = lax.rem(number, 2)
            for copy in inputs(number):
                copy.wait()

            @pl.when(number + 1 < 2 * spots)
            def _():
                for copy in inputs(number + 1):
                    copy.start()

            for index, kind in enumerate(source_kinds):
                if kind:

                    def fetch(index=index, kind=kind):
                        copy = pltpu.make_async_copy(
                            window(sources[index], kind, at, c), source_tiles[index], tile_sem.at[0, index]
                        )
                        copy.start()
                        copy.wait()

                    pl.when(inside)(fetch)

            @pl.when(number == 0)
            def _():
                for copy in early:
                    copy.wait()
                for index in later:
                    loads[index].start()

            @pl.when(number == min(1, spots - 1))
            def _():
                for index in later:
                    loads[index].wait()

            @pl.when(number >= 2)
            def _():
                for index, kind in enumerate(result_kinds):
                    if not kind:
                        outward(index, which, at, c).wait()

            tiles = [
                target if kind else target.at[which] for target, kind in zip(source_tiles, source_kinds)
            ]
            body(
                inside,
                [tiles[0][...], small_ref, *tiles[1:]],
                weights,
                [*(target.at[which] for target in result_tiles), x_buf.at[at * 2 + c]],
                scratch,
            )
            for part in range(parts):
                pair(at, c, part).start()
            for index, kind in enumerate(result_kinds):
                if kind:

                    def put(index=index):
                        copy = outward(index, which, at, c)
                        copy.start()
                        copy.wait()

                    pl.when(inside)(put)
                else:
                    outward(index, which, at, c).start()
            for number_of in range(spots):
                pl.when(number == 2 * number_of)(functools.partial(across, number_of))
                pl.when(number == 2 * number_of + late)(functools.partial(along, number_of))
            return carry

        lax.fori_loop(0, 2 * spots, step, 0)
        for number_of in range(spots):
            pl.when(2 * number_of + late >= 2 * spots)(functools.partial(along, number_of))
        for which in range(2):
            for index, kind in enumerate(result_kinds):
                if not kind:
                    outward(index, which, spot, chip).wait()
        for part in range(parts):
            for number_of in range(spots):
                at = order(number_of)
                pair(at, 0, part).wait_send()
                pair(at, 1, part).wait_send()
                over(at, part).wait_send()
                if number_of < spots - 1:
                    up(at, part).wait_send()

    pl.when(lax.axis_index(SECTION) == active)(run)


def sum_call(rows, number, active, body, small, sources, weights, later, results, into, scratch=(), parts=4):
    spots = lax.axis_size(PACKS)
    width = weights[-1][0].shape[1]
    tile = 2 * rows
    dma = pltpu.SemaphoreType.DMA
    anywhere = pl.BlockSpec(memory_space=pl.ANY)
    inside = pl.BlockSpec(memory_space=pltpu.VMEM)
    pieces = [piece for weight in weights for piece in weight]
    first = 1 + len(sources) + len(pieces)
    held = lambda *lead: pltpu.VMEM((*lead, rows, width), jnp.bfloat16)

    def hold(array, kind, *lead):
        if kind:
            return pltpu.VMEM((*lead, 2, tile, array.shape[2]), array.dtype)
        return pltpu.VMEM((2, tile, array.shape[1]), array.dtype)

    outs = pl.pallas_call(
        functools.partial(
            sum_kernel,
            spots,
            parts,
            active,
            body,
            ([kind for _, kind in sources], [kind for _, kind in results]),
            [len(weight) for weight in weights],
            later,
            len(into),
        ),
        out_shape=[jax.ShapeDtypeStruct((rows, width), jnp.float32), *(shape for shape, _ in results)],
        in_specs=[inside, *([anywhere] * (len(sources) + len(pieces) + len(into)))],
        out_specs=[inside, *([anywhere] * len(results))],
        input_output_aliases={first + index: 1 + index for index in range(len(into))},
        scratch_shapes=[
            *(hold(array, kind) for array, kind in sources),
            *(hold(shape, kind, 2) for shape, kind in results),
            *(hold_weight(weight) for weight in weights),
            pltpu.VMEM((2 * spots, tile, width), jnp.bfloat16),
            held(spots, 2),
            held(spots),
            held(spots),
            held(spots),
            held(spots),
            held(spots),
            dma((len(pieces),)),
            dma((2, len(sources))),
            dma((2, max(len(results), 1))),
            dma((spots, 2, parts)),
            dma((spots, 2, parts)),
            dma((spots, parts)),
            dma((spots, parts)),
            dma((spots, parts)),
            dma((spots, parts)),
            dma((spots, parts)),
            *scratch,
        ],
        compiler_params=pltpu.CompilerParams(collective_id=number, has_side_effects=True),
        name=f"sum{number}",
    )(small, *(array for array, _ in sources), *pieces, *into)
    return outs[0], list(outs[1:])


def body(
    boundary,
    lengths,
    routes,
    attn_gain,
    query_weight,
    compress_weight,
    latent_gain,
    expand_weight,
    output_weight,
    ffn_gain,
    router_weight,
    shared_in,
    shared_out,
    expert_in,
    expert_out,
):
    attn_gain, latent_gain, ffn_gain = attn_gain[0], latent_gain[0], ffn_gain[0]
    query_weight, compress_weight = query_weight[0], compress_weight[0]
    expand_weight, output_weight = expand_weight[0], output_weight[0]
    router_weight, shared_out, expert_out = router_weight[0], shared_out[0], expert_out[0, 0]
    width = boundary.shape[3]
    rows = boundary.shape[2]
    half = shared_out.shape[0]
    units = expert_out.shape[0]
    experts_count = router_weight.shape[1]
    shared_in_t = jnp.transpose(shared_in[0], (1, 2, 0)).reshape(2 * half, width)
    joined_in = (
        expert_in.reshape(width, 2 * units),
        jnp.pad(router_weight, ((0, 0), (0, -experts_count % 128))),
    )
    joined_width = sum(piece.shape[1] for piece in joined_in)

    packs, members = lax.axis_size(PACKS), lax.axis_size(MEMBERS)
    count = packs * members
    pack, member = lax.axis_index(PACKS), lax.axis_index(MEMBERS)
    me = pack * members + member
    is_first = lax.axis_index(SECTION) == 0
    pack_rows = members * rows
    all_rows = count * rows
    heads = output_weight.shape[0] // VD
    top = routes.shape[3]
    tiles = [Tiles(all_rows, pack_rows, pack, active) for active in range(2)]
    fusing = members == 4 and tiles[0].tile == 2 * rows

    def own_pack(value):
        size = value.shape[0] // packs
        return lax.dynamic_slice_in_dim(value, pack * size, size, 0)

    freqs = rope_base ** (-jnp.arange(HALF, dtype=jnp.float32) / HALF)
    angles = jnp.arange(rows, dtype=jnp.float32)[:, None] * freqs[None, :]
    turns = jnp.concatenate([jnp.cos(angles), jnp.sin(angles)], axis=1)

    def tables_of(block_lengths):
        segment, position = block_layout(block_lengths, rows)
        blocks = segment.shape[0]
        chosen = position.reshape(-1)[:, None] == jnp.arange(rows, dtype=jnp.int32)[None, :]
        found = jnp.dot(
            chosen.astype(jnp.float32),
            turns,
            precision=lax.Precision.HIGHEST,
            preferred_element_type=jnp.float32,
        )
        return (
            found[:, :HALF],
            found[:, HALF:],
            segment.reshape(blocks * rows, 1),
            segment.reshape(blocks, 1, rows),
        )

    own_lengths = lax.dynamic_index_in_dim(lengths[0, 0], member, 0, keepdims=False)
    layout = jnp.concatenate(
        [
            jnp.transpose(routes[0, 0]),
            jnp.pad(own_lengths, (0, rows - own_lengths.shape[0]))[None],
            jnp.zeros((-(top + 1) % 8, rows), jnp.int32),
        ],
        axis=0,
    )


    def routed_of(layout_all):
        named = layout_all.reshape(count, -1, rows)[:, :top] == me
        return jnp.any(named, axis=1).astype(jnp.float32).reshape(all_rows, 1)

    tables_pack = tables_of(lengths[0, 0])
    tables_own = tables_of(own_lengths[None])
    own_cos, own_sin = tables_own[:2]
    own_column = (lax.broadcasted_iota(jnp.int32, (1, experts_count), 1) == me).astype(jnp.float32)

    def inputs_of(hidden):
        normed32, scale_attn = rms_forward(hidden, attn_gain)
        normed = bf16(normed32)
        compressed = dot(normed, compress_weight)
        latent32, scale_latent = rms_forward(compressed[:, :LAT], latent_gain)
        keyed = bf16(
            jnp.concatenate([latent32, rotate(compressed[:, LAT:], own_cos, own_sin)], axis=1)
        )
        return normed, keyed, (compressed, scale_attn, scale_latent)

    def run_experts(section, x, routed, gathered, into, number, full):
        at = tiles[section]
        results = [
            at.result(2 * units),
            at.result(units),
            at.result(experts_count, jnp.float32),
            at.pair_result(half),
            at.result(half),
        ]
        weights = [joined_in, (shared_in_t,)]
        if full:
            results.append(at.result(width))
            weights += [(expert_out,), (shared_out,)]
        if fusing:
            shapes = [(shape, index == 3) for index, (shape, _) in enumerate(results)]
            return fused_call(
                at, x, number, section, experts_body, own_column, [(routed, False)], weights, shapes, gathered, into
            )
        (x_all,) = gather_blocks([x], True, number, section, [gathered])
        return x_all, at.call(
            tiled(experts_body),
            "experts",
            [(x_all, at.source(width)), (own_column, at.small(own_column)), (routed, at.source(1))],
            weights,
            results,
            into[:5],
        )

    def summed_over(section, number, body_of, name, sources, weights, later, results, into, scratch=()):
        at = tiles[section]
        if fusing:
            shapes = [(shape, shape.ndim == 3) for shape, _ in results]
            return sum_call(rows, number, section, body_of, own_column, sources, weights, later, shapes, into, scratch)
        specs = [(array, at.pair_source(half) if kind else at.source(array.shape[1])) for array, kind in sources]
        specs.insert(1, (own_column, at.small(own_column)))
        *found, partial = at.call(
            tiled(body_of), name, specs, weights, [*results, at.result(width)], into, scratch
        )
        return scatter_blocks(partial, rows, True, number, section), found

    def run_experts_back(section, number, grad_all, routed, stored, into):
        at = tiles[section]
        pre, _, prob, shared_pre, _ = stored
        return summed_over(
            section,
            number,
            experts_back_body,
            "experts_back",
            [(grad_all, False), (pre, False), (prob, False), (routed, False), (shared_pre, True)],
            [joined_in, (shared_in_t,), (expert_out,), (shared_out,)],
            [2, 4],
            [at.result(2 * units), at.result(1, jnp.float32)],
            into,
            [pltpu.VMEM((at.tile, joined_width), jnp.bfloat16)],
        )

    def run_heads(section, normed_all, keyed_all, tables, into):
        at = tiles[section]
        cosine, sine, seg_col, seg_row = tables
        blocks = at.tile // rows
        row_spec = pl.BlockSpec((blocks, 1, rows), lambda i, control: (i * control[2], 0, 0))
        return at.call(
            tiled(functools.partial(heads_body, rows)),
            "heads",
            [
                (normed_all, at.source(width)),
                (keyed_all, at.source(LAT + ROPE)),
                (cosine, at.source(HALF)),
                (sine, at.source(HALF)),
                (seg_col, at.source(1)),
                (seg_row, row_spec),
            ],
            [(query_weight,), (expand_weight,)],
            [at.result(heads * VD), at.result(heads * QK), at.result(heads * KV)],
            into,
            [pltpu.VMEM((at.tile, heads * QK), jnp.float32)],
            flops=4 * all_rows * width * heads * QK,
        )

    def run_shared(section, ffn_all, into):
        at = tiles[section]
        return at.call(
            tiled(shared_body),
            "shared",
            [(ffn_all, at.source(width))],
            [(shared_in_t,)],
            [at.pair_result(half), at.result(half)],
            into,
            flops=4 * all_rows * width * half,
        )

    fresh = boundary[0, 0].astype(jnp.float32)

    normed, keyed, _ = inputs_of(fresh)
    normed_pack, keyed_pack, layout_all = gather_blocks(
        [normed, keyed, layout], True, 0, 0, wide=[False, False, True]
    )
    attended, _ = attend(
        dot(normed_pack, query_weight),
        bf16(dot(keyed_pack[:, :LAT], expand_weight)),
        keyed_pack,
        tables_pack,
    )
    mixed_first = fresh + scatter_blocks(bf16(dot(attended, output_weight)), rows, False, 1, 0)
    empty = [
        blank((all_rows, width), jnp.bfloat16),
        *(
            blank(shape, dtype)
            for shape, dtype in (
                ((all_rows + tiles[0].tile, 2 * units), jnp.bfloat16),
                ((all_rows + tiles[0].tile, units), jnp.bfloat16),
                ((all_rows + tiles[0].tile, experts_count), jnp.float32),
                ((2, all_rows + tiles[0].tile, half), jnp.bfloat16),
                ((all_rows + tiles[0].tile, half), jnp.bfloat16),
            )
        ),
    ]
    ffn_all, (*stored, partial) = run_experts(
        0, bf16(rms_forward(mixed_first, ffn_gain)[0]), routed_of(layout_all), empty[0], empty[1:], 2, True
    )
    result_first = mixed_first + scatter_blocks(partial, rows, True, 3, 0)
    heads_weights = spread_blocks([query_weight, expand_weight, output_weight], 4, 1)
    target_all, layout_all = gather_blocks(
        [boundary[0, 0], layout], True, 5, 1, [blank((all_rows, width), jnp.bfloat16), layout_all]
    )
    sent, target_all, layout_all, heads_weights = lax.optimization_barrier(
        (bf16(result_first), target_all, layout_all, heads_weights)
    )
    inbound = lax.ppermute(sent, SECTION, [(0, 1)])
    routed = routed_of(layout_all)
    tables_all = tables_of(layout_all.reshape(count, -1, rows)[:, top, : lengths.shape[3]])

    normed, keyed, ffn_all, _ = lax.optimization_barrier((normed, keyed, ffn_all, sent))
    all_inputs = gather_blocks([normed, keyed], True, 8, 0)
    prepared = run_heads(0, *all_inputs, tables_all, ())
    stored[3:] = run_shared(0, ffn_all, stored[3:])
    inbound, prepared, all_inputs, stored = lax.optimization_barrier((inbound, prepared, all_inputs, stored))
    query_heads, expand_heads, output_heads = (
        value.reshape(members, -1, value.shape[1]) for value in heads_weights
    )

    hidden = jnp.where(is_first, fresh, inbound.astype(jnp.float32))
    normed, keyed, (compressed, scale_attn, scale_latent) = inputs_of(hidden)
    latent = bf16(jnp.einsum("rd,mdc->mrc", keyed[:, :LAT], expand_heads, preferred_element_type=jnp.float32))
    latent = latent.reshape(members * rows, -1)
    query_raw = jnp.einsum("rd,mdc->mrc", normed, query_heads, preferred_element_type=jnp.float32)
    attended, query = attend(query_raw.reshape(members * rows, -1), latent, keyed, tables_own, members)
    mixed = hidden + jnp.einsum(
        "mrc,mcd->rd", attended.reshape(members, rows, -1), output_heads, preferred_element_type=jnp.float32
    )
    mixed = jnp.where(is_first, mixed_first, mixed)
    ffn32, scale_ffn = rms_forward(mixed, ffn_gain)
    ffn_all, stored = run_experts(1, bf16(ffn32), routed, ffn_all, stored, 6, False)

    def latent_back(own):
        grad_latent, grad_latent_gain = rms_backward(
            compressed[:, :LAT], scale_latent, latent_gain, own[:, width : width + LAT]
        )
        grad_compressed = bf16(
            jnp.concatenate([grad_latent, rotate(own[:, width + LAT :], own_cos, -own_sin)], axis=1)
        )
        grad_normed = own[:, :width] + dot_t(grad_compressed, compress_weight)
        grad_hidden_norm, grad_attn_gain = rms_backward(hidden, scale_attn, attn_gain, grad_normed)
        return grad_compressed, grad_hidden_norm, grad_attn_gain, grad_latent_gain

    grad_ffn_second, grad_units = run_experts_back(1, 7, target_all, routed, stored, ())
    grad_mixed = fresh + rms_backward(mixed, scale_ffn, ffn_gain, grad_ffn_second)[0]
    grad_attended = jnp.einsum(
        "rd,mcd->mrc", bf16(grad_mixed), output_heads, preferred_element_type=jnp.float32
    )
    grad_query, grad_latent_heads, grad_shared_key = attend_back(
        query, latent, keyed, bf16(grad_attended).reshape(members * rows, -1), tables_own, members
    )
    own_second = jnp.concatenate(
        [
            jnp.einsum(
                "mrc,mdc->rd",
                grad_query.reshape(members, rows, -1),
                query_heads,
                preferred_element_type=jnp.float32,
            ),
            jnp.einsum(
                "mrc,mdc->rd",
                grad_latent_heads.reshape(members, rows, -1),
                expand_heads,
                preferred_element_type=jnp.float32,
            ),
            jnp.sum(grad_shared_key.reshape(members, rows, -1), axis=0),
        ],
        axis=1,
    )
    grad_second = bf16(grad_mixed + latent_back(own_second)[1])

    downbound = lax.ppermute(grad_second, SECTION, [(1, 0)]).astype(jnp.float32)

    normed_late, keyed_late, gated_late, _ = lax.optimization_barrier((normed, keyed, stored[1], grad_second))
    finished, _ = summed_over(
        1,
        10,
        finish_body,
        "finish",
        [(gated_late, False), (stored[3], True)],
        [(expert_out,), (shared_out,)],
        [1],
        [],
        (),
    )
    result = mixed + finished
    upstream = jnp.where(is_first, downbound, fresh)
    (upstream_all,) = gather_blocks([bf16(upstream)], True, 11, 0, [target_all])
    grad_ffn, (grad_pre, moved) = run_experts_back(0, 12, upstream_all, routed, stored, grad_units)
    grad_ffn = jnp.where(is_first, grad_ffn, grad_ffn_second)
    normed_late, keyed_late, _ = lax.optimization_barrier((normed_late, keyed_late, finished))
    normed_all, keyed_all = gather_blocks([normed_late, keyed_late], True, 9, 1, all_inputs)
    attended_all, query_all, latent_all = run_heads(1, normed_all, keyed_all, tables_all, prepared)
    shared_pre, shared_hid = stored[3:]
    attended_all, shared_hid = attended_all[:all_rows], shared_hid[:all_rows]
    grad_mixed_norm, grad_ffn_gain = rms_backward(mixed, scale_ffn, ffn_gain, grad_ffn)
    grad_mixed = upstream + grad_mixed_norm
    grad_mixed_all = lax.all_gather(bf16(grad_mixed), BOTH, axis=0, tiled=True)
    grad_attended = bf16(dot_t(grad_mixed_all, output_weight))
    grad_query, grad_latent_heads, grad_shared_key = attend_back(
        query_all, latent_all, keyed_all, grad_attended, tables_all
    )
    own = lax.psum_scatter(
        bf16(
            jnp.concatenate(
                [
                    dot_t(own_pack(grad_query), query_weight),
                    dot_t(own_pack(grad_latent_heads), expand_weight),
                    own_pack(grad_shared_key),
                ],
                axis=1,
            )
        ),
        MEMBERS,
        scatter_dimension=0,
        tiled=True,
    ).astype(jnp.float32)
    grad_compressed, grad_hidden_norm, grad_attn_gain, grad_latent_gain = latent_back(own)
    grad_hidden = grad_mixed + grad_hidden_norm

    gains = jnp.concatenate([grad_attn_gain, grad_latent_gain, grad_ffn_gain])
    rounded = lax.reduce_precision(gains, 8, 7)
    small = jnp.concatenate([bf16(rounded), bf16(gains - rounded), bf16(moved[:all_rows, 0])])
    small = jnp.pad(small, (0, -small.shape[0] % rows)).reshape(rows, -1)
    last = lax.all_gather(jnp.concatenate([grad_compressed, small], axis=1), BOTH, axis=0, tiled=True)
    grad_compressed_all = last[:, : LAT + ROPE]
    small_all = last[:, LAT + ROPE :].reshape(count, -1).astype(jnp.float32)
    many = 2 * width + LAT
    gains = jnp.sum(small_all[:, :many] + small_all[:, many : 2 * many], axis=0)
    moved_all = small_all[:, 2 * many : 2 * many + all_rows].T
    prob = stored[2][:all_rows]
    grad_logits = bf16(moved_all - prob * jnp.sum(moved_all, axis=1, keepdims=True))
    left, right = gated_back(
        shared_pre[0, :all_rows].astype(jnp.float32),
        shared_pre[1, :all_rows].astype(jnp.float32),
        dot_t(upstream_all, shared_out),
    )
    grad_shared_in = lax.dot_general(
        jnp.stack([left, right]), ffn_all, (((1,), (0,)), ((), ())), preferred_element_type=jnp.float32
    )
    ends = jnp.where(is_first, grad_hidden, result)
    return (
        ends[None, None],
        gains[:width][None],
        t_dot(normed_all, grad_query)[None],
        t_dot(normed_all, grad_compressed_all)[None],
        gains[width : width + LAT][None],
        t_dot(keyed_all[:, :LAT], grad_latent_heads)[None],
        t_dot(attended_all, grad_mixed_all)[None],
        gains[width + LAT :][None],
        t_dot(ffn_all, grad_logits)[None],
        jnp.transpose(grad_shared_in, (2, 0, 1))[None],
        t_dot(shared_hid, upstream_all)[None],
        pair_grad(ffn_all, grad_pre)[None, None],
        t_dot(stored[1][:all_rows], upstream_all)[None, None],
    )


def solution(mesh):
    return jax.shard_map(
        body,
        mesh=mesh,
        in_specs=(
            P(SECTION, None, BOTH, None),
            P(None, PACKS, None, None),
            P(SECTION, None, BOTH, None),
            P(SECTION, None),
            P(SECTION, None, MEMBERS),
            P(SECTION, None, None),
            P(SECTION, None),
            P(SECTION, None, MEMBERS),
            P(SECTION, MEMBERS, None),
            P(SECTION, None),
            P(SECTION, None, None),
            P(SECTION, None, None, MEMBERS),
            P(SECTION, MEMBERS, None),
            P(SECTION, BOTH, None, None, None),
            P(SECTION, BOTH, None, None),
        ),
        out_specs=(
            P(SECTION, None, BOTH, None),
            P(SECTION, None),
            P(SECTION, None, MEMBERS),
            P(SECTION, None, None),
            P(SECTION, None),
            P(SECTION, None, MEMBERS),
            P(SECTION, MEMBERS, None),
            P(SECTION, None),
            P(SECTION, None, None),
            P(SECTION, None, None, MEMBERS),
            P(SECTION, MEMBERS, None),
            P(SECTION, BOTH, None, None, None),
            P(SECTION, BOTH, None, None),
        ),
        check_vma=False,
    )
```
